32 devices in a mesh: batch: 1 (over z), row: 4 (over y), col: 8 (over x, core).
Axes of the slice: x: 4, y: 4, z: 1, core: 2. Of those that a mesh axis runs over, the one named last changes fastest.
The devices are a block of a 4x4x8 slice.
Arguments:
- left_op: bfloat16 [16384, 16384], P(('batch', 'row'), 'col')
- left_start: float32 [16384, 256], P(('batch', 'row', 'col'))
- right_op: bfloat16 [16384, 16384], P(('batch', 'row'), 'col')
- right_start: float32 [16384, 256], P(('batch', 'row', 'col'))
Outputs:
- output 1: float32 [16384, 256], P(('batch', 'row', 'col'))
- output 2: float32 [256, 256], P('batch')
- output 3: float32 [16384, 256], P(('batch', 'row', 'col'))
- output 4: float32 [256, 256], P('batch')
All inputs are finite; a program needn't handle non-finite values.
Results may differ from the reference program's by a relative error of at most 0.001.
Values are sent between devices in bfloat16 or wider.
A program may use at most 768 MiB of HBM per device.

```python
import jax
import jax.numpy as jnp
from jax import lax

N = 16384
N2 = 16384
S = 256
SWEEPS = 4


def build_operator(key, size):
    key_vec, key_val, key_noise = jax.random.split(key, 3)
    eig_basis = jax.random.normal(key_vec, (size, S), jnp.float32) * (size ** -0.5)
    levels = 1.5 * 4.0 ** jax.random.uniform(key_val, (S,), jnp.float32)
    noise_mat = jax.random.normal(key_noise, (size, size), jnp.float32) * (0.1 * size ** -0.5)
    full_mat = jnp.dot(eig_basis * levels, eig_basis.T) + noise_mat
    symmetric = 0.5 * (full_mat + full_mat.T) + 0.5 * jnp.eye(size, dtype=jnp.float32)
    return symmetric.astype(jnp.bfloat16)


def setup_inputs(seed: int = 0, part: int = 0) -> dict:
    base_key = jax.random.fold_in(jax.random.key(seed), part)
    key_left_op, key_left_start, key_right_op, key_right_start = jax.random.split(base_key, 4)
    return {
        "left_op": build_operator(key_left_op, N),
        "left_start": jax.random.normal(key_left_start, (N, S), jnp.float32),
        "right_op": build_operator(key_right_op, N2),
        "right_start": jax.random.normal(key_right_start, (N2, S), jnp.float32),
    }


def cholqr_step(y_mat, gram_mat):
    chol_low = jnp.linalg.cholesky(gram_mat)
    return lax.linalg.triangular_solve(chol_low, y_mat, left_side=False, lower=True, transpose_a=True)


def orthonormalize(y_mat):
    row_count = y_mat.shape[0]
    y_half = y_mat.astype(jnp.bfloat16)
    gram_one = jnp.dot(y_half.T, y_half, preferred_element_type=jnp.float32) / row_count
    y_one = cholqr_step(y_mat, gram_one)
    gram_two = jnp.dot(y_one.T, y_one, precision=lax.Precision.HIGHEST) / row_count
    return cholqr_step(y_one, gram_two)


def iterate(operator, start_block):
    def one_sweep(x_cur, unused):
        y_mat = jnp.dot(operator, x_cur.astype(jnp.bfloat16), preferred_element_type=jnp.float32)
        return orthonormalize(y_mat), None

    x_final, scan_rest = lax.scan(one_sweep, start_block, None, length=SWEEPS)
    z_mat = jnp.dot(operator, x_final.astype(jnp.bfloat16), preferred_element_type=jnp.float32)
    rayleigh = jnp.dot(x_final.T, z_mat, precision=lax.Precision.HIGHEST) / x_final.shape[0]
    return x_final, rayleigh


def reference(left_op, left_start, right_op, right_start):
    left_basis, left_rayleigh = iterate(left_op, left_start)
    right_basis, right_rayleigh = iterate(right_op, right_start)
    return (left_basis, left_rayleigh, right_basis, right_rayleigh)
```

```python
import functools

import jax
import jax.numpy as jnp
from jax import lax
from jax.experimental import pallas as pl
from jax.experimental.pallas import tpu as pltpu
from jax.sharding import PartitionSpec as P

SWEEPS = 4
CORES = 2
RING = 4
PIVOTS = 32
GROUP = 8
VMEM_BYTES = 67043328
F32, BF16 = jnp.float32, jnp.bfloat16
TN = (((0,), (0,)), ((), ()))
NT = (((1,), (1,)), ((), ()))

AG_T, AG_A, RELAY, RS_T, RS_A, PAIR, GRAM_PAIR, GRAM_RS, GRAM_AG, LINV, MOVE = 0, 6, 12, 17, 23, 29, 33, 34, 35, 36, 37
COPIES = 40


def split3(v):
    high = v.astype(BF16)
    rest = v - high.astype(F32)
    mid = rest.astype(BF16)
    return high, mid, (rest - mid.astype(F32)).astype(BF16)


def dot_f32(lhs, rhs, dims):
    lh, lm, ll = split3(lhs)
    rh, rm, rl = split3(rhs)

    def one(a, b):
        return lax.dot_general(a, b, dims, preferred_element_type=F32)

    small = one(ll, rh) + one(lh, rl) + one(lm, rm)
    return (small + (one(lm, rh) + one(lh, rm))) + one(lh, rh)


def rows_of(ref, part, parts=2):
    size = ref.shape[0] // parts
    return ref.at[pl.ds(part * size, size)]


def inverse_factor(gram, work, store):
    tile = gram.shape[1]
    width = 2 * tile
    work[0:tile, 0:tile] = gram[0:tile]
    work[0:tile, tile:width] = gram[tile : 2 * tile]
    work[tile:width, tile:width] = gram[2 * tile : 3 * tile]
    at_row = lax.broadcasted_iota(jnp.int32, (width, width), 0)
    at_col = lax.broadcasted_iota(jnp.int32, (width, width), 1)
    work[:, width : 2 * width] = jnp.where(at_row == at_col, 1.0, 0.0).astype(F32)
    sub = lax.broadcasted_iota(jnp.int32, (GROUP, tile), 0)
    groups = PIVOTS // GROUP
    full = (GROUP, tile)

    def lane(row):
        return jnp.broadcast_to(row, full)

    for first in range(0, width, PIVOTS):
        near = first // tile
        offset = first - near * tile
        gram_tiles = list(range(near, 2))
        tiles = gram_tiles + [2 + i for i in range(near + 1)]
        data = {
            t: [work[pl.ds(first + GROUP * g, GROUP), t * tile : (t + 1) * tile] for g in range(groups)] for t in tiles
        }
        cols = [
            {g: jnp.broadcast_to(data[near][g][:, offset + j : offset + j + 1], full) for g in range(j // GROUP, groups)}
            for j in range(PIVOTS)
        ]
        pivots = [jnp.ones(full, F32) for _ in range(groups)]
        for j in range(PIVOTS):
            gj, rj = divmod(j, GROUP)
            col = cols[j]
            pivot = lane(col[gj][rj : rj + 1])
            inv = 1.0 / pivot
            pivots[gj] = jnp.where(sub == rj, pivot, pivots[gj])
            for nxt in range(j + 1, PIVOTS):
                gn, rn = divmod(nxt, GROUP)
                entry = lane(col[gn][rn : rn + 1])
                if nxt == j + 1:
                    for g in range(gn, groups):
                        cols[nxt][g] = cols[nxt][g] - (col[g] * entry) * inv
                else:
                    scaled = entry * inv
                    for g in range(gn, groups):
                        cols[nxt][g] = cols[nxt][g] - col[g] * scaled
            for g in range(gj, groups):
                factor = col[g] * inv
                if g == gj:
                    if rj == GROUP - 1:
                        continue
                    factor = jnp.where(sub > rj, factor, 0.0)
                for t in tiles:
                    data[t][g] = data[t][g] - factor * lane(data[t][gj][rj : rj + 1])
        scale = [lax.rsqrt(p) for p in pivots]
        for t in tiles:
            data[t] = [d * s for d, s in zip(data[t], scale, strict=True)]
        for t in tiles:
            if t >= 2:
                for g in range(groups):
                    store(first + GROUP * g, t - 2, data[t][g])
        nxt = first + PIVOTS
        if nxt == width:
            break
        parts = {t: split3(jnp.concatenate(data[t], axis=0)) for t in tiles}
        below = [t for t in gram_tiles if (t + 1) * tile > nxt]
        low = below[0] * tile
        order_l, order_r = (0, 0, 1, 0, 2, 1), (0, 1, 0, 2, 0, 1)
        lhs = jnp.concatenate([jnp.concatenate([parts[t][i] for i in order_l], axis=0) for t in below], axis=1)
        right_tiles = below + [t for t in tiles if t >= 2]
        rhs = jnp.concatenate([jnp.concatenate([parts[t][i] for i in order_r], axis=0) for t in right_tiles], axis=1)
        upd = lax.dot_general(lhs, rhs, TN, preferred_element_type=F32)
        for n, t in enumerate(right_tiles):
            where = pl.ds(nxt, width - nxt), slice(t * tile, (t + 1) * tile)
            work[where] = work[where] - upd[nxt - low :, n * tile : (n + 1) * tile]


def kernel(
    sizes, left_op, left_start, right_op, right_start, left_out, left_ray, right_out, right_ray,
    ops, ycur, ag_t, ag_a, p_t, p_a, d_a, r_t, r_a, x_half, x_move, g_loc, g_pair, g_sum, g_in, g_all, h_all, work, linv,
    send, recv, load_sem,
):
    nrow, ncol, total_rows = sizes
    sub, width = ycur.shape[1:]
    tile = width // 2
    nchips = RING * RING
    y = lax.axis_index("row")
    c = lax.axis_index("col")
    x, k = lax.div(c, CORES), lax.rem(c, CORES)
    other = 1 - k
    xp, xm, xf = (lax.rem(x + d, RING) for d in (1, 3, 2))
    yp, ym, yf = (lax.rem(y + d, RING) for d in (1, 3, 2))

    def dev(row, chip, core):
        return {"row": row, "col": chip * CORES + core}

    partner = dev(y, x, other)

    def push(i, src, dst, to):
        return pltpu.make_async_remote_copy(
            src_ref=src, dst_ref=dst, send_sem=send.at[i], recv_sem=recv.at[i], device_id=to, device_id_type=pl.DeviceIdType.MESH
        )

    loads = []
    for n, (xi, yi) in enumerate(((x, y), (xm, ym), (xp, yp), (xf, yf))):
        take = pl.ds(pl.multiple_of(xi * CORES * sub, sub), CORES * sub)
        loads.append(pltpu.make_async_copy(left_op.at[take], ops.at[0, take], load_sem.at[2 * n]))
        take = pl.ds(pl.multiple_of(yi * sub, sub), sub)
        loads.append(pltpu.make_async_copy(right_op.at[:, take], ops.at[1, :, take], load_sem.at[2 * n + 1]))
    starts = [
        pltpu.make_async_copy(left_start, ycur.at[0], load_sem.at[8]),
        pltpu.make_async_copy(right_start, ycur.at[1], load_sem.at[9]),
    ]
    for copy in starts + loads:
        copy.start()

    barrier = pltpu.get_barrier_semaphore()
    here = y * ncol + c
    for o in range(1, nrow * ncol):
        there = lax.rem(here + o, nrow * ncol)
        pl.semaphore_signal(
            barrier, inc=1, device_id={"row": lax.div(there, ncol), "col": lax.rem(there, ncol)}, device_id_type=pl.DeviceIdType.MESH
        )
    pl.semaphore_wait(barrier, nrow * ncol - 1)

    by_row, by_col = y * ncol + c, c * nrow + y
    to_col_y, to_col_c = lax.rem(by_row, nrow), lax.div(by_row, nrow)
    to_row_y, to_row_c = lax.div(by_col, ncol), lax.rem(by_col, ncol)
    stays = by_row == by_col

    for copy in starts:
        copy.wait()
    ag_t[c] = ycur[0].T.astype(BF16)
    x_half[...] = ycur[1].astype(BF16)
    first_move = push(MOVE, x_half, ag_a.at[to_col_y], {"row": to_col_y, "col": to_col_c})

    @pl.when(stays)
    def _():
        ag_a[y] = x_half[...]

    @pl.when(jnp.logical_not(stays))
    def _():
        first_move.start()
        first_move.wait()

    def ring_gather(base, blk, me, plus, minus, far, to):
        own = [rows_of(blk(me), h) for h in range(2)]
        first = [
            push(base + 0, own[0], own[0], to(plus)),
            push(base + 1, own[1], own[1], to(plus)),
            push(base + 2, own[1], own[1], to(minus)),
            push(base + 3, own[0], own[0], to(minus)),
        ]
        got0, got1 = rows_of(blk(minus), 0), rows_of(blk(plus), 1)
        return first, [push(base + 4, got0, got0, to(plus)), push(base + 5, got1, got1, to(minus))]

    def apply(p):
        t = lax.rem(p, 2)
        a = 1 - t

        def mm_t(chip, owner, first):
            lanes = pl.ds(pl.multiple_of(owner * sub, sub), sub)
            acc = None
            for core in range(CORES):
                b = chip * CORES + core
                rows = pl.ds(pl.multiple_of(b * sub, sub), sub)
                one = jnp.dot(ag_t[b], ops[t, rows, lanes], preferred_element_type=F32)
                acc = one if acc is None else acc + one
            p_t[owner] = acc if first else p_t[owner] + acc

        def mm_a(chip, owner, first):
            rows = pl.ds(pl.multiple_of(owner * sub, sub), sub)
            lanes = pl.ds(pl.multiple_of(chip * sub, sub), sub)
            acc = jnp.dot(ops[a, rows, lanes], ag_a[chip], preferred_element_type=F32)
            p_a[owner] = acc if first else p_a[owner] + acc

        def loaded(n):
            @pl.when(p == 0)
            def _():
                loads[n].wait()

        send_t, fwd_t = ring_gather(AG_T, lambda i: ag_t.at[i * CORES + k], x, xp, xm, xf, lambda i: dev(y, i, k))
        send_a, fwd_a = ring_gather(AG_A, lambda i: ag_a.at[i], y, yp, ym, yf, lambda i: dev(i, x, k))

        def relay(n, i, h=None):
            ref = ag_t.at[i * CORES + k]
            ref = ref if h is None else rows_of(ref, h)
            return push(RELAY + n, ref, ref, partner)

        relays = [relay(0, x), relay(1, xm), relay(2, xp), relay(3, xf, 0), relay(4, xf, 1)]
        for n in (0, 2, 1, 3):
            send_t[n].start()
            send_a[n].start()
        relays[0].start()
        loaded(1)
        for owner in range(RING * CORES):
            mm_a(y, owner, True)
        relays[0].wait_recv()
        loaded(0)
        for owner in range(RING):
            mm_t(x, owner, True)
        send_t[0].wait_recv()
        fwd_t[0].start()
        send_a[0].wait_recv()
        fwd_a[0].start()
        send_t[2].wait_recv()
        fwd_t[1].start()
        send_a[2].wait_recv()
        fwd_a[1].start()
        send_t[1].wait_recv()
        relays[1].start()
        send_t[3].wait_recv()
        relays[2].start()
        send_a[1].wait_recv()
        loaded(3)
        for owner in range(RING * CORES):
            mm_a(ym, owner, False)
        send_a[3].wait_recv()
        loaded(5)
        for owner in range(RING * CORES):
            mm_a(yp, owner, False)
        relays[1].wait_recv()
        loaded(2)
        for owner in range(RING):
            mm_t(xm, owner, False)
        relays[2].wait_recv()
        loaded(4)
        for owner in range(RING):
            mm_t(xp, owner, False)
        fwd_t[0].wait_recv()
        relays[3].start()
        fwd_t[1].wait_recv()
        relays[4].start()
        fwd_a[0].wait_recv()
        fwd_a[1].wait_recv()

        loaded(7)
        pairs = []
        for n, i in enumerate((xf, xp, xm, x)):
            mm_a(yf, i * CORES + other, False)
            pairs.append(push(PAIR + n, p_a.at[i * CORES + other], d_a.at[i], partner))
            pairs[n].start()

        def ring_scatter(base, part, got, plus, minus, far, to):
            def half(i, h):
                return rows_of(part(i), h)

            return [
                push(base + 0, half(far, 0), got.at[0], to(plus)),
                push(base + 1, half(far, 1), got.at[1], to(minus)),
                push(base + 2, half(plus, 1), got.at[2], to(plus)),
                push(base + 3, half(minus, 0), got.at[3], to(minus)),
                push(base + 4, half(plus, 0), got.at[4], to(plus)),
                push(base + 5, half(minus, 1), got.at[5], to(minus)),
            ]

        out_t = ring_scatter(RS_T, lambda i: p_t.at[i], r_t, yp, ym, yf, lambda i: dev(i, x, k))
        out_a = ring_scatter(RS_A, lambda i: p_a.at[i * CORES + k], r_a, xp, xm, xf, lambda i: dev(y, i, k))
        relays[3].wait_recv()
        relays[4].wait_recv()
        loaded(6)
        for n, i in enumerate((yf, yp, ym, y)):
            mm_t(xf, i, False)
            for q in ((0, 1), (2,), (3,), ())[n]:
                out_t[q].start()
        for n, i in enumerate((xf, xp, xm, x)):
            mm_a(yf, i * CORES + k, False)
            pairs[n].wait_recv()
            p_a[i * CORES + k] = p_a[i * CORES + k] + d_a[i]
            for q in ((0, 1), (2,), (3,), ())[n]:
                out_a[q].start()
        ht, ha = width // 2, sub // 2
        out_t[0].wait_recv()
        p_t[yp, 0:ht] = p_t[yp, 0:ht] + r_t[0]
        out_t[4].start()
        out_t[1].wait_recv()
        p_t[ym, ht:width] = p_t[ym, ht:width] + r_t[1]
        out_t[5].start()
        out_a[0].wait_recv()
        kp, km, kk = xp * CORES + k, xm * CORES + k, x * CORES + k
        p_a[kp, 0:ha] = p_a[kp, 0:ha] + r_a[0]
        out_a[4].start()
        out_a[1].wait_recv()
        p_a[km, ha:sub] = p_a[km, ha:sub] + r_a[1]
        out_a[5].start()
        for n in (2, 3, 4, 5):
            out_t[n].wait_recv()
            out_a[n].wait_recv()
        ycur[t, :, 0:ht] = (p_t[y, 0:ht] + r_t[3] + r_t[4]).T
        ycur[t, :, ht:width] = (p_t[y, ht:width] + r_t[2] + r_t[5]).T
        ycur[a, 0:ha] = p_a[kk, 0:ha] + r_a[3] + r_a[4]
        ycur[a, ha:sub] = p_a[kk, ha:sub] + r_a[2] + r_a[5]
        for copy in send_t + fwd_t + send_a + fwd_a + relays + pairs + out_t + out_a:
            copy.wait_send()

    def all_reduce(rows):
        piece = rows // nchips
        pair = push(GRAM_PAIR, g_loc.at[other, pl.ds(0, rows)], g_pair.at[pl.ds(0, rows)], partner)
        pair.start()
        pair.wait_recv()
        g_sum[0:rows] = g_loc[k, 0:rows] + g_pair[0:rows]

        def chunk(ref, q):
            return ref.at[pl.ds(pl.multiple_of(q * piece, GROUP), piece)]

        def chips():
            for o in range(1, nchips):
                to_y, to_x = lax.rem(y + o // RING, RING), lax.rem(x + o % RING, RING)
                yield o, to_y * RING + to_x, dev(to_y, to_x, k)

        mine = y * RING + x
        for o, q, to in chips():
            push(GRAM_RS, chunk(g_sum, q), chunk(g_in, o - 1), to).start()
        others = pl.ds(0, (nchips - 1) * piece)
        pltpu.make_async_copy(g_in.at[others], g_in.at[others], recv.at[GRAM_RS]).wait()
        total = chunk(g_sum, mine)[...]
        for o in range(1, nchips):
            total = total + g_in[(o - 1) * piece : o * piece]
        chunk(g_all, mine)[...] = total / total_rows
        for o, q, to in chips():
            push(GRAM_AG, chunk(g_all, mine), chunk(g_all, mine), to).start()
        pltpu.make_async_copy(g_in.at[others], g_in.at[others], recv.at[GRAM_AG]).wait()
        pair.wait_send()
        for i in (GRAM_RS, GRAM_AG):
            pltpu.make_async_copy(g_in.at[others], g_in.at[others], send.at[i]).wait()

    def gram_blocks(op, dot):
        lo, hi = ycur[op, :, 0:tile], ycur[op, :, tile:width]
        g_loc[op, 0:tile] = dot(lo, lo)
        g_loc[op, tile : 2 * tile] = dot(lo, hi)
        g_loc[op, 2 * tile : 3 * tile] = dot(hi, hi)

    def half_dot(u, v):
        return lax.dot_general(u.astype(BF16), v.astype(BF16), TN, preferred_element_type=F32)

    def full_dot(u, v):
        return dot_f32(u, v, TN)

    def normalize(q):
        @pl.when(q == 0)
        def _():
            for op in range(2):
                gram_blocks(op, half_dot)

        @pl.when(q == 1)
        def _():
            for op in range(2):
                gram_blocks(op, full_dot)

        all_reduce(3 * tile)

        def store(first, t, value):
            linv[k, pl.ds(first, GROUP), t * tile : (t + 1) * tile] = value

        linv[k, 0:tile, tile:width] = jnp.zeros((tile, tile), F32)
        inverse_factor(g_all, work, store)
        swap = push(LINV, linv.at[k], linv.at[k], partner)
        swap.start()
        ycur[k] = dot_f32(ycur[k], linv[k], NT)
        swap.wait_recv()
        ycur[other] = dot_f32(ycur[other], linv[other], NT)
        swap.wait_send()

    keep_left = push(MOVE + 1, ycur.at[0], x_move.at[0], {"row": to_col_y, "col": to_col_c})
    keep_right = push(MOVE + 2, ycur.at[1], x_move.at[1], {"row": to_row_y, "col": to_row_c})

    def sweep(p, carry):
        apply(p)

        @pl.when(p < SWEEPS)
        def _():
            def one(q, carry):
                normalize(q)
                return carry

            lax.fori_loop(0, 2, one, 0)
            nxt = lax.rem(p + 1, 2)
            ag_t[c] = ycur[nxt].T.astype(BF16)
            ag_a[y] = ycur[1 - nxt].astype(BF16)

        @pl.when(p == SWEEPS - 1)
        def _():
            left_out[...] = ycur[0]

            @pl.when(stays)
            def _():
                x_move[...] = ycur[...]

            @pl.when(jnp.logical_not(stays))
            def _():
                keep_left.start()
                keep_right.start()
                keep_left.wait()
                keep_right.wait()

        return carry

    lax.fori_loop(0, SWEEPS + 1, sweep, 0)
    right_out[...] = x_move[1]
    for op in range(2):
        for n, (i, j) in enumerate(((0, 0), (0, 1), (1, 0), (1, 1))):
            xs, zs = slice(i * tile, (i + 1) * tile), slice(j * tile, (j + 1) * tile)
            g_loc[op, n * tile : (n + 1) * tile] = dot_f32(x_move[op, :, xs], ycur[op, :, zs], TN)
    all_reduce(4 * tile)
    swap = push(LINV, g_all, h_all, partner)
    swap.start()
    swap.wait()
    for n, (i, j) in enumerate(((0, 0), (0, 1), (1, 0), (1, 1))):
        rows, at = slice(n * tile, (n + 1) * tile), (slice(i * tile, (i + 1) * tile), slice(j * tile, (j + 1) * tile))
        left_ray[at] = jnp.where(k == 0, g_all[rows], h_all[rows])
        right_ray[at] = jnp.where(k == 0, h_all[rows], g_all[rows])


def solution(mesh):
    nrow, ncol = mesh.shape["row"], mesh.shape["col"]
    assert nrow == RING and ncol == RING * CORES

    def local_program(left_op, left_start, right_op, right_start):
        rows, cols = left_op.shape
        sub, width = left_start.shape
        tile = width // 2
        vmem = pltpu.VMEM
        dma = pltpu.SemaphoreType.DMA
        out = [
            jax.ShapeDtypeStruct((sub, width), F32),
            jax.ShapeDtypeStruct((width, width), F32),
        ] * 2
        return pl.pallas_call(
            functools.partial(kernel, (nrow, ncol, rows * nrow)),
            out_shape=out,
            in_specs=[pl.BlockSpec(memory_space=pl.ANY)] * 4,
            out_specs=[pl.BlockSpec(memory_space=vmem)] * 4,
            scratch_shapes=[
                vmem((2, rows, cols), BF16),
                vmem((2, sub, width), F32),
                vmem((ncol, width, sub), BF16),
                vmem((nrow, sub, width), BF16),
                vmem((nrow, width, sub), F32),
                vmem((ncol, sub, width), F32),
                vmem((RING, sub, width), F32),
                vmem((6, width // 2, sub), F32),
                vmem((6, sub // 2, width), F32),
                vmem((sub, width), BF16),
                vmem((2, sub, width), F32),
                vmem((2, 4 * tile, tile), F32),
                vmem((4 * tile, tile), F32),
                vmem((4 * tile, tile), F32),
                vmem((4 * tile, tile), F32),
                vmem((4 * tile, tile), F32),
                vmem((4 * tile, tile), F32),
                vmem((width, 2 * width), F32),
                vmem((2, width, width), F32),
                dma((COPIES,)),
                dma((COPIES,)),
                dma((10,)),
            ],
            compiler_params=pltpu.CompilerParams(collective_id=0, has_side_effects=True, vmem_limit_bytes=VMEM_BYTES),
            name="subspace",
        )(left_op, left_start, right_op, right_start)

    op_spec = P(("batch", "row"), "col")
    vec_spec = P(("batch", "row", "col"), None)
    small_spec = P("batch", None)
    return jax.shard_map(
        local_program,
        mesh=mesh,
        in_specs=(op_spec, vec_spec, op_spec, vec_spec),
        out_specs=(vec_spec, small_spec, vec_spec, small_spec),
        check_vma=False,
    )
```

```python
import functools

import jax
import jax.numpy as jnp
from jax import lax
from jax.experimental import pallas as pl
from jax.experimental.pallas import tpu as pltpu
from jax.sharding import PartitionSpec as P

SWEEPS = 4
CORES = 2
RING = 4
PIVOTS = 32
GROUP = 8
VMEM_BYTES = 67043328
F32, BF16 = jnp.float32, jnp.bfloat16
TN = (((0,), (0,)), ((), ()))
NT = (((1,), (1,)), ((), ()))

AG_T, AG_A, RELAY, RS_T, RS_A, PAIR, GRAM_PAIR, GRAM_RS, GRAM_AG, LINV, MOVE = 0, 6, 12, 19, 25, 31, 35, 36, 37, 38, 39
COPIES = 42


def split3(v):
    high = v.astype(BF16)
    rest = v - high.astype(F32)
    mid = rest.astype(BF16)
    return high, mid, (rest - mid.astype(F32)).astype(BF16)


def dot_f32(lhs, rhs, dims):
    lh, lm, ll = split3(lhs)
    rh, rm, rl = split3(rhs)

    def one(a, b):
        return lax.dot_general(a, b, dims, preferred_element_type=F32)

    small = one(ll, rh) + one(lh, rl) + one(lm, rm)
    return (small + (one(lm, rh) + one(lh, rm))) + one(lh, rh)


class Phases:
    def __init__(self):
        self.scope = None

    def __call__(self, name=None):
        if self.scope is not None:
            self.scope.__exit__(None, None, None)
        self.scope = None
        if name is not None:
            self.scope = jax.named_scope(name)
            self.scope.__enter__()


def rows_of(ref, part, parts=2):
    size = ref.shape[0] // parts
    return ref.at[pl.ds(part * size, size)]


def inverse_factor(gram, work, store):
    tile = gram.shape[1]
    width = 2 * tile
    work[0:tile, 0:tile] = gram[0:tile]
    work[0:tile, tile:width] = gram[tile : 2 * tile]
    work[tile:width, tile:width] = gram[2 * tile : 3 * tile]
    at_row = lax.broadcasted_iota(jnp.int32, (width, width), 0)
    at_col = lax.broadcasted_iota(jnp.int32, (width, width), 1)
    work[:, width : 2 * width] = jnp.where(at_row == at_col, 1.0, 0.0).astype(F32)
    sub = lax.broadcasted_iota(jnp.int32, (GROUP, tile), 0)
    groups = PIVOTS // GROUP
    full = (GROUP, tile)

    def lane(row):
        return jnp.broadcast_to(row, full)

    for first in range(0, width, PIVOTS):
        near = first // tile
        offset = first - near * tile
        gram_tiles = list(range(near, 2))
        tiles = gram_tiles + [2 + i for i in range(near + 1)]
        data = {
            t: [work[pl.ds(first + GROUP * g, GROUP), t * tile : (t + 1) * tile] for g in range(groups)] for t in tiles
        }
        cols = [
            {g: jnp.broadcast_to(data[near][g][:, offset + j : offset + j + 1], full) for g in range(j // GROUP, groups)}
            for j in range(PIVOTS)
        ]
        pivots = [jnp.ones(full, F32) for _ in range(groups)]
        for j in range(PIVOTS):
            gj, rj = divmod(j, GROUP)
            col = cols[j]
            pivot = lane(col[gj][rj : rj + 1])
            inv = 1.0 / pivot
            pivots[gj] = jnp.where(sub == rj, pivot, pivots[gj])
            for nxt in range(j + 1, PIVOTS):
                gn, rn = divmod(nxt, GROUP)
                entry = lane(col[gn][rn : rn + 1])
                if nxt == j + 1:
                    for g in range(gn, groups):
                        cols[nxt][g] = cols[nxt][g] - (col[g] * entry) * inv
                else:
                    scaled = entry * inv
                    for g in range(gn, groups):
                        cols[nxt][g] = cols[nxt][g] - col[g] * scaled
            for g in range(gj, groups):
                factor = col[g] * inv
                if g == gj:
                    if rj == GROUP - 1:
                        continue
                    factor = jnp.where(sub > rj, factor, 0.0)
                for t in tiles:
                    data[t][g] = data[t][g] - factor * lane(data[t][gj][rj : rj + 1])
        scale = [lax.rsqrt(p) for p in pivots]
        for t in tiles:
            data[t] = [d * s for d, s in zip(data[t], scale, strict=True)]
        for t in tiles:
            if t >= 2:
                for g in range(groups):
                    store(first + GROUP * g, t - 2, data[t][g])
        nxt = first + PIVOTS
        if nxt == width:
            break
        parts = {t: split3(jnp.concatenate(data[t], axis=0)) for t in tiles}
        below = [t for t in gram_tiles if (t + 1) * tile > nxt]
        low = below[0] * tile
        order_l, order_r = (0, 0, 1, 0, 2, 1), (0, 1, 0, 2, 0, 1)
        lhs = jnp.concatenate([jnp.concatenate([parts[t][i] for i in order_l], axis=0) for t in below], axis=1)
        right_tiles = below + [t for t in tiles if t >= 2]
        rhs = jnp.concatenate([jnp.concatenate([parts[t][i] for i in order_r], axis=0) for t in right_tiles], axis=1)
        upd = lax.dot_general(lhs, rhs, TN, preferred_element_type=F32)
        for n, t in enumerate(right_tiles):
            where = pl.ds(nxt, width - nxt), slice(t * tile, (t + 1) * tile)
            work[where] = work[where] - upd[nxt - low :, n * tile : (n + 1) * tile]


def kernel(
    sizes, left_op, left_start, right_op, right_start, x_out, h_out,
    ops, ycur, ag_t, ag_a, p_t, p_a, d_a, r_t, r_a, x_half, y_keep, x_move, g_loc, g_pair, g_sum, g_in, g_all, h_all, work, linv,
    send, recv, load_sem,
):
    nrow, ncol, total_rows = sizes
    sub, width = ycur.shape[1:]
    tile, hsub = width // 2, sub // 2
    nchips = RING * RING
    y = lax.axis_index("row")
    c = lax.axis_index("col")
    x, k = lax.div(c, CORES), lax.rem(c, CORES)
    other = 1 - k
    xp, xm, xf = (lax.rem(x + d, RING) for d in (1, 3, 2))
    yp, ym, yf = (lax.rem(y + d, RING) for d in (1, 3, 2))

    def dev(row, chip, core):
        return {"row": row, "col": chip * CORES + core}

    partner = dev(y, x, other)

    def push(i, src, dst, to):
        return pltpu.make_async_remote_copy(
            src_ref=src, dst_ref=dst, send_sem=send.at[i], recv_sem=recv.at[i], device_id=to, device_id_type=pl.DeviceIdType.MESH
        )

    def spot(i):
        return lax.rem(i + RING - x, RING)

    def run(index, size):
        return pl.ds(pl.multiple_of(index * size, size), size)

    phase = Phases()
    phase("boot")
    starts = [
        pltpu.make_async_copy(left_start, ycur.at[0], load_sem.at[8]),
        pltpu.make_async_copy(right_start, ycur.at[1], load_sem.at[9]),
    ]
    loads_t, loads_a = [], []
    for n, (xi, yi) in enumerate(((x, y), (xm, ym), (xp, yp), (xf, yf))):
        take = run(xi, CORES * sub)
        loads_t.append(pltpu.make_async_copy(left_op.at[take], ops.at[0, take], load_sem.at[2 * n]))
        take = run(spot(yi), sub)
        loads_a.append(pltpu.make_async_copy(right_op.at[:, take], ops.at[1, :, take], load_sem.at[2 * n + 1]))
    for copy in starts + loads_t + loads_a:
        copy.start()

    barrier = pltpu.get_barrier_semaphore()
    here = y * ncol + c
    for o in range(1, nrow * ncol):
        there = lax.rem(here + o, nrow * ncol)
        pl.semaphore_signal(
            barrier, inc=1, device_id={"row": lax.div(there, ncol), "col": lax.rem(there, ncol)}, device_id_type=pl.DeviceIdType.MESH
        )

    in_col = lax.rem(c, nrow)
    to_col_c = y * CORES + lax.div(c, nrow)
    to_col_y = lax.rem(y + in_col, RING)
    to_row_y = x
    to_row_c = k * nrow + spot(y)
    stays = jnp.logical_and(to_col_c == c, to_col_y == y)
    leaves = jnp.logical_not(stays)

    for copy in starts:
        copy.wait()
    for h in range(2):
        ag_t[c, h] = ycur[0, h * hsub : (h + 1) * hsub].T.astype(BF16)
    x_half[...] = ycur[1].astype(BF16)
    pl.semaphore_wait(barrier, nrow * ncol - 1)
    first_moves = [
        push(MOVE + h, x_half.at[pl.ds(h * hsub, hsub)], ag_a.at[to_col_y, h], {"row": to_col_y, "col": to_col_c}) for h in range(2)
    ]

    @pl.when(leaves)
    def _():
        for copy in first_moves:
            copy.start()

    phase()

    def ring_gather(base, blk, me, plus, minus, to):
        own = [blk(me, h) for h in range(2)]
        first = [
            push(base + 0, own[0], own[0], to(plus)),
            push(base + 1, own[1], own[1], to(plus)),
            push(base + 2, own[1], own[1], to(minus)),
            push(base + 3, own[0], own[0], to(minus)),
        ]
        got0, got1 = blk(minus, 0), blk(plus, 1)
        return first, [push(base + 4, got0, got0, to(plus)), push(base + 5, got1, got1, to(minus))]

    def ring_scatter(base, part, got, plus, minus, far, to):
        def half(i, h):
            return rows_of(part(i), h)

        return [
            push(base + 0, half(far, 0), got.at[0], to(plus)),
            push(base + 1, half(far, 1), got.at[1], to(minus)),
            push(base + 2, half(plus, 1), got.at[2], to(plus)),
            push(base + 3, half(minus, 0), got.at[3], to(minus)),
            push(base + 4, half(plus, 0), got.at[4], to(plus)),
            push(base + 5, half(minus, 1), got.at[5], to(minus)),
        ]

    keep_left = push(MOVE, y_keep.at[0], x_move.at[0], {"row": to_col_y, "col": to_col_c})
    keep_right = push(MOVE + 1, y_keep.at[1], x_move.at[1], {"row": to_row_y, "col": to_row_c})
    out_left = pltpu.make_async_copy(y_keep.at[0], x_out.at[0], load_sem.at[0])
    out_right = pltpu.make_async_copy(x_move.at[1], x_out.at[1], load_sem.at[1])

    def apply(p):
        t = lax.rem(p, 2)
        a = 1 - t

        def mm_t(pieces, owner, first=False):
            acc = None
            for chip, h in pieces:
                for core in range(CORES):
                    b = chip * CORES + core
                    one = jnp.dot(ag_t[b, h], ops[t, run(b * 2 + h, hsub), run(spot(owner), sub)], preferred_element_type=F32)
                    acc = one if acc is None else acc + one
            p_t[owner] = acc if first else p_t[owner] + acc

        def mm_a(pieces, owner, first=False):
            acc = None
            for i, h in pieces:
                one = jnp.dot(ops[a, run(owner, sub), run(spot(i) * 2 + h, hsub)], ag_a[i, h], preferred_element_type=F32)
                acc = one if acc is None else acc + one
            p_a[owner] = acc if first else p_a[owner] + acc

        def loaded(copy):
            @pl.when(p == 0)
            def _():
                copy.wait()

        send_t, fwd_t = ring_gather(AG_T, lambda i, h: ag_t.at[i * CORES + k, h], x, xp, xm, lambda i: dev(y, i, k))
        send_a, fwd_a = ring_gather(AG_A, lambda i, h: ag_a.at[i, h], y, yp, ym, lambda i: dev(i, x, k))

        def relay(n, i, h=None):
            ref = ag_t.at[i * CORES + k] if h is None else ag_t.at[i * CORES + k, h]
            return push(RELAY + n, ref, ref, partner)

        relays = [relay(0, x)] + [relay(1 + n, i, h) for n, (i, h) in enumerate(((xm, 0), (xp, 1), (xm, 1), (xp, 0), (xf, 0), (xf, 1)))]
        own_y = [(y, 0), (y, 1)]
        phase("ag_own")
        for n in (0, 2, 1, 3):
            send_t[n].start()
        relays[0].start()

        @pl.when(p > 0)
        def _():
            for n in (0, 2, 1, 3):
                send_a[n].start()
            for owner in range(RING * CORES):
                mm_a(own_y, owner, True)

        relays[0].wait_recv()
        loaded(loads_t[0])
        for owner in range(RING):
            mm_t([(x, 0), (x, 1)], owner, True)

        @pl.when(p == 0)
        def _():
            @pl.when(leaves)
            def _():
                for copy in first_moves:
                    copy.wait()

            @pl.when(stays)
            def _():
                for h in range(2):
                    ag_a[y, h] = x_half[h * hsub : (h + 1) * hsub]

            for n in (0, 2, 1, 3):
                send_a[n].start()
            loads_a[0].wait()
            for owner in range(RING * CORES):
                mm_a(own_y, owner, True)

        phase("ag_wait1")
        for n, fwd in ((0, 0), (2, 1)):
            send_t[n].wait_recv()
            fwd_t[fwd].start()
            relays[1 + fwd].start()
        for n, fwd in ((0, 0), (2, 1)):
            send_a[n].wait_recv()
            fwd_a[fwd].start()
        phase("mm_near1")
        loaded(loads_a[1])
        loaded(loads_a[2])
        for owner in range(RING * CORES):
            mm_a([(ym, 0), (yp, 1)], owner)
        relays[1].wait_recv()
        relays[2].wait_recv()
        loaded(loads_t[1])
        loaded(loads_t[2])
        for owner in range(RING):
            mm_t([(xm, 0), (xp, 1)], owner)
        phase("mm_near2")
        for n in (1, 3):
            send_t[n].wait_recv()
            relays[3 + n // 2].start()
        for n in (1, 3):
            send_a[n].wait_recv()
        for owner in range(RING * CORES):
            mm_a([(ym, 1), (yp, 0)], owner)
        for n in range(2):
            fwd_t[n].wait_recv()
            relays[5 + n].start()
        relays[3].wait_recv()
        relays[4].wait_recv()
        for owner in range(RING):
            mm_t([(xm, 1), (xp, 0)], owner)
        phase("ag_far")
        fwd_a[0].wait_recv()
        fwd_a[1].wait_recv()
        phase("mm_far")

        loaded(loads_a[3])
        pairs = []
        far_y = [(yf, 0), (yf, 1)]
        for n, i in enumerate((xf, xp, xm, x)):
            mm_a(far_y, i * CORES + other)
            pairs.append(push(PAIR + n, p_a.at[i * CORES + other], d_a.at[i], partner))
            pairs[n].start()
        out_t = ring_scatter(RS_T, lambda i: p_t.at[i], r_t, yp, ym, yf, lambda i: dev(i, x, k))
        out_a = ring_scatter(RS_A, lambda i: p_a.at[i * CORES + k], r_a, xp, xm, xf, lambda i: dev(y, i, k))
        for i in (xf, xp, xm, x):
            mm_a(far_y, i * CORES + k)
        relays[5].wait_recv()
        relays[6].wait_recv()
        loaded(loads_t[3])
        for n, (iy, ix) in enumerate(((yf, xf), (yp, xp), (ym, xm), (y, x))):
            mm_t([(xf, 0), (xf, 1)], iy)
            for q in ((0, 1), (2,), (3,), ())[n]:
                out_t[q].start()
            pairs[n].wait_recv()
            p_a[ix * CORES + k] = p_a[ix * CORES + k] + d_a[ix]
            for q in ((0, 1), (2,), (3,), ())[n]:
                out_a[q].start()
        phase("rs_mid")

        @pl.when(p == SWEEPS)
        def _():
            @pl.when(leaves)
            def _():
                keep_left.wait()
                keep_right.wait()

            @pl.when(stays)
            def _():
                x_move[...] = y_keep[...]

            for op in range(2):
                for q in range(2):
                    x_move[op] = dot_f32(x_move[op], linv[q, op], NT)
            out_right.start()
            y_keep[0] = ycur[0]
            out_left.start()

        ht = width // 2
        out_t[0].wait_recv()
        p_t[yp, 0:ht] = p_t[yp, 0:ht] + r_t[0]
        out_t[4].start()
        out_t[1].wait_recv()
        p_t[ym, ht:width] = p_t[ym, ht:width] + r_t[1]
        out_t[5].start()
        out_a[0].wait_recv()
        kp, km, kk = xp * CORES + k, xm * CORES + k, x * CORES + k
        p_a[kp, 0:hsub] = p_a[kp, 0:hsub] + r_a[0]
        out_a[4].start()
        out_a[1].wait_recv()
        p_a[km, hsub:sub] = p_a[km, hsub:sub] + r_a[1]
        out_a[5].start()
        phase("rs_end")
        for n in (2, 3, 4, 5):
            out_t[n].wait_recv()
            out_a[n].wait_recv()
        phase("rs_sum")
        ycur[t, :, 0:ht] = (p_t[y, 0:ht] + r_t[3] + r_t[4]).T
        ycur[t, :, ht:width] = (p_t[y, ht:width] + r_t[2] + r_t[5]).T
        ycur[a, 0:hsub] = p_a[kk, 0:hsub] + r_a[3] + r_a[4]
        ycur[a, hsub:sub] = p_a[kk, hsub:sub] + r_a[2] + r_a[5]
        phase("rs_drain")
        for copy in send_t + fwd_t + send_a + fwd_a + relays + pairs + out_t + out_a:
            copy.wait_send()
        phase()

    def all_reduce(rows, local):
        piece = rows // nchips
        phase("ar_pair")
        local(other)
        pair = push(GRAM_PAIR, g_loc.at[other, pl.ds(0, rows)], g_pair.at[pl.ds(0, rows)], partner)
        pair.start()
        local(k)
        pair.wait_recv()
        g_sum[0:rows] = g_loc[k, 0:rows] + g_pair[0:rows]

        def chunk(ref, q):
            return ref.at[pl.ds(pl.multiple_of(q * piece, GROUP), piece)]

        def chips():
            for o in range(1, nchips):
                to_y, to_x = lax.rem(y + o // RING, RING), lax.rem(x + o % RING, RING)
                yield o, to_y * RING + to_x, dev(to_y, to_x, k)

        phase("ar_rs")
        mine = y * RING + x
        for o, q, to in chips():
            push(GRAM_RS, chunk(g_sum, q), chunk(g_in, o - 1), to).start()
        others = pl.ds(0, (nchips - 1) * piece)
        pltpu.make_async_copy(g_in.at[others], g_in.at[others], recv.at[GRAM_RS]).wait()
        phase("ar_ag")
        total = chunk(g_sum, mine)[...]
        for o in range(1, nchips):
            total = total + g_in[(o - 1) * piece : o * piece]
        chunk(g_all, mine)[...] = total / total_rows
        for o, q, to in chips():
            push(GRAM_AG, chunk(g_all, mine), chunk(g_all, mine), to).start()
        pltpu.make_async_copy(g_in.at[others], g_in.at[others], recv.at[GRAM_AG]).wait()
        phase("ar_drain")
        pair.wait_send()
        for i in (GRAM_RS, GRAM_AG):
            pltpu.make_async_copy(g_in.at[others], g_in.at[others], send.at[i]).wait()
        phase()

    def gram_blocks(op, dot):
        lo, hi = ycur[op, :, 0:tile], ycur[op, :, tile:width]
        g_loc[op, 0:tile] = dot(lo, lo)
        g_loc[op, tile : 2 * tile] = dot(lo, hi)
        g_loc[op, 2 * tile : 3 * tile] = dot(hi, hi)

    def half_dot(u, v):
        return lax.dot_general(u.astype(BF16), v.astype(BF16), TN, preferred_element_type=F32)

    def full_dot(u, v):
        return dot_f32(u, v, TN)

    def normalize(p, q):
        def local(op):
            @pl.when(q == 0)
            def _():
                gram_blocks(op, half_dot)

            @pl.when(q == 1)
            def _():
                gram_blocks(op, full_dot)

        all_reduce(3 * tile, local)
        last = p == SWEEPS - 1

        @pl.when(jnp.logical_and(last, q == 0))
        def _():
            y_keep[...] = ycur[...]

            @pl.when(leaves)
            def _():
                keep_right.start()

        @pl.when(jnp.logical_and(jnp.logical_and(last, q == 1), leaves))
        def _():
            keep_left.start()

        phase("chol")

        def store(first, t, value):
            linv[q, k, pl.ds(first, GROUP), t * tile : (t + 1) * tile] = value

        linv[q, k, 0:tile, tile:width] = jnp.zeros((tile, tile), F32)
        inverse_factor(g_all, work, store)
        phase("mul_own")
        swap = push(LINV, linv.at[q, k], linv.at[q, k], partner)
        swap.start()
        ycur[k] = dot_f32(ycur[k], linv[q, k], NT)
        phase("mul_other")
        swap.wait_recv()
        ycur[other] = dot_f32(ycur[other], linv[q, other], NT)
        swap.wait_send()
        phase()

    def sweep(p, carry):
        apply(p)

        @pl.when(p < SWEEPS)
        def _():
            def one(q, carry):
                normalize(p, q)
                return carry

            lax.fori_loop(0, 2, one, 0)
            phase("next_x")
            nxt = lax.rem(p + 1, 2)
            for h in range(2):
                rows = slice(h * hsub, (h + 1) * hsub)
                ag_t[c, h] = ycur[nxt, rows].T.astype(BF16)
                ag_a[y, h] = ycur[1 - nxt, rows].astype(BF16)
            phase()

        return carry

    lax.fori_loop(0, SWEEPS + 1, sweep, 0)
    corners = ((0, 0), (0, 1), (1, 0), (1, 1))

    def rayleigh(op):
        for n, (i, j) in enumerate(corners):
            xs, zs = slice(i * tile, (i + 1) * tile), slice(j * tile, (j + 1) * tile)
            g_loc[op, n * tile : (n + 1) * tile] = dot_f32(x_move[op, :, xs], ycur[op, :, zs], TN)

    all_reduce(4 * tile, rayleigh)
    phase("h_swap")
    swap = push(LINV, g_all, h_all, partner)
    swap.start()
    swap.wait()
    for n, (i, j) in enumerate(corners):
        rows, at = slice(n * tile, (n + 1) * tile), (slice(i * tile, (i + 1) * tile), slice(j * tile, (j + 1) * tile))
        for op in range(2):
            h_out[(op, *at)] = jnp.where(k == op, g_all[rows], h_all[rows])
    out_left.wait()
    out_right.wait()
    phase()


def hand_over(x_ref, h_ref, left_x, left_h, right_x, right_h):
    left_x[...] = x_ref[0]
    left_h[...] = h_ref[0]
    right_x[...] = x_ref[1]
    right_h[...] = h_ref[1]


def solution(mesh):
    nrow, ncol = mesh.shape["row"], mesh.shape["col"]
    assert nrow == RING and ncol == RING * CORES

    def local_program(left_op, left_start, right_op, right_start):
        rows, cols = left_op.shape
        sub, width = left_start.shape
        tile = width // 2
        vmem = pltpu.VMEM
        dma = pltpu.SemaphoreType.DMA
        basis, ray = jax.ShapeDtypeStruct((sub, width), F32), jax.ShapeDtypeStruct((width, width), F32)
        both_x, both_h = pl.pallas_call(
            functools.partial(kernel, (nrow, ncol, rows * nrow)),
            out_shape=[jax.ShapeDtypeStruct((2, sub, width), F32), jax.ShapeDtypeStruct((2, width, width), F32)],
            in_specs=[pl.BlockSpec(memory_space=pl.ANY)] * 4,
            out_specs=[pl.BlockSpec(memory_space=pl.ANY), pl.BlockSpec(memory_space=vmem)],
            scratch_shapes=[
                vmem((2, rows, cols), BF16),
                vmem((2, sub, width), F32),
                vmem((ncol, 2, width, sub // 2), BF16),
                vmem((nrow, 2, sub // 2, width), BF16),
                vmem((nrow, width, sub), F32),
                vmem((ncol, sub, width), F32),
                vmem((RING, sub, width), F32),
                vmem((6, width // 2, sub), F32),
                vmem((6, sub // 2, width), F32),
                vmem((sub, width), BF16),
                vmem((2, sub, width), F32),
                vmem((2, sub, width), F32),
                vmem((2, 4 * tile, tile), F32),
                vmem((4 * tile, tile), F32),
                vmem((4 * tile, tile), F32),
                vmem((4 * tile, tile), F32),
                vmem((4 * tile, tile), F32),
                vmem((4 * tile, tile), F32),
                vmem((width, 2 * width), F32),
                vmem((2, 2, width, width), F32),
                dma((COPIES,)),
                dma((COPIES,)),
                dma((10,)),
            ],
            compiler_params=pltpu.CompilerParams(collective_id=0, has_side_effects=True, vmem_limit_bytes=VMEM_BYTES),
            name="subspace",
        )(left_op, left_start, right_op, right_start)
        whole = pl.BlockSpec(memory_space=vmem)
        return pl.pallas_call(
            hand_over, out_shape=[basis, ray, basis, ray], in_specs=[whole] * 2, out_specs=[whole] * 4, name="hand_over"
        )(both_x, both_h)

    op_spec = P(("batch", "row"), "col")
    vec_spec = P(("batch", "row", "col"), None)
    small_spec = P("batch", None)
    return jax.shard_map(
        local_program,
        mesh=mesh,
        in_specs=(op_spec, vec_spec, op_spec, vec_spec),
        out_specs=(vec_spec, small_spec, vec_spec, small_spec),
        check_vma=False,
    )
```

```python
import functools

import jax
import jax.numpy as jnp
from jax import lax
from jax.experimental import pallas as pl
from jax.experimental.pallas import tpu as pltpu
from jax.sharding import PartitionSpec as P

SWEEPS = 4
CORES = 2
RING = 4
PIVOTS = 32
STEP = 16
LEFT_PARTS, RIGHT_PARTS = (2, 0, 1, 1, 0, 0), (0, 2, 1, 0, 1, 0)
GROUP = 8
VMEM_BYTES = 67043328
F32, BF16 = jnp.float32, jnp.bfloat16
TN = (((0,), (0,)), ((), ()))
NT = (((1,), (1,)), ((), ()))

AG_T, AG_A, RELAY, RS_T, RS_A, PAIR, GRAM_PAIR, GRAM_RS, GRAM_AG, LINV, MOVE = 0, 6, 12, 19, 25, 31, 35, 36, 37, 38, 39
COPIES = 42


def split3(v):
    high = v.astype(BF16)
    rest = v - high.astype(F32)
    mid = rest.astype(BF16)
    return high, mid, (rest - mid.astype(F32)).astype(BF16)


def dot_f32(lhs, rhs, dims):
    left, right = split3(lhs), split3(rhs)
    (lk,), (rk,) = dims[0]
    lhs = jnp.concatenate([left[i] for i in LEFT_PARTS], axis=lk)
    rhs = jnp.concatenate([right[i] for i in RIGHT_PARTS], axis=rk)
    return lax.dot_general(lhs, rhs, dims, preferred_element_type=F32)


def gram_f32(v):
    high, mid, low = split3(v)
    mixed = lax.dot_general(
        jnp.concatenate([high, high], axis=0), jnp.concatenate([low, mid], axis=0), TN, preferred_element_type=F32
    )
    small = lax.dot_general(mid, mid, TN, preferred_element_type=F32)
    return (small + (mixed + mixed.T)) + lax.dot_general(high, high, TN, preferred_element_type=F32)


class Phases:
    def __init__(self):
        self.scope = None

    def __call__(self, name=None):
        if self.scope is not None:
            self.scope.__exit__(None, None, None)
        self.scope = None
        if name is not None:
            self.scope = jax.named_scope(name)
            self.scope.__enter__()


def rows_of(ref, part, parts=2):
    size = ref.shape[0] // parts
    return ref.at[pl.ds(part * size, size)]


def inverse_factor(gram, work, store):
    tile = gram.shape[1]
    width = 2 * tile
    work[0:tile, 0:tile] = gram[0:tile]
    work[0:tile, tile:width] = gram[tile : 2 * tile]
    work[tile:width, tile:width] = gram[2 * tile : 3 * tile]
    at_row = lax.broadcasted_iota(jnp.int32, (width, width), 0)
    at_col = lax.broadcasted_iota(jnp.int32, (width, width), 1)
    work[:, width : 2 * width] = jnp.where(at_row == at_col, 1.0, 0.0).astype(F32)
    sub = lax.broadcasted_iota(jnp.int32, (GROUP, tile), 0)
    groups = PIVOTS // GROUP
    full = (GROUP, tile)

    def lane(row):
        return jnp.broadcast_to(row, full)

    for first in range(0, width, PIVOTS):
        near = first // tile
        gram_tiles = list(range(near, 2))
        tiles = gram_tiles + [2 + i for i in range(near + 1)]
        data = {
            t: [work[pl.ds(first + GROUP * g, GROUP), t * tile : (t + 1) * tile] for g in range(groups)] for t in tiles
        }
        pivots = [jnp.ones(full, F32) for _ in range(groups)]
        for start in range(0, PIVOTS, STEP):
            at = first - near * tile + start
            end = start + STEP
            cols = {
                j: {
                    g: jnp.broadcast_to(data[near][g][:, at + j - start : at + j - start + 1], full)
                    for g in range(j // GROUP, groups)
                }
                for j in range(start, end)
            }
            for j in range(start, end):
                gj, rj = divmod(j, GROUP)
                col = cols[j]
                pivot = lane(col[gj][rj : rj + 1])
                inv = 1.0 / pivot
                pivots[gj] = jnp.where(sub == rj, pivot, pivots[gj])
                for nxt in range(j + 1, end):
                    gn, rn = divmod(nxt, GROUP)
                    entry = lane(col[gn][rn : rn + 1])
                    if nxt == j + 1:
                        for g in range(gn, groups):
                            cols[nxt][g] = cols[nxt][g] - (col[g] * entry) * inv
                    else:
                        scaled = entry * inv
                        for g in range(gn, groups):
                            cols[nxt][g] = cols[nxt][g] - col[g] * scaled
                for g in range(gj, groups):
                    factor = col[g] * inv
                    if g == gj:
                        if rj == GROUP - 1:
                            continue
                        factor = jnp.where(sub > rj, factor, 0.0)
                    for t in tiles:
                        data[t][g] = data[t][g] - factor * lane(data[t][gj][rj : rj + 1])
        scale = [lax.rsqrt(p) for p in pivots]
        for t in tiles:
            data[t] = [d * s for d, s in zip(data[t], scale, strict=True)]
        for t in tiles:
            if t >= 2:
                for g in range(groups):
                    store(first + GROUP * g, t - 2, data[t][g])
        nxt = first + PIVOTS
        if nxt == width:
            break
        parts = {t: split3(jnp.concatenate(data[t], axis=0)) for t in tiles}
        below = [t for t in gram_tiles if (t + 1) * tile > nxt]
        low = below[0] * tile
        lhs = jnp.concatenate([jnp.concatenate([parts[t][i] for i in LEFT_PARTS], axis=0) for t in below], axis=1)
        right_tiles = below + [t for t in tiles if t >= 2]
        rhs = jnp.concatenate([jnp.concatenate([parts[t][i] for i in RIGHT_PARTS], axis=0) for t in right_tiles], axis=1)
        upd = lax.dot_general(lhs, rhs, TN, preferred_element_type=F32)
        for n, t in enumerate(right_tiles):
            where = pl.ds(nxt, width - nxt), slice(t * tile, (t + 1) * tile)
            work[where] = work[where] - upd[nxt - low :, n * tile : (n + 1) * tile]


def kernel(
    sizes, left_op, left_start, right_op, right_start, x_out, h_out,
    ops, ycur, ag_t, ag_a, p_t, p_a, d_a, r_t, r_a, x_half, y_keep, x_move, g_loc, g_pair, g_sum, g_in, g_all, h_all, work, linv,
    send, recv, load_sem,
):
    nrow, ncol, total_rows = sizes
    sub, width = ycur.shape[1:]
    tile, hsub = width // 2, sub // 2
    nchips = RING * RING
    y = lax.axis_index("row")
    c = lax.axis_index("col")
    x, k = lax.div(c, CORES), lax.rem(c, CORES)
    other = 1 - k
    xp, xm, xf = (lax.rem(x + d, RING) for d in (1, 3, 2))
    yp, ym, yf = (lax.rem(y + d, RING) for d in (1, 3, 2))

    def dev(row, chip, core):
        return {"row": row, "col": chip * CORES + core}

    partner = dev(y, x, other)

    def push(i, src, dst, to):
        return pltpu.make_async_remote_copy(
            src_ref=src, dst_ref=dst, send_sem=send.at[i], recv_sem=recv.at[i], device_id=to, device_id_type=pl.DeviceIdType.MESH
        )

    def spot(i):
        return lax.rem(i + RING - x, RING)

    def run(index, size):
        return pl.ds(pl.multiple_of(index * size, size), size)

    phase = Phases()
    phase("boot")
    starts = [
        pltpu.make_async_copy(left_start, ycur.at[0], load_sem.at[8]),
        pltpu.make_async_copy(right_start, ycur.at[1], load_sem.at[9]),
    ]
    loads_t, loads_a = [], []
    for n, (xi, yi) in enumerate(((x, y), (xm, ym), (xp, yp), (xf, yf))):
        take = run(xi, CORES * sub)
        loads_t.append(pltpu.make_async_copy(left_op.at[take], ops.at[0, take], load_sem.at[2 * n]))
        take = run(spot(yi), sub)
        loads_a.append(pltpu.make_async_copy(right_op.at[:, take], ops.at[1, :, take], load_sem.at[2 * n + 1]))
    for copy in starts + loads_t + loads_a:
        copy.start()

    barrier = pltpu.get_barrier_semaphore()
    here = y * ncol + c
    for o in range(1, nrow * ncol):
        there = lax.rem(here + o, nrow * ncol)
        pl.semaphore_signal(
            barrier, inc=1, device_id={"row": lax.div(there, ncol), "col": lax.rem(there, ncol)}, device_id_type=pl.DeviceIdType.MESH
        )

    in_col = lax.rem(c, nrow)
    to_col_c = y * CORES + lax.div(c, nrow)
    to_col_y = lax.rem(y + in_col, RING)
    to_row_y = x
    to_row_c = k * nrow + spot(y)
    stays = jnp.logical_and(to_col_c == c, to_col_y == y)
    leaves = jnp.logical_not(stays)

    for copy in starts:
        copy.wait()
    for h in range(2):
        ag_t[c, h] = ycur[0, h * hsub : (h + 1) * hsub].T.astype(BF16)
    x_half[...] = ycur[1].astype(BF16)
    pl.semaphore_wait(barrier, nrow * ncol - 1)
    first_moves = [
        push(MOVE + h, x_half.at[pl.ds(h * hsub, hsub)], ag_a.at[to_col_y, h], {"row": to_col_y, "col": to_col_c}) for h in range(2)
    ]

    @pl.when(leaves)
    def _():
        for copy in first_moves:
            copy.start()

    phase()

    def ring_gather(base, blk, me, plus, minus, to):
        own = [blk(me, h) for h in range(2)]
        first = [
            push(base + 0, own[0], own[0], to(plus)),
            push(base + 1, own[1], own[1], to(plus)),
            push(base + 2, own[1], own[1], to(minus)),
            push(base + 3, own[0], own[0], to(minus)),
        ]
        got0, got1 = blk(minus, 0), blk(plus, 1)
        return first, [push(base + 4, got0, got0, to(plus)), push(base + 5, got1, got1, to(minus))]

    def ring_scatter(base, part, got, plus, minus, far, to):
        def half(i, h):
            return rows_of(part(i), h)

        return [
            push(base + 0, half(far, 0), got.at[0], to(plus)),
            push(base + 1, half(far, 1), got.at[1], to(minus)),
            push(base + 2, half(plus, 1), got.at[2], to(plus)),
            push(base + 3, half(minus, 0), got.at[3], to(minus)),
            push(base + 4, half(plus, 0), got.at[4], to(plus)),
            push(base + 5, half(minus, 1), got.at[5], to(minus)),
        ]

    keep_left = push(MOVE, y_keep.at[0], x_move.at[0], {"row": to_col_y, "col": to_col_c})
    keep_right = push(MOVE + 1, y_keep.at[1], x_move.at[1], {"row": to_row_y, "col": to_row_c})
    out_left = pltpu.make_async_copy(y_keep.at[0], x_out.at[0], load_sem.at[0])
    out_right = pltpu.make_async_copy(x_move.at[1], x_out.at[1], load_sem.at[1])

    def apply(p):
        t = lax.rem(p, 2)
        a = 1 - t

        def mm_t(pieces, owner, first=False):
            acc = None
            for chip, h in pieces:
                for core in range(CORES):
                    b = chip * CORES + core
                    one = jnp.dot(ag_t[b, h], ops[t, run(b * 2 + h, hsub), run(spot(owner), sub)], preferred_element_type=F32)
                    acc = one if acc is None else acc + one
            p_t[owner] = acc if first else p_t[owner] + acc

        def mm_a(pieces, owner, first=False):
            acc = None
            for i, h in pieces:
                one = jnp.dot(ops[a, run(owner, sub), run(spot(i) * 2 + h, hsub)], ag_a[i, h], preferred_element_type=F32)
                acc = one if acc is None else acc + one
            p_a[owner] = acc if first else p_a[owner] + acc

        def loaded(copy):
            @pl.when(p == 0)
            def _():
                copy.wait()

        send_t, fwd_t = ring_gather(AG_T, lambda i, h: ag_t.at[i * CORES + k, h], x, xp, xm, lambda i: dev(y, i, k))
        send_a, fwd_a = ring_gather(AG_A, lambda i, h: ag_a.at[i, h], y, yp, ym, lambda i: dev(i, x, k))

        def relay(n, i, h=None):
            ref = ag_t.at[i * CORES + k] if h is None else ag_t.at[i * CORES + k, h]
            return push(RELAY + n, ref, ref, partner)

        relays = [relay(0, x)] + [relay(1 + n, i, h) for n, (i, h) in enumerate(((xm, 0), (xp, 1), (xm, 1), (xp, 0), (xf, 0), (xf, 1)))]
        own_y = [(y, 0), (y, 1)]
        phase("ag_own")
        for n in (0, 2, 1, 3):
            send_t[n].start()
        relays[0].start()

        @pl.when(p > 0)
        def _():
            for n in (0, 2, 1, 3):
                send_a[n].start()
            for owner in range(RING * CORES):
                mm_a(own_y, owner, True)

        relays[0].wait_recv()
        loaded(loads_t[0])
        for owner in range(RING):
            mm_t([(x, 0), (x, 1)], owner, True)

        @pl.when(p == 0)
        def _():
            @pl.when(leaves)
            def _():
                for copy in first_moves:
                    copy.wait()

            @pl.when(stays)
            def _():
                for h in range(2):
                    ag_a[y, h] = x_half[h * hsub : (h + 1) * hsub]

            for n in (0, 2, 1, 3):
                send_a[n].start()
            loads_a[0].wait()
            for owner in range(RING * CORES):
                mm_a(own_y, owner, True)

        phase("ag_wait1")
        for n, fwd in ((0, 0), (2, 1)):
            send_t[n].wait_recv()
            fwd_t[fwd].start()
            relays[1 + fwd].start()
        for n, fwd in ((0, 0), (2, 1)):
            send_a[n].wait_recv()
            fwd_a[fwd].start()
        phase("mm_near1")
        loaded(loads_a[1])
        loaded(loads_a[2])
        for owner in range(RING * CORES):
            mm_a([(ym, 0), (yp, 1)], owner)
        relays[1].wait_recv()
        relays[2].wait_recv()
        loaded(loads_t[1])
        loaded(loads_t[2])
        for owner in range(RING):
            mm_t([(xm, 0), (xp, 1)], owner)
        phase("mm_near2")
        for n in (1, 3):
            send_t[n].wait_recv()
            relays[3 + n // 2].start()
        for n in (1, 3):
            send_a[n].wait_recv()
        for owner in range(RING * CORES):
            mm_a([(ym, 1), (yp, 0)], owner)
        for n in range(2):
            fwd_t[n].wait_recv()
            relays[5 + n].start()
        relays[3].wait_recv()
        relays[4].wait_recv()
        for owner in range(RING):
            mm_t([(xm, 1), (xp, 0)], owner)
        phase("ag_far")
        fwd_a[0].wait_recv()
        fwd_a[1].wait_recv()
        phase("mm_far")

        loaded(loads_a[3])
        pairs = []
        far_y = [(yf, 0), (yf, 1)]
        for n, i in enumerate((xf, xp, xm, x)):
            mm_a(far_y, i * CORES + other)
            pairs.append(push(PAIR + n, p_a.at[i * CORES + other], d_a.at[i], partner))
            pairs[n].start()
        out_t = ring_scatter(RS_T, lambda i: p_t.at[i], r_t, yp, ym, yf, lambda i: dev(i, x, k))
        out_a = ring_scatter(RS_A, lambda i: p_a.at[i * CORES + k], r_a, xp, xm, xf, lambda i: dev(y, i, k))
        for i in (xf, xp, xm, x):
            mm_a(far_y, i * CORES + k)
        relays[5].wait_recv()
        relays[6].wait_recv()
        loaded(loads_t[3])
        for n, (iy, ix) in enumerate(((yf, xf), (yp, xp), (ym, xm), (y, x))):
            mm_t([(xf, 0), (xf, 1)], iy)
            for q in ((0, 1), (2,), (3,), ())[n]:
                out_t[q].start()
            pairs[n].wait_recv()
            p_a[ix * CORES + k] = p_a[ix * CORES + k] + d_a[ix]
            for q in ((0, 1), (2,), (3,), ())[n]:
                out_a[q].start()
        phase("rs_mid")

        @pl.when(p == SWEEPS)
        def _():
            @pl.when(leaves)
            def _():
                keep_left.wait()
                keep_right.wait()

            @pl.when(stays)
            def _():
                x_move[...] = y_keep[...]

            for op in range(2):
                for q in range(2):
                    x_move[op] = dot_f32(x_move[op], linv[q, op], NT)
            out_right.start()
            y_keep[0] = ycur[0]
            out_left.start()

        ht = width // 2
        out_t[0].wait_recv()
        p_t[yp, 0:ht] = p_t[yp, 0:ht] + r_t[0]
        out_t[4].start()
        out_t[1].wait_recv()
        p_t[ym, ht:width] = p_t[ym, ht:width] + r_t[1]
        out_t[5].start()
        out_a[0].wait_recv()
        kp, km, kk = xp * CORES + k, xm * CORES + k, x * CORES + k
        p_a[kp, 0:hsub] = p_a[kp, 0:hsub] + r_a[0]
        out_a[4].start()
        out_a[1].wait_recv()
        p_a[km, hsub:sub] = p_a[km, hsub:sub] + r_a[1]
        out_a[5].start()
        phase("rs_end")
        for n in (2, 3, 4, 5):
            out_t[n].wait_recv()
            out_a[n].wait_recv()
        phase("rs_sum")
        ycur[t, :, 0:ht] = (p_t[y, 0:ht] + r_t[3] + r_t[4]).T
        ycur[t, :, ht:width] = (p_t[y, ht:width] + r_t[2] + r_t[5]).T
        ycur[a, 0:hsub] = p_a[kk, 0:hsub] + r_a[3] + r_a[4]
        ycur[a, hsub:sub] = p_a[kk, hsub:sub] + r_a[2] + r_a[5]
        phase("rs_drain")
        for copy in send_t + fwd_t + send_a + fwd_a + relays + pairs + out_t + out_a:
            copy.wait_send()
        phase()

    def all_reduce(rows, local):
        piece = rows // nchips
        phase("ar_pair")
        local(other)
        pair = push(GRAM_PAIR, g_loc.at[other, pl.ds(0, rows)], g_pair.at[pl.ds(0, rows)], partner)
        pair.start()
        local(k)
        pair.wait_recv()
        g_sum[0:rows] = g_loc[k, 0:rows] + g_pair[0:rows]

        def chunk(ref, q):
            return ref.at[pl.ds(pl.multiple_of(q * piece, GROUP), piece)]

        def chips():
            for o in range(1, nchips):
                to_y, to_x = lax.rem(y + o // RING, RING), lax.rem(x + o % RING, RING)
                yield o, to_y * RING + to_x, dev(to_y, to_x, k)

        phase("ar_rs")
        mine = y * RING + x
        for o, q, to in chips():
            push(GRAM_RS, chunk(g_sum, q), chunk(g_in, o - 1), to).start()
        others = pl.ds(0, (nchips - 1) * piece)
        pltpu.make_async_copy(g_in.at[others], g_in.at[others], recv.at[GRAM_RS]).wait()
        phase("ar_ag")
        total = chunk(g_sum, mine)[...]
        for o in range(1, nchips):
            total = total + g_in[(o - 1) * piece : o * piece]
        chunk(g_all, mine)[...] = total / total_rows
        for o, q, to in chips():
            push(GRAM_AG, chunk(g_all, mine), chunk(g_all, mine), to).start()
        pltpu.make_async_copy(g_in.at[others], g_in.at[others], recv.at[GRAM_AG]).wait()
        phase("ar_drain")
        pair.wait_send()
        for i in (GRAM_RS, GRAM_AG):
            pltpu.make_async_copy(g_in.at[others], g_in.at[others], send.at[i]).wait()
        phase()

    corners = ((0, 0), (0, 1), (1, 1), (1, 0))

    def put_gram(op, full, count):
        for n, (i, j) in enumerate(corners[:count]):
            g_loc[op, n * tile : (n + 1) * tile] = full[i * tile : (i + 1) * tile, j * tile : (j + 1) * tile]

    def half_gram(op):
        half = ycur[op].astype(BF16)
        put_gram(op, lax.dot_general(half, half, TN, preferred_element_type=F32), 3)

    def full_gram(op):
        put_gram(op, gram_f32(ycur[op]), 3)

    def normalize(p, q):
        def local(op):
            @pl.when(q == 0)
            def _():
                half_gram(op)

            @pl.when(q == 1)
            def _():
                full_gram(op)

        all_reduce(3 * tile, local)
        last = p == SWEEPS - 1

        @pl.when(jnp.logical_and(last, q == 0))
        def _():
            y_keep[...] = ycur[...]

            @pl.when(leaves)
            def _():
                keep_right.start()

        @pl.when(jnp.logical_and(jnp.logical_and(last, q == 1), leaves))
        def _():
            keep_left.start()

        phase("chol")

        def store(first, t, value):
            linv[q, k, pl.ds(first, GROUP), t * tile : (t + 1) * tile] = value

        linv[q, k, 0:tile, tile:width] = jnp.zeros((tile, tile), F32)
        inverse_factor(g_all, work, store)
        phase("mul_own")
        swap = push(LINV, linv.at[q, k], linv.at[q, k], partner)
        swap.start()
        ycur[k] = dot_f32(ycur[k], linv[q, k], NT)
        phase("mul_other")
        swap.wait_recv()
        ycur[other] = dot_f32(ycur[other], linv[q, other], NT)
        swap.wait_send()
        phase()

    def sweep(p, carry):
        apply(p)

        @pl.when(p < SWEEPS)
        def _():
            def one(q, carry):
                normalize(p, q)
                return carry

            lax.fori_loop(0, 2, one, 0)
            phase("next_x")
            nxt = lax.rem(p + 1, 2)
            for h in range(2):
                rows = slice(h * hsub, (h + 1) * hsub)
                ag_t[c, h] = ycur[nxt, rows].T.astype(BF16)
                ag_a[y, h] = ycur[1 - nxt, rows].astype(BF16)
            phase()

        return carry

    lax.fori_loop(0, SWEEPS + 1, sweep, 0)

    def rayleigh(op):
        put_gram(op, dot_f32(x_move[op], ycur[op], TN), 4)

    all_reduce(4 * tile, rayleigh)
    phase("h_swap")
    swap = push(LINV, g_all, h_all, partner)
    swap.start()
    swap.wait()
    for n, (i, j) in enumerate(corners):
        rows, at = slice(n * tile, (n + 1) * tile), (slice(i * tile, (i + 1) * tile), slice(j * tile, (j + 1) * tile))
        for op in range(2):
            h_out[(op, *at)] = jnp.where(k == op, g_all[rows], h_all[rows])
    out_left.wait()
    out_right.wait()
    phase()


def hand_over(x_ref, h_ref, left_x, left_h, right_x, right_h):
    left_x[...] = x_ref[0]
    left_h[...] = h_ref[0]
    right_x[...] = x_ref[1]
    right_h[...] = h_ref[1]


def solution(mesh):
    nrow, ncol = mesh.shape["row"], mesh.shape["col"]
    assert nrow == RING and ncol == RING * CORES

    def local_program(left_op, left_start, right_op, right_start):
        rows, cols = left_op.shape
        sub, width = left_start.shape
        tile = width // 2
        vmem = pltpu.VMEM
        dma = pltpu.SemaphoreType.DMA
        basis, ray = jax.ShapeDtypeStruct((sub, width), F32), jax.ShapeDtypeStruct((width, width), F32)
        both_x, both_h = pl.pallas_call(
            functools.partial(kernel, (nrow, ncol, rows * nrow)),
            out_shape=[jax.ShapeDtypeStruct((2, sub, width), F32), jax.ShapeDtypeStruct((2, width, width), F32)],
            in_specs=[pl.BlockSpec(memory_space=pl.ANY)] * 4,
            out_specs=[pl.BlockSpec(memory_space=pl.ANY), pl.BlockSpec(memory_space=vmem)],
            scratch_shapes=[
                vmem((2, rows, cols), BF16),
                vmem((2, sub, width), F32),
                vmem((ncol, 2, width, sub // 2), BF16),
                vmem((nrow, 2, sub // 2, width), BF16),
                vmem((nrow, width, sub), F32),
                vmem((ncol, sub, width), F32),
                vmem((RING, sub, width), F32),
                vmem((6, width // 2, sub), F32),
                vmem((6, sub // 2, width), F32),
                vmem((sub, width), BF16),
                vmem((2, sub, width), F32),
                vmem((2, sub, width), F32),
                vmem((2, 4 * tile, tile), F32),
                vmem((4 * tile, tile), F32),
                vmem((4 * tile, tile), F32),
                vmem((4 * tile, tile), F32),
                vmem((4 * tile, tile), F32),
                vmem((4 * tile, tile), F32),
                vmem((width, 2 * width), F32),
                vmem((2, 2, width, width), F32),
                dma((COPIES,)),
                dma((COPIES,)),
                dma((10,)),
            ],
            compiler_params=pltpu.CompilerParams(collective_id=0, has_side_effects=True, vmem_limit_bytes=VMEM_BYTES),
            name="subspace",
        )(left_op, left_start, right_op, right_start)
        whole = pl.BlockSpec(memory_space=vmem)
        return pl.pallas_call(
            hand_over, out_shape=[basis, ray, basis, ray], in_specs=[whole] * 2, out_specs=[whole] * 4, name="hand_over"
        )(both_x, both_h)

    op_spec = P(("batch", "row"), "col")
    vec_spec = P(("batch", "row", "col"), None)
    small_spec = P("batch", None)
    return jax.shard_map(
        local_program,
        mesh=mesh,
        in_specs=(op_spec, vec_spec, op_spec, vec_spec),
        out_specs=(vec_spec, small_spec, vec_spec, small_spec),
        check_vma=False,
    )
```

```python
import functools

import jax
import jax.numpy as jnp
from jax import lax
from jax.experimental import pallas as pl
from jax.experimental.pallas import tpu as pltpu
from jax.sharding import PartitionSpec as P

SWEEPS = 4
CORES = 2
RING = 4
PIVOTS = 32
STEP = 16
LEFT_PARTS, RIGHT_PARTS = (2, 0, 1, 1, 0, 0), (0, 2, 1, 0, 1, 0)
GROUP = 8
VMEM_BYTES = 67043328
F32, BF16 = jnp.float32, jnp.bfloat16
TN = (((0,), (0,)), ((), ()))
NT = (((1,), (1,)), ((), ()))

AG_T, AG_A, RELAY, RS_T, RS_A, PAIR, GRAM_PAIR, GRAM_RS, GRAM_AG, LINV, MOVE = 0, 6, 12, 19, 25, 31, 35, 36, 38, 40, 41
COPIES = 45
OFFSETS = sorted(
    ((dy, dx) for dy in range(RING) for dx in range(RING) if dy or dx),
    key=lambda o: -min(o[0], RING - o[0]) - min(o[1], RING - o[1]),
)


def split3(v):
    high = v.astype(BF16)
    rest = v - high.astype(F32)
    mid = rest.astype(BF16)
    return high, mid, (rest - mid.astype(F32)).astype(BF16)


def halves_dot(lhs, rhs, dims):
    axis = 1 - dims[0][0][0]
    size = lhs.shape[axis] // 2
    parts = [lax.slice_in_dim(lhs, i * size, (i + 1) * size, axis=axis) for i in range(2)]
    return jnp.concatenate([lax.dot_general(part, rhs, dims, preferred_element_type=F32) for part in parts], axis=0)


def dot_f32(lhs, rhs, dims):
    left, right = split3(lhs), split3(rhs)
    (lk,), (rk,) = dims[0]
    lhs = jnp.concatenate([left[i] for i in LEFT_PARTS], axis=lk)
    rhs = jnp.concatenate([right[i] for i in RIGHT_PARTS], axis=rk)
    return halves_dot(lhs, rhs, dims)


def gram_f32(v):
    high, mid, low = split3(v)
    mixed = halves_dot(jnp.concatenate([high, high], axis=0), jnp.concatenate([low, mid], axis=0), TN)
    return (halves_dot(mid, mid, TN) + (mixed + mixed.T)) + halves_dot(high, high, TN)


class Phases:
    def __init__(self):
        self.scope = None

    def __call__(self, name=None):
        if self.scope is not None:
            self.scope.__exit__(None, None, None)
        self.scope = None
        if name is not None:
            self.scope = jax.named_scope(name)
            self.scope.__enter__()


def rows_of(ref, part, parts=2):
    size = ref.shape[0] // parts
    return ref.at[pl.ds(part * size, size)]


def inverse_factor(gram, work, store):
    tile = gram.shape[1]
    width = 2 * tile
    work[0:tile, 0:tile] = gram[0:tile]
    work[0:tile, tile:width] = gram[tile : 2 * tile]
    work[tile:width, tile:width] = gram[2 * tile : 3 * tile]
    at_row = lax.broadcasted_iota(jnp.int32, (width, width), 0)
    at_col = lax.broadcasted_iota(jnp.int32, (width, width), 1)
    work[:, width : 2 * width] = jnp.where(at_row == at_col, 1.0, 0.0).astype(F32)
    sub = lax.broadcasted_iota(jnp.int32, (GROUP, tile), 0)
    groups = PIVOTS // GROUP
    full = (GROUP, tile)

    def lane(row):
        return jnp.broadcast_to(row, full)

    for first in range(0, width, PIVOTS):
        near = first // tile
        gram_tiles = list(range(near, 2))
        tiles = gram_tiles + [2 + i for i in range(near + 1)]
        data = {
            t: [work[pl.ds(first + GROUP * g, GROUP), t * tile : (t + 1) * tile] for g in range(groups)] for t in tiles
        }
        pivots = [jnp.ones(full, F32) for _ in range(groups)]
        for start in range(0, PIVOTS, STEP):
            at = first - near * tile + start
            end = start + STEP
            cols = {
                j: {
                    g: jnp.broadcast_to(data[near][g][:, at + j - start : at + j - start + 1], full)
                    for g in range(j // GROUP, groups)
                }
                for j in range(start, end)
            }
            for j in range(start, end):
                gj, rj = divmod(j, GROUP)
                col = cols[j]
                pivot = lane(col[gj][rj : rj + 1])
                inv = 1.0 / pivot
                pivots[gj] = jnp.where(sub == rj, pivot, pivots[gj])
                for nxt in range(j + 1, end):
                    gn, rn = divmod(nxt, GROUP)
                    entry = lane(col[gn][rn : rn + 1])
                    if nxt == j + 1:
                        for g in range(gn, groups):
                            cols[nxt][g] = cols[nxt][g] - (col[g] * entry) * inv
                    else:
                        scaled = entry * inv
                        for g in range(gn, groups):
                            cols[nxt][g] = cols[nxt][g] - col[g] * scaled
                for g in range(gj, groups):
                    factor = col[g] * inv
                    if g == gj:
                        if rj == GROUP - 1:
                            continue
                        factor = jnp.where(sub > rj, factor, 0.0)
                    for t in tiles:
                        data[t][g] = data[t][g] - factor * lane(data[t][gj][rj : rj + 1])
        scale = [lax.rsqrt(p) for p in pivots]
        for t in tiles:
            data[t] = [d * s for d, s in zip(data[t], scale, strict=True)]
        for t in tiles:
            if t >= 2:
                for g in range(groups):
                    store(first + GROUP * g, t - 2, data[t][g])
        nxt = first + PIVOTS
        if nxt == width:
            break
        parts = {t: split3(jnp.concatenate(data[t], axis=0)) for t in tiles}
        below = [t for t in gram_tiles if (t + 1) * tile > nxt]
        low = below[0] * tile
        lhs = jnp.concatenate([jnp.concatenate([parts[t][i] for i in LEFT_PARTS], axis=0) for t in below], axis=1)
        right_tiles = below + [t for t in tiles if t >= 2]
        rhs = jnp.concatenate([jnp.concatenate([parts[t][i] for i in RIGHT_PARTS], axis=0) for t in right_tiles], axis=1)
        upd = lax.dot_general(lhs, rhs, TN, preferred_element_type=F32)
        for n, t in enumerate(right_tiles):
            where = pl.ds(nxt, width - nxt), slice(t * tile, (t + 1) * tile)
            work[where] = work[where] - upd[nxt - low :, n * tile : (n + 1) * tile]


def kernel(
    sizes, left_op, left_start, right_op, right_start, x_out, h_out,
    ops, ycur, y_one, ag_t, ag_a, p_t, p_a, d_a, r_t, r_a, x_half, x_via, x_move, g_loc, g_pair, g_sum, g_in, g_red, g_all, h_all, work, linv,
    send, recv, load_sem,
):
    nrow, ncol, total_rows = sizes
    sub, width = ycur.shape[1:]
    tile, hsub = width // 2, sub // 2
    nchips = RING * RING
    y = lax.axis_index("row")
    c = lax.axis_index("col")
    x, k = lax.div(c, CORES), lax.rem(c, CORES)
    other = 1 - k
    xp, xm, xf = (lax.rem(x + d, RING) for d in (1, 3, 2))
    yp, ym, yf = (lax.rem(y + d, RING) for d in (1, 3, 2))

    def dev(row, chip, core):
        return {"row": row, "col": chip * CORES + core}

    partner = dev(y, x, other)

    def push(i, src, dst, to):
        return pltpu.make_async_remote_copy(
            src_ref=src, dst_ref=dst, send_sem=send.at[i], recv_sem=recv.at[i], device_id=to, device_id_type=pl.DeviceIdType.MESH
        )

    def spot(i):
        return lax.rem(i + RING - x, RING)

    def run(index, size):
        return pl.ds(pl.multiple_of(index * size, size), size)

    phase = Phases()
    phase("boot")
    starts = [
        pltpu.make_async_copy(left_start, ycur.at[0], load_sem.at[8]),
        pltpu.make_async_copy(right_start, ycur.at[1], load_sem.at[9]),
    ]
    loads_t, loads_a = [], []
    for n, (xi, yi) in enumerate(((x, y), (xm, ym), (xp, yp), (xf, yf))):
        take = run(xi, CORES * sub)
        loads_t.append(pltpu.make_async_copy(left_op.at[take], ops.at[0, take], load_sem.at[2 * n]))
        take = run(spot(yi), sub)
        loads_a.append(pltpu.make_async_copy(right_op.at[:, take], ops.at[1, :, take], load_sem.at[2 * n + 1]))
    for copy in starts + loads_t + loads_a:
        copy.start()

    barrier = pltpu.get_barrier_semaphore()
    here = y * ncol + c
    for o in range(1, nrow * ncol):
        there = lax.rem(here + o, nrow * ncol)
        pl.semaphore_signal(
            barrier, inc=1, device_id={"row": lax.div(there, ncol), "col": lax.rem(there, ncol)}, device_id_type=pl.DeviceIdType.MESH
        )

    shift = CORES * lax.rem(x, 2) + k
    behind = spot(y)
    up, down = lax.rem(y + shift, RING), lax.rem(y + RING - shift, RING)

    def move(i, src, dst, row, chip, core):
        stays = jnp.logical_and(row == y, jnp.logical_and(chip == x, core == k))
        return push(i, src, dst, dev(row, chip, core)), stays, src, dst

    def start_moves(*moves):
        for copy, stays, src, dst in moves:

            @pl.when(stays)
            def _():
                dst[...] = src[...]

            @pl.when(jnp.logical_not(stays))
            def _():
                copy.start()

    def end_moves(*moves):
        for copy, stays, _, _ in moves:

            @pl.when(jnp.logical_not(stays))
            def _():
                copy.wait()

    for copy in starts:
        copy.wait()
    for h in range(2):
        ag_t[c, h] = ycur[0, h * hsub : (h + 1) * hsub].T.astype(BF16)
    x_half[...] = ycur[1].astype(BF16)
    pl.semaphore_wait(barrier, nrow * ncol - 1)
    first_moves = [move(MOVE + h, x_half.at[pl.ds(h * hsub, hsub)], ag_a.at[up, h], up, y, lax.div(x, 2)) for h in range(2)]
    start_moves(*first_moves)
    phase()

    def ring_gather(base, blk, me, plus, minus, to):
        own = [blk(me, h) for h in range(2)]
        first = [
            push(base + 0, own[0], own[0], to(plus)),
            push(base + 1, own[1], own[1], to(plus)),
            push(base + 2, own[1], own[1], to(minus)),
            push(base + 3, own[0], own[0], to(minus)),
        ]
        got0, got1 = blk(minus, 0), blk(plus, 1)
        return first, [push(base + 4, got0, got0, to(plus)), push(base + 5, got1, got1, to(minus))]

    def ring_scatter(base, part, got, plus, minus, far, to):
        def half(i, h):
            return rows_of(part(i), h)

        return [
            push(base + 0, half(far, 0), got.at[0], to(plus)),
            push(base + 1, half(far, 1), got.at[1], to(minus)),
            push(base + 2, half(plus, 1), got.at[2], to(plus)),
            push(base + 3, half(minus, 0), got.at[3], to(minus)),
            push(base + 4, half(plus, 0), got.at[4], to(plus)),
            push(base + 5, half(minus, 1), got.at[5], to(minus)),
        ]

    step_one = [
        move(MOVE, ycur.at[0], x_via.at[0], up, x, k),
        move(MOVE + 1, ycur.at[1], x_via.at[1], y, CORES * k + lax.div(behind, 2), lax.rem(behind, 2)),
    ]
    step_two = [
        move(MOVE + 2, x_via.at[0], x_move.at[0], y, down, lax.div(x, 2)),
        move(MOVE + 3, x_via.at[1], x_move.at[1], down, x, k),
    ]
    out_left = pltpu.make_async_copy(x_via.at[0], x_out.at[0], load_sem.at[0])
    out_right = pltpu.make_async_copy(x_move.at[1], x_out.at[1], load_sem.at[1])

    def apply(p):
        t = lax.rem(p, 2)
        a = 1 - t

        def mm_t(pieces, owner, first=False):
            acc = None
            for chip, h in pieces:
                for core in range(CORES):
                    b = chip * CORES + core
                    one = jnp.dot(ag_t[b, h], ops[t, run(b * 2 + h, hsub), run(spot(owner), sub)], preferred_element_type=F32)
                    acc = one if acc is None else acc + one
            p_t[owner] = acc if first else p_t[owner] + acc

        def mm_a(pieces, owner, first=False):
            acc = None
            for i, h in pieces:
                one = jnp.dot(ops[a, run(owner, sub), run(spot(i) * 2 + h, hsub)], ag_a[i, h], preferred_element_type=F32)
                acc = one if acc is None else acc + one
            p_a[owner] = acc if first else p_a[owner] + acc

        def loaded(copy):
            @pl.when(p == 0)
            def _():
                copy.wait()

        send_t, fwd_t = ring_gather(AG_T, lambda i, h: ag_t.at[i * CORES + k, h], x, xp, xm, lambda i: dev(y, i, k))
        send_a, fwd_a = ring_gather(AG_A, lambda i, h: ag_a.at[i, h], y, yp, ym, lambda i: dev(i, x, k))

        def relay(n, i, h=None):
            ref = ag_t.at[i * CORES + k] if h is None else ag_t.at[i * CORES + k, h]
            return push(RELAY + n, ref, ref, partner)

        relays = [relay(0, x)] + [relay(1 + n, i, h) for n, (i, h) in enumerate(((xm, 0), (xp, 1), (xm, 1), (xp, 0), (xf, 0), (xf, 1)))]
        own_y = [(y, 0), (y, 1)]
        phase("ag_own")
        for n in (0, 2, 1, 3):
            send_t[n].start()
        relays[0].start()

        @pl.when(p > 0)
        def _():
            for n in (0, 2, 1, 3):
                send_a[n].start()
            for owner in range(RING * CORES):
                mm_a(own_y, owner, True)

        relays[0].wait_recv()
        loaded(loads_t[0])
        for owner in range(RING):
            mm_t([(x, 0), (x, 1)], owner, True)

        @pl.when(p == 0)
        def _():
            end_moves(*first_moves)
            for n in (0, 2, 1, 3):
                send_a[n].start()
            loads_a[0].wait()
            for owner in range(RING * CORES):
                mm_a(own_y, owner, True)

        phase("ag_wait1")
        for n, fwd in ((0, 0), (2, 1)):
            send_t[n].wait_recv()
            fwd_t[fwd].start()
            relays[1 + fwd].start()
        for n, fwd in ((0, 0), (2, 1)):
            send_a[n].wait_recv()
            fwd_a[fwd].start()
        phase("mm_near1")
        loaded(loads_a[1])
        loaded(loads_a[2])
        for owner in range(RING * CORES):
            mm_a([(ym, 0), (yp, 1)], owner)
        relays[1].wait_recv()
        relays[2].wait_recv()
        loaded(loads_t[1])
        loaded(loads_t[2])
        for owner in range(RING):
            mm_t([(xm, 0), (xp, 1)], owner)
        phase("mm_near2")
        for n in (1, 3):
            send_t[n].wait_recv()
            relays[3 + n // 2].start()
        for n in (1, 3):
            send_a[n].wait_recv()
        for owner in range(RING * CORES):
            mm_a([(ym, 1), (yp, 0)], owner)
        for n in range(2):
            fwd_t[n].wait_recv()
            relays[5 + n].start()
        relays[3].wait_recv()
        relays[4].wait_recv()
        for owner in range(RING):
            mm_t([(xm, 1), (xp, 0)], owner)
        phase("ag_far")
        fwd_a[0].wait_recv()
        fwd_a[1].wait_recv()
        phase("mm_far")

        loaded(loads_a[3])
        pairs = []
        far_y = [(yf, 0), (yf, 1)]
        along = (xf, xp, xm, x)
        for i in along:
            mm_a(far_y, i * CORES + other)
        for n, i in enumerate(along):
            pairs.append(push(PAIR + n, p_a.at[i * CORES + other], d_a.at[i], partner))
            pairs[n].start()
        out_t = ring_scatter(RS_T, lambda i: p_t.at[i], r_t, yp, ym, yf, lambda i: dev(i, x, k))
        out_a = ring_scatter(RS_A, lambda i: p_a.at[i * CORES + k], r_a, xp, xm, xf, lambda i: dev(y, i, k))

        def add_pair(n):
            i = along[n]
            pairs[n].wait_recv()
            p_a[i * CORES + k] = p_a[i * CORES + k] + d_a[i]

        for i in along:
            mm_a(far_y, i * CORES + k)
        relays[5].wait_recv()
        relays[6].wait_recv()
        loaded(loads_t[3])
        far_x = [(xf, 0), (xf, 1)]
        mm_t(far_x, yf)
        out_t[0].start()
        out_t[1].start()
        mm_t(far_x, yp)
        mm_t(far_x, ym)
        out_t[2].start()
        out_t[3].start()
        add_pair(0)
        out_a[0].start()
        out_a[1].start()
        add_pair(1)
        add_pair(2)
        out_a[2].start()
        out_a[3].start()
        mm_t(far_x, y)
        add_pair(3)
        phase("rs_mid")

        @pl.when(p == SWEEPS)
        def _():
            end_moves(*step_two)
            for op in range(2):
                y_one[op] = dot_f32(x_move[op], linv[0, op], NT)
                x_move[op] = dot_f32(y_one[op], linv[1, op], NT)
            out_right.start()
            x_via[0] = ycur[0]
            out_left.start()

        ht = width // 2
        out_t[0].wait_recv()
        p_t[yp, 0:ht] = p_t[yp, 0:ht] + r_t[0]
        out_t[4].start()
        out_t[1].wait_recv()
        p_t[ym, ht:width] = p_t[ym, ht:width] + r_t[1]
        out_t[5].start()
        out_a[0].wait_recv()
        kp, km, kk = xp * CORES + k, xm * CORES + k, x * CORES + k
        p_a[kp, 0:hsub] = p_a[kp, 0:hsub] + r_a[0]
        out_a[4].start()
        out_a[1].wait_recv()
        p_a[km, hsub:sub] = p_a[km, hsub:sub] + r_a[1]
        out_a[5].start()
        phase("rs_end")
        for n in (2, 3, 4, 5):
            out_t[n].wait_recv()
            out_a[n].wait_recv()
        phase("rs_sum")
        ycur[t, :, 0:ht] = (p_t[y, 0:ht] + r_t[3] + r_t[4]).T
        ycur[t, :, ht:width] = (p_t[y, ht:width] + r_t[2] + r_t[5]).T
        ycur[a, 0:hsub] = p_a[kk, 0:hsub] + r_a[3] + r_a[4]
        ycur[a, hsub:sub] = p_a[kk, hsub:sub] + r_a[2] + r_a[5]
        phase("rs_drain")
        for copy in send_t + fwd_t + send_a + fwd_a + relays + pairs + out_t + out_a:
            copy.wait_send()
        phase()

    def all_reduce(rows, local):
        piece = rows // nchips
        phase("ar_pair")
        local(other)
        pair = push(GRAM_PAIR, g_loc.at[other, pl.ds(0, rows)], g_pair.at[pl.ds(0, rows)], partner)
        pair.start()
        local(k)
        pair.wait_recv()
        g_sum[0:rows] = g_loc[k, 0:rows] + g_pair[0:rows]

        def chunk(ref, q):
            return ref.at[pl.ds(pl.multiple_of(q * piece, GROUP), piece)]

        def count(copies):
            return g_all.at[pl.ds(0, copies * piece)]

        def await_copies(sem, copies):
            pltpu.make_async_copy(count(copies), count(copies), sem).wait()

        phase("ar_rs")
        mine = y * RING + x
        routes = []
        for dy, dx in OFFSETS:
            to_y, to_x = (y, yp, yf, ym)[dy], (x, xp, xf, xm)[dx]
            routes.append((dy * RING + dx, to_y * RING + to_x, to_y, to_x))
        owner = CORES - 1

        def spread(o, q, to_y, to_x):
            pltpu.make_async_remote_copy(
                src_ref=chunk(g_sum, q), dst_ref=g_in.at[k, pl.ds(o * piece, piece)], send_sem=send.at[GRAM_RS],
                recv_sem=recv.at[GRAM_RS + k], device_id=dev(to_y, to_x, owner), device_id_type=pl.DeviceIdType.MESH,
            ).start()

        for route in routes:
            spread(*route)

        @pl.when(k == 0)
        def _():
            spread(0, mine, y, x)
            await_copies(send.at[GRAM_RS], nchips)
            phase("ar_ag")
            await_copies(recv.at[GRAM_AG], nchips)
            phase("ar_drain")

        @pl.when(k == 1)
        def _():
            def hand_out(i, src, q, to_y, to_x, core):
                pltpu.make_async_remote_copy(
                    src_ref=src, dst_ref=chunk(g_all, q), send_sem=send.at[GRAM_AG + i], recv_sem=recv.at[GRAM_AG],
                    device_id=dev(to_y, to_x, core), device_id_type=pl.DeviceIdType.MESH,
                ).start()

            await_copies(recv.at[GRAM_RS], nchips)
            total = g_in[0, 0:piece]
            for o in range(1, nchips):
                total = total + g_in[0, o * piece : (o + 1) * piece]
            g_red[0:piece] = total / total_rows
            for _, _, to_y, to_x in routes:
                hand_out(1, g_red.at[pl.ds(0, piece)], mine, to_y, to_x, 0)
            hand_out(1, g_red.at[pl.ds(0, piece)], mine, y, x, 0)
            phase("ar_ag")
            await_copies(recv.at[GRAM_RS + 1], nchips - 1)
            total = chunk(g_sum, mine)[...]
            for o in range(1, nchips):
                total = total + g_in[1, o * piece : (o + 1) * piece]
            chunk(g_all, mine)[...] = total / total_rows
            for _, _, to_y, to_x in routes:
                hand_out(0, chunk(g_all, mine), mine, to_y, to_x, 1)
            await_copies(recv.at[GRAM_AG], nchips - 1)
            phase("ar_drain")
            await_copies(send.at[GRAM_RS], nchips - 1)
            await_copies(send.at[GRAM_AG], nchips - 1)
            await_copies(send.at[GRAM_AG + 1], nchips)

        pair.wait_send()
        phase()

    corners = ((0, 0), (0, 1), (1, 1), (1, 0))

    def put_gram(op, full, count):
        for n, (i, j) in enumerate(corners[:count]):
            g_loc[op, n * tile : (n + 1) * tile] = full[i * tile : (i + 1) * tile, j * tile : (j + 1) * tile]

    def half_gram(op):
        half = ycur[op].astype(BF16)
        put_gram(op, lax.dot_general(half, half, TN, preferred_element_type=F32), 3)

    def full_gram(op):
        put_gram(op, gram_f32(y_one[op]), 3)

    def normalize(p, q):
        def local(op):
            @pl.when(q == 0)
            def _():
                half_gram(op)

            @pl.when(q == 1)
            def _():
                full_gram(op)

        all_reduce(3 * tile, local)
        last = p == SWEEPS - 1

        @pl.when(jnp.logical_and(last, q == 0))
        def _():
            start_moves(*step_one)

        @pl.when(jnp.logical_and(last, q == 1))
        def _():
            end_moves(*step_one)
            start_moves(*step_two)

        phase("chol")

        def store(first, t, value):
            linv[q, k, pl.ds(first, GROUP), t * tile : (t + 1) * tile] = value

        linv[q, k, 0:tile, tile:width] = jnp.zeros((tile, tile), F32)
        inverse_factor(g_all, work, store)
        phase("mul_own")
        swap = push(LINV, linv.at[q, k], linv.at[q, k], partner)
        swap.start()

        def multiply(src, dst):
            dst[k] = dot_f32(src[k], linv[q, k], NT)
            swap.wait_recv()
            dst[other] = dot_f32(src[other], linv[q, other], NT)

        @pl.when(q == 0)
        def _():
            multiply(ycur, y_one)

        @pl.when(q == 1)
        def _():
            multiply(y_one, ycur)

        swap.wait_send()
        phase()

    def sweep(p, carry):
        apply(p)

        @pl.when(p < SWEEPS)
        def _():
            def one(q, carry):
                normalize(p, q)
                return carry

            lax.fori_loop(0, 2, one, 0)
            phase("next_x")
            nxt = lax.rem(p + 1, 2)
            for h in range(2):
                rows = slice(h * hsub, (h + 1) * hsub)
                ag_t[c, h] = ycur[nxt, rows].T.astype(BF16)
                ag_a[y, h] = ycur[1 - nxt, rows].astype(BF16)
            phase()

        return carry

    lax.fori_loop(0, SWEEPS + 1, sweep, 0)

    def rayleigh(op):
        put_gram(op, dot_f32(x_move[op], ycur[op], TN), 4)

    all_reduce(4 * tile, rayleigh)
    phase("h_swap")
    swap = push(LINV, g_all, h_all, partner)
    swap.start()
    swap.wait()
    for n, (i, j) in enumerate(corners):
        rows, at = slice(n * tile, (n + 1) * tile), (slice(i * tile, (i + 1) * tile), slice(j * tile, (j + 1) * tile))
        for op in range(2):
            h_out[(op, *at)] = jnp.where(k == op, g_all[rows], h_all[rows])
    out_left.wait()
    out_right.wait()
    phase()


def hand_over(x_ref, h_ref, left_x, left_h, right_x, right_h):
    left_x[...] = x_ref[0]
    left_h[...] = h_ref[0]
    right_x[...] = x_ref[1]
    right_h[...] = h_ref[1]


def solution(mesh):
    nrow, ncol = mesh.shape["row"], mesh.shape["col"]
    assert nrow == RING and ncol == RING * CORES

    def local_program(left_op, left_start, right_op, right_start):
        rows, cols = left_op.shape
        sub, width = left_start.shape
        tile = width // 2
        vmem = pltpu.VMEM
        dma = pltpu.SemaphoreType.DMA
        basis, ray = jax.ShapeDtypeStruct((sub, width), F32), jax.ShapeDtypeStruct((width, width), F32)
        both_x, both_h = pl.pallas_call(
            functools.partial(kernel, (nrow, ncol, rows * nrow)),
            out_shape=[jax.ShapeDtypeStruct((2, sub, width), F32), jax.ShapeDtypeStruct((2, width, width), F32)],
            in_specs=[pl.BlockSpec(memory_space=pl.ANY)] * 4,
            out_specs=[pl.BlockSpec(memory_space=pl.ANY), pl.BlockSpec(memory_space=vmem)],
            scratch_shapes=[
                vmem((2, rows, cols), BF16),
                vmem((2, sub, width), F32),
                vmem((2, sub, width), F32),
                vmem((ncol, 2, width, sub // 2), BF16),
                vmem((nrow, 2, sub // 2, width), BF16),
                vmem((nrow, width, sub), F32),
                vmem((ncol, sub, width), F32),
                vmem((RING, sub, width), F32),
                vmem((6, width // 2, sub), F32),
                vmem((6, sub // 2, width), F32),
                vmem((sub, width), BF16),
                vmem((2, sub, width), F32),
                vmem((2, sub, width), F32),
                vmem((2, 4 * tile, tile), F32),
                vmem((4 * tile, tile), F32),
                vmem((4 * tile, tile), F32),
                vmem((2, 4 * tile, tile), F32),
                vmem((4 * tile // (RING * RING), tile), F32),
                vmem((4 * tile, tile), F32),
                vmem((4 * tile, tile), F32),
                vmem((width, 2 * width), F32),
                vmem((2, 2, width, width), F32),
                dma((COPIES,)),
                dma((COPIES,)),
                dma((10,)),
            ],
            compiler_params=pltpu.CompilerParams(collective_id=0, has_side_effects=True, vmem_limit_bytes=VMEM_BYTES),
            name="subspace",
        )(left_op, left_start, right_op, right_start)
        whole = pl.BlockSpec(memory_space=vmem)
        return pl.pallas_call(
            hand_over, out_shape=[basis, ray, basis, ray], in_specs=[whole] * 2, out_specs=[whole] * 4, name="hand_over"
        )(both_x, both_h)

    op_spec = P(("batch", "row"), "col")
    vec_spec = P(("batch", "row", "col"), None)
    small_spec = P("batch", None)
    return jax.shard_map(
        local_program,
        mesh=mesh,
        in_specs=(op_spec, vec_spec, op_spec, vec_spec),
        out_specs=(vec_spec, small_spec, vec_spec, small_spec),
        check_vma=False,
    )
```

```python
import functools

import jax
import jax.numpy as jnp
from jax import lax
from jax.experimental import pallas as pl
from jax.experimental.pallas import tpu as pltpu
from jax.sharding import PartitionSpec as P

SWEEPS = 4
CORES = 2
RING = 4
PIVOTS = 32
STEP = 16
LEFT_PARTS, RIGHT_PARTS = (2, 0, 1, 1, 0, 0), (0, 2, 1, 0, 1, 0)
GROUP = 8
VMEM_BYTES = 67043328
F32, BF16 = jnp.float32, jnp.bfloat16
TN = (((0,), (0,)), ((), ()))
NT = (((1,), (1,)), ((), ()))

AG_T, AG_A, RELAY, RS_T, RS_A, PAIR, GRAM_PAIR, GRAM_RS, GRAM_AG, LINV, MOVE = 0, 6, 12, 19, 25, 31, 36, 37, 39, 41, 42
COPIES = 46
OFFSETS = sorted(
    ((dy, dx) for dy in range(RING) for dx in range(RING) if dy or dx),
    key=lambda o: -min(o[0], RING - o[0]) - min(o[1], RING - o[1]),
)


def split3(v):
    high = v.astype(BF16)
    rest = v - high.astype(F32)
    mid = rest.astype(BF16)
    return high, mid, (rest - mid.astype(F32)).astype(BF16)


def halves_dot(lhs, rhs, dims):
    axis = 1 - dims[0][0][0]
    size = lhs.shape[axis] // 2
    parts = [lax.slice_in_dim(lhs, i * size, (i + 1) * size, axis=axis) for i in range(2)]
    return jnp.concatenate([lax.dot_general(part, rhs, dims, preferred_element_type=F32) for part in parts], axis=0)


def dot_f32(lhs, rhs, dims):
    left, right = split3(lhs), split3(rhs)
    (lk,), (rk,) = dims[0]
    lhs = jnp.concatenate([left[i] for i in LEFT_PARTS], axis=lk)
    rhs = jnp.concatenate([right[i] for i in RIGHT_PARTS], axis=rk)
    return halves_dot(lhs, rhs, dims)


def gram_f32(v):
    high, mid, low = split3(v)
    mixed = halves_dot(jnp.concatenate([high, high], axis=0), jnp.concatenate([low, mid], axis=0), TN)
    return (halves_dot(mid, mid, TN) + (mixed + mixed.T)) + halves_dot(high, high, TN)


class Phases:
    def __init__(self):
        self.scope = None

    def __call__(self, name=None):
        if self.scope is not None:
            self.scope.__exit__(None, None, None)
        self.scope = None
        if name is not None:
            self.scope = jax.named_scope(name)
            self.scope.__enter__()


def rows_of(ref, part, parts=2):
    size = ref.shape[0] // parts
    return ref.at[pl.ds(part * size, size)]


def inverse_factor(gram, work, store):
    tile = gram.shape[1]
    width = 2 * tile
    work[0:tile, 0:tile] = gram[0:tile]
    work[0:tile, tile:width] = gram[tile : 2 * tile]
    work[tile:width, tile:width] = gram[2 * tile : 3 * tile]
    at_row = lax.broadcasted_iota(jnp.int32, (width, width), 0)
    at_col = lax.broadcasted_iota(jnp.int32, (width, width), 1)
    work[:, width : 2 * width] = jnp.where(at_row == at_col, 1.0, 0.0).astype(F32)
    sub = lax.broadcasted_iota(jnp.int32, (GROUP, tile), 0)
    groups = PIVOTS // GROUP
    full = (GROUP, tile)

    def lane(row):
        return jnp.broadcast_to(row, full)

    for first in range(0, width, PIVOTS):
        near = first // tile
        gram_tiles = list(range(near, 2))
        tiles = gram_tiles + [2 + i for i in range(near + 1)]
        data = {
            t: [work[pl.ds(first + GROUP * g, GROUP), t * tile : (t + 1) * tile] for g in range(groups)] for t in tiles
        }
        pivots = [jnp.ones(full, F32) for _ in range(groups)]
        for start in range(0, PIVOTS, STEP):
            at = first - near * tile + start
            end = start + STEP
            cols = {
                j: {
                    g: jnp.broadcast_to(data[near][g][:, at + j - start : at + j - start + 1], full)
                    for g in range(j // GROUP, groups)
                }
                for j in range(start, end)
            }
            for j in range(start, end):
                gj, rj = divmod(j, GROUP)
                col = cols[j]
                pivot = lane(col[gj][rj : rj + 1])
                inv = 1.0 / pivot
                pivots[gj] = jnp.where(sub == rj, pivot, pivots[gj])
                for nxt in range(j + 1, end):
                    gn, rn = divmod(nxt, GROUP)
                    entry = lane(col[gn][rn : rn + 1])
                    if nxt == j + 1:
                        for g in range(gn, groups):
                            cols[nxt][g] = cols[nxt][g] - (col[g] * entry) * inv
                    else:
                        scaled = entry * inv
                        for g in range(gn, groups):
                            cols[nxt][g] = cols[nxt][g] - col[g] * scaled
                for g in range(gj, groups):
                    factor = col[g] * inv
                    if g == gj:
                        if rj == GROUP - 1:
                            continue
                        factor = jnp.where(sub > rj, factor, 0.0)
                    for t in tiles:
                        data[t][g] = data[t][g] - factor * lane(data[t][gj][rj : rj + 1])
        scale = [lax.rsqrt(p) for p in pivots]
        for t in tiles:
            data[t] = [d * s for d, s in zip(data[t], scale, strict=True)]
        for t in tiles:
            if t >= 2:
                for g in range(groups):
                    store(first + GROUP * g, t - 2, data[t][g])
        nxt = first + PIVOTS
        if nxt == width:
            break
        parts = {t: split3(jnp.concatenate(data[t], axis=0)) for t in tiles}
        below = [t for t in gram_tiles if (t + 1) * tile > nxt]
        low = below[0] * tile
        lhs = jnp.concatenate([jnp.concatenate([parts[t][i] for i in LEFT_PARTS], axis=0) for t in below], axis=1)
        right_tiles = below + [t for t in tiles if t >= 2]
        rhs = jnp.concatenate([jnp.concatenate([parts[t][i] for i in RIGHT_PARTS], axis=0) for t in right_tiles], axis=1)
        upd = lax.dot_general(lhs, rhs, TN, preferred_element_type=F32)
        for n, t in enumerate(right_tiles):
            where = pl.ds(nxt, width - nxt), slice(t * tile, (t + 1) * tile)
            work[where] = work[where] - upd[nxt - low :, n * tile : (n + 1) * tile]


def kernel(
    sizes, left_op, left_start, right_op, right_start, x_out, h_out,
    ops, ycur, y_one, ag_t, ag_a, p_t, p_a, d_a, r_t, r_a, x_half, x_via, x_move, g_loc, g_pair, g_sum, g_in, g_red, g_all, h_all, work, linv,
    send, recv, load_sem,
):
    nrow, ncol, total_rows = sizes
    sub, width = ycur.shape[1:]
    tile, hsub = width // 2, sub // 2
    nchips = RING * RING
    y = lax.axis_index("row")
    c = lax.axis_index("col")
    x, k = lax.div(c, CORES), lax.rem(c, CORES)
    other = 1 - k
    xp, xm, xf = (lax.rem(x + d, RING) for d in (1, 3, 2))
    yp, ym, yf = (lax.rem(y + d, RING) for d in (1, 3, 2))

    def dev(row, chip, core):
        return {"row": row, "col": chip * CORES + core}

    partner = dev(y, x, other)

    def push(i, src, dst, to):
        return pltpu.make_async_remote_copy(
            src_ref=src, dst_ref=dst, send_sem=send.at[i], recv_sem=recv.at[i], device_id=to, device_id_type=pl.DeviceIdType.MESH
        )

    def spot(i):
        return lax.rem(i + RING - x, RING)

    def run(index, size):
        return pl.ds(pl.multiple_of(index * size, size), size)

    phase = Phases()
    phase("boot")
    starts = [
        pltpu.make_async_copy(left_start, ycur.at[0], load_sem.at[8]),
        pltpu.make_async_copy(right_start, ycur.at[1], load_sem.at[9]),
    ]
    loads_t, loads_a = [], []
    for n, (xi, yi) in enumerate(((x, y), (xm, ym), (xp, yp), (xf, yf))):
        take = run(xi, CORES * sub)
        loads_t.append(pltpu.make_async_copy(left_op.at[take], ops.at[0, take], load_sem.at[2 * n]))
        take = run(spot(yi), sub)
        loads_a.append(pltpu.make_async_copy(right_op.at[:, take], ops.at[1, :, take], load_sem.at[2 * n + 1]))
    for copy in starts + loads_t + loads_a:
        copy.start()

    barrier = pltpu.get_barrier_semaphore()
    here = y * ncol + c
    for o in range(1, nrow * ncol):
        there = lax.rem(here + o, nrow * ncol)
        pl.semaphore_signal(
            barrier, inc=1, device_id={"row": lax.div(there, ncol), "col": lax.rem(there, ncol)}, device_id_type=pl.DeviceIdType.MESH
        )

    shift = CORES * lax.rem(x, 2) + k
    behind = spot(y)
    up, down = lax.rem(y + shift, RING), lax.rem(y + RING - shift, RING)

    def move(i, src, dst, row, chip, core):
        stays = jnp.logical_and(row == y, jnp.logical_and(chip == x, core == k))
        return push(i, src, dst, dev(row, chip, core)), stays, src, dst

    def start_moves(*moves):
        for copy, stays, src, dst in moves:

            @pl.when(stays)
            def _():
                dst[...] = src[...]

            @pl.when(jnp.logical_not(stays))
            def _():
                copy.start()

    def end_moves(*moves):
        for copy, stays, _, _ in moves:

            @pl.when(jnp.logical_not(stays))
            def _():
                copy.wait()

    for copy in starts:
        copy.wait()
    for h in range(2):
        ag_t[c, h] = ycur[0, h * hsub : (h + 1) * hsub].T.astype(BF16)
    for h in range(2):
        x_half[0, h] = ycur[1, h * hsub : (h + 1) * hsub].astype(BF16)
    pl.semaphore_wait(barrier, nrow * ncol - 1)
    first_one = [move(MOVE + h, x_half.at[0, h], x_half.at[1, h], up, x, k) for h in range(2)]
    first_two = [move(MOVE + 2 + h, x_half.at[1, h], ag_a.at[y, h], y, down, lax.div(x, 2)) for h in range(2)]
    start_moves(*first_one)
    phase()

    def ring_gather(base, blk, me, plus, minus, to):
        own = [blk(me, h) for h in range(2)]
        first = [
            push(base + 0, own[0], own[0], to(plus)),
            push(base + 1, own[1], own[1], to(plus)),
            push(base + 2, own[1], own[1], to(minus)),
            push(base + 3, own[0], own[0], to(minus)),
        ]
        got0, got1 = blk(minus, 0), blk(plus, 1)
        return first, [push(base + 4, got0, got0, to(plus)), push(base + 5, got1, got1, to(minus))]

    def ring_scatter(base, part, got, plus, minus, far, to):
        def half(i, h):
            return rows_of(part(i), h)

        return [
            push(base + 0, half(far, 0), got.at[0], to(plus)),
            push(base + 1, half(far, 1), got.at[1], to(minus)),
            push(base + 2, half(plus, 1), got.at[2], to(plus)),
            push(base + 3, half(minus, 0), got.at[3], to(minus)),
            push(base + 4, half(plus, 0), got.at[4], to(plus)),
            push(base + 5, half(minus, 1), got.at[5], to(minus)),
        ]

    step_one = [
        move(MOVE, ycur.at[0], x_via.at[0], up, x, k),
        move(MOVE + 1, ycur.at[1], x_via.at[1], y, CORES * k + lax.div(behind, 2), lax.rem(behind, 2)),
    ]
    step_two = [
        move(MOVE + 2, x_via.at[0], x_move.at[0], y, down, lax.div(x, 2)),
        move(MOVE + 3, x_via.at[1], x_move.at[1], down, x, k),
    ]
    out_left = pltpu.make_async_copy(x_via.at[0], x_out.at[0], load_sem.at[0])
    out_right = pltpu.make_async_copy(x_move.at[1], x_out.at[1], load_sem.at[1])

    def apply(p):
        t = lax.rem(p, 2)
        a = 1 - t

        def mm_t(pieces, owner, first=False):
            acc = None
            for chip, h in pieces:
                for core in range(CORES):
                    b = chip * CORES + core
                    one = jnp.dot(ag_t[b, h], ops[t, run(b * 2 + h, hsub), run(spot(owner), sub)], preferred_element_type=F32)
                    acc = one if acc is None else acc + one
            p_t[owner] = acc if first else p_t[owner] + acc

        def mm_a(pieces, owner, first=False):
            acc = None
            for i, h in pieces:
                one = jnp.dot(ops[a, run(owner, sub), run(spot(i) * 2 + h, hsub)], ag_a[i, h], preferred_element_type=F32)
                acc = one if acc is None else acc + one
            p_a[owner] = acc if first else p_a[owner] + acc

        def loaded(copy):
            @pl.when(p == 0)
            def _():
                copy.wait()

        send_t, fwd_t = ring_gather(AG_T, lambda i, h: ag_t.at[i * CORES + k, h], x, xp, xm, lambda i: dev(y, i, k))
        send_a, fwd_a = ring_gather(AG_A, lambda i, h: ag_a.at[i, h], y, yp, ym, lambda i: dev(i, x, k))

        def relay(n, i, h=None):
            ref = ag_t.at[i * CORES + k] if h is None else ag_t.at[i * CORES + k, h]
            return push(RELAY + n, ref, ref, partner)

        relays = [relay(0, x)] + [relay(1 + n, i, h) for n, (i, h) in enumerate(((xm, 0), (xp, 1), (xm, 1), (xp, 0), (xf, 0), (xf, 1)))]
        own_y = [(y, 0), (y, 1)]
        phase("ag_own")
        relays[0].start()

        @pl.when(p == 0)
        def _():
            for h in range(2):
                end_moves(first_one[h])
                start_moves(first_two[h])

        for n in (0, 2, 1, 3):
            send_t[n].start()

        @pl.when(p > 0)
        def _():
            for n in (0, 2, 1, 3):
                send_a[n].start()
            for owner in range(RING * CORES):
                mm_a(own_y, owner, True)

        relays[0].wait_recv()
        loaded(loads_t[0])
        for owner in range(RING):
            mm_t([(x, 0), (x, 1)], owner, True)

        @pl.when(p == 0)
        def _():
            end_moves(first_two[0])
            send_a[0].start()
            send_a[3].start()
            end_moves(first_two[1])
            send_a[2].start()
            send_a[1].start()
            loads_a[0].wait()
            for owner in range(RING * CORES):
                mm_a(own_y, owner, True)

        phase("ag_wait1")
        for n, fwd in ((0, 0), (2, 1)):
            send_t[n].wait_recv()
            fwd_t[fwd].start()
            relays[1 + fwd].start()
        for n, fwd in ((0, 0), (2, 1)):
            send_a[n].wait_recv()
            fwd_a[fwd].start()
        phase("mm_near1")
        loaded(loads_a[1])
        loaded(loads_a[2])
        for owner in range(RING * CORES):
            mm_a([(ym, 0), (yp, 1)], owner)
        relays[1].wait_recv()
        relays[2].wait_recv()
        loaded(loads_t[1])
        loaded(loads_t[2])
        for owner in range(RING):
            mm_t([(xm, 0), (xp, 1)], owner)
        phase("mm_near2")
        for n in (1, 3):
            send_t[n].wait_recv()
            relays[3 + n // 2].start()
        for n in (1, 3):
            send_a[n].wait_recv()
        for owner in range(RING * CORES):
            mm_a([(ym, 1), (yp, 0)], owner)
        for n in range(2):
            fwd_t[n].wait_recv()
            relays[5 + n].start()
        relays[3].wait_recv()
        relays[4].wait_recv()
        for owner in range(RING):
            mm_t([(xm, 1), (xp, 0)], owner)
        phase("ag_far")
        fwd_a[0].wait_recv()
        fwd_a[1].wait_recv()
        phase("mm_far")

        loaded(loads_a[3])
        pairs = []
        far_y = [(yf, 0), (yf, 1)]
        out_t = ring_scatter(RS_T, lambda i: p_t.at[i], r_t, yp, ym, yf, lambda i: dev(i, x, k))
        out_a = ring_scatter(RS_A, lambda i: p_a.at[i * CORES + k], r_a, xp, xm, xf, lambda i: dev(y, i, k))

        def pair(n, i, rows):
            pairs.append(push(PAIR + n, p_a.at[i * CORES + other, rows], d_a.at[i, rows], partner))
            pairs[n].start()

        def add_pair(n, i, rows):
            pairs[n].wait_recv()
            p_a[i * CORES + k, rows] = p_a[i * CORES + k, rows] + d_a[i, rows]

        every, half_rows = pl.ds(0, sub), [pl.ds(h * hsub, hsub) for h in range(2)]
        far_x = [(xf, 0), (xf, 1)]
        mm_a(far_y, xf * CORES + other)
        for h in range(2):
            pair(h, xf, half_rows[h])
        for n, i in enumerate((xp, xm, x)):
            mm_a(far_y, i * CORES + other)
        for n, i in enumerate((xp, xm, x)):
            pair(2 + n, i, every)
        relays[5].wait_recv()
        relays[6].wait_recv()
        loaded(loads_t[3])
        mm_t(far_x, yf)
        out_t[0].start()
        out_t[1].start()
        mm_a(far_y, xf * CORES + k)
        for h in range(2):
            add_pair(h, xf, half_rows[h])
            out_a[h].start()
        mm_t(far_x, yp)
        mm_t(far_x, ym)
        out_t[2].start()
        out_t[3].start()
        for i in (xp, xm, x):
            mm_a(far_y, i * CORES + k)
        add_pair(2, xp, every)
        add_pair(3, xm, every)
        out_a[2].start()
        out_a[3].start()
        mm_t(far_x, y)
        add_pair(4, x, every)
        phase("rs_mid")

        @pl.when(p == SWEEPS)
        def _():
            end_moves(*step_two)
            for op in range(2):
                y_one[op] = dot_f32(x_move[op], linv[0, op], NT)
                x_move[op] = dot_f32(y_one[op], linv[1, op], NT)
            out_right.start()
            x_via[0] = ycur[0]
            out_left.start()

        ht = width // 2
        out_t[0].wait_recv()
        p_t[yp, 0:ht] = p_t[yp, 0:ht] + r_t[0]
        out_t[4].start()
        out_t[1].wait_recv()
        p_t[ym, ht:width] = p_t[ym, ht:width] + r_t[1]
        out_t[5].start()
        out_a[0].wait_recv()
        kp, km, kk = xp * CORES + k, xm * CORES + k, x * CORES + k
        p_a[kp, 0:hsub] = p_a[kp, 0:hsub] + r_a[0]
        out_a[4].start()
        out_a[1].wait_recv()
        p_a[km, hsub:sub] = p_a[km, hsub:sub] + r_a[1]
        out_a[5].start()
        phase("rs_end")
        for n in (2, 3, 4, 5):
            out_t[n].wait_recv()
            out_a[n].wait_recv()
        phase("rs_sum")
        ycur[t, :, 0:ht] = (p_t[y, 0:ht] + r_t[3] + r_t[4]).T
        ycur[t, :, ht:width] = (p_t[y, ht:width] + r_t[2] + r_t[5]).T
        ycur[a, 0:hsub] = p_a[kk, 0:hsub] + r_a[3] + r_a[4]
        ycur[a, hsub:sub] = p_a[kk, hsub:sub] + r_a[2] + r_a[5]
        phase("rs_drain")
        for copy in send_t + fwd_t + send_a + fwd_a + relays + pairs + out_t + out_a:
            copy.wait_send()
        phase()

    def all_reduce(rows, local):
        piece = rows // nchips
        phase("ar_pair")
        local(other)
        pair = push(GRAM_PAIR, g_loc.at[other, pl.ds(0, rows)], g_pair.at[pl.ds(0, rows)], partner)
        pair.start()
        local(k)
        pair.wait_recv()
        g_sum[0:rows] = g_loc[k, 0:rows] + g_pair[0:rows]

        def chunk(ref, q):
            return ref.at[pl.ds(pl.multiple_of(q * piece, GROUP), piece)]

        def count(copies):
            return g_all.at[pl.ds(0, copies * piece)]

        def await_copies(sem, copies):
            pltpu.make_async_copy(count(copies), count(copies), sem).wait()

        phase("ar_rs")
        mine = y * RING + x
        routes = []
        for dy, dx in OFFSETS:
            to_y, to_x = (y, yp, yf, ym)[dy], (x, xp, xf, xm)[dx]
            routes.append((dy * RING + dx, to_y * RING + to_x, to_y, to_x))
        owner = CORES - 1

        def spread(o, q, to_y, to_x):
            pltpu.make_async_remote_copy(
                src_ref=chunk(g_sum, q), dst_ref=g_in.at[k, pl.ds(o * piece, piece)], send_sem=send.at[GRAM_RS],
                recv_sem=recv.at[GRAM_RS + k], device_id=dev(to_y, to_x, owner), device_id_type=pl.DeviceIdType.MESH,
            ).start()

        for route in routes:
            spread(*route)

        @pl.when(k == 0)
        def _():
            spread(0, mine, y, x)
            await_copies(send.at[GRAM_RS], nchips)
            phase("ar_ag")
            await_copies(recv.at[GRAM_AG], nchips)
            phase("ar_drain")

        @pl.when(k == 1)
        def _():
            def hand_out(i, src, q, to_y, to_x, core):
                pltpu.make_async_remote_copy(
                    src_ref=src, dst_ref=chunk(g_all, q), send_sem=send.at[GRAM_AG + i], recv_sem=recv.at[GRAM_AG],
                    device_id=dev(to_y, to_x, core), device_id_type=pl.DeviceIdType.MESH,
                ).start()

            await_copies(recv.at[GRAM_RS], nchips)
            total = g_in[0, 0:piece]
            for o in range(1, nchips):
                total = total + g_in[0, o * piece : (o + 1) * piece]
            g_red[0:piece] = total / total_rows
            for _, _, to_y, to_x in routes:
                hand_out(1, g_red.at[pl.ds(0, piece)], mine, to_y, to_x, 0)
            hand_out(1, g_red.at[pl.ds(0, piece)], mine, y, x, 0)
            phase("ar_ag")
            await_copies(recv.at[GRAM_RS + 1], nchips - 1)
            total = chunk(g_sum, mine)[...]
            for o in range(1, nchips):
                total = total + g_in[1, o * piece : (o + 1) * piece]
            chunk(g_all, mine)[...] = total / total_rows
            for _, _, to_y, to_x in routes:
                hand_out(0, chunk(g_all, mine), mine, to_y, to_x, 1)
            await_copies(recv.at[GRAM_AG], nchips - 1)
            phase("ar_drain")
            await_copies(send.at[GRAM_RS], nchips - 1)
            await_copies(send.at[GRAM_AG], nchips - 1)
            await_copies(send.at[GRAM_AG + 1], nchips)

        pair.wait_send()
        phase()

    corners = ((0, 0), (0, 1), (1, 1), (1, 0))

    def put_gram(op, full, count):
        for n, (i, j) in enumerate(corners[:count]):
            g_loc[op, n * tile : (n + 1) * tile] = full[i * tile : (i + 1) * tile, j * tile : (j + 1) * tile]

    def half_gram(op):
        half = ycur[op].astype(BF16)
        put_gram(op, lax.dot_general(half, half, TN, preferred_element_type=F32), 3)

    def full_gram(op):
        put_gram(op, gram_f32(y_one[op]), 3)

    def normalize(p, q):
        def local(op):
            @pl.when(q == 0)
            def _():
                half_gram(op)

            @pl.when(q == 1)
            def _():
                full_gram(op)

        all_reduce(3 * tile, local)
        last = p == SWEEPS - 1

        @pl.when(jnp.logical_and(last, q == 0))
        def _():
            start_moves(*step_one)

        @pl.when(jnp.logical_and(last, q == 1))
        def _():
            end_moves(*step_one)
            start_moves(*step_two)

        phase("chol")

        def store(first, t, value):
            linv[q, k, pl.ds(first, GROUP), t * tile : (t + 1) * tile] = value

        linv[q, k, 0:tile, tile:width] = jnp.zeros((tile, tile), F32)
        inverse_factor(g_all, work, store)
        phase("mul_own")
        swap = push(LINV, linv.at[q, k], linv.at[q, k], partner)
        swap.start()

        def multiply(src, dst):
            dst[k] = dot_f32(src[k], linv[q, k], NT)
            swap.wait_recv()
            dst[other] = dot_f32(src[other], linv[q, other], NT)

        @pl.when(q == 0)
        def _():
            multiply(ycur, y_one)

        @pl.when(q == 1)
        def _():
            multiply(y_one, ycur)

        swap.wait_send()
        phase()

    def sweep(p, carry):
        apply(p)

        @pl.when(p < SWEEPS)
        def _():
            def one(q, carry):
                normalize(p, q)
                return carry

            lax.fori_loop(0, 2, one, 0)
            phase("next_x")
            nxt = lax.rem(p + 1, 2)
            for h in range(2):
                rows = slice(h * hsub, (h + 1) * hsub)
                ag_t[c, h] = ycur[nxt, rows].T.astype(BF16)
                ag_a[y, h] = ycur[1 - nxt, rows].astype(BF16)
            phase()

        return carry

    lax.fori_loop(0, SWEEPS + 1, sweep, 0)

    def rayleigh(op):
        put_gram(op, dot_f32(x_move[op], ycur[op], TN), 4)

    all_reduce(4 * tile, rayleigh)
    phase("h_swap")
    swap = push(LINV, g_all, h_all, partner)
    swap.start()
    swap.wait()
    for n, (i, j) in enumerate(corners):
        rows, at = slice(n * tile, (n + 1) * tile), (slice(i * tile, (i + 1) * tile), slice(j * tile, (j + 1) * tile))
        for op in range(2):
            h_out[(op, *at)] = jnp.where(k == op, g_all[rows], h_all[rows])
    out_left.wait()
    out_right.wait()
    phase()


def hand_over(x_ref, h_ref, left_x, left_h, right_x, right_h):
    left_x[...] = x_ref[0]
    left_h[...] = h_ref[0]
    right_x[...] = x_ref[1]
    right_h[...] = h_ref[1]


def solution(mesh):
    nrow, ncol = mesh.shape["row"], mesh.shape["col"]
    assert nrow == RING and ncol == RING * CORES

    def local_program(left_op, left_start, right_op, right_start):
        rows, cols = left_op.shape
        sub, width = left_start.shape
        tile = width // 2
        vmem = pltpu.VMEM
        dma = pltpu.SemaphoreType.DMA
        basis, ray = jax.ShapeDtypeStruct((sub, width), F32), jax.ShapeDtypeStruct((width, width), F32)
        both_x, both_h = pl.pallas_call(
            functools.partial(kernel, (nrow, ncol, rows * nrow)),
            out_shape=[jax.ShapeDtypeStruct((2, sub, width), F32), jax.ShapeDtypeStruct((2, width, width), F32)],
            in_specs=[pl.BlockSpec(memory_space=pl.ANY)] * 4,
            out_specs=[pl.BlockSpec(memory_space=pl.ANY), pl.BlockSpec(memory_space=vmem)],
            scratch_shapes=[
                vmem((2, rows, cols), BF16),
                vmem((2, sub, width), F32),
                vmem((2, sub, width), F32),
                vmem((ncol, 2, width, sub // 2), BF16),
                vmem((nrow, 2, sub // 2, width), BF16),
                vmem((nrow, width, sub), F32),
                vmem((ncol, sub, width), F32),
                vmem((RING, sub, width), F32),
                vmem((6, width // 2, sub), F32),
                vmem((6, sub // 2, width), F32),
                vmem((2, 2, sub // 2, width), BF16),
                vmem((2, sub, width), F32),
                vmem((2, sub, width), F32),
                vmem((2, 4 * tile, tile), F32),
                vmem((4 * tile, tile), F32),
                vmem((4 * tile, tile), F32),
                vmem((2, 4 * tile, tile), F32),
                vmem((4 * tile // (RING * RING), tile), F32),
                vmem((4 * tile, tile), F32),
                vmem((4 * tile, tile), F32),
                vmem((width, 2 * width), F32),
                vmem((2, 2, width, width), F32),
                dma((COPIES,)),
                dma((COPIES,)),
                dma((10,)),
            ],
            compiler_params=pltpu.CompilerParams(collective_id=0, has_side_effects=True, vmem_limit_bytes=VMEM_BYTES),
            name="subspace",
        )(left_op, left_start, right_op, right_start)
        whole = pl.BlockSpec(memory_space=vmem)
        return pl.pallas_call(
            hand_over, out_shape=[basis, ray, basis, ray], in_specs=[whole] * 2, out_specs=[whole] * 4, name="hand_over"
        )(both_x, both_h)

    op_spec = P(("batch", "row"), "col")
    vec_spec = P(("batch", "row", "col"), None)
    small_spec = P("batch", None)
    return jax.shard_map(
        local_program,
        mesh=mesh,
        in_specs=(op_spec, vec_spec, op_spec, vec_spec),
        out_specs=(vec_spec, small_spec, vec_spec, small_spec),
        check_vma=False,
    )
```

```python
import functools

import jax
import jax.numpy as jnp
from jax import lax
from jax.experimental import pallas as pl
from jax.experimental.pallas import tpu as pltpu
from jax.sharding import PartitionSpec as P

SWEEPS = 4
CORES = 2
RING = 4
PIVOTS = 32
STEP = 16
LEFT_PARTS, RIGHT_PARTS = (2, 0, 1, 1, 0, 0), (0, 2, 1, 0, 1, 0)
GROUP = 8
VMEM_BYTES = 67043328
F32, BF16 = jnp.float32, jnp.bfloat16
TN = (((0,), (0,)), ((), ()))
NT = (((1,), (1,)), ((), ()))

AG_T, AG_A, RELAY, RS_T, RS_A, PAIR, GRAM_PAIR, GRAM_RS, GRAM_AG, LINV, MOVE = 0, 6, 12, 19, 25, 31, 36, 37, 39, 41, 43
AG_B, RELAY_A, START, SWAP_Y, SWAP_H = 47, 51, 52, 54, 55
COPIES = 56
OFFSETS = sorted(
    ((dy, dx) for dy in range(RING) for dx in range(RING) if dy or dx),
    key=lambda o: -min(o[0], RING - o[0]) - min(o[1], RING - o[1]),
)


def split3(v):
    high = v.astype(BF16)
    rest = v - high.astype(F32)
    mid = rest.astype(BF16)
    return high, mid, (rest - mid.astype(F32)).astype(BF16)


def halves_dot(lhs, rhs, dims):
    axis = 1 - dims[0][0][0]
    size = lhs.shape[axis] // 2
    parts = [lax.slice_in_dim(lhs, i * size, (i + 1) * size, axis=axis) for i in range(2)]
    return jnp.concatenate([lax.dot_general(part, rhs, dims, preferred_element_type=F32) for part in parts], axis=0)


def dot_f32(lhs, rhs, dims):
    left, right = split3(lhs), split3(rhs)
    (lk,), (rk,) = dims[0]
    lhs = jnp.concatenate([left[i] for i in LEFT_PARTS], axis=lk)
    rhs = jnp.concatenate([right[i] for i in RIGHT_PARTS], axis=rk)
    return halves_dot(lhs, rhs, dims)


def gram_f32(v):
    high, mid, low = split3(v)
    mixed = halves_dot(jnp.concatenate([high, high], axis=0), jnp.concatenate([low, mid], axis=0), TN)
    return (halves_dot(mid, mid, TN) + (mixed + mixed.T)) + halves_dot(high, high, TN)


class Phases:
    def __init__(self):
        self.scope = None

    def __call__(self, name=None):
        if self.scope is not None:
            self.scope.__exit__(None, None, None)
        self.scope = None
        if name is not None:
            self.scope = jax.named_scope(name)
            self.scope.__enter__()


def rows_of(ref, part, parts=2):
    size = ref.shape[0] // parts
    return ref.at[pl.ds(part * size, size)]


def inverse_factor(gram, work, store):
    tile = gram.shape[1]
    width = 2 * tile
    work[0:tile, 0:tile] = gram[0:tile]
    work[0:tile, tile:width] = gram[tile : 2 * tile]
    work[tile:width, tile:width] = gram[2 * tile : 3 * tile]
    at_row = lax.broadcasted_iota(jnp.int32, (width, width), 0)
    at_col = lax.broadcasted_iota(jnp.int32, (width, width), 1)
    work[:, width : 2 * width] = jnp.where(at_row == at_col, 1.0, 0.0).astype(F32)
    sub = lax.broadcasted_iota(jnp.int32, (GROUP, tile), 0)
    groups = PIVOTS // GROUP
    full = (GROUP, tile)

    def lane(row):
        return jnp.broadcast_to(row, full)

    for first in range(0, width, PIVOTS):
        near = first // tile
        gram_tiles = list(range(near, 2))
        tiles = gram_tiles + [2 + i for i in range(near + 1)]
        data = {
            t: [work[pl.ds(first + GROUP * g, GROUP), t * tile : (t + 1) * tile] for g in range(groups)] for t in tiles
        }
        pivots = [jnp.ones(full, F32) for _ in range(groups)]
        for start in range(0, PIVOTS, STEP):
            at = first - near * tile + start
            end = start + STEP
            cols = {
                j: {
                    g: jnp.broadcast_to(data[near][g][:, at + j - start : at + j - start + 1], full)
                    for g in range(j // GROUP, groups)
                }
                for j in range(start, end)
            }
            for j in range(start, end):
                gj, rj = divmod(j, GROUP)
                col = cols[j]
                pivot = lane(col[gj][rj : rj + 1])
                inv = 1.0 / pivot
                pivots[gj] = jnp.where(sub == rj, pivot, pivots[gj])
                for nxt in range(j + 1, end):
                    gn, rn = divmod(nxt, GROUP)
                    entry = lane(col[gn][rn : rn + 1])
                    if nxt == j + 1:
                        for g in range(gn, groups):
                            cols[nxt][g] = cols[nxt][g] - (col[g] * entry) * inv
                    else:
                        scaled = entry * inv
                        for g in range(gn, groups):
                            cols[nxt][g] = cols[nxt][g] - col[g] * scaled
                for g in range(gj, groups):
                    factor = col[g] * inv
                    if g == gj:
                        if rj == GROUP - 1:
                            continue
                        factor = jnp.where(sub > rj, factor, 0.0)
                    for t in tiles:
                        data[t][g] = data[t][g] - factor * lane(data[t][gj][rj : rj + 1])
        scale = [lax.rsqrt(p) for p in pivots]
        for t in tiles:
            data[t] = [d * s for d, s in zip(data[t], scale, strict=True)]
        for t in tiles:
            if t >= 2:
                for g in range(groups):
                    store(first + GROUP * g, t - 2, data[t][g])
        nxt = first + PIVOTS
        if nxt == width:
            break
        parts = {t: split3(jnp.concatenate(data[t], axis=0)) for t in tiles}
        below = [t for t in gram_tiles if (t + 1) * tile > nxt]
        low = below[0] * tile
        lhs = jnp.concatenate([jnp.concatenate([parts[t][i] for i in LEFT_PARTS], axis=0) for t in below], axis=1)
        right_tiles = below + [t for t in tiles if t >= 2]
        rhs = jnp.concatenate([jnp.concatenate([parts[t][i] for i in RIGHT_PARTS], axis=0) for t in right_tiles], axis=1)
        upd = lax.dot_general(lhs, rhs, TN, preferred_element_type=F32)
        for n, t in enumerate(right_tiles):
            where = pl.ds(nxt, width - nxt), slice(t * tile, (t + 1) * tile)
            work[where] = work[where] - upd[nxt - low :, n * tile : (n + 1) * tile]


def kernel(
    sizes, left_op, left_start, right_op, right_start, x_out, h_out,
    ops, ycur, y_one, ag_t, ag_a, p_t, p_a, d_a, r_t, r_a, x_half, x_via, x_move, y_in, g_loc, g_pair, g_sum, g_in, g_red, g_all, h_all, work, linv,
    send, recv, load_sem,
):
    nrow, ncol, total_rows = sizes
    sub, width = ycur.shape[1:]
    tile, hsub = width // 2, sub // 2
    nchips = RING * RING
    y = lax.axis_index("row")
    c = lax.axis_index("col")
    x, k = lax.div(c, CORES), lax.rem(c, CORES)
    other = 1 - k
    xp, xm, xf = (lax.rem(x + d, RING) for d in (1, 3, 2))
    yp, ym, yf = (lax.rem(y + d, RING) for d in (1, 3, 2))

    def dev(row, chip, core):
        return {"row": row, "col": chip * CORES + core}

    partner = dev(y, x, other)

    def push(i, src, dst, to):
        return pltpu.make_async_remote_copy(
            src_ref=src, dst_ref=dst, send_sem=send.at[i], recv_sem=recv.at[i], device_id=to, device_id_type=pl.DeviceIdType.MESH
        )

    def spot(i):
        return lax.rem(i + RING - x, RING)

    def run(index, size):
        return pl.ds(pl.multiple_of(index * size, size), size)

    phase = Phases()
    phase("boot")
    starts = [
        pltpu.make_async_copy(left_start, ycur.at[0], load_sem.at[8]),
        pltpu.make_async_copy(right_start, ycur.at[1], load_sem.at[9]),
    ]
    loads_t, loads_a = [], []
    for n, (xi, yi) in enumerate(((x, y), (xm, ym), (xp, yp), (xf, yf))):
        take = run(xi, CORES * sub)
        loads_t.append(pltpu.make_async_copy(left_op.at[take], ops.at[0, take], load_sem.at[2 * n]))
        take = run(spot(yi), sub)
        loads_a.append(pltpu.make_async_copy(right_op.at[:, take], ops.at[1, :, take], load_sem.at[2 * n + 1]))
    for copy in starts + loads_t + loads_a:
        copy.start()

    barrier = pltpu.get_barrier_semaphore()
    here = y * ncol + c
    for o in range(1, nrow * ncol):
        there = lax.rem(here + o, nrow * ncol)
        pl.semaphore_signal(
            barrier, inc=1, device_id={"row": lax.div(there, ncol), "col": lax.rem(there, ncol)}, device_id_type=pl.DeviceIdType.MESH
        )

    shift = CORES * lax.rem(x, 2) + k
    behind = spot(y)
    up, down = lax.rem(y + shift, RING), lax.rem(y + RING - shift, RING)

    def move(i, src, dst, row, chip, core):
        stays = jnp.logical_and(row == y, jnp.logical_and(chip == x, core == k))
        return push(i, src, dst, dev(row, chip, core)), stays, src, dst

    def start_moves(*moves):
        for copy, stays, src, dst in moves:

            @pl.when(stays)
            def _():
                dst[...] = src[...]

            @pl.when(jnp.logical_not(stays))
            def _():
                copy.start()

    def end_moves(*moves):
        for copy, stays, _, _ in moves:

            @pl.when(jnp.logical_not(stays))
            def _():
                copy.wait()

    for copy in starts:
        copy.wait()
    for h in range(2):
        ag_t[x, h, k] = ycur[0, h * hsub : (h + 1) * hsub].T.astype(BF16)
    for h in range(2):
        x_half[0, h] = ycur[1, h * hsub : (h + 1) * hsub].astype(BF16)
    pl.semaphore_wait(barrier, nrow * ncol - 1)
    first_one = [move(MOVE + h, x_half.at[0, h], x_half.at[1, h], up, x, k) for h in range(2)]
    first_two = [move(MOVE + 2 + h, x_half.at[1, h], ag_a.at[y, h], y, down, lax.div(x, 2)) for h in range(2)]
    start_moves(*first_one)
    first_swap = [push(START + h, ag_t.at[x, h, k], ag_t.at[x, h, k], partner) for h in range(2)]
    for copy in first_swap:
        copy.start()
    phase()

    def piece_t(chip, h):
        return ag_t.at[chip, h]

    def gather_t():
        to_p, to_m = dev(y, xp, k), dev(y, xm, k)
        sends = [
            push(AG_T + n, piece_t(x, h), piece_t(x, h), to) for n, (h, to) in enumerate(((0, to_p), (1, to_p), (1, to_m), (0, to_m)))
        ]
        onward = [
            push(AG_T + 4, piece_t(xm, 0), piece_t(xm, 0), to_p),
            push(AG_T + 5, piece_t(xp, 1), piece_t(xp, 1), to_m),
        ]
        relays = [push(RELAY, ag_t.at[x], ag_t.at[x], partner)] + [
            push(RELAY + 1 + n, piece_t(i, h), piece_t(i, h), partner)
            for n, (i, h) in enumerate(((xm, 0), (xp, 1), (xm, 1), (xp, 0), (xf, 0), (xf, 1)))
        ]
        return sends, onward, relays

    def gather_a():
        routes = ((0, yp), (1, yp), (1, ym), (0, ym))
        sends = [push(AG_A + n, ag_a.at[y, h], ag_a.at[y, h], dev(i, x, k)) for n, (h, i) in enumerate(routes)]
        onward = [
            push(AG_A + 4, ag_a.at[ym, 0], ag_a.at[ym, 0], dev(yp, x, k)),
            push(AG_A + 5, ag_a.at[yp, 1], ag_a.at[yp, 1], dev(ym, x, k)),
        ]
        for_other = [
            pltpu.make_async_remote_copy(
                src_ref=x_half.at[0, h], dst_ref=ag_a.at[y, h], send_sem=send.at[AG_B + n], recv_sem=recv.at[AG_A + n],
                device_id=dev(i, x, other), device_id_type=pl.DeviceIdType.MESH,
            )
            for n, (h, i) in enumerate(routes)
        ]
        return sends, onward, for_other, push(RELAY_A, x_half.at[0], ag_a.at[y], partner)

    def ring_scatter(base, part, got, plus, minus, far, to):
        def half(i, h):
            return rows_of(part(i), h)

        return [
            push(base + 0, half(far, 0), got.at[0], to(plus)),
            push(base + 1, half(far, 1), got.at[1], to(minus)),
            push(base + 2, half(plus, 1), got.at[2], to(plus)),
            push(base + 3, half(minus, 0), got.at[3], to(minus)),
            push(base + 4, half(plus, 0), got.at[4], to(plus)),
            push(base + 5, half(minus, 1), got.at[5], to(minus)),
        ]

    step_one = [
        move(MOVE, ycur.at[0], x_via.at[0], up, x, k),
        move(MOVE + 1, ycur.at[1], x_via.at[1], y, CORES * k + lax.div(behind, 2), lax.rem(behind, 2)),
    ]
    step_two = [
        move(MOVE + 2, x_via.at[0], x_move.at[0], y, down, lax.div(x, 2)),
        move(MOVE + 3, x_via.at[1], x_move.at[1], down, x, k),
    ]
    out_left = pltpu.make_async_copy(x_via.at[0], x_out.at[0], load_sem.at[0])
    out_right = pltpu.make_async_copy(x_move.at[1], x_out.at[1], load_sem.at[1])

    def share_linv(q):
        return push(LINV + q, linv.at[q, k], linv.at[q, k], partner)

    swap_y = push(SWAP_Y, ycur.at[other], y_in, partner)

    def apply(p):
        t = lax.rem(p, 2)
        a = 1 - t

        def mm_t(pieces, owner, first=False):
            acc = None
            for chip, h in pieces:
                for core in range(CORES):
                    b = chip * CORES + core
                    one = jnp.dot(ag_t[chip, h, core], ops[t, run(b * 2 + h, hsub), run(spot(owner), sub)], preferred_element_type=F32)
                    acc = one if acc is None else acc + one
            p_t[owner] = acc if first else p_t[owner] + acc

        def mm_a(pieces, owner, first=False):
            acc = None
            for i, h in pieces:
                one = jnp.dot(ops[a, run(owner, sub), run(spot(i) * 2 + h, hsub)], ag_a[i, h], preferred_element_type=F32)
                acc = one if acc is None else acc + one
            p_a[owner] = acc if first else p_a[owner] + acc

        def loaded(copy):
            @pl.when(p == 0)
            def _():
                copy.wait()

        send_t, fwd_t, relays = gather_t()
        send_a, fwd_a, send_b, relay_a = gather_a()
        drives_t, drives_a = k == t, k == a
        own_y = [(y, 0), (y, 1)]
        phase("ag_own")

        @pl.when(p == 0)
        def _():
            for h in range(2):
                end_moves(first_one[h])
                start_moves(first_two[h])
            for copy in first_swap:
                copy.wait()

            @pl.when(drives_t)
            def _():
                for n in (0, 2, 1, 3):
                    send_t[n].start()

        @pl.when(p > 0)
        def _():
            @pl.when(jnp.logical_not(drives_a))
            def _():
                relay_a.wait_recv()

            for owner in range(RING * CORES):
                mm_a(own_y, owner, True)

            @pl.when(jnp.logical_not(drives_t))
            def _():
                relays[0].wait_recv()

        loaded(loads_t[0])
        for owner in range(RING):
            mm_t([(x, 0), (x, 1)], owner, True)

        @pl.when(p == 0)
        def _():
            end_moves(first_two[0])
            send_a[0].start()
            send_a[3].start()
            end_moves(first_two[1])
            send_a[2].start()
            send_a[1].start()
            loads_a[0].wait()
            for owner in range(RING * CORES):
                mm_a(own_y, owner, True)

        def take_t(arrived, then):
            @pl.when(drives_t)
            def _():
                for copy, follow in zip(arrived, then, strict=True):
                    copy.wait_recv()
                    for nxt in follow:
                        nxt.start()

        def relayed(*copies):
            @pl.when(jnp.logical_not(drives_t))
            def _():
                for copy in copies:
                    copy.wait_recv()

        phase("ag_wait1")
        take_t((send_t[0], send_t[2]), ((fwd_t[0], relays[1]), (fwd_t[1], relays[2])))
        for n, fwd in ((0, 0), (2, 1)):
            send_a[n].wait_recv()
            fwd_a[fwd].start()
        phase("mm_near1")
        loaded(loads_a[1])
        loaded(loads_a[2])
        for owner in range(RING * CORES):
            mm_a([(ym, 0), (yp, 1)], owner)
        relayed(relays[1], relays[2])
        loaded(loads_t[1])
        loaded(loads_t[2])
        for owner in range(RING):
            mm_t([(xm, 0), (xp, 1)], owner)
        phase("mm_near2")
        take_t((send_t[1], send_t[3]), ((relays[3],), (relays[4],)))
        for n in (1, 3):
            send_a[n].wait_recv()
        for owner in range(RING * CORES):
            mm_a([(ym, 1), (yp, 0)], owner)
        take_t(fwd_t, ((relays[5],), (relays[6],)))
        relayed(relays[3], relays[4])
        for owner in range(RING):
            mm_t([(xm, 1), (xp, 0)], owner)
        phase("ag_far")
        fwd_a[0].wait_recv()
        fwd_a[1].wait_recv()
        phase("mm_far")

        loaded(loads_a[3])
        pairs = []
        far_y = [(yf, 0), (yf, 1)]
        out_t = ring_scatter(RS_T, lambda i: p_t.at[i], r_t, yp, ym, yf, lambda i: dev(i, x, k))
        out_a = ring_scatter(RS_A, lambda i: p_a.at[i * CORES + k], r_a, xp, xm, xf, lambda i: dev(y, i, k))

        def pair(n, i, rows):
            pairs.append(push(PAIR + n, p_a.at[i * CORES + other, rows], d_a.at[i, rows], partner))
            pairs[n].start()

        def add_pair(n, i, rows):
            pairs[n].wait_recv()
            p_a[i * CORES + k, rows] = p_a[i * CORES + k, rows] + d_a[i, rows]

        every, half_rows = pl.ds(0, sub), [pl.ds(h * hsub, hsub) for h in range(2)]
        far_x = [(xf, 0), (xf, 1)]
        mm_a(far_y, xf * CORES + other)
        for h in range(2):
            pair(h, xf, half_rows[h])
        for n, i in enumerate((xp, xm, x)):
            mm_a(far_y, i * CORES + other)
        for n, i in enumerate((xp, xm, x)):
            pair(2 + n, i, every)
        relayed(relays[5], relays[6])
        loaded(loads_t[3])
        mm_t(far_x, yf)
        out_t[0].start()
        out_t[1].start()
        mm_a(far_y, xf * CORES + k)
        for h in range(2):
            add_pair(h, xf, half_rows[h])
            out_a[h].start()
        mm_t(far_x, yp)
        mm_t(far_x, ym)
        out_t[2].start()
        out_t[3].start()
        for i in (xp, xm, x):
            mm_a(far_y, i * CORES + k)
        add_pair(2, xp, every)
        add_pair(3, xm, every)
        out_a[2].start()
        out_a[3].start()
        mm_t(far_x, y)
        add_pair(4, x, every)
        phase("rs_mid")

        @pl.when(p == SWEEPS)
        def _():
            end_moves(*step_two)
            for q in range(2):
                share_linv(q).wait()
            for op in range(2):
                y_one[op] = dot_f32(x_move[op], linv[0, op], NT)
                x_move[op] = dot_f32(y_one[op], linv[1, op], NT)
            out_right.start()
            y_one[0] = dot_f32(ycur[0], linv[0, 0], NT)
            x_via[0] = dot_f32(y_one[0], linv[1, 0], NT)
            out_left.start()

        ht = width // 2
        out_t[0].wait_recv()
        p_t[yp, 0:ht] = p_t[yp, 0:ht] + r_t[0]
        out_t[4].start()
        out_t[1].wait_recv()
        p_t[ym, ht:width] = p_t[ym, ht:width] + r_t[1]
        out_t[5].start()
        out_a[0].wait_recv()
        kp, km, kk = xp * CORES + k, xm * CORES + k, x * CORES + k
        p_a[kp, 0:hsub] = p_a[kp, 0:hsub] + r_a[0]
        out_a[4].start()
        out_a[1].wait_recv()
        p_a[km, hsub:sub] = p_a[km, hsub:sub] + r_a[1]
        out_a[5].start()
        phase("rs_end")
        for n in (2, 3, 4, 5):
            out_t[n].wait_recv()
            out_a[n].wait_recv()
        phase("rs_sum")
        ycur[t, :, 0:ht] = (p_t[y, 0:ht] + r_t[3] + r_t[4]).T
        ycur[t, :, ht:width] = (p_t[y, ht:width] + r_t[2] + r_t[5]).T
        ycur[a, 0:hsub] = p_a[kk, 0:hsub] + r_a[3] + r_a[4]
        ycur[a, hsub:sub] = p_a[kk, hsub:sub] + r_a[2] + r_a[5]
        phase("rs_drain")
        for copy in fwd_a + pairs + out_t + out_a:
            copy.wait_send()

        @pl.when(drives_t)
        def _():
            for copy in send_t + fwd_t + relays[1:]:
                copy.wait_send()

            @pl.when(p > 0)
            def _():
                relays[0].wait_send()

        @pl.when(jnp.logical_or(p == 0, drives_a))
        def _():
            for copy in send_a:
                copy.wait_send()

        @pl.when(jnp.logical_and(p > 0, drives_a))
        def _():
            for copy in send_b + [relay_a]:
                copy.wait_send()

        phase()

    def pair_sum(rows, local):
        phase("ar_pair")
        local(other)
        pair = push(GRAM_PAIR, g_loc.at[other, pl.ds(0, rows)], g_pair.at[pl.ds(0, rows)], partner)
        pair.start()
        local(k)
        pair.wait_recv()
        g_sum[0:rows] = g_loc[k, 0:rows] + g_pair[0:rows]
        pair.wait_send()
        phase()

    def all_reduce(rows):
        piece = rows // nchips

        def chunk(ref, q):
            return ref.at[pl.ds(pl.multiple_of(q * piece, GROUP), piece)]

        def count(copies):
            return g_all.at[pl.ds(0, copies * piece)]

        def await_copies(sem, copies):
            pltpu.make_async_copy(count(copies), count(copies), sem).wait()

        phase("ar_rs")
        mine = y * RING + x
        routes = []
        for dy, dx in OFFSETS:
            to_y, to_x = (y, yp, yf, ym)[dy], (x, xp, xf, xm)[dx]
            routes.append((dy * RING + dx, to_y * RING + to_x, to_y, to_x))
        owner = CORES - 1

        def spread(o, q, to_y, to_x):
            pltpu.make_async_remote_copy(
                src_ref=chunk(g_sum, q), dst_ref=g_in.at[k, pl.ds(o * piece, piece)], send_sem=send.at[GRAM_RS],
                recv_sem=recv.at[GRAM_RS + k], device_id=dev(to_y, to_x, owner), device_id_type=pl.DeviceIdType.MESH,
            ).start()

        for route in routes:
            spread(*route)

        @pl.when(k == 0)
        def _():
            spread(0, mine, y, x)
            await_copies(send.at[GRAM_RS], nchips)
            phase("ar_ag")
            await_copies(recv.at[GRAM_AG], nchips)
            phase("ar_drain")

        @pl.when(k == 1)
        def _():
            def hand_out(i, src, q, to_y, to_x, core):
                pltpu.make_async_remote_copy(
                    src_ref=src, dst_ref=chunk(g_all, q), send_sem=send.at[GRAM_AG + i], recv_sem=recv.at[GRAM_AG],
                    device_id=dev(to_y, to_x, core), device_id_type=pl.DeviceIdType.MESH,
                ).start()

            await_copies(recv.at[GRAM_RS], nchips)
            total = g_in[0, 0:piece]
            for o in range(1, nchips):
                total = total + g_in[0, o * piece : (o + 1) * piece]
            g_red[0:piece] = total / total_rows
            for _, _, to_y, to_x in routes:
                hand_out(1, g_red.at[pl.ds(0, piece)], mine, to_y, to_x, 0)
            hand_out(1, g_red.at[pl.ds(0, piece)], mine, y, x, 0)
            phase("ar_ag")
            await_copies(recv.at[GRAM_RS + 1], nchips - 1)
            total = chunk(g_sum, mine)[...]
            for o in range(1, nchips):
                total = total + g_in[1, o * piece : (o + 1) * piece]
            chunk(g_all, mine)[...] = total / total_rows
            for _, _, to_y, to_x in routes:
                hand_out(0, chunk(g_all, mine), mine, to_y, to_x, 1)
            await_copies(recv.at[GRAM_AG], nchips - 1)
            phase("ar_drain")
            await_copies(send.at[GRAM_RS], nchips - 1)
            await_copies(send.at[GRAM_AG], nchips - 1)
            await_copies(send.at[GRAM_AG + 1], nchips)

        phase()

    corners = ((0, 0), (0, 1), (1, 1), (1, 0))

    def put_gram(into, full, count):
        for n, (i, j) in enumerate(corners[:count]):
            into[n * tile : (n + 1) * tile] = full[i * tile : (i + 1) * tile, j * tile : (j + 1) * tile]

    def half_gram(op):
        half = ycur[op].astype(BF16)
        put_gram(g_loc.at[op], lax.dot_general(half, half, TN, preferred_element_type=F32), 3)

    def normalize(p, q):
        @pl.when(q == 0)
        def _():
            swap_y.start()
            pair_sum(3 * tile, half_gram)

        @pl.when(q == 1)
        def _():
            phase("gram2")
            put_gram(g_sum, gram_f32(y_one[0]) + gram_f32(y_one[1]), 3)
            phase()

        all_reduce(3 * tile)
        last = p == SWEEPS - 1

        @pl.when(jnp.logical_and(last, q == 0))
        def _():
            start_moves(*step_one)

        @pl.when(jnp.logical_and(last, q == 1))
        def _():
            end_moves(*step_one)
            start_moves(*step_two)

        phase("chol")

        def store(first, t, value):
            linv[q, k, pl.ds(first, GROUP), t * tile : (t + 1) * tile] = value

        linv[q, k, 0:tile, tile:width] = jnp.zeros((tile, tile), F32)
        inverse_factor(g_all, work, store)
        phase("mul")

        @pl.when(last)
        def _():
            share_linv(q).start()

        @pl.when(q == 0)
        def _():
            y_one[0] = dot_f32(ycur[k], linv[0, k], NT)
            swap_y.wait()
            y_one[1] = dot_f32(y_in[...], linv[0, k], NT)

        phase()

    def launch(p):
        t = lax.rem(p, 2)

        def new_x(i):
            d_a[i] = dot_f32(y_one[i], linv[1, k], NT)
            return [d_a[i, h * hsub : (h + 1) * hsub] for h in range(2)]

        phase("launch")

        @pl.when(k == t)
        def _():
            sends, _, relays = gather_t()
            for i, core in enumerate((k, other)):
                for h, rows in enumerate(new_x(i)):
                    ag_t[x, h, core] = rows.T.astype(BF16)
            for n in (0, 2, 1, 3):
                sends[n].start()
            relays[0].start()

        @pl.when(k != t)
        def _():
            sends, _, for_other, relay_a = gather_a()
            for h, rows in enumerate(new_x(0)):
                ag_a[y, h] = rows.astype(BF16)
            for n in (0, 2, 1, 3):
                sends[n].start()
            for h, rows in enumerate(new_x(1)):
                x_half[0, h] = rows.astype(BF16)
            for n in (0, 2, 1, 3):
                for_other[n].start()
            relay_a.start()

        phase()

    def sweep(p, carry):
        apply(p)

        @pl.when(p < SWEEPS)
        def _():
            def one(q, carry):
                normalize(p, q)
                return carry

            lax.fori_loop(0, 2, one, 0)
            launch(p + 1)

        return carry

    lax.fori_loop(0, SWEEPS + 1, sweep, 0)

    def rayleigh(op):
        put_gram(g_loc.at[op], dot_f32(x_move[op], ycur[op], TN), 4)

    pair_sum(4 * tile, rayleigh)
    all_reduce(4 * tile)
    phase("h_swap")
    swap = push(SWAP_H, g_all, h_all, partner)
    swap.start()
    swap.wait()
    for n, (i, j) in enumerate(corners):
        rows, at = slice(n * tile, (n + 1) * tile), (slice(i * tile, (i + 1) * tile), slice(j * tile, (j + 1) * tile))
        for op in range(2):
            h_out[(op, *at)] = jnp.where(k == op, g_all[rows], h_all[rows])
    out_left.wait()
    out_right.wait()
    phase()


def hand_over(x_ref, h_ref, left_x, left_h, right_x, right_h):
    left_x[...] = x_ref[0]
    left_h[...] = h_ref[0]
    right_x[...] = x_ref[1]
    right_h[...] = h_ref[1]


def solution(mesh):
    nrow, ncol = mesh.shape["row"], mesh.shape["col"]
    assert nrow == RING and ncol == RING * CORES

    def local_program(left_op, left_start, right_op, right_start):
        rows, cols = left_op.shape
        sub, width = left_start.shape
        tile = width // 2
        vmem = pltpu.VMEM
        dma = pltpu.SemaphoreType.DMA
        basis, ray = jax.ShapeDtypeStruct((sub, width), F32), jax.ShapeDtypeStruct((width, width), F32)
        both_x, both_h = pl.pallas_call(
            functools.partial(kernel, (nrow, ncol, rows * nrow)),
            out_shape=[jax.ShapeDtypeStruct((2, sub, width), F32), jax.ShapeDtypeStruct((2, width, width), F32)],
            in_specs=[pl.BlockSpec(memory_space=pl.ANY)] * 4,
            out_specs=[pl.BlockSpec(memory_space=pl.ANY), pl.BlockSpec(memory_space=vmem)],
            scratch_shapes=[
                vmem((2, rows, cols), BF16),
                vmem((2, sub, width), F32),
                vmem((2, sub, width), F32),
                vmem((RING, 2, CORES, width, sub // 2), BF16),
                vmem((nrow, 2, sub // 2, width), BF16),
                vmem((nrow, width, sub), F32),
                vmem((ncol, sub, width), F32),
                vmem((RING, sub, width), F32),
                vmem((6, width // 2, sub), F32),
                vmem((6, sub // 2, width), F32),
                vmem((2, 2, sub // 2, width), BF16),
                vmem((2, sub, width), F32),
                vmem((2, sub, width), F32),
                vmem((sub, width), F32),
                vmem((2, 4 * tile, tile), F32),
                vmem((4 * tile, tile), F32),
                vmem((4 * tile, tile), F32),
                vmem((2, 4 * tile, tile), F32),
                vmem((4 * tile // (RING * RING), tile), F32),
                vmem((4 * tile, tile), F32),
                vmem((4 * tile, tile), F32),
                vmem((width, 2 * width), F32),
                vmem((2, 2, width, width), F32),
                dma((COPIES,)),
                dma((COPIES,)),
                dma((10,)),
            ],
            compiler_params=pltpu.CompilerParams(collective_id=0, has_side_effects=True, vmem_limit_bytes=VMEM_BYTES),
            name="subspace",
        )(left_op, left_start, right_op, right_start)
        whole = pl.BlockSpec(memory_space=vmem)
        return pl.pallas_call(
            hand_over, out_shape=[basis, ray, basis, ray], in_specs=[whole] * 2, out_specs=[whole] * 4, name="hand_over"
        )(both_x, both_h)

    op_spec = P(("batch", "row"), "col")
    vec_spec = P(("batch", "row", "col"), None)
    small_spec = P("batch", None)
    return jax.shard_map(
        local_program,
        mesh=mesh,
        in_specs=(op_spec, vec_spec, op_spec, vec_spec),
        out_specs=(vec_spec, small_spec, vec_spec, small_spec),
        check_vma=False,
    )
```

```python
import functools

import jax
import jax.numpy as jnp
from jax import lax
from jax.experimental import pallas as pl
from jax.experimental.pallas import tpu as pltpu
from jax.sharding import PartitionSpec as P

SWEEPS = 4
CORES = 2
RING = 4
PIVOTS = 32
STEP = 16
LEFT_PARTS, RIGHT_PARTS = (2, 0, 1, 1, 0, 0), (0, 2, 1, 0, 1, 0)
GROUP = 8
VMEM_BYTES = 67043328
F32, BF16 = jnp.float32, jnp.bfloat16
TN = (((0,), (0,)), ((), ()))
NT = (((1,), (1,)), ((), ()))

AG_T, AG_A, RELAY, RS_T, RS_A, PAIR, GRAM_PAIR, GRAM_RS, GRAM_AG, LINV, MOVE = 0, 6, 12, 19, 25, 31, 36, 37, 39, 41, 43
AG_B, RELAY_A, START, SWAP_Y, SWAP_H = 47, 51, 52, 54, 55
COPIES = 56
OFFSETS = sorted(
    ((dy, dx) for dy in range(RING) for dx in range(RING) if dy or dx),
    key=lambda o: -min(o[0], RING - o[0]) - min(o[1], RING - o[1]),
)


def split3(v):
    high = v.astype(BF16)
    rest = v - high.astype(F32)
    mid = rest.astype(BF16)
    return high, mid, (rest - mid.astype(F32)).astype(BF16)


def halves_dot(lhs, rhs, dims):
    axis = 1 - dims[0][0][0]
    size = lhs.shape[axis] // 2
    parts = [lax.slice_in_dim(lhs, i * size, (i + 1) * size, axis=axis) for i in range(2)]
    return jnp.concatenate([lax.dot_general(part, rhs, dims, preferred_element_type=F32) for part in parts], axis=0)


def dot_f32(lhs, rhs, dims):
    left, right = split3(lhs), split3(rhs)
    (lk,), (rk,) = dims[0]
    lhs = jnp.concatenate([left[i] for i in LEFT_PARTS], axis=lk)
    rhs = jnp.concatenate([right[i] for i in RIGHT_PARTS], axis=rk)
    return halves_dot(lhs, rhs, dims)


def gram_f32(v):
    high, mid, low = split3(v)
    mixed = halves_dot(jnp.concatenate([high, high], axis=0), jnp.concatenate([low, mid], axis=0), TN)
    return (halves_dot(mid, mid, TN) + (mixed + mixed.T)) + halves_dot(high, high, TN)


class Phases:
    def __init__(self):
        self.scope = None

    def __call__(self, name=None):
        if self.scope is not None:
            self.scope.__exit__(None, None, None)
        self.scope = None
        if name is not None:
            self.scope = jax.named_scope(name)
            self.scope.__enter__()


def rows_of(ref, part, parts=2):
    size = ref.shape[0] // parts
    return ref.at[pl.ds(part * size, size)]


def inverse_factor(gram, work, store):
    tile = gram.shape[1]
    width = 2 * tile
    work[0:tile, 0:tile] = gram[0:tile]
    work[0:tile, tile:width] = gram[tile : 2 * tile]
    work[tile:width, tile:width] = gram[2 * tile : 3 * tile]
    at_row = lax.broadcasted_iota(jnp.int32, (width, width), 0)
    at_col = lax.broadcasted_iota(jnp.int32, (width, width), 1)
    work[:, width : 2 * width] = jnp.where(at_row == at_col, 1.0, 0.0).astype(F32)
    sub = lax.broadcasted_iota(jnp.int32, (GROUP, tile), 0)
    groups = PIVOTS // GROUP
    full = (GROUP, tile)

    def lane(row):
        return jnp.broadcast_to(row, full)

    for first in range(0, width, PIVOTS):
        near = first // tile
        gram_tiles = list(range(near, 2))
        tiles = gram_tiles + [2 + i for i in range(near + 1)]
        data = {
            t: [work[pl.ds(first + GROUP * g, GROUP), t * tile : (t + 1) * tile] for g in range(groups)] for t in tiles
        }
        pivots = [jnp.ones(full, F32) for _ in range(groups)]
        for start in range(0, PIVOTS, STEP):
            at = first - near * tile + start
            end = start + STEP
            cols = {
                j: {
                    g: jnp.broadcast_to(data[near][g][:, at + j - start : at + j - start + 1], full)
                    for g in range(j // GROUP, groups)
                }
                for j in range(start, end)
            }
            for j in range(start, end):
                gj, rj = divmod(j, GROUP)
                col = cols[j]
                pivot = lane(col[gj][rj : rj + 1])
                inv = 1.0 / pivot
                pivots[gj] = jnp.where(sub == rj, pivot, pivots[gj])
                for nxt in range(j + 1, end):
                    gn, rn = divmod(nxt, GROUP)
                    entry = lane(col[gn][rn : rn + 1])
                    if nxt == j + 1:
                        for g in range(gn, groups):
                            cols[nxt][g] = cols[nxt][g] - (col[g] * entry) * inv
                    else:
                        scaled = entry * inv
                        for g in range(gn, groups):
                            cols[nxt][g] = cols[nxt][g] - col[g] * scaled
                for g in range(gj, groups):
                    factor = col[g] * inv
                    if g == gj:
                        if rj == GROUP - 1:
                            continue
                        factor = jnp.where(sub > rj, factor, 0.0)
                    for t in tiles:
                        data[t][g] = data[t][g] - factor * lane(data[t][gj][rj : rj + 1])
        scale = [lax.rsqrt(p) for p in pivots]
        for t in tiles:
            data[t] = [d * s for d, s in zip(data[t], scale, strict=True)]
        for t in tiles:
            if t >= 2:
                for g in range(groups):
                    store(first + GROUP * g, t - 2, data[t][g])
        nxt = first + PIVOTS
        if nxt == width:
            break
        parts = {t: split3(jnp.concatenate(data[t], axis=0)) for t in tiles}
        below = [t for t in gram_tiles if (t + 1) * tile > nxt]
        low = below[0] * tile
        lhs = jnp.concatenate([jnp.concatenate([parts[t][i] for i in LEFT_PARTS], axis=0) for t in below], axis=1)
        right_tiles = below + [t for t in tiles if t >= 2]
        rhs = jnp.concatenate([jnp.concatenate([parts[t][i] for i in RIGHT_PARTS], axis=0) for t in right_tiles], axis=1)
        upd = lax.dot_general(lhs, rhs, TN, preferred_element_type=F32)
        for n, t in enumerate(right_tiles):
            where = pl.ds(nxt, width - nxt), slice(t * tile, (t + 1) * tile)
            work[where] = work[where] - upd[nxt - low :, n * tile : (n + 1) * tile]


def kernel(
    sizes, left_op, left_start, right_op, right_start, x_out, h_out,
    ops, ycur, y_one, ag_t, ag_a, p_t, p_a, d_a, r_t, r_a, x_half, x_via, x_move, y_in, g_loc, g_pair, g_sum, g_in, g_red, g_all, h_all, work, linv,
    send, recv, load_sem,
):
    nrow, ncol, total_rows = sizes
    sub, width = ycur.shape[1:]
    tile, hsub = width // 2, sub // 2
    nchips = RING * RING
    y = lax.axis_index("row")
    c = lax.axis_index("col")
    x, k = lax.div(c, CORES), lax.rem(c, CORES)
    other = 1 - k
    xp, xm, xf = (lax.rem(x + d, RING) for d in (1, 3, 2))
    yp, ym, yf = (lax.rem(y + d, RING) for d in (1, 3, 2))

    def dev(row, chip, core):
        return {"row": row, "col": chip * CORES + core}

    partner = dev(y, x, other)

    def push(i, src, dst, to):
        return pltpu.make_async_remote_copy(
            src_ref=src, dst_ref=dst, send_sem=send.at[i], recv_sem=recv.at[i], device_id=to, device_id_type=pl.DeviceIdType.MESH
        )

    def spot(i):
        return lax.rem(i + RING - x, RING)

    def run(index, size):
        return pl.ds(pl.multiple_of(index * size, size), size)

    phase = Phases()
    phase("boot")
    starts = [
        pltpu.make_async_copy(left_start, ycur.at[0], load_sem.at[8]),
        pltpu.make_async_copy(right_start, ycur.at[1], load_sem.at[9]),
    ]
    loads_t, loads_a = [], []
    for n, (xi, yi) in enumerate(((x, y), (xm, ym), (xp, yp), (xf, yf))):
        take = run(xi, CORES * sub)
        loads_t.append(pltpu.make_async_copy(left_op.at[take], ops.at[0, take], load_sem.at[2 * n]))
        take = run(spot(yi), sub)
        loads_a.append(pltpu.make_async_copy(right_op.at[:, take], ops.at[1, :, take], load_sem.at[2 * n + 1]))
    for copy in starts + loads_t + loads_a:
        copy.start()

    barrier = pltpu.get_barrier_semaphore()
    here = y * ncol + c
    for o in range(1, nrow * ncol):
        there = lax.rem(here + o, nrow * ncol)
        pl.semaphore_signal(
            barrier, inc=1, device_id={"row": lax.div(there, ncol), "col": lax.rem(there, ncol)}, device_id_type=pl.DeviceIdType.MESH
        )

    shift = CORES * lax.rem(x, 2) + k
    behind = spot(y)
    up, down = lax.rem(y + shift, RING), lax.rem(y + RING - shift, RING)

    def move(i, src, dst, row, chip, core):
        stays = jnp.logical_and(row == y, jnp.logical_and(chip == x, core == k))
        return push(i, src, dst, dev(row, chip, core)), stays, src, dst

    def start_moves(*moves):
        for copy, stays, src, dst in moves:

            @pl.when(stays)
            def _():
                dst[...] = src[...]

            @pl.when(jnp.logical_not(stays))
            def _():
                copy.start()

    def end_moves(*moves):
        for copy, stays, _, _ in moves:

            @pl.when(jnp.logical_not(stays))
            def _():
                copy.wait()

    for copy in starts:
        copy.wait()
    for h in range(2):
        ag_t[x, h, k] = ycur[0, h * hsub : (h + 1) * hsub].T.astype(BF16)
    for h in range(2):
        x_half[0, h] = ycur[1, h * hsub : (h + 1) * hsub].astype(BF16)
    pl.semaphore_wait(barrier, nrow * ncol - 1)
    first_one = [move(MOVE + h, x_half.at[0, h], x_half.at[1, h], up, x, k) for h in range(2)]
    first_two = [move(MOVE + 2 + h, x_half.at[1, h], ag_a.at[y, h], y, down, lax.div(x, 2)) for h in range(2)]
    start_moves(*first_one)
    first_swap = [push(START + h, ag_t.at[x, h, k], ag_t.at[x, h, k], partner) for h in range(2)]
    for copy in first_swap:
        copy.start()
    phase()

    def piece_t(chip, h):
        return ag_t.at[chip, h]

    def gather_t():
        to_p, to_m = dev(y, xp, k), dev(y, xm, k)
        sends = [
            push(AG_T + n, piece_t(x, h), piece_t(x, h), to) for n, (h, to) in enumerate(((0, to_p), (1, to_p), (1, to_m), (0, to_m)))
        ]
        onward = [
            push(AG_T + 4, piece_t(xm, 0), piece_t(xm, 0), to_p),
            push(AG_T + 5, piece_t(xp, 1), piece_t(xp, 1), to_m),
        ]
        relays = [push(RELAY, ag_t.at[x], ag_t.at[x], partner)] + [
            push(RELAY + 1 + n, piece_t(i, h), piece_t(i, h), partner)
            for n, (i, h) in enumerate(((xm, 0), (xp, 1), (xm, 1), (xp, 0), (xf, 0), (xf, 1)))
        ]
        return sends, onward, relays

    def gather_a():
        routes = ((0, yp), (1, yp), (1, ym), (0, ym))
        sends = [push(AG_A + n, ag_a.at[y, h], ag_a.at[y, h], dev(i, x, k)) for n, (h, i) in enumerate(routes)]
        onward = [
            push(AG_A + 4, ag_a.at[ym, 0], ag_a.at[ym, 0], dev(yp, x, k)),
            push(AG_A + 5, ag_a.at[yp, 1], ag_a.at[yp, 1], dev(ym, x, k)),
        ]
        for_other = [
            pltpu.make_async_remote_copy(
                src_ref=x_half.at[0, h], dst_ref=ag_a.at[y, h], send_sem=send.at[AG_B + n], recv_sem=recv.at[AG_A + n],
                device_id=dev(i, x, other), device_id_type=pl.DeviceIdType.MESH,
            )
            for n, (h, i) in enumerate(routes)
        ]
        return sends, onward, for_other, push(RELAY_A, x_half.at[0], ag_a.at[y], partner)

    def ring_scatter(base, part, got, plus, minus, far, to):
        def half(i, h):
            return rows_of(part(i), h)

        return [
            push(base + 0, half(far, 0), got.at[0], to(plus)),
            push(base + 1, half(far, 1), got.at[1], to(minus)),
            push(base + 2, half(plus, 1), got.at[2], to(plus)),
            push(base + 3, half(minus, 0), got.at[3], to(minus)),
            push(base + 4, half(plus, 0), got.at[4], to(plus)),
            push(base + 5, half(minus, 1), got.at[5], to(minus)),
        ]

    step_one = [
        move(MOVE, ycur.at[0], x_via.at[0], up, x, k),
        move(MOVE + 1, ycur.at[1], x_via.at[1], y, CORES * k + lax.div(behind, 2), lax.rem(behind, 2)),
    ]
    step_two = [
        move(MOVE + 2, x_via.at[0], x_move.at[0], y, down, lax.div(x, 2)),
        move(MOVE + 3, x_via.at[1], x_move.at[1], down, x, k),
    ]
    out_left = pltpu.make_async_copy(x_via.at[0], x_out.at[0], load_sem.at[0])
    out_right = pltpu.make_async_copy(x_move.at[1], x_out.at[1], load_sem.at[1])

    def share_linv(q):
        return push(LINV + q, linv.at[q, k], linv.at[q, k], partner)

    swap_y = push(SWAP_Y, ycur.at[other], y_in, partner)

    def apply(p):
        t = lax.rem(p, 2)
        a = 1 - t

        def mm_t(pieces, owner, first=False):
            acc = None
            for chip, h in pieces:
                for core in range(CORES):
                    b = chip * CORES + core
                    one = jnp.dot(ag_t[chip, h, core], ops[t, run(b * 2 + h, hsub), run(spot(owner), sub)], preferred_element_type=F32)
                    acc = one if acc is None else acc + one
            p_t[owner] = acc if first else p_t[owner] + acc

        def mm_a(pieces, owner, first=False):
            acc = None
            for i, h in pieces:
                one = jnp.dot(ops[a, run(owner, sub), run(spot(i) * 2 + h, hsub)], ag_a[i, h], preferred_element_type=F32)
                acc = one if acc is None else acc + one
            p_a[owner] = acc if first else p_a[owner] + acc

        def loaded(copy):
            @pl.when(p == 0)
            def _():
                copy.wait()

        send_t, fwd_t, relays = gather_t()
        send_a, fwd_a, send_b, relay_a = gather_a()
        drives_t, drives_a = k == t, k == a
        own_y = [(y, 0), (y, 1)]
        phase("ag_own")

        @pl.when(p == 0)
        def _():
            for h in range(2):
                end_moves(first_one[h])
                start_moves(first_two[h])
            for copy in first_swap:
                copy.wait()

            @pl.when(drives_t)
            def _():
                for n in (0, 2, 1, 3):
                    send_t[n].start()

        @pl.when(p > 0)
        def _():
            @pl.when(jnp.logical_not(drives_a))
            def _():
                relay_a.wait_recv()

            for owner in range(RING * CORES):
                mm_a(own_y, owner, True)

            @pl.when(jnp.logical_not(drives_t))
            def _():
                relays[0].wait_recv()

        loaded(loads_t[0])
        for owner in range(RING):
            mm_t([(x, 0), (x, 1)], owner, True)

        @pl.when(p == 0)
        def _():
            end_moves(first_two[0])
            send_a[0].start()
            send_a[3].start()
            end_moves(first_two[1])
            send_a[2].start()
            send_a[1].start()
            loads_a[0].wait()
            for owner in range(RING * CORES):
                mm_a(own_y, owner, True)

        def take_t(arrived, then):
            @pl.when(drives_t)
            def _():
                for copy, follow in zip(arrived, then, strict=True):
                    copy.wait_recv()
                    for nxt in follow:
                        nxt.start()

        def relayed(*copies):
            @pl.when(jnp.logical_not(drives_t))
            def _():
                for copy in copies:
                    copy.wait_recv()

        phase("ag_wait1")
        take_t((send_t[0], send_t[2]), ((fwd_t[0], relays[1]), (fwd_t[1], relays[2])))
        for n, fwd in ((0, 0), (2, 1)):
            send_a[n].wait_recv()
            fwd_a[fwd].start()
        phase("mm_near1")
        loaded(loads_a[1])
        loaded(loads_a[2])
        for owner in range(RING * CORES):
            mm_a([(ym, 0), (yp, 1)], owner)
        relayed(relays[1], relays[2])
        loaded(loads_t[1])
        loaded(loads_t[2])
        for owner in range(RING):
            mm_t([(xm, 0), (xp, 1)], owner)
        phase("mm_near2")
        take_t((send_t[1], send_t[3]), ((relays[3],), (relays[4],)))
        for n in (1, 3):
            send_a[n].wait_recv()
        for owner in range(RING * CORES):
            mm_a([(ym, 1), (yp, 0)], owner)
        relayed(relays[3], relays[4])
        for owner in range(RING):
            mm_t([(xm, 1), (xp, 0)], owner)
        phase("ag_far")
        take_t(fwd_t, ((relays[5],), (relays[6],)))
        fwd_a[0].wait_recv()
        fwd_a[1].wait_recv()
        phase("mm_far")

        loaded(loads_a[3])
        pairs = []
        far_y = [(yf, 0), (yf, 1)]
        out_t = ring_scatter(RS_T, lambda i: p_t.at[i], r_t, yp, ym, yf, lambda i: dev(i, x, k))
        out_a = ring_scatter(RS_A, lambda i: p_a.at[i * CORES + k], r_a, xp, xm, xf, lambda i: dev(y, i, k))

        def pair(n, i, rows):
            pairs.append(push(PAIR + n, p_a.at[i * CORES + other, rows], d_a.at[i, rows], partner))
            pairs[n].start()

        def add_pair(n, i, rows):
            pairs[n].wait_recv()
            p_a[i * CORES + k, rows] = p_a[i * CORES + k, rows] + d_a[i, rows]

        every, half_rows = pl.ds(0, sub), [pl.ds(h * hsub, hsub) for h in range(2)]
        far_x = [(xf, 0), (xf, 1)]
        mm_a(far_y, xf * CORES + other)
        for h in range(2):
            pair(h, xf, half_rows[h])
        relayed(relays[5], relays[6])
        loaded(loads_t[3])
        mm_t(far_x, yf)
        out_t[0].start()
        out_t[1].start()
        mm_a(far_y, xf * CORES + k)
        for h in range(2):
            add_pair(h, xf, half_rows[h])
            out_a[h].start()
        for n, i in enumerate((xp, xm, x)):
            mm_a(far_y, i * CORES + other)
        for n, i in enumerate((xp, xm, x)):
            pair(2 + n, i, every)
        mm_t(far_x, yp)
        mm_t(far_x, ym)
        out_t[2].start()
        out_t[3].start()
        for i in (xp, xm, x):
            mm_a(far_y, i * CORES + k)
        add_pair(2, xp, every)
        add_pair(3, xm, every)
        out_a[2].start()
        out_a[3].start()
        mm_t(far_x, y)
        add_pair(4, x, every)
        phase("rs_mid")

        @pl.when(p == SWEEPS)
        def _():
            end_moves(*step_two)
            for q in range(2):
                share_linv(q).wait()
            for op in range(2):
                y_one[op] = dot_f32(x_move[op], linv[0, op], NT)
                x_move[op] = dot_f32(y_one[op], linv[1, op], NT)
            out_right.start()
            y_one[0] = dot_f32(ycur[0], linv[0, 0], NT)
            x_via[0] = dot_f32(y_one[0], linv[1, 0], NT)
            out_left.start()

        ht = width // 2
        out_t[0].wait_recv()
        p_t[yp, 0:ht] = p_t[yp, 0:ht] + r_t[0]
        out_t[4].start()
        out_t[1].wait_recv()
        p_t[ym, ht:width] = p_t[ym, ht:width] + r_t[1]
        out_t[5].start()
        out_a[0].wait_recv()
        kp, km, kk = xp * CORES + k, xm * CORES + k, x * CORES + k
        p_a[kp, 0:hsub] = p_a[kp, 0:hsub] + r_a[0]
        out_a[4].start()
        out_a[1].wait_recv()
        p_a[km, hsub:sub] = p_a[km, hsub:sub] + r_a[1]
        out_a[5].start()
        phase("rs_end")
        for n in (2, 3, 4, 5):
            out_t[n].wait_recv()
            out_a[n].wait_recv()
        phase("rs_sum")
        ycur[t, :, 0:ht] = (p_t[y, 0:ht] + r_t[3] + r_t[4]).T
        ycur[t, :, ht:width] = (p_t[y, ht:width] + r_t[2] + r_t[5]).T
        ycur[a, 0:hsub] = p_a[kk, 0:hsub] + r_a[3] + r_a[4]
        ycur[a, hsub:sub] = p_a[kk, hsub:sub] + r_a[2] + r_a[5]
        phase("rs_drain")
        for copy in fwd_a + pairs + out_t + out_a:
            copy.wait_send()

        @pl.when(drives_t)
        def _():
            for copy in send_t + fwd_t + relays[1:]:
                copy.wait_send()

            @pl.when(p > 0)
            def _():
                relays[0].wait_send()

        @pl.when(jnp.logical_or(p == 0, drives_a))
        def _():
            for copy in send_a:
                copy.wait_send()

        @pl.when(jnp.logical_and(p > 0, drives_a))
        def _():
            for copy in send_b + [relay_a]:
                copy.wait_send()

        phase()

    def pair_sum(rows, local, behind=None):
        phase("ar_pair")
        local(other)
        pair = push(GRAM_PAIR, g_loc.at[other, pl.ds(0, rows)], g_pair.at[pl.ds(0, rows)], partner)
        pair.start()
        local(k)
        pair.wait_recv()
        if behind is not None:
            behind.start()
        g_sum[0:rows] = g_loc[k, 0:rows] + g_pair[0:rows]
        pair.wait_send()
        phase()

    def all_reduce(rows):
        piece = rows // nchips

        def chunk(ref, q):
            return ref.at[pl.ds(pl.multiple_of(q * piece, GROUP), piece)]

        def count(copies):
            return g_all.at[pl.ds(0, copies * piece)]

        def await_copies(sem, copies):
            pltpu.make_async_copy(count(copies), count(copies), sem).wait()

        phase("ar_rs")
        mine = y * RING + x
        routes = []
        for dy, dx in OFFSETS:
            to_y, to_x = (y, yp, yf, ym)[dy], (x, xp, xf, xm)[dx]
            routes.append((dy * RING + dx, to_y * RING + to_x, to_y, to_x))
        owner = CORES - 1

        def spread(o, q, to_y, to_x):
            pltpu.make_async_remote_copy(
                src_ref=chunk(g_sum, q), dst_ref=g_in.at[k, pl.ds(o * piece, piece)], send_sem=send.at[GRAM_RS],
                recv_sem=recv.at[GRAM_RS + k], device_id=dev(to_y, to_x, owner), device_id_type=pl.DeviceIdType.MESH,
            ).start()

        for route in routes:
            spread(*route)

        @pl.when(k == 0)
        def _():
            spread(0, mine, y, x)
            await_copies(send.at[GRAM_RS], nchips)
            phase("ar_ag")
            await_copies(recv.at[GRAM_AG], nchips)
            phase("ar_drain")

        @pl.when(k == 1)
        def _():
            def hand_out(i, src, q, to_y, to_x, core):
                pltpu.make_async_remote_copy(
                    src_ref=src, dst_ref=chunk(g_all, q), send_sem=send.at[GRAM_AG + i], recv_sem=recv.at[GRAM_AG],
                    device_id=dev(to_y, to_x, core), device_id_type=pl.DeviceIdType.MESH,
                ).start()

            await_copies(recv.at[GRAM_RS], nchips)
            total = g_in[0, 0:piece]
            for o in range(1, nchips):
                total = total + g_in[0, o * piece : (o + 1) * piece]
            g_red[0:piece] = total / total_rows
            for _, _, to_y, to_x in routes:
                hand_out(1, g_red.at[pl.ds(0, piece)], mine, to_y, to_x, 0)
            hand_out(1, g_red.at[pl.ds(0, piece)], mine, y, x, 0)
            phase("ar_ag")
            await_copies(recv.at[GRAM_RS + 1], nchips - 1)
            total = chunk(g_sum, mine)[...]
            for o in range(1, nchips):
                total = total + g_in[1, o * piece : (o + 1) * piece]
            chunk(g_all, mine)[...] = total / total_rows
            for _, _, to_y, to_x in routes:
                hand_out(0, chunk(g_all, mine), mine, to_y, to_x, 1)
            await_copies(recv.at[GRAM_AG], nchips - 1)
            phase("ar_drain")
            await_copies(send.at[GRAM_RS], nchips - 1)
            await_copies(send.at[GRAM_AG], nchips - 1)
            await_copies(send.at[GRAM_AG + 1], nchips)

        phase()

    corners = ((0, 0), (0, 1), (1, 1), (1, 0))

    def put_gram(into, full, count):
        for n, (i, j) in enumerate(corners[:count]):
            into[n * tile : (n + 1) * tile] = full[i * tile : (i + 1) * tile, j * tile : (j + 1) * tile]

    def half_gram(op):
        half = ycur[op].astype(BF16)
        put_gram(g_loc.at[op], lax.dot_general(half, half, TN, preferred_element_type=F32), 3)

    def normalize(p, q):
        @pl.when(q == 0)
        def _():
            pair_sum(3 * tile, half_gram, swap_y)

        @pl.when(q == 1)
        def _():
            phase("gram2")
            put_gram(g_sum, gram_f32(y_one[0]) + gram_f32(y_one[1]), 3)
            phase()

        all_reduce(3 * tile)
        last = p == SWEEPS - 1

        @pl.when(jnp.logical_and(last, q == 0))
        def _():
            start_moves(*step_one)

        @pl.when(jnp.logical_and(last, q == 1))
        def _():
            end_moves(*step_one)
            start_moves(*step_two)

        phase("chol")

        def store(first, t, value):
            linv[q, k, pl.ds(first, GROUP), t * tile : (t + 1) * tile] = value

        linv[q, k, 0:tile, tile:width] = jnp.zeros((tile, tile), F32)
        inverse_factor(g_all, work, store)
        phase("mul")

        @pl.when(last)
        def _():
            share_linv(q).start()

        @pl.when(q == 0)
        def _():
            y_one[0] = dot_f32(ycur[k], linv[0, k], NT)
            swap_y.wait()
            y_one[1] = dot_f32(y_in[...], linv[0, k], NT)

        phase()

    def launch(p):
        t = lax.rem(p, 2)

        def new_x(i):
            d_a[i] = dot_f32(y_one[i], linv[1, k], NT)
            return [d_a[i, h * hsub : (h + 1) * hsub] for h in range(2)]

        phase("launch")

        @pl.when(k == t)
        def _():
            sends, _, relays = gather_t()
            for i, core in enumerate((k, other)):
                for h, rows in enumerate(new_x(i)):
                    ag_t[x, h, core] = rows.T.astype(BF16)
            for n in (0, 2, 1, 3):
                sends[n].start()
            relays[0].start()

        @pl.when(k != t)
        def _():
            sends, _, for_other, relay_a = gather_a()
            for h, rows in enumerate(new_x(0)):
                ag_a[y, h] = rows.astype(BF16)
            for n in (0, 2, 1, 3):
                sends[n].start()
            for h, rows in enumerate(new_x(1)):
                x_half[0, h] = rows.astype(BF16)
            for n in (0, 2, 1, 3):
                for_other[n].start()
            relay_a.start()

        phase()

    def sweep(p, carry):
        apply(p)

        @pl.when(p < SWEEPS)
        def _():
            def one(q, carry):
                normalize(p, q)
                return carry

            lax.fori_loop(0, 2, one, 0)
            launch(p + 1)

        return carry

    lax.fori_loop(0, SWEEPS + 1, sweep, 0)

    def rayleigh(op):
        put_gram(g_loc.at[op], dot_f32(x_move[op], ycur[op], TN), 4)

    pair_sum(4 * tile, rayleigh)
    all_reduce(4 * tile)
    phase("h_swap")
    swap = push(SWAP_H, g_all, h_all, partner)
    swap.start()
    swap.wait()
    for n, (i, j) in enumerate(corners):
        rows, at = slice(n * tile, (n + 1) * tile), (slice(i * tile, (i + 1) * tile), slice(j * tile, (j + 1) * tile))
        for op in range(2):
            h_out[(op, *at)] = jnp.where(k == op, g_all[rows], h_all[rows])
    out_left.wait()
    out_right.wait()
    phase()


def hand_over(x_ref, h_ref, left_x, left_h, right_x, right_h):
    left_x[...] = x_ref[0]
    left_h[...] = h_ref[0]
    right_x[...] = x_ref[1]
    right_h[...] = h_ref[1]


def solution(mesh):
    nrow, ncol = mesh.shape["row"], mesh.shape["col"]
    assert nrow == RING and ncol == RING * CORES

    def local_program(left_op, left_start, right_op, right_start):
        rows, cols = left_op.shape
        sub, width = left_start.shape
        tile = width // 2
        vmem = pltpu.VMEM
        dma = pltpu.SemaphoreType.DMA
        basis, ray = jax.ShapeDtypeStruct((sub, width), F32), jax.ShapeDtypeStruct((width, width), F32)
        both_x, both_h = pl.pallas_call(
            functools.partial(kernel, (nrow, ncol, rows * nrow)),
            out_shape=[jax.ShapeDtypeStruct((2, sub, width), F32), jax.ShapeDtypeStruct((2, width, width), F32)],
            in_specs=[pl.BlockSpec(memory_space=pl.ANY)] * 4,
            out_specs=[pl.BlockSpec(memory_space=pl.ANY), pl.BlockSpec(memory_space=vmem)],
            scratch_shapes=[
                vmem((2, rows, cols), BF16),
                vmem((2, sub, width), F32),
                vmem((2, sub, width), F32),
                vmem((RING, 2, CORES, width, sub // 2), BF16),
                vmem((nrow, 2, sub // 2, width), BF16),
                vmem((nrow, width, sub), F32),
                vmem((ncol, sub, width), F32),
                vmem((RING, sub, width), F32),
                vmem((6, width // 2, sub), F32),
                vmem((6, sub // 2, width), F32),
                vmem((2, 2, sub // 2, width), BF16),
                vmem((2, sub, width), F32),
                vmem((2, sub, width), F32),
                vmem((sub, width), F32),
                vmem((2, 4 * tile, tile), F32),
                vmem((4 * tile, tile), F32),
                vmem((4 * tile, tile), F32),
                vmem((2, 4 * tile, tile), F32),
                vmem((4 * tile // (RING * RING), tile), F32),
                vmem((4 * tile, tile), F32),
                vmem((4 * tile, tile), F32),
                vmem((width, 2 * width), F32),
                vmem((2, 2, width, width), F32),
                dma((COPIES,)),
                dma((COPIES,)),
                dma((10,)),
            ],
            compiler_params=pltpu.CompilerParams(collective_id=0, has_side_effects=True, vmem_limit_bytes=VMEM_BYTES),
            name="subspace",
        )(left_op, left_start, right_op, right_start)
        whole = pl.BlockSpec(memory_space=vmem)
        return pl.pallas_call(
            hand_over, out_shape=[basis, ray, basis, ray], in_specs=[whole] * 2, out_specs=[whole] * 4, name="hand_over"
        )(both_x, both_h)

    op_spec = P(("batch", "row"), "col")
    vec_spec = P(("batch", "row", "col"), None)
    small_spec = P("batch", None)
    return jax.shard_map(
        local_program,
        mesh=mesh,
        in_specs=(op_spec, vec_spec, op_spec, vec_spec),
        out_specs=(vec_spec, small_spec, vec_spec, small_spec),
        check_vma=False,
    )
```

```python
import functools

import jax
import jax.numpy as jnp
from jax import lax
from jax.experimental import pallas as pl
from jax.experimental.pallas import tpu as pltpu
from jax.sharding import PartitionSpec as P

SWEEPS = 4
CORES = 2
RING = 4
PIVOTS = 32
STEP = 16
LEFT_PARTS, RIGHT_PARTS = (2, 0, 1, 1, 0, 0), (0, 2, 1, 0, 1, 0)
GROUP = 8
VMEM_BYTES = 67043328
F32, BF16 = jnp.float32, jnp.bfloat16
TN = (((0,), (0,)), ((), ()))
NT = (((1,), (1,)), ((), ()))

SLOTS = 8
KINDS = range(0, 17 * SLOTS, SLOTS)
AG_T, AG_TX, AG_A, AG_B, RELAY, RELAY_A, RS_T, RS_A, PAIR, GRAM_PAIR, GRAM_RS, GRAM_AG, LINV, MOVE, START, SWAP_Y, SWAP_H = KINDS
ORDER = (0, 2, 1, 3)
OFFSETS = sorted(
    ((dy, dx) for dy in range(RING) for dx in range(RING) if dy or dx),
    key=lambda o: -min(o[0], RING - o[0]) - min(o[1], RING - o[1]),
)


def split3(v):
    high = v.astype(BF16)
    rest = v - high.astype(F32)
    mid = rest.astype(BF16)
    return high, mid, (rest - mid.astype(F32)).astype(BF16)


def halves_dot(lhs, rhs, dims):
    axis = 1 - dims[0][0][0]
    size = lhs.shape[axis] // 2
    parts = [lax.slice_in_dim(lhs, i * size, (i + 1) * size, axis=axis) for i in range(2)]
    return jnp.concatenate([lax.dot_general(part, rhs, dims, preferred_element_type=F32) for part in parts], axis=0)


def dot_f32(lhs, rhs, dims):
    left, right = split3(lhs), split3(rhs)
    (lk,), (rk,) = dims[0]
    lhs = jnp.concatenate([left[i] for i in LEFT_PARTS], axis=lk)
    rhs = jnp.concatenate([right[i] for i in RIGHT_PARTS], axis=rk)
    return halves_dot(lhs, rhs, dims)


def gram_f32(v):
    high, mid, low = split3(v)
    mixed = halves_dot(jnp.concatenate([high, high], axis=0), jnp.concatenate([low, mid], axis=0), TN)
    return (halves_dot(mid, mid, TN) + (mixed + mixed.T)) + halves_dot(high, high, TN)


class Phases:
    def __init__(self):
        self.scope = None

    def __call__(self, name=None):
        if self.scope is not None:
            self.scope.__exit__(None, None, None)
        self.scope = None
        if name is not None:
            self.scope = jax.named_scope(name)
            self.scope.__enter__()


def rows_of(ref, part, parts=2):
    size = ref.shape[0] // parts
    return ref.at[pl.ds(part * size, size)]


def set_identity(work):
    width = work.shape[0]
    at_row = lax.broadcasted_iota(jnp.int32, (width, width), 0)
    at_col = lax.broadcasted_iota(jnp.int32, (width, width), 1)
    work[:, width : 2 * width] = jnp.where(at_row == at_col, 1.0, 0.0).astype(F32)


def inverse_factor(gram, work, store):
    tile = gram.shape[1]
    width = 2 * tile
    work[0:tile, 0:tile] = gram[0:tile]
    work[0:tile, tile:width] = gram[tile : 2 * tile]
    work[tile:width, tile:width] = gram[2 * tile : 3 * tile]
    sub = lax.broadcasted_iota(jnp.int32, (GROUP, tile), 0)
    groups = PIVOTS // GROUP
    full = (GROUP, tile)

    def lane(row):
        return jnp.broadcast_to(row, full)

    for first in range(0, width, PIVOTS):
        near = first // tile
        gram_tiles = list(range(near, 2))
        tiles = gram_tiles + [2 + i for i in range(near + 1)]
        data = {
            t: [work[pl.ds(first + GROUP * g, GROUP), t * tile : (t + 1) * tile] for g in range(groups)] for t in tiles
        }
        pivots = [jnp.ones(full, F32) for _ in range(groups)]
        for start in range(0, PIVOTS, STEP):
            at = first - near * tile + start
            end = start + STEP
            cols = {
                j: {
                    g: jnp.broadcast_to(data[near][g][:, at + j - start : at + j - start + 1], full)
                    for g in range(j // GROUP, groups)
                }
                for j in range(start, end)
            }
            for j in range(start, end):
                gj, rj = divmod(j, GROUP)
                col = cols[j]
                pivot = lane(col[gj][rj : rj + 1])
                inv = 1.0 / pivot
                pivots[gj] = jnp.where(sub == rj, pivot, pivots[gj])
                for nxt in range(j + 1, end):
                    gn, rn = divmod(nxt, GROUP)
                    entry = lane(col[gn][rn : rn + 1])
                    if nxt == j + 1:
                        for g in range(gn, groups):
                            cols[nxt][g] = cols[nxt][g] - (col[g] * entry) * inv
                    else:
                        scaled = entry * inv
                        for g in range(gn, groups):
                            cols[nxt][g] = cols[nxt][g] - col[g] * scaled
                for g in range(gj, groups):
                    factor = col[g] * inv
                    if g == gj:
                        if rj == GROUP - 1:
                            continue
                        factor = jnp.where(sub > rj, factor, 0.0)
                    for t in tiles:
                        data[t][g] = data[t][g] - factor * lane(data[t][gj][rj : rj + 1])
        scale = [lax.rsqrt(p) for p in pivots]
        for t in tiles:
            data[t] = [d * s for d, s in zip(data[t], scale, strict=True)]
        for t in tiles:
            if t >= 2:
                for g in range(groups):
                    store(first + GROUP * g, t - 2, data[t][g])
        nxt = first + PIVOTS
        if nxt == width:
            break
        parts = {t: split3(jnp.concatenate(data[t], axis=0)) for t in tiles}
        below = [t for t in gram_tiles if (t + 1) * tile > nxt]
        low = below[0] * tile
        lhs = jnp.concatenate([jnp.concatenate([parts[t][i] for i in LEFT_PARTS], axis=0) for t in below], axis=1)
        right_tiles = below + [t for t in tiles if t >= 2]
        rhs = jnp.concatenate([jnp.concatenate([parts[t][i] for i in RIGHT_PARTS], axis=0) for t in right_tiles], axis=1)
        upd = lax.dot_general(lhs, rhs, TN, preferred_element_type=F32)
        for n, t in enumerate(right_tiles):
            where = pl.ds(nxt, width - nxt), slice(t * tile, (t + 1) * tile)
            work[where] = work[where] - upd[nxt - low :, n * tile : (n + 1) * tile]


def kernel(
    sizes, left_op, left_start, right_op, right_start, x_out, h_out,
    ops, ycur, y_one, ag_t, ag_a, p_t, p_a, d_a, r_t, r_a, x_half, x_via, x_move, y_in, g_loc, g_pair, g_sum, g_in, g_red, g_all, h_all, work, linv,
    send, recv, load_sem,
):
    nrow, ncol, total_rows = sizes
    sub, width = ycur.shape[1:]
    tile, hsub = width // 2, sub // 2
    nchips = RING * RING
    y = lax.axis_index("row")
    c = lax.axis_index("col")
    x, k = lax.div(c, CORES), lax.rem(c, CORES)
    other = 1 - k
    xp, xm, xf = (lax.rem(x + d, RING) for d in (1, 3, 2))
    yp, ym, yf = (lax.rem(y + d, RING) for d in (1, 3, 2))

    def dev(row, chip, core):
        return {"row": row, "col": chip * CORES + core}

    partner = dev(y, x, other)

    def push(i, src, dst, to):
        return pltpu.make_async_remote_copy(
            src_ref=src, dst_ref=dst, send_sem=send.at[i], recv_sem=recv.at[i], device_id=to, device_id_type=pl.DeviceIdType.MESH
        )

    def spot(i):
        return lax.rem(i + RING - x, RING)

    def run(index, size):
        return pl.ds(pl.multiple_of(index * size, size), size)

    phase = Phases()
    phase("boot")
    starts = [
        pltpu.make_async_copy(left_start, ycur.at[0], load_sem.at[8]),
        pltpu.make_async_copy(right_start, ycur.at[1], load_sem.at[9]),
    ]
    loads_t, loads_a = [], []
    for n, (xi, yi) in enumerate(((x, y), (xm, ym), (xp, yp), (xf, yf))):
        take = run(xi, CORES * sub)
        loads_t.append(pltpu.make_async_copy(left_op.at[take], ops.at[0, take], load_sem.at[2 * n]))
        take = run(spot(yi), sub)
        loads_a.append(pltpu.make_async_copy(right_op.at[:, take], ops.at[1, :, take], load_sem.at[2 * n + 1]))
    for copy in starts + loads_t + loads_a:
        copy.start()

    barrier = pltpu.get_barrier_semaphore()
    here = y * ncol + c
    for o in range(1, nrow * ncol):
        there = lax.rem(here + o, nrow * ncol)
        pl.semaphore_signal(
            barrier, inc=1, device_id={"row": lax.div(there, ncol), "col": lax.rem(there, ncol)}, device_id_type=pl.DeviceIdType.MESH
        )

    shift = CORES * lax.rem(x, 2) + k
    behind = spot(y)
    up, down = lax.rem(y + shift, RING), lax.rem(y + RING - shift, RING)

    def move(i, src, dst, row, chip, core):
        stays = jnp.logical_and(row == y, jnp.logical_and(chip == x, core == k))
        return push(i, src, dst, dev(row, chip, core)), stays, src, dst

    def start_moves(*moves):
        for copy, stays, src, dst in moves:

            @pl.when(stays)
            def _():
                dst[...] = src[...]

            @pl.when(jnp.logical_not(stays))
            def _():
                copy.start()

    def end_moves(*moves):
        for copy, stays, _, _ in moves:

            @pl.when(jnp.logical_not(stays))
            def _():
                copy.wait()

    for copy in starts:
        copy.wait()
    for h in range(2):
        ag_t[x, h, k] = ycur[0, h * hsub : (h + 1) * hsub].T.astype(BF16)
    for h in range(2):
        x_half[0, h] = ycur[1, h * hsub : (h + 1) * hsub].astype(BF16)
    pl.semaphore_wait(barrier, nrow * ncol - 1)
    first_one = [move(MOVE + h, x_half.at[0, h], x_half.at[1, h], up, x, k) for h in range(2)]
    first_two = [move(MOVE + 2 + h, x_half.at[1, h], ag_a.at[y, h], y, down, lax.div(x, 2)) for h in range(2)]
    start_moves(*first_one)
    first_swap = [push(START + h, ag_t.at[x, h, k], ag_t.at[x, h, k], partner) for h in range(2)]
    for copy in first_swap:
        copy.start()
    phase()

    def piece_t(chip, h):
        return ag_t.at[chip, h]

    def gather_t():
        to_p, to_m = dev(y, xp, k), dev(y, xm, k)
        routes = ((0, to_p), (1, to_p), (1, to_m), (0, to_m))
        sends = [
            [push(kind + n, ag_t.at[x, h, core], ag_t.at[x, h, core], to) for kind, core in ((AG_T, k), (AG_TX, other))]
            for n, (h, to) in enumerate(routes)
        ]
        onward = [
            push(AG_T + 4, piece_t(xm, 0), piece_t(xm, 0), to_p),
            push(AG_T + 5, piece_t(xp, 1), piece_t(xp, 1), to_m),
        ]
        relays = [push(RELAY, ag_t.at[x], ag_t.at[x], partner)] + [
            push(RELAY + 1 + n, piece_t(i, h), piece_t(i, h), partner)
            for n, (i, h) in enumerate(((xm, 0), (xp, 1), (xm, 1), (xp, 0), (xf, 0), (xf, 1)))
        ]
        return sends, onward, relays

    def gather_a():
        routes = ((0, yp), (1, yp), (1, ym), (0, ym))
        sends = [push(AG_A + n, ag_a.at[y, h], ag_a.at[y, h], dev(i, x, k)) for n, (h, i) in enumerate(routes)]
        onward = [
            push(AG_A + 4, ag_a.at[ym, 0], ag_a.at[ym, 0], dev(yp, x, k)),
            push(AG_A + 5, ag_a.at[yp, 1], ag_a.at[yp, 1], dev(ym, x, k)),
        ]
        for_other = [
            pltpu.make_async_remote_copy(
                src_ref=x_half.at[0, h], dst_ref=ag_a.at[y, h], send_sem=send.at[AG_B + n], recv_sem=recv.at[AG_A + n],
                device_id=dev(i, x, other), device_id_type=pl.DeviceIdType.MESH,
            )
            for n, (h, i) in enumerate(routes)
        ]
        return sends, onward, for_other, push(RELAY_A, x_half.at[0], ag_a.at[y], partner)

    def ring_scatter(base, part, got, plus, minus, far, to):
        def half(i, h):
            return rows_of(part(i), h)

        return [
            push(base + 0, half(far, 0), got.at[0], to(plus)),
            push(base + 1, half(far, 1), got.at[1], to(minus)),
            push(base + 2, half(plus, 1), got.at[2], to(plus)),
            push(base + 3, half(minus, 0), got.at[3], to(minus)),
            push(base + 4, half(plus, 0), got.at[4], to(plus)),
            push(base + 5, half(minus, 1), got.at[5], to(minus)),
        ]

    step_one = [
        move(MOVE, ycur.at[0], x_via.at[0], up, x, k),
        move(MOVE + 1, ycur.at[1], x_via.at[1], y, CORES * k + lax.div(behind, 2), lax.rem(behind, 2)),
    ]
    step_two = [
        move(MOVE + 2, x_via.at[0], x_move.at[0], y, down, lax.div(x, 2)),
        move(MOVE + 3, x_via.at[1], x_move.at[1], down, x, k),
    ]
    out_left = pltpu.make_async_copy(x_via.at[0], x_out.at[0], load_sem.at[0])
    out_right = pltpu.make_async_copy(x_move.at[1], x_out.at[1], load_sem.at[1])

    def share_linv(q):
        return push(LINV + q, linv.at[q, k], linv.at[q, k], partner)

    swap_y = push(SWAP_Y, ycur.at[other], y_in, partner)

    def apply(p):
        t = lax.rem(p, 2)
        a = 1 - t

        def mm_t(pieces, owner, first=False):
            for n in range(2):
                acc, lanes = None, slice(n * hsub, (n + 1) * hsub)
                for chip, h in pieces:
                    for core in range(CORES):
                        rows = run((chip * CORES + core) * 2 + h, hsub)
                        one = jnp.dot(ag_t[chip, h, core], ops[t, rows, run(spot(owner) * 2 + n, hsub)], preferred_element_type=F32)
                        acc = one if acc is None else acc + one
                p_t[owner, :, lanes] = acc if first else p_t[owner, :, lanes] + acc

        def mm_a(pieces, owner, first=False):
            for n in range(2):
                acc, rows = None, slice(n * hsub, (n + 1) * hsub)
                for i, h in pieces:
                    one = jnp.dot(ops[a, run(owner * 2 + n, hsub), run(spot(i) * 2 + h, hsub)], ag_a[i, h], preferred_element_type=F32)
                    acc = one if acc is None else acc + one
                p_a[owner, rows] = acc if first else p_a[owner, rows] + acc

        def loaded(copy):
            @pl.when(p == 0)
            def _():
                copy.wait()

        send_t, fwd_t, relays = gather_t()
        send_a, fwd_a, send_b, relay_a = gather_a()
        drives_t, drives_a = k == t, k == a
        own_y = [(y, 0), (y, 1)]
        phase("ag_own")

        @pl.when(p == 0)
        def _():
            for h in range(2):
                end_moves(first_one[h])
                start_moves(first_two[h])
            for copy in first_swap:
                copy.wait()

            @pl.when(drives_t)
            def _():
                for n in ORDER:
                    for copy in send_t[n]:
                        copy.start()

        @pl.when(p > 0)
        def _():
            @pl.when(jnp.logical_not(drives_a))
            def _():
                relay_a.wait_recv()

            for owner in range(RING * CORES):
                mm_a(own_y, owner, True)

            @pl.when(jnp.logical_not(drives_t))
            def _():
                relays[0].wait_recv()

        loaded(loads_t[0])
        for owner in range(RING):
            mm_t([(x, 0), (x, 1)], owner, True)

        @pl.when(p == 0)
        def _():
            end_moves(first_two[0])
            send_a[0].start()
            send_a[3].start()
            end_moves(first_two[1])
            send_a[2].start()
            send_a[1].start()
            loads_a[0].wait()
            for owner in range(RING * CORES):
                mm_a(own_y, owner, True)

        def take_t(arrived, then):
            @pl.when(drives_t)
            def _():
                for copies, follow in zip(arrived, then):
                    for copy in copies:
                        copy.wait_recv()
                    for nxt in follow:
                        nxt.start()

        def relayed(*copies):
            @pl.when(jnp.logical_not(drives_t))
            def _():
                for copy in copies:
                    copy.wait_recv()

        phase("ag_wait1")
        take_t([send_t[n] for n in ORDER[:2]], zip(fwd_t, relays[1:3]))
        for n, copy in zip(ORDER, fwd_a):
            send_a[n].wait_recv()
            copy.start()
        phase("mm_near1")
        loaded(loads_a[1])
        loaded(loads_a[2])
        for owner in range(RING * CORES):
            mm_a([(ym, 0), (yp, 1)], owner)
        relayed(*relays[1:3])
        loaded(loads_t[1])
        loaded(loads_t[2])
        for owner in range(RING):
            mm_t([(xm, 0), (xp, 1)], owner)
        phase("mm_near2")
        take_t([send_t[n] for n in ORDER[2:]], zip(relays[3:5]))
        for n in ORDER[2:]:
            send_a[n].wait_recv()
        for owner in range(RING * CORES):
            mm_a([(ym, 1), (yp, 0)], owner)
        relayed(*relays[3:5])
        for owner in range(RING):
            mm_t([(xm, 1), (xp, 0)], owner)
        phase("ag_far")
        take_t(zip(fwd_t), zip(relays[5:]))
        for copy in fwd_a:
            copy.wait_recv()
        phase("mm_far")

        loaded(loads_a[3])
        pairs = []
        far_y = [(yf, 0), (yf, 1)]
        out_t = ring_scatter(RS_T, lambda i: p_t.at[i], r_t, yp, ym, yf, lambda i: dev(i, x, k))
        out_a = ring_scatter(RS_A, lambda i: p_a.at[i * CORES + k], r_a, xp, xm, xf, lambda i: dev(y, i, k))

        def pair(n, i, rows):
            pairs.append(push(PAIR + n, p_a.at[i * CORES + other, rows], d_a.at[i, rows], partner))
            pairs[n].start()

        def add_pair(n, i, rows):
            pairs[n].wait_recv()
            p_a[i * CORES + k, rows] = p_a[i * CORES + k, rows] + d_a[i, rows]

        every, half_rows = pl.ds(0, sub), [pl.ds(h * hsub, hsub) for h in range(2)]
        far_x = [(xf, 0), (xf, 1)]
        mm_a(far_y, xf * CORES + other)
        for h in range(2):
            pair(h, xf, half_rows[h])
        relayed(*relays[5:])
        loaded(loads_t[3])
        mm_t(far_x, yf)
        out_t[0].start()
        out_t[1].start()
        mm_a(far_y, xf * CORES + k)
        for h in range(2):
            add_pair(h, xf, half_rows[h])
            out_a[h].start()
        for n, i in enumerate((xp, xm, x)):
            mm_a(far_y, i * CORES + other)
        for n, i in enumerate((xp, xm, x)):
            pair(2 + n, i, every)
        mm_t(far_x, yp)
        mm_t(far_x, ym)
        out_t[2].start()
        out_t[3].start()
        for i in (xp, xm, x):
            mm_a(far_y, i * CORES + k)
        add_pair(2, xp, every)
        add_pair(3, xm, every)
        out_a[2].start()
        out_a[3].start()
        mm_t(far_x, y)
        add_pair(4, x, every)
        phase("rs_mid")

        ht = width // 2
        out_t[0].wait_recv()
        p_t[yp, 0:ht] = p_t[yp, 0:ht] + r_t[0]
        out_t[4].start()
        out_t[1].wait_recv()
        p_t[ym, ht:width] = p_t[ym, ht:width] + r_t[1]
        out_t[5].start()
        out_a[0].wait_recv()
        kp, km, kk = xp * CORES + k, xm * CORES + k, x * CORES + k
        p_a[kp, 0:hsub] = p_a[kp, 0:hsub] + r_a[0]
        out_a[4].start()
        out_a[1].wait_recv()
        p_a[km, hsub:sub] = p_a[km, hsub:sub] + r_a[1]
        out_a[5].start()
        phase("rs_end")

        @pl.when(p == SWEEPS)
        def _():
            end_moves(*step_two)
            for q in range(2):
                share_linv(q).wait()
            for op in range(2):
                y_one[op] = dot_f32(x_move[op], linv[0, op], NT)
                x_move[op] = dot_f32(y_one[op], linv[1, op], NT)
            out_right.start()
            y_one[0] = dot_f32(ycur[0], linv[0, 0], NT)
            x_via[0] = dot_f32(y_one[0], linv[1, 0], NT)
            out_left.start()

        for copy in out_t[2:] + out_a[2:]:
            copy.wait_recv()
        phase("rs_sum")
        ycur[t, :, 0:ht] = (p_t[y, 0:ht] + r_t[3] + r_t[4]).T
        ycur[t, :, ht:width] = (p_t[y, ht:width] + r_t[2] + r_t[5]).T
        ycur[a, 0:hsub] = p_a[kk, 0:hsub] + r_a[3] + r_a[4]
        ycur[a, hsub:sub] = p_a[kk, hsub:sub] + r_a[2] + r_a[5]
        phase("rs_drain")
        for copy in fwd_a + pairs + out_t + out_a:
            copy.wait_send()

        @pl.when(drives_t)
        def _():
            for copy in [copy for pieces in send_t for copy in pieces] + fwd_t + relays[1:]:
                copy.wait_send()

            @pl.when(p > 0)
            def _():
                relays[0].wait_send()

        @pl.when(jnp.logical_or(p == 0, drives_a))
        def _():
            for copy in send_a:
                copy.wait_send()

        @pl.when(jnp.logical_and(p > 0, drives_a))
        def _():
            for copy in send_b + [relay_a]:
                copy.wait_send()

        phase()

    def pair_of(rows):
        return push(GRAM_PAIR, g_loc.at[other, pl.ds(0, rows)], g_pair.at[pl.ds(0, rows)], partner)

    def pair_sum(rows, local, behind=None):
        phase("ar_pair")
        local(other)
        pair = pair_of(rows)
        pair.start()
        local(k)
        pair.wait_recv()
        if behind is not None:
            behind.start()
        g_sum[0:rows] = g_loc[k, 0:rows] + g_pair[0:rows]
        phase()

    def all_reduce(rows, meanwhile=None, both=False):
        piece = rows // nchips

        def chunk(ref, q):
            return ref.at[pl.ds(pl.multiple_of(q * piece, GROUP), piece)]

        def count(copies):
            return g_all.at[pl.ds(0, copies * piece)]

        def await_copies(sem, copies):
            pltpu.make_async_copy(count(copies), count(copies), sem).wait()

        phase("ar_rs")
        mine = y * RING + x
        routes = []
        for dy, dx in OFFSETS:
            to_y, to_x = (y, yp, yf, ym)[dy], (x, xp, xf, xm)[dx]
            routes.append((dy * RING + dx, to_y * RING + to_x, to_y, to_x))
        owner = CORES - 1

        def spread(o, q, to_y, to_x):
            pltpu.make_async_remote_copy(
                src_ref=chunk(g_sum, q), dst_ref=g_in.at[k, pl.ds(o * piece, piece)], send_sem=send.at[GRAM_RS],
                recv_sem=recv.at[GRAM_RS + k], device_id=dev(to_y, to_x, owner), device_id_type=pl.DeviceIdType.MESH,
            ).start()

        for route in routes:
            spread(*route)
        if meanwhile is not None:
            meanwhile()

        @pl.when(k == 0)
        def _():
            spread(0, mine, y, x)
            await_copies(send.at[GRAM_RS], nchips)
            phase("ar_ag")
            await_copies(recv.at[GRAM_AG], nchips)
            if both:
                await_copies(recv.at[SWAP_H], nchips)
            phase("ar_drain")

        @pl.when(k == 1)
        def _():
            def hand_out(i, src, dst, sem, to_y, to_x, core):
                pltpu.make_async_remote_copy(
                    src_ref=src, dst_ref=chunk(dst, mine), send_sem=send.at[i], recv_sem=recv.at[sem],
                    device_id=dev(to_y, to_x, core), device_id_type=pl.DeviceIdType.MESH,
                ).start()

            left, right = g_red.at[pl.ds(0, piece)], chunk(g_all, mine)
            await_copies(recv.at[GRAM_RS], nchips)
            total = g_in[0, 0:piece]
            for o in range(1, nchips):
                total = total + g_in[0, o * piece : (o + 1) * piece]
            g_red[0:piece] = total / total_rows
            for _, _, to_y, to_x in routes:
                hand_out(GRAM_AG + 1, left, g_all, GRAM_AG, to_y, to_x, 0)
            hand_out(GRAM_AG + 1, left, g_all, GRAM_AG, y, x, 0)
            phase("ar_ag")
            await_copies(recv.at[GRAM_RS + 1], nchips - 1)
            total = chunk(g_sum, mine)[...]
            for o in range(1, nchips):
                total = total + g_in[1, o * piece : (o + 1) * piece]
            chunk(g_all, mine)[...] = total / total_rows
            for _, _, to_y, to_x in routes:
                hand_out(GRAM_AG, right, g_all, GRAM_AG, to_y, to_x, 1)
            if both:
                for _, _, to_y, to_x in routes:
                    hand_out(SWAP_H, left, h_all, SWAP_H, to_y, to_x, 1)
                    hand_out(SWAP_H + 1, right, h_all, SWAP_H, to_y, to_x, 0)
                hand_out(SWAP_H + 1, right, h_all, SWAP_H, y, x, 0)
                chunk(h_all, mine)[...] = left[...]
            await_copies(recv.at[GRAM_AG], nchips - 1)
            phase("ar_drain")
            await_copies(send.at[GRAM_RS], nchips - 1)
            await_copies(send.at[GRAM_AG], nchips - 1)
            await_copies(send.at[GRAM_AG + 1], nchips)
            if both:
                await_copies(recv.at[SWAP_H], nchips - 1)
                await_copies(send.at[SWAP_H], nchips - 1)
                await_copies(send.at[SWAP_H + 1], nchips)

        phase()

    corners = ((0, 0), (0, 1), (1, 1), (1, 0))

    def put_gram(into, full, count):
        for n, (i, j) in enumerate(corners[:count]):
            into[n * tile : (n + 1) * tile] = full[i * tile : (i + 1) * tile, j * tile : (j + 1) * tile]

    def half_gram(op):
        half = ycur[op].astype(BF16)
        put_gram(g_loc.at[op], lax.dot_general(half, half, TN, preferred_element_type=F32), 3)

    def normalize(p, q):
        @pl.when(q == 0)
        def _():
            pair_sum(3 * tile, half_gram, swap_y)
            phase()

        @pl.when(q == 1)
        def _():
            phase("gram2")
            put_gram(g_sum, gram_f32(y_one[0]) + gram_f32(y_one[1]), 3)
            phase()

        def clear():
            set_identity(work)
            linv[q, k, 0:tile, tile:width] = jnp.zeros((tile, tile), F32)

        all_reduce(3 * tile, clear)

        @pl.when(q == 0)
        def _():
            pair_of(3 * tile).wait_send()

        last = p == SWEEPS - 1

        @pl.when(jnp.logical_and(last, q == 0))
        def _():
            start_moves(*step_one)

        @pl.when(jnp.logical_and(last, q == 1))
        def _():
            end_moves(*step_one)
            start_moves(*step_two)

        phase("chol")

        def store(first, t, value):
            linv[q, k, pl.ds(first, GROUP), t * tile : (t + 1) * tile] = value

        inverse_factor(g_all, work, store)
        phase("mul")

        @pl.when(last)
        def _():
            share_linv(q).start()

        @pl.when(q == 0)
        def _():
            y_one[0] = dot_f32(ycur[k], linv[0, k], NT)
            swap_y.wait()
            y_one[1] = dot_f32(y_in[...], linv[0, k], NT)

        phase()

    def launch(p):
        t = lax.rem(p, 2)

        def new_x(i):
            d_a[i] = dot_f32(y_one[i], linv[1, k], NT)
            return [d_a[i, h * hsub : (h + 1) * hsub] for h in range(2)]

        phase("launch")

        @pl.when(k == t)
        def _():
            sends, _, relays = gather_t()
            for i, core in enumerate((k, other)):
                for h, rows in enumerate(new_x(i)):
                    ag_t[x, h, core] = rows.T.astype(BF16)
                for n in ORDER[:2]:
                    sends[n][i].start()
            for n in ORDER[2:]:
                for copy in sends[n]:
                    copy.start()
            relays[0].start()

        @pl.when(k != t)
        def _():
            sends, _, for_other, relay_a = gather_a()
            for h, rows in enumerate(new_x(0)):
                ag_a[y, h] = rows.astype(BF16)
            for n in ORDER:
                sends[n].start()
            for h, rows in enumerate(new_x(1)):
                x_half[0, h] = rows.astype(BF16)
            for n in ORDER:
                for_other[n].start()
            relay_a.start()

        phase()

    def sweep(p, carry):
        apply(p)

        @pl.when(p < SWEEPS)
        def _():
            def one(q, carry):
                normalize(p, q)
                return carry

            lax.fori_loop(0, 2, one, 0)
            launch(p + 1)

        return carry

    lax.fori_loop(0, SWEEPS + 1, sweep, 0)

    def rayleigh(op):
        put_gram(g_loc.at[op], dot_f32(x_move[op], ycur[op], TN), 4)

    pair_sum(4 * tile, rayleigh)
    all_reduce(4 * tile, both=True)
    pair_of(4 * tile).wait_send()
    phase("h_swap")
    for n, (i, j) in enumerate(corners):
        rows, at = slice(n * tile, (n + 1) * tile), (slice(i * tile, (i + 1) * tile), slice(j * tile, (j + 1) * tile))
        for op in range(2):
            h_out[(op, *at)] = jnp.where(k == op, g_all[rows], h_all[rows])
    out_left.wait()
    out_right.wait()
    phase()


def hand_over(x_ref, h_ref, left_x, left_h, right_x, right_h):
    left_x[...] = x_ref[0]
    left_h[...] = h_ref[0]
    right_x[...] = x_ref[1]
    right_h[...] = h_ref[1]


def solution(mesh):
    nrow, ncol = mesh.shape["row"], mesh.shape["col"]
    assert nrow == RING and ncol == RING * CORES

    def local_program(left_op, left_start, right_op, right_start):
        rows, cols = left_op.shape
        sub, width = left_start.shape
        tile = width // 2
        vmem = pltpu.VMEM
        dma = pltpu.SemaphoreType.DMA
        basis, ray = jax.ShapeDtypeStruct((sub, width), F32), jax.ShapeDtypeStruct((width, width), F32)
        both_x, both_h = pl.pallas_call(
            functools.partial(kernel, (nrow, ncol, rows * nrow)),
            out_shape=[jax.ShapeDtypeStruct((2, sub, width), F32), jax.ShapeDtypeStruct((2, width, width), F32)],
            in_specs=[pl.BlockSpec(memory_space=pl.ANY)] * 4,
            out_specs=[pl.BlockSpec(memory_space=pl.ANY), pl.BlockSpec(memory_space=vmem)],
            scratch_shapes=[
                vmem((2, rows, cols), BF16),
                vmem((2, sub, width), F32),
                vmem((2, sub, width), F32),
                vmem((RING, 2, CORES, width, sub // 2), BF16),
                vmem((nrow, 2, sub // 2, width), BF16),
                vmem((nrow, width, sub), F32),
                vmem((ncol, sub, width), F32),
                vmem((RING, sub, width), F32),
                vmem((6, width // 2, sub), F32),
                vmem((6, sub // 2, width), F32),
                vmem((2, 2, sub // 2, width), BF16),
                vmem((2, sub, width), F32),
                vmem((2, sub, width), F32),
                vmem((sub, width), F32),
                vmem((2, 4 * tile, tile), F32),
                vmem((4 * tile, tile), F32),
                vmem((4 * tile, tile), F32),
                vmem((2, 4 * tile, tile), F32),
                vmem((4 * tile // (RING * RING), tile), F32),
                vmem((4 * tile, tile), F32),
                vmem((4 * tile, tile), F32),
                vmem((width, 2 * width), F32),
                vmem((2, 2, width, width), F32),
                dma((KINDS.stop,)),
                dma((KINDS.stop,)),
                dma((10,)),
            ],
            compiler_params=pltpu.CompilerParams(collective_id=0, has_side_effects=True, vmem_limit_bytes=VMEM_BYTES),
            name="subspace",
        )(left_op, left_start, right_op, right_start)
        whole = pl.BlockSpec(memory_space=vmem)
        return pl.pallas_call(
            hand_over, out_shape=[basis, ray, basis, ray], in_specs=[whole] * 2, out_specs=[whole] * 4, name="hand_over"
        )(both_x, both_h)

    op_spec = P(("batch", "row"), "col")
    vec_spec = P(("batch", "row", "col"), None)
    small_spec = P("batch", None)
    return jax.shard_map(
        local_program,
        mesh=mesh,
        in_specs=(op_spec, vec_spec, op_spec, vec_spec),
        out_specs=(vec_spec, small_spec, vec_spec, small_spec),
        check_vma=False,
    )
```

```python
import functools

import jax
import jax.numpy as jnp
from jax import lax
from jax.experimental import pallas as pl
from jax.experimental.pallas import tpu as pltpu
from jax.sharding import PartitionSpec as P

SWEEPS = 4
CORES = 2
RING = 4
PIVOTS = 32
STEP = 12
LEFT_PARTS, RIGHT_PARTS = (2, 0, 1, 1, 0, 0), (0, 2, 1, 0, 1, 0)
GROUP = 8
VMEM_BYTES = 67043328
F32, BF16 = jnp.float32, jnp.bfloat16
TN = (((0,), (0,)), ((), ()))
NT = (((1,), (1,)), ((), ()))

SLOTS = 8
KINDS = range(0, 16 * SLOTS, SLOTS)
AG_T, AG_A, AG_B, RELAY, RELAY_A, RS_T, RS_A, PAIR, GRAM_PAIR, GRAM_RS, GRAM_AG, LINV, MOVE, START, SWAP_Y, SWAP_H = KINDS
ORDER = (0, 2, 1, 3)
OFFSETS = sorted(
    ((dy, dx) for dy in range(RING) for dx in range(RING) if dy or dx),
    key=lambda o: -min(o[0], RING - o[0]) - min(o[1], RING - o[1]),
)


def split3(v):
    high = v.astype(BF16)
    rest = v - high.astype(F32)
    mid = rest.astype(BF16)
    return high, mid, (rest - mid.astype(F32)).astype(BF16)


def halves_dot(lhs, rhs, dims):
    axis = 1 - dims[0][0][0]
    size = lhs.shape[axis] // 2
    parts = [lax.slice_in_dim(lhs, i * size, (i + 1) * size, axis=axis) for i in range(2)]
    return jnp.concatenate([lax.dot_general(part, rhs, dims, preferred_element_type=F32) for part in parts], axis=0)


def dot_f32(lhs, rhs, dims):
    left, right = split3(lhs), split3(rhs)
    (lk,), (rk,) = dims[0]
    lhs = jnp.concatenate([left[i] for i in LEFT_PARTS], axis=lk)
    rhs = jnp.concatenate([right[i] for i in RIGHT_PARTS], axis=rk)
    return halves_dot(lhs, rhs, dims)


def gram_f32(v):
    high, mid, low = split3(v)
    mixed = halves_dot(jnp.concatenate([high, high], axis=0), jnp.concatenate([low, mid], axis=0), TN)
    return (halves_dot(mid, mid, TN) + (mixed + mixed.T)) + halves_dot(high, high, TN)


class Phases:
    def __init__(self):
        self.scope = None

    def __call__(self, name=None):
        if self.scope is not None:
            self.scope.__exit__(None, None, None)
        self.scope = None
        if name is not None:
            self.scope = jax.named_scope(name)
            self.scope.__enter__()


def rows_of(ref, part, parts=2):
    size = ref.shape[0] // parts
    return ref.at[pl.ds(part * size, size)]


def set_identity(work):
    width = work.shape[0]
    at_row = lax.broadcasted_iota(jnp.int32, (width, width), 0)
    at_col = lax.broadcasted_iota(jnp.int32, (width, width), 1)
    work[:, width : 2 * width] = jnp.where(at_row == at_col, 1.0, 0.0).astype(F32)


def inverse_factor(gram, work, store):
    tile = gram.shape[1]
    width = 2 * tile
    work[0:tile, 0:tile] = gram[0:tile]
    work[0:tile, tile:width] = gram[tile : 2 * tile]
    work[tile:width, tile:width] = gram[2 * tile : 3 * tile]
    sub = lax.broadcasted_iota(jnp.int32, (GROUP, tile), 0)
    groups = PIVOTS // GROUP
    full = (GROUP, tile)

    def lane(row):
        return jnp.broadcast_to(row, full)

    for first in range(0, width, PIVOTS):
        near = first // tile
        gram_tiles = list(range(near, 2))
        tiles = gram_tiles + [2 + i for i in range(near + 1)]
        data = {
            t: [work[pl.ds(first + GROUP * g, GROUP), t * tile : (t + 1) * tile] for g in range(groups)] for t in tiles
        }
        pivots = [jnp.ones(full, F32) for _ in range(groups)]
        for start, end in ((0, STEP), (STEP, PIVOTS)):
            at = first - near * tile + start
            cols = {
                j: {
                    g: jnp.broadcast_to(data[near][g][:, at + j - start : at + j - start + 1], full)
                    for g in range(j // GROUP, groups)
                }
                for j in range(start, end)
            }
            for j in range(start, end):
                gj, rj = divmod(j, GROUP)
                col = cols[j]
                pivot = lane(col[gj][rj : rj + 1])
                inv = 1.0 / pivot
                pivots[gj] = jnp.where(sub == rj, pivot, pivots[gj])
                for nxt in range(j + 1, end):
                    gn, rn = divmod(nxt, GROUP)
                    entry = lane(col[gn][rn : rn + 1])
                    if nxt == j + 1:
                        for g in range(gn, groups):
                            cols[nxt][g] = cols[nxt][g] - (col[g] * entry) * inv
                    else:
                        scaled = entry * inv
                        for g in range(gn, groups):
                            cols[nxt][g] = cols[nxt][g] - col[g] * scaled
                for g in range(gj, groups):
                    factor = col[g] * inv
                    if g == gj:
                        if rj == GROUP - 1:
                            continue
                        factor = jnp.where(sub > rj, factor, 0.0)
                    for t in tiles:
                        data[t][g] = data[t][g] - factor * lane(data[t][gj][rj : rj + 1])
        scale = [lax.rsqrt(p) for p in pivots]
        for t in tiles:
            data[t] = [d * s for d, s in zip(data[t], scale, strict=True)]
        for t in tiles:
            if t >= 2:
                for g in range(groups):
                    store(first + GROUP * g, t - 2, data[t][g])
        nxt = first + PIVOTS
        if nxt == width:
            break
        parts = {t: split3(jnp.concatenate(data[t], axis=0)) for t in tiles}
        below = [t for t in gram_tiles if (t + 1) * tile > nxt]
        low = below[0] * tile
        lhs = jnp.concatenate([jnp.concatenate([parts[t][i] for i in LEFT_PARTS], axis=0) for t in below], axis=1)
        right_tiles = below + [t for t in tiles if t >= 2]
        rhs = jnp.concatenate([jnp.concatenate([parts[t][i] for i in RIGHT_PARTS], axis=0) for t in right_tiles], axis=1)
        upd = lax.dot_general(lhs, rhs, TN, preferred_element_type=F32)
        for n, t in enumerate(right_tiles):
            where = pl.ds(nxt, width - nxt), slice(t * tile, (t + 1) * tile)
            work[where] = work[where] - upd[nxt - low :, n * tile : (n + 1) * tile]


def kernel(
    sizes, left_op, left_start, right_op, right_start, x_out, h_out,
    ops, ycur, y_one, ag_t, ag_a, p_t, p_a, d_a, r_t, r_a, x_half, x_via, x_move, y_in, g_loc, g_pair, g_sum, g_in, g_red, g_all, h_all, work, linv,
    send, recv, load_sem,
):
    nrow, ncol, total_rows = sizes
    sub, width = ycur.shape[1:]
    tile, hsub = width // 2, sub // 2
    nchips = RING * RING
    y = lax.axis_index("row")
    c = lax.axis_index("col")
    x, k = lax.div(c, CORES), lax.rem(c, CORES)
    other = 1 - k
    xp, xm, xf = (lax.rem(x + d, RING) for d in (1, 3, 2))
    yp, ym, yf = (lax.rem(y + d, RING) for d in (1, 3, 2))

    def dev(row, chip, core):
        return {"row": row, "col": chip * CORES + core}

    partner = dev(y, x, other)

    def push(i, src, dst, to):
        return pltpu.make_async_remote_copy(
            src_ref=src, dst_ref=dst, send_sem=send.at[i], recv_sem=recv.at[i], device_id=to, device_id_type=pl.DeviceIdType.MESH
        )

    def spot(i):
        return lax.rem(i + RING - x, RING)

    def run(index, size):
        return pl.ds(pl.multiple_of(index * size, size), size)

    phase = Phases()
    phase("boot")
    starts = [
        pltpu.make_async_copy(left_start, ycur.at[0], load_sem.at[8]),
        pltpu.make_async_copy(right_start, ycur.at[1], load_sem.at[9]),
    ]
    loads_t, loads_a = [], []
    for n, (xi, yi) in enumerate(((x, y), (xm, ym), (xp, yp), (xf, yf))):
        take = run(xi, CORES * sub)
        loads_t.append(pltpu.make_async_copy(left_op.at[take], ops.at[0, take], load_sem.at[2 * n]))
        take = run(spot(yi), sub)
        loads_a.append(pltpu.make_async_copy(right_op.at[:, take], ops.at[1, :, take], load_sem.at[2 * n + 1]))
    for copy in starts + loads_t + loads_a:
        copy.start()

    barrier = pltpu.get_barrier_semaphore()
    here = y * ncol + c
    for o in range(1, nrow * ncol):
        there = lax.rem(here + o, nrow * ncol)
        pl.semaphore_signal(
            barrier, inc=1, device_id={"row": lax.div(there, ncol), "col": lax.rem(there, ncol)}, device_id_type=pl.DeviceIdType.MESH
        )

    shift = CORES * lax.rem(x, 2) + k
    behind = spot(y)
    up, down = lax.rem(y + shift, RING), lax.rem(y + RING - shift, RING)

    def move(i, src, dst, row, chip, core):
        stays = jnp.logical_and(row == y, jnp.logical_and(chip == x, core == k))
        return push(i, src, dst, dev(row, chip, core)), stays, src, dst

    def start_moves(*moves):
        for copy, stays, src, dst in moves:

            @pl.when(stays)
            def _():
                dst[...] = src[...]

            @pl.when(jnp.logical_not(stays))
            def _():
                copy.start()

    def end_moves(*moves):
        for copy, stays, _, _ in moves:

            @pl.when(jnp.logical_not(stays))
            def _():
                copy.wait()

    for copy in starts:
        copy.wait()
    for h in range(2):
        ag_t[x, h, k] = ycur[0, h * hsub : (h + 1) * hsub].T.astype(BF16)
    for h in range(2):
        x_half[0, h] = ycur[1, h * hsub : (h + 1) * hsub].astype(BF16)
    pl.semaphore_wait(barrier, nrow * ncol - 1)
    first_one = [move(MOVE + h, x_half.at[0, h], x_half.at[1, h], up, x, k) for h in range(2)]
    first_two = [move(MOVE + 2 + h, x_half.at[1, h], ag_a.at[y, h], y, down, lax.div(x, 2)) for h in range(2)]
    start_moves(*first_one)
    first_swap = [push(START + h, ag_t.at[x, h, k], ag_t.at[x, h, k], partner) for h in range(2)]
    for copy in first_swap:
        copy.start()
    phase()

    def piece_t(chip, h):
        return ag_t.at[chip, h]

    def gather_t():
        to_p, to_m = dev(y, xp, k), dev(y, xm, k)
        sends = [
            push(AG_T + n, piece_t(x, h), piece_t(x, h), to) for n, (h, to) in enumerate(((0, to_p), (1, to_p), (1, to_m), (0, to_m)))
        ]
        onward = [
            push(AG_T + 4, piece_t(xm, 0), piece_t(xm, 0), to_p),
            push(AG_T + 5, piece_t(xp, 1), piece_t(xp, 1), to_m),
        ]
        relays = [push(RELAY, ag_t.at[x], ag_t.at[x], partner)] + [
            push(RELAY + 1 + n, piece_t(i, h), piece_t(i, h), partner)
            for n, (i, h) in enumerate(((xm, 0), (xp, 1), (xm, 1), (xp, 0), (xf, 0), (xf, 1)))
        ]
        return sends, onward, relays

    def gather_a():
        routes = ((0, yp), (1, yp), (1, ym), (0, ym))
        sends = [push(AG_A + n, ag_a.at[y, h], ag_a.at[y, h], dev(i, x, k)) for n, (h, i) in enumerate(routes)]
        onward = [
            push(AG_A + 4, ag_a.at[ym, 0], ag_a.at[ym, 0], dev(yp, x, k)),
            push(AG_A + 5, ag_a.at[yp, 1], ag_a.at[yp, 1], dev(ym, x, k)),
        ]
        for_other = [
            pltpu.make_async_remote_copy(
                src_ref=x_half.at[0, h], dst_ref=ag_a.at[y, h], send_sem=send.at[AG_B + n], recv_sem=recv.at[AG_A + n],
                device_id=dev(i, x, other), device_id_type=pl.DeviceIdType.MESH,
            )
            for n, (h, i) in enumerate(routes)
        ]
        return sends, onward, for_other, push(RELAY_A, x_half.at[0], ag_a.at[y], partner)

    def ring_scatter(base, part, got, plus, minus, far, to):
        def half(i, h):
            return rows_of(part(i), h)

        return [
            push(base + 0, half(far, 0), got.at[0], to(plus)),
            push(base + 1, half(far, 1), got.at[1], to(minus)),
            push(base + 2, half(plus, 1), got.at[2], to(plus)),
            push(base + 3, half(minus, 0), got.at[3], to(minus)),
            push(base + 4, half(plus, 0), got.at[4], to(plus)),
            push(base + 5, half(minus, 1), got.at[5], to(minus)),
        ]

    step_one = [
        move(MOVE, ycur.at[0], x_via.at[0], up, x, k),
        move(MOVE + 1, ycur.at[1], x_via.at[1], y, CORES * k + lax.div(behind, 2), lax.rem(behind, 2)),
    ]
    step_two = [
        move(MOVE + 2, x_via.at[0], x_move.at[0], y, down, lax.div(x, 2)),
        move(MOVE + 3, x_via.at[1], x_move.at[1], down, x, k),
    ]
    out_left = pltpu.make_async_copy(x_via.at[0], x_out.at[0], load_sem.at[0])
    out_right = pltpu.make_async_copy(x_move.at[1], x_out.at[1], load_sem.at[1])

    def share_linv(q):
        return push(LINV + q, linv.at[q, k], linv.at[q, k], partner)

    swap_y = push(SWAP_Y, ycur.at[other], y_in, partner)

    def apply(p):
        t = lax.rem(p, 2)
        a = 1 - t

        def mm_t(pieces, owner, first=False, cuts=1):
            size = sub // cuts
            for n in range(cuts):
                acc, lanes = None, slice(n * size, (n + 1) * size)
                for chip, h in pieces:
                    for core in range(CORES):
                        rows = run((chip * CORES + core) * 2 + h, hsub)
                        one = jnp.dot(ag_t[chip, h, core], ops[t, rows, run(spot(owner) * cuts + n, size)], preferred_element_type=F32)
                        acc = one if acc is None else acc + one
                p_t[owner, :, lanes] = acc if first else p_t[owner, :, lanes] + acc

        def mm_a(pieces, owner, first=False, cuts=1):
            size = sub // cuts
            for n in range(cuts):
                acc, rows = None, slice(n * size, (n + 1) * size)
                for i, h in pieces:
                    one = jnp.dot(ops[a, run(owner * cuts + n, size), run(spot(i) * 2 + h, hsub)], ag_a[i, h], preferred_element_type=F32)
                    acc = one if acc is None else acc + one
                p_a[owner, rows] = acc if first else p_a[owner, rows] + acc

        def loaded(copy):
            @pl.when(p == 0)
            def _():
                copy.wait()

        send_t, fwd_t, relays = gather_t()
        send_a, fwd_a, send_b, relay_a = gather_a()
        drives_t, drives_a = k == t, k == a
        own_y = [(y, 0), (y, 1)]
        phase("ag_own")

        @pl.when(p == 0)
        def _():
            for h in range(2):
                end_moves(first_one[h])
                start_moves(first_two[h])
            for copy in first_swap:
                copy.wait()

            @pl.when(drives_t)
            def _():
                for n in ORDER:
                    send_t[n].start()

        @pl.when(p > 0)
        def _():
            @pl.when(jnp.logical_not(drives_a))
            def _():
                relay_a.wait_recv()

            for owner in range(RING * CORES):
                mm_a(own_y, owner, True)

            @pl.when(jnp.logical_not(drives_t))
            def _():
                relays[0].wait_recv()

        loaded(loads_t[0])
        for owner in range(RING):
            mm_t([(x, 0), (x, 1)], owner, True)

        @pl.when(p == 0)
        def _():
            end_moves(first_two[0])
            send_a[0].start()
            send_a[3].start()
            end_moves(first_two[1])
            send_a[2].start()
            send_a[1].start()
            loads_a[0].wait()
            for owner in range(RING * CORES):
                mm_a(own_y, owner, True)

        def take_t(arrived, then):
            @pl.when(drives_t)
            def _():
                for copy, follow in zip(arrived, then):
                    copy.wait_recv()
                    for nxt in follow:
                        nxt.start()

        def relayed(*copies):
            @pl.when(jnp.logical_not(drives_t))
            def _():
                for copy in copies:
                    copy.wait_recv()

        phase("ag_wait1")
        take_t([send_t[n] for n in ORDER[:2]], zip(fwd_t, relays[1:3]))
        for n, copy in zip(ORDER, fwd_a):
            send_a[n].wait_recv()
            copy.start()
        phase("mm_near1")
        loaded(loads_a[1])
        loaded(loads_a[2])
        for owner in range(RING * CORES):
            mm_a([(ym, 0), (yp, 1)], owner)
        relayed(*relays[1:3])
        loaded(loads_t[1])
        loaded(loads_t[2])
        for owner in range(RING):
            mm_t([(xm, 0), (xp, 1)], owner)
        phase("mm_near2")
        take_t([send_t[n] for n in ORDER[2:]], zip(relays[3:5]))
        for n in ORDER[2:]:
            send_a[n].wait_recv()
        for owner in range(RING * CORES):
            mm_a([(ym, 1), (yp, 0)], owner)
        relayed(*relays[3:5])
        for owner in range(RING):
            mm_t([(xm, 1), (xp, 0)], owner)
        phase("ag_far")
        take_t(fwd_t, zip(relays[5:]))
        for copy in fwd_a:
            copy.wait_recv()
        phase("mm_far")

        loaded(loads_a[3])
        pairs = []
        far_y = [(yf, 0), (yf, 1)]
        out_t = ring_scatter(RS_T, lambda i: p_t.at[i], r_t, yp, ym, yf, lambda i: dev(i, x, k))
        out_a = ring_scatter(RS_A, lambda i: p_a.at[i * CORES + k], r_a, xp, xm, xf, lambda i: dev(y, i, k))

        def pair(n, i, rows):
            pairs.append(push(PAIR + n, p_a.at[i * CORES + other, rows], d_a.at[i, rows], partner))
            pairs[n].start()

        def add_pair(n, i, rows):
            pairs[n].wait_recv()
            p_a[i * CORES + k, rows] = p_a[i * CORES + k, rows] + d_a[i, rows]

        every, half_rows = pl.ds(0, sub), [pl.ds(h * hsub, hsub) for h in range(2)]
        far_x = [(xf, 0), (xf, 1)]
        mm_a(far_y, xf * CORES + other, cuts=2)
        for h in range(2):
            pair(h, xf, half_rows[h])
        relayed(*relays[5:])
        loaded(loads_t[3])
        mm_t(far_x, yf, cuts=2)
        out_t[0].start()
        out_t[1].start()
        mm_a(far_y, xf * CORES + k, cuts=2)
        for h in range(2):
            add_pair(h, xf, half_rows[h])
            out_a[h].start()
        for n, i in enumerate((xp, xm, x)):
            mm_a(far_y, i * CORES + other)
        for n, i in enumerate((xp, xm, x)):
            pair(2 + n, i, every)
        mm_t(far_x, yp)
        mm_t(far_x, ym)
        out_t[2].start()
        out_t[3].start()
        for i in (xp, xm, x):
            mm_a(far_y, i * CORES + k)
        add_pair(2, xp, every)
        add_pair(3, xm, every)
        out_a[2].start()
        out_a[3].start()
        mm_t(far_x, y)
        phase("rs_mid")

        ht = width // 2
        out_t[0].wait_recv()
        p_t[yp, 0:ht] = p_t[yp, 0:ht] + r_t[0]
        out_t[4].start()
        out_t[1].wait_recv()
        p_t[ym, ht:width] = p_t[ym, ht:width] + r_t[1]
        out_t[5].start()
        out_a[0].wait_recv()
        kp, km, kk = xp * CORES + k, xm * CORES + k, x * CORES + k
        p_a[kp, 0:hsub] = p_a[kp, 0:hsub] + r_a[0]
        out_a[4].start()
        out_a[1].wait_recv()
        p_a[km, hsub:sub] = p_a[km, hsub:sub] + r_a[1]
        out_a[5].start()
        phase("rs_end")

        @pl.when(p == SWEEPS)
        def _():
            end_moves(*step_two)
            for q in range(2):
                share_linv(q).wait()
            for op in range(2):
                y_one[op] = dot_f32(x_move[op], linv[0, op], NT)
                x_move[op] = dot_f32(y_one[op], linv[1, op], NT)
            out_right.start()
            y_one[0] = dot_f32(ycur[0], linv[0, 0], NT)
            x_via[0] = dot_f32(y_one[0], linv[1, 0], NT)
            out_left.start()

        add_pair(4, x, every)
        for copy in out_t[2:] + out_a[2:]:
            copy.wait_recv()
        phase("rs_sum")
        ycur[t, :, 0:ht] = (p_t[y, 0:ht] + r_t[3] + r_t[4]).T
        ycur[t, :, ht:width] = (p_t[y, ht:width] + r_t[2] + r_t[5]).T
        ycur[a, 0:hsub] = p_a[kk, 0:hsub] + r_a[3] + r_a[4]
        ycur[a, hsub:sub] = p_a[kk, hsub:sub] + r_a[2] + r_a[5]
        phase("rs_drain")
        for copy in fwd_a + pairs + out_t + out_a:
            copy.wait_send()

        @pl.when(drives_t)
        def _():
            for copy in send_t + fwd_t + relays[1:]:
                copy.wait_send()

            @pl.when(p > 0)
            def _():
                relays[0].wait_send()

        @pl.when(jnp.logical_or(p == 0, drives_a))
        def _():
            for copy in send_a:
                copy.wait_send()

        @pl.when(jnp.logical_and(p > 0, drives_a))
        def _():
            for copy in send_b + [relay_a]:
                copy.wait_send()

        phase()

    def pair_of(rows):
        return push(GRAM_PAIR, g_loc.at[other, pl.ds(0, rows)], g_pair.at[pl.ds(0, rows)], partner)

    def pair_sum(rows, local, behind=None):
        phase("ar_pair")
        local(other)
        pair = pair_of(rows)
        pair.start()
        local(k)
        pair.wait_recv()
        if behind is not None:
            behind.start()
        g_sum[0:rows] = g_loc[k, 0:rows] + g_pair[0:rows]
        phase()

    def all_reduce(rows, meanwhile=None, sent=None):
        piece = rows // nchips

        def chunk(ref, q):
            return ref.at[pl.ds(pl.multiple_of(q * piece, GROUP), piece)]

        def count(copies):
            return g_all.at[pl.ds(0, copies * piece)]

        def await_copies(sem, copies):
            pltpu.make_async_copy(count(copies), count(copies), sem).wait()

        phase("ar_rs")
        mine = y * RING + x
        routes = []
        for dy, dx in OFFSETS:
            to_y, to_x = (y, yp, yf, ym)[dy], (x, xp, xf, xm)[dx]
            routes.append((dy * RING + dx, to_y * RING + to_x, to_y, to_x))
        owner = CORES - 1

        def spread(o, q, to_y, to_x):
            pltpu.make_async_remote_copy(
                src_ref=chunk(g_sum, q), dst_ref=g_in.at[k, pl.ds(o * piece, piece)], send_sem=send.at[GRAM_RS],
                recv_sem=recv.at[GRAM_RS + k], device_id=dev(to_y, to_x, owner), device_id_type=pl.DeviceIdType.MESH,
            ).start()

        for route in routes:
            spread(*route)
        if meanwhile is not None:
            meanwhile()

        @pl.when(k == 0)
        def _():
            spread(0, mine, y, x)
            if sent is not None:
                sent()
            await_copies(send.at[GRAM_RS], nchips)
            phase("ar_ag")
            await_copies(recv.at[GRAM_AG], nchips)
            phase("ar_drain")

        @pl.when(k == 1)
        def _():
            def hand_out(i, src, q, to_y, to_x, core):
                pltpu.make_async_remote_copy(
                    src_ref=src, dst_ref=chunk(g_all, q), send_sem=send.at[GRAM_AG + i], recv_sem=recv.at[GRAM_AG],
                    device_id=dev(to_y, to_x, core), device_id_type=pl.DeviceIdType.MESH,
                ).start()

            await_copies(recv.at[GRAM_RS], nchips)
            total = g_in[0, 0:piece]
            for o in range(1, nchips):
                total = total + g_in[0, o * piece : (o + 1) * piece]
            g_red[0:piece] = total / total_rows
            for _, _, to_y, to_x in routes:
                hand_out(1, g_red.at[pl.ds(0, piece)], mine, to_y, to_x, 0)
            hand_out(1, g_red.at[pl.ds(0, piece)], mine, y, x, 0)
            phase("ar_ag")
            await_copies(recv.at[GRAM_RS + 1], nchips - 1)
            total = chunk(g_sum, mine)[...]
            for o in range(1, nchips):
                total = total + g_in[1, o * piece : (o + 1) * piece]
            chunk(g_all, mine)[...] = total / total_rows
            for _, _, to_y, to_x in routes:
                hand_out(0, chunk(g_all, mine), mine, to_y, to_x, 1)
            if sent is not None:
                sent()
            await_copies(recv.at[GRAM_AG], nchips - 1)
            phase("ar_drain")
            await_copies(send.at[GRAM_RS], nchips - 1)
            await_copies(send.at[GRAM_AG], nchips - 1)
            await_copies(send.at[GRAM_AG + 1], nchips)

        phase()

    corners = ((0, 0), (0, 1), (1, 1), (1, 0))

    def put_gram(into, full, count):
        for n, (i, j) in enumerate(corners[:count]):
            into[n * tile : (n + 1) * tile] = full[i * tile : (i + 1) * tile, j * tile : (j + 1) * tile]

    def half_gram(op):
        half = ycur[op].astype(BF16)
        put_gram(g_loc.at[op], lax.dot_general(half, half, TN, preferred_element_type=F32), 3)

    def normalize(p, q):
        @pl.when(q == 0)
        def _():
            pair_sum(3 * tile, half_gram, swap_y)
            phase()

        @pl.when(q == 1)
        def _():
            phase("gram2")
            put_gram(g_sum, gram_f32(y_one[0]) + gram_f32(y_one[1]), 3)
            phase()

        last = p == SWEEPS - 1

        def clear():
            set_identity(work)
            linv[q, k, 0:tile, tile:width] = jnp.zeros((tile, tile), F32)

        def move_y():
            @pl.when(jnp.logical_and(last, q == 0))
            def _():
                start_moves(*step_one)

            @pl.when(jnp.logical_and(last, q == 1))
            def _():
                end_moves(*step_one)
                start_moves(*step_two)

        all_reduce(3 * tile, clear, move_y)

        @pl.when(q == 0)
        def _():
            pair_of(3 * tile).wait_send()

        phase("chol")

        def store(first, t, value):
            linv[q, k, pl.ds(first, GROUP), t * tile : (t + 1) * tile] = value

        inverse_factor(g_all, work, store)
        phase("mul")

        @pl.when(last)
        def _():
            share_linv(q).start()

        @pl.when(q == 0)
        def _():
            y_one[0] = dot_f32(ycur[k], linv[0, k], NT)
            swap_y.wait()
            y_one[1] = dot_f32(y_in[...], linv[0, k], NT)

        phase()

    def launch(p):
        t = lax.rem(p, 2)

        def new_x(i):
            d_a[i] = dot_f32(y_one[i], linv[1, k], NT)
            return [d_a[i, h * hsub : (h + 1) * hsub] for h in range(2)]

        phase("launch")

        @pl.when(k == t)
        def _():
            sends, _, relays = gather_t()
            for i, core in enumerate((k, other)):
                for h, rows in enumerate(new_x(i)):
                    ag_t[x, h, core] = rows.T.astype(BF16)
            for n in ORDER:
                sends[n].start()
            relays[0].start()

        @pl.when(k != t)
        def _():
            sends, _, for_other, relay_a = gather_a()
            for h, rows in enumerate(new_x(0)):
                ag_a[y, h] = rows.astype(BF16)
            for n in ORDER:
                sends[n].start()
            for h, rows in enumerate(new_x(1)):
                x_half[0, h] = rows.astype(BF16)
            for n in ORDER:
                for_other[n].start()
            relay_a.start()

        phase()

    def sweep(p, carry):
        apply(p)

        @pl.when(p < SWEEPS)
        def _():
            def one(q, carry):
                normalize(p, q)
                return carry

            lax.fori_loop(0, 2, one, 0)
            launch(p + 1)

        return carry

    lax.fori_loop(0, SWEEPS + 1, sweep, 0)

    def rayleigh(op):
        put_gram(g_loc.at[op], dot_f32(x_move[op], ycur[op], TN), 4)

    pair_sum(4 * tile, rayleigh)
    all_reduce(4 * tile)
    pair_of(4 * tile).wait_send()
    phase("h_swap")
    swap = push(SWAP_H, g_all, h_all, partner)
    swap.start()
    swap.wait()
    for n, (i, j) in enumerate(corners):
        rows, at = slice(n * tile, (n + 1) * tile), (slice(i * tile, (i + 1) * tile), slice(j * tile, (j + 1) * tile))
        for op in range(2):
            h_out[(op, *at)] = jnp.where(k == op, g_all[rows], h_all[rows])
    out_left.wait()
    out_right.wait()
    phase()


def hand_over(x_ref, h_ref, left_x, left_h, right_x, right_h):
    left_x[...] = x_ref[0]
    left_h[...] = h_ref[0]
    right_x[...] = x_ref[1]
    right_h[...] = h_ref[1]


def solution(mesh):
    nrow, ncol = mesh.shape["row"], mesh.shape["col"]
    assert nrow == RING and ncol == RING * CORES

    def local_program(left_op, left_start, right_op, right_start):
        rows, cols = left_op.shape
        sub, width = left_start.shape
        tile = width // 2
        vmem = pltpu.VMEM
        dma = pltpu.SemaphoreType.DMA
        basis, ray = jax.ShapeDtypeStruct((sub, width), F32), jax.ShapeDtypeStruct((width, width), F32)
        both_x, both_h = pl.pallas_call(
            functools.partial(kernel, (nrow, ncol, rows * nrow)),
            out_shape=[jax.ShapeDtypeStruct((2, sub, width), F32), jax.ShapeDtypeStruct((2, width, width), F32)],
            in_specs=[pl.BlockSpec(memory_space=pl.ANY)] * 4,
            out_specs=[pl.BlockSpec(memory_space=pl.ANY), pl.BlockSpec(memory_space=vmem)],
            scratch_shapes=[
                vmem((2, rows, cols), BF16),
                vmem((2, sub, width), F32),
                vmem((2, sub, width), F32),
                vmem((RING, 2, CORES, width, sub // 2), BF16),
                vmem((nrow, 2, sub // 2, width), BF16),
                vmem((nrow, width, sub), F32),
                vmem((ncol, sub, width), F32),
                vmem((RING, sub, width), F32),
                vmem((6, width // 2, sub), F32),
                vmem((6, sub // 2, width), F32),
                vmem((2, 2, sub // 2, width), BF16),
                vmem((2, sub, width), F32),
                vmem((2, sub, width), F32),
                vmem((sub, width), F32),
                vmem((2, 4 * tile, tile), F32),
                vmem((4 * tile, tile), F32),
                vmem((4 * tile, tile), F32),
                vmem((2, 4 * tile, tile), F32),
                vmem((4 * tile // (RING * RING), tile), F32),
                vmem((4 * tile, tile), F32),
                vmem((4 * tile, tile), F32),
                vmem((width, 2 * width), F32),
                vmem((2, 2, width, width), F32),
                dma((KINDS.stop,)),
                dma((KINDS.stop,)),
                dma((10,)),
            ],
            compiler_params=pltpu.CompilerParams(collective_id=0, has_side_effects=True, vmem_limit_bytes=VMEM_BYTES),
            name="subspace",
        )(left_op, left_start, right_op, right_start)
        whole = pl.BlockSpec(memory_space=vmem)
        return pl.pallas_call(
            hand_over, out_shape=[basis, ray, basis, ray], in_specs=[whole] * 2, out_specs=[whole] * 4, name="hand_over"
        )(both_x, both_h)

    op_spec = P(("batch", "row"), "col")
    vec_spec = P(("batch", "row", "col"), None)
    small_spec = P("batch", None)
    return jax.shard_map(
        local_program,
        mesh=mesh,
        in_specs=(op_spec, vec_spec, op_spec, vec_spec),
        out_specs=(vec_spec, small_spec, vec_spec, small_spec),
        check_vma=False,
    )
```

```python
import functools

import jax
import jax.numpy as jnp
from jax import lax
from jax.experimental import pallas as pl
from jax.experimental.pallas import tpu as pltpu
from jax.sharding import PartitionSpec as P

SWEEPS = 4
CORES = 2
RING = 4
PIVOTS = 32
STEP = 12
LEFT_PARTS, RIGHT_PARTS = (2, 0, 1, 1, 0, 0), (0, 2, 1, 0, 1, 0)
GROUP = 8
VMEM_BYTES = 67043328
F32, BF16 = jnp.float32, jnp.bfloat16
TN = (((0,), (0,)), ((), ()))
NT = (((1,), (1,)), ((), ()))

SLOTS = 8
KINDS = range(0, 17 * SLOTS, SLOTS)
AG_T, AG_A, AG_B, RELAY, RELAY_A, RS_T, RS_A, PAIR, GRAM_PAIR, GRAM_RS, GRAM_AG, LINV, MOVE, START, SWAP_Y, SWAP_H, DIAGONAL = KINDS
ORDER = (0, 2, 1, 3)
OFFSETS = sorted(
    ((dy, dx) for dy in range(RING) for dx in range(RING) if dy or dx),
    key=lambda o: -min(o[0], RING - o[0]) - min(o[1], RING - o[1]),
)


def split3(v):
    high = v.astype(BF16)
    rest = v - high.astype(F32)
    mid = rest.astype(BF16)
    return high, mid, (rest - mid.astype(F32)).astype(BF16)


def halves_dot(lhs, rhs, dims):
    axis = 1 - dims[0][0][0]
    size = lhs.shape[axis] // 2
    parts = [lax.slice_in_dim(lhs, i * size, (i + 1) * size, axis=axis) for i in range(2)]
    return jnp.concatenate([lax.dot_general(part, rhs, dims, preferred_element_type=F32) for part in parts], axis=0)


def dot_f32(lhs, rhs, dims):
    left, right = split3(lhs), split3(rhs)
    (lk,), (rk,) = dims[0]
    lhs = jnp.concatenate([left[i] for i in LEFT_PARTS], axis=lk)
    rhs = jnp.concatenate([right[i] for i in RIGHT_PARTS], axis=rk)
    return halves_dot(lhs, rhs, dims)


def gram_f32(v):
    high, mid, low = split3(v)
    mixed = halves_dot(jnp.concatenate([high, high], axis=0), jnp.concatenate([low, mid], axis=0), TN)
    return (halves_dot(mid, mid, TN) + (mixed + mixed.T)) + halves_dot(high, high, TN)


class Phases:
    def __init__(self):
        self.scope = None

    def __call__(self, name=None):
        if self.scope is not None:
            self.scope.__exit__(None, None, None)
        self.scope = None
        if name is not None:
            self.scope = jax.named_scope(name)
            self.scope.__enter__()


def rows_of(ref, part, parts=2):
    size = ref.shape[0] // parts
    return ref.at[pl.ds(part * size, size)]


def set_identity(work):
    width = work.shape[0]
    at_row = lax.broadcasted_iota(jnp.int32, (width, width), 0)
    at_col = lax.broadcasted_iota(jnp.int32, (width, width), 1)
    work[:, width : 2 * width] = jnp.where(at_row == at_col, 1.0, 0.0).astype(F32)


def inverse_factor(gram, diagonal, work, store):
    tile = gram.shape[1]
    width = 2 * tile
    at_row, at_col = (lax.broadcasted_iota(jnp.int32, (tile, tile), i) for i in range(2))
    packed = gram[0:tile]
    turned = packed.T
    work[0:tile, 0:tile] = jnp.where(at_row <= at_col, packed, turned)
    work[0:tile, tile:width] = gram[tile : 2 * tile]
    work[tile:width, tile:width] = jnp.where(at_row == at_col, diagonal, jnp.where(at_row > at_col, packed, turned))
    sub = lax.broadcasted_iota(jnp.int32, (GROUP, tile), 0)
    groups = PIVOTS // GROUP
    full = (GROUP, tile)

    def lane(row):
        return jnp.broadcast_to(row, full)

    for first in range(0, width, PIVOTS):
        near = first // tile
        gram_tiles = list(range(near, 2))
        tiles = gram_tiles + [2 + i for i in range(near + 1)]
        data = {
            t: [work[pl.ds(first + GROUP * g, GROUP), t * tile : (t + 1) * tile] for g in range(groups)] for t in tiles
        }
        pivots = [jnp.ones(full, F32) for _ in range(groups)]
        for start, end in ((0, STEP), (STEP, PIVOTS)):
            at = first - near * tile + start
            cols = {
                j: {
                    g: jnp.broadcast_to(data[near][g][:, at + j - start : at + j - start + 1], full)
                    for g in range(j // GROUP, groups)
                }
                for j in range(start, end)
            }
            for j in range(start, end):
                gj, rj = divmod(j, GROUP)
                col = cols[j]
                pivot = lane(col[gj][rj : rj + 1])
                inv = 1.0 / pivot
                pivots[gj] = jnp.where(sub == rj, pivot, pivots[gj])
                for nxt in range(j + 1, end):
                    gn, rn = divmod(nxt, GROUP)
                    entry = lane(col[gn][rn : rn + 1])
                    if nxt == j + 1:
                        for g in range(gn, groups):
                            cols[nxt][g] = cols[nxt][g] - (col[g] * entry) * inv
                    else:
                        scaled = entry * inv
                        for g in range(gn, groups):
                            cols[nxt][g] = cols[nxt][g] - col[g] * scaled
                for g in range(gj, groups):
                    factor = col[g] * inv
                    if g == gj:
                        if rj == GROUP - 1:
                            continue
                        factor = jnp.where(sub > rj, factor, 0.0)
                    for t in tiles:
                        data[t][g] = data[t][g] - factor * lane(data[t][gj][rj : rj + 1])
        scale = [lax.rsqrt(p) for p in pivots]
        for t in tiles:
            data[t] = [d * s for d, s in zip(data[t], scale, strict=True)]
        for t in tiles:
            if t >= 2:
                for g in range(groups):
                    store(first + GROUP * g, t - 2, data[t][g])
        nxt = first + PIVOTS
        if nxt == width:
            break
        parts = {t: split3(jnp.concatenate(data[t], axis=0)) for t in tiles}
        below = [t for t in gram_tiles if (t + 1) * tile > nxt]
        low = below[0] * tile
        lhs = jnp.concatenate([jnp.concatenate([parts[t][i] for i in LEFT_PARTS], axis=0) for t in below], axis=1)
        right_tiles = below + [t for t in tiles if t >= 2]
        rhs = jnp.concatenate([jnp.concatenate([parts[t][i] for i in RIGHT_PARTS], axis=0) for t in right_tiles], axis=1)
        upd = lax.dot_general(lhs, rhs, TN, preferred_element_type=F32)
        for n, t in enumerate(right_tiles):
            where = pl.ds(nxt, width - nxt), slice(t * tile, (t + 1) * tile)
            work[where] = work[where] - upd[nxt - low :, n * tile : (n + 1) * tile]


def kernel(
    sizes, left_op, left_start, right_op, right_start, x_out, h_out,
    ops, ycur, y_one, ag_t, ag_a, p_t, p_a, d_a, r_t, r_a, x_half, x_via, x_move, y_in, g_loc, g_pair, g_sum, g_in, g_red, g_all, h_all, d_all, work, linv,
    send, recv, load_sem,
):
    nrow, ncol, total_rows = sizes
    sub, width = ycur.shape[1:]
    tile, hsub = width // 2, sub // 2
    nchips = RING * RING
    y = lax.axis_index("row")
    c = lax.axis_index("col")
    x, k = lax.div(c, CORES), lax.rem(c, CORES)
    other = 1 - k
    xp, xm, xf = (lax.rem(x + d, RING) for d in (1, 3, 2))
    yp, ym, yf = (lax.rem(y + d, RING) for d in (1, 3, 2))

    def dev(row, chip, core):
        return {"row": row, "col": chip * CORES + core}

    partner = dev(y, x, other)

    def push(i, src, dst, to):
        return pltpu.make_async_remote_copy(
            src_ref=src, dst_ref=dst, send_sem=send.at[i], recv_sem=recv.at[i], device_id=to, device_id_type=pl.DeviceIdType.MESH
        )

    def spot(i):
        return lax.rem(i + RING - x, RING)

    def run(index, size):
        return pl.ds(pl.multiple_of(index * size, size), size)

    phase = Phases()
    phase("boot")
    barrier = pltpu.get_barrier_semaphore()
    here = y * ncol + c
    for o in range(1, nrow * ncol):
        there = lax.rem(here + o, nrow * ncol)
        pl.semaphore_signal(
            barrier, inc=1, device_id={"row": lax.div(there, ncol), "col": lax.rem(there, ncol)}, device_id_type=pl.DeviceIdType.MESH
        )

    starts = [
        pltpu.make_async_copy(left_start, ycur.at[0], load_sem.at[8]),
        pltpu.make_async_copy(right_start, ycur.at[1], load_sem.at[9]),
    ]
    loads_t, loads_a = [], []
    for n, (xi, yi) in enumerate(((x, y), (xm, ym), (xp, yp), (xf, yf))):
        take = run(xi, CORES * sub)
        loads_t.append(pltpu.make_async_copy(left_op.at[take], ops.at[0, take], load_sem.at[2 * n]))
        take = run(spot(yi), sub)
        loads_a.append(pltpu.make_async_copy(right_op.at[:, take], ops.at[1, :, take], load_sem.at[2 * n + 1]))
    for copy in starts + loads_t + loads_a:
        copy.start()

    shift = CORES * lax.rem(x, 2) + k
    behind = spot(y)
    up, down = lax.rem(y + shift, RING), lax.rem(y + RING - shift, RING)

    def move(i, src, dst, row, chip, core):
        stays = jnp.logical_and(row == y, jnp.logical_and(chip == x, core == k))
        return push(i, src, dst, dev(row, chip, core)), stays, src, dst

    def start_moves(*moves):
        for copy, stays, src, dst in moves:

            @pl.when(stays)
            def _():
                dst[...] = src[...]

            @pl.when(jnp.logical_not(stays))
            def _():
                copy.start()

    def end_moves(*moves):
        for copy, stays, _, _ in moves:

            @pl.when(jnp.logical_not(stays))
            def _():
                copy.wait()

    for copy in starts:
        copy.wait()
    for h in range(2):
        ag_t[x, h, k] = ycur[0, h * hsub : (h + 1) * hsub].T.astype(BF16)
    for h in range(2):
        x_half[0, h] = ycur[1, h * hsub : (h + 1) * hsub].astype(BF16)
    pl.semaphore_wait(barrier, nrow * ncol - 1)
    first_one = [move(MOVE + h, x_half.at[0, h], x_half.at[1, h], up, x, k) for h in range(2)]
    first_two = [move(MOVE + 2 + h, x_half.at[1, h], ag_a.at[y, h], y, down, lax.div(x, 2)) for h in range(2)]
    start_moves(*first_one)
    first_swap = [push(START + h, ag_t.at[x, h, k], ag_t.at[x, h, k], partner) for h in range(2)]
    for copy in first_swap:
        copy.start()
    phase()

    def piece_t(chip, h):
        return ag_t.at[chip, h]

    def gather_t():
        to_p, to_m = dev(y, xp, k), dev(y, xm, k)
        sends = [
            push(AG_T + n, piece_t(x, h), piece_t(x, h), to) for n, (h, to) in enumerate(((0, to_p), (1, to_p), (1, to_m), (0, to_m)))
        ]
        onward = [
            push(AG_T + 4, piece_t(xm, 0), piece_t(xm, 0), to_p),
            push(AG_T + 5, piece_t(xp, 1), piece_t(xp, 1), to_m),
        ]
        relays = [push(RELAY, ag_t.at[x], ag_t.at[x], partner)] + [
            push(RELAY + 1 + n, piece_t(i, h), piece_t(i, h), partner)
            for n, (i, h) in enumerate(((xm, 0), (xp, 1), (xm, 1), (xp, 0), (xf, 0), (xf, 1)))
        ]
        return sends, onward, relays

    def gather_a():
        routes = ((0, yp), (1, yp), (1, ym), (0, ym))
        sends = [push(AG_A + n, ag_a.at[y, h], ag_a.at[y, h], dev(i, x, k)) for n, (h, i) in enumerate(routes)]
        onward = [
            push(AG_A + 4, ag_a.at[ym, 0], ag_a.at[ym, 0], dev(yp, x, k)),
            push(AG_A + 5, ag_a.at[yp, 1], ag_a.at[yp, 1], dev(ym, x, k)),
        ]
        for_other = [
            pltpu.make_async_remote_copy(
                src_ref=x_half.at[0, h], dst_ref=ag_a.at[y, h], send_sem=send.at[AG_B + n], recv_sem=recv.at[AG_A + n],
                device_id=dev(i, x, other), device_id_type=pl.DeviceIdType.MESH,
            )
            for n, (h, i) in enumerate(routes)
        ]
        return sends, onward, for_other, push(RELAY_A, x_half.at[0], ag_a.at[y], partner)

    def ring_scatter(base, part, got, plus, minus, far, to):
        def half(i, h):
            return rows_of(part(i), h)

        return [
            push(base + 0, half(far, 0), got.at[0], to(plus)),
            push(base + 1, half(far, 1), got.at[1], to(minus)),
            push(base + 2, half(plus, 1), got.at[2], to(plus)),
            push(base + 3, half(minus, 0), got.at[3], to(minus)),
            push(base + 4, half(plus, 0), got.at[4], to(plus)),
            push(base + 5, half(minus, 1), got.at[5], to(minus)),
        ]

    step_one = [
        move(MOVE, ycur.at[0], x_via.at[0], up, x, k),
        move(MOVE + 1, ycur.at[1], x_via.at[1], y, CORES * k + lax.div(behind, 2), lax.rem(behind, 2)),
    ]
    step_two = [
        move(MOVE + 2, x_via.at[0], x_move.at[0], y, down, lax.div(x, 2)),
        move(MOVE + 3, x_via.at[1], x_move.at[1], down, x, k),
    ]
    out_left = pltpu.make_async_copy(x_via.at[0], x_out.at[0], load_sem.at[0])
    out_right = pltpu.make_async_copy(x_move.at[1], x_out.at[1], load_sem.at[1])

    def share_linv(q):
        return push(LINV + q, linv.at[q, k], linv.at[q, k], partner)

    swap_y = push(SWAP_Y, ycur.at[other], y_in, partner)

    def apply(p):
        t = lax.rem(p, 2)
        a = 1 - t

        def mm_t(pieces, owner, first=False, cuts=1):
            size = sub // cuts
            for n in range(cuts):
                acc, lanes = None, slice(n * size, (n + 1) * size)
                for chip, h in pieces:
                    for core in range(CORES):
                        rows = run((chip * CORES + core) * 2 + h, hsub)
                        one = jnp.dot(ag_t[chip, h, core], ops[t, rows, run(spot(owner) * cuts + n, size)], preferred_element_type=F32)
                        acc = one if acc is None else acc + one
                p_t[owner, :, lanes] = acc if first else p_t[owner, :, lanes] + acc

        def mm_a(pieces, owner, first=False, cuts=1):
            size = sub // cuts
            for n in range(cuts):
                acc, rows = None, slice(n * size, (n + 1) * size)
                for i, h in pieces:
                    one = jnp.dot(ops[a, run(owner * cuts + n, size), run(spot(i) * 2 + h, hsub)], ag_a[i, h], preferred_element_type=F32)
                    acc = one if acc is None else acc + one
                p_a[owner, rows] = acc if first else p_a[owner, rows] + acc

        def loaded(copy):
            @pl.when(p == 0)
            def _():
                copy.wait()

        send_t, fwd_t, relays = gather_t()
        send_a, fwd_a, send_b, relay_a = gather_a()
        drives_t, drives_a = k == t, k == a
        own_y = [(y, 0), (y, 1)]
        phase("ag_own")

        @pl.when(p == 0)
        def _():
            for h in range(2):
                end_moves(first_one[h])
                start_moves(first_two[h])
            for copy in first_swap:
                copy.wait()

            @pl.when(drives_t)
            def _():
                for n in ORDER:
                    send_t[n].start()

        @pl.when(p > 0)
        def _():
            @pl.when(jnp.logical_not(drives_a))
            def _():
                relay_a.wait_recv()

            for owner in range(RING * CORES):
                mm_a(own_y, owner, True)

            @pl.when(jnp.logical_not(drives_t))
            def _():
                relays[0].wait_recv()

        loaded(loads_t[0])
        for owner in range(RING):
            mm_t([(x, 0), (x, 1)], owner, True)

        @pl.when(p == 0)
        def _():
            end_moves(first_two[0])
            send_a[0].start()
            send_a[3].start()
            end_moves(first_two[1])
            send_a[2].start()
            send_a[1].start()
            loads_a[0].wait()
            for owner in range(RING * CORES):
                mm_a(own_y, owner, True)

        def take_t(arrived, then):
            @pl.when(drives_t)
            def _():
                for copy, follow in zip(arrived, then):
                    copy.wait_recv()
                    for nxt in follow:
                        nxt.start()

        def relayed(*copies):
            @pl.when(jnp.logical_not(drives_t))
            def _():
                for copy in copies:
                    copy.wait_recv()

        phase("ag_wait1")
        take_t([send_t[n] for n in ORDER[:2]], zip(fwd_t, relays[1:3]))
        for n, copy in zip(ORDER, fwd_a):
            send_a[n].wait_recv()
            copy.start()
        phase("mm_near1")
        loaded(loads_a[1])
        loaded(loads_a[2])
        for owner in range(RING * CORES):
            mm_a([(ym, 0), (yp, 1)], owner)
        relayed(*relays[1:3])
        loaded(loads_t[1])
        loaded(loads_t[2])
        for owner in range(RING):
            mm_t([(xm, 0), (xp, 1)], owner)
        phase("mm_near2")
        take_t([send_t[n] for n in ORDER[2:]], zip(relays[3:5]))
        for n in ORDER[2:]:
            send_a[n].wait_recv()
        for owner in range(RING * CORES):
            mm_a([(ym, 1), (yp, 0)], owner)
        relayed(*relays[3:5])
        for owner in range(RING):
            mm_t([(xm, 1), (xp, 0)], owner)
        phase("ag_far")
        take_t(fwd_t, zip(relays[5:]))
        for copy in fwd_a:
            copy.wait_recv()
        phase("mm_far")

        loaded(loads_a[3])
        pairs = []
        far_y = [(yf, 0), (yf, 1)]
        out_t = ring_scatter(RS_T, lambda i: p_t.at[i], r_t, yp, ym, yf, lambda i: dev(i, x, k))
        out_a = ring_scatter(RS_A, lambda i: p_a.at[i * CORES + k], r_a, xp, xm, xf, lambda i: dev(y, i, k))

        def pair(n, i, rows):
            pairs.append(push(PAIR + n, p_a.at[i * CORES + other, rows], d_a.at[i, rows], partner))
            pairs[n].start()

        def add_pair(n, i, rows):
            pairs[n].wait_recv()
            p_a[i * CORES + k, rows] = p_a[i * CORES + k, rows] + d_a[i, rows]

        every, half_rows = pl.ds(0, sub), [pl.ds(h * hsub, hsub) for h in range(2)]
        far_x = [(xf, 0), (xf, 1)]
        mm_a(far_y, xf * CORES + other, cuts=2)
        for h in range(2):
            pair(h, xf, half_rows[h])
        relayed(*relays[5:])
        loaded(loads_t[3])
        mm_t(far_x, yf, cuts=2)
        out_t[0].start()
        out_t[1].start()
        mm_a(far_y, xf * CORES + k, cuts=2)
        for h in range(2):
            add_pair(h, xf, half_rows[h])
            out_a[h].start()
        for n, i in enumerate((xp, xm, x)):
            mm_a(far_y, i * CORES + other)
        for n, i in enumerate((xp, xm, x)):
            pair(2 + n, i, every)
        mm_t(far_x, yp)
        mm_t(far_x, ym)
        out_t[2].start()
        out_t[3].start()
        for i in (xp, xm, x):
            mm_a(far_y, i * CORES + k)
        add_pair(2, xp, every)
        add_pair(3, xm, every)
        out_a[2].start()
        out_a[3].start()
        mm_t(far_x, y)
        phase("rs_mid")

        ht = width // 2
        out_t[0].wait_recv()
        p_t[yp, 0:ht] = p_t[yp, 0:ht] + r_t[0]
        out_t[4].start()
        out_t[1].wait_recv()
        p_t[ym, ht:width] = p_t[ym, ht:width] + r_t[1]
        out_t[5].start()
        out_a[0].wait_recv()
        kp, km, kk = xp * CORES + k, xm * CORES + k, x * CORES + k
        p_a[kp, 0:hsub] = p_a[kp, 0:hsub] + r_a[0]
        out_a[4].start()
        out_a[1].wait_recv()
        p_a[km, hsub:sub] = p_a[km, hsub:sub] + r_a[1]
        out_a[5].start()
        phase("rs_end")

        @pl.when(p == SWEEPS)
        def _():
            end_moves(*step_two)
            for q in range(2):
                share_linv(q).wait()
            for op in range(2):
                y_one[op] = dot_f32(x_move[op], linv[0, op], NT)
                x_move[op] = dot_f32(y_one[op], linv[1, op], NT)
            out_right.start()
            y_one[0] = dot_f32(ycur[0], linv[0, 0], NT)
            x_via[0] = dot_f32(y_one[0], linv[1, 0], NT)
            out_left.start()

        add_pair(4, x, every)
        for copy in out_t[2:] + out_a[2:]:
            copy.wait_recv()
        phase("rs_sum")
        ycur[t, :, 0:ht] = (p_t[y, 0:ht] + r_t[3] + r_t[4]).T
        ycur[t, :, ht:width] = (p_t[y, ht:width] + r_t[2] + r_t[5]).T
        ycur[a, 0:hsub] = p_a[kk, 0:hsub] + r_a[3] + r_a[4]
        ycur[a, hsub:sub] = p_a[kk, hsub:sub] + r_a[2] + r_a[5]
        phase("rs_drain")
        for copy in fwd_a + pairs + out_t + out_a:
            copy.wait_send()

        @pl.when(drives_t)
        def _():
            for copy in send_t + fwd_t + relays[1:]:
                copy.wait_send()

            @pl.when(p > 0)
            def _():
                relays[0].wait_send()

        @pl.when(jnp.logical_or(p == 0, drives_a))
        def _():
            for copy in send_a:
                copy.wait_send()

        @pl.when(jnp.logical_and(p > 0, drives_a))
        def _():
            for copy in send_b + [relay_a]:
                copy.wait_send()

        phase()

    def routes():
        for dy, dx in OFFSETS:
            to_y, to_x = (y, yp, yf, ym)[dy], (x, xp, xf, xm)[dx]
            yield dy * RING + dx, to_y * RING + to_x, to_y, to_x

    def pair_of(rows):
        return push(GRAM_PAIR, g_loc.at[other, pl.ds(0, rows)], g_pair.at[pl.ds(0, rows)], partner)

    def pair_sum(rows, local, behind=None):
        phase("ar_pair")
        local(other)
        pair = pair_of(rows)
        pair.start()
        local(k)
        pair.wait_recv()
        if behind is not None:
            behind.start()
        g_sum[0:rows] = g_loc[k, 0:rows] + g_pair[0:rows]
        phase()

    def all_reduce(rows, meanwhile=None):
        piece = rows // nchips

        def chunk(ref, q):
            return ref.at[pl.ds(pl.multiple_of(q * piece, GROUP), piece)]

        def count(copies):
            return g_all.at[pl.ds(0, copies * piece)]

        def await_copies(sem, copies):
            pltpu.make_async_copy(count(copies), count(copies), sem).wait()

        phase("ar_rs")
        mine = y * RING + x
        owner = CORES - 1

        def spread(o, q, to_y, to_x):
            pltpu.make_async_remote_copy(
                src_ref=chunk(g_sum, q), dst_ref=g_in.at[k, pl.ds(o * piece, piece)], send_sem=send.at[GRAM_RS],
                recv_sem=recv.at[GRAM_RS + k], device_id=dev(to_y, to_x, owner), device_id_type=pl.DeviceIdType.MESH,
            ).start()

        for route in routes():
            spread(*route)
        if meanwhile is not None:
            meanwhile()

        @pl.when(k == 0)
        def _():
            spread(0, mine, y, x)
            await_copies(send.at[GRAM_RS], nchips)
            phase("ar_ag")
            await_copies(recv.at[GRAM_AG], nchips)
            phase("ar_drain")

        @pl.when(k == 1)
        def _():
            def hand_out(i, src, q, to_y, to_x, core):
                pltpu.make_async_remote_copy(
                    src_ref=src, dst_ref=chunk(g_all, q), send_sem=send.at[GRAM_AG + i], recv_sem=recv.at[GRAM_AG],
                    device_id=dev(to_y, to_x, core), device_id_type=pl.DeviceIdType.MESH,
                ).start()

            await_copies(recv.at[GRAM_RS], nchips)
            total = g_in[0, 0:piece]
            for o in range(1, nchips):
                total = total + g_in[0, o * piece : (o + 1) * piece]
            g_red[0:piece] = total / total_rows
            for _, _, to_y, to_x in routes():
                hand_out(1, g_red.at[pl.ds(0, piece)], mine, to_y, to_x, 0)
            hand_out(1, g_red.at[pl.ds(0, piece)], mine, y, x, 0)
            phase("ar_ag")
            await_copies(recv.at[GRAM_RS + 1], nchips - 1)
            total = chunk(g_sum, mine)[...]
            for o in range(1, nchips):
                total = total + g_in[1, o * piece : (o + 1) * piece]
            chunk(g_all, mine)[...] = total / total_rows
            for _, _, to_y, to_x in routes():
                hand_out(0, chunk(g_all, mine), mine, to_y, to_x, 1)
            await_copies(recv.at[GRAM_AG], nchips - 1)
            phase("ar_drain")
            await_copies(send.at[GRAM_RS], nchips - 1)
            await_copies(send.at[GRAM_AG], nchips - 1)
            await_copies(send.at[GRAM_AG + 1], nchips)

        phase()

    corners = ((0, 0), (0, 1), (1, 1), (1, 0))

    def put_gram(into, full):
        at_row, at_col = (lax.broadcasted_iota(jnp.int32, (tile, tile), i) for i in range(2))
        low = full[tile:width, tile:width]
        into[0:tile] = jnp.where(at_row <= at_col, full[0:tile, 0:tile], low)
        into[tile : 2 * tile] = full[0:tile, tile:width]
        diagonal = jnp.sum(jnp.where(at_row == at_col, low, 0.0), axis=0, keepdims=True)
        into[2 * tile : 2 * tile + GROUP] = jnp.broadcast_to(diagonal, (GROUP, tile))

    def half_gram(op):
        half = ycur[op].astype(BF16)
        put_gram(g_loc.at[op], lax.dot_general(half, half, TN, preferred_element_type=F32))

    def normalize(p, q):
        @pl.when(q == 0)
        def _():
            pair_sum(2 * tile + GROUP, half_gram, swap_y)
            phase()

        @pl.when(q == 1)
        def _():
            phase("gram2")
            put_gram(g_sum, gram_f32(y_one[0]) + gram_f32(y_one[1]))
            phase()

        last = p == SWEEPS - 1

        def clear():
            set_identity(work)
            linv[q, k, 0:tile, tile:width] = jnp.zeros((tile, tile), F32)

        own = d_all.at[q, y * RING + x]
        own[...] = g_sum[2 * tile : 2 * tile + 1]
        for _, _, to_y, to_x in routes():
            push(DIAGONAL + q, own, own, dev(to_y, to_x, k)).start()


        all_reduce(2 * tile, clear)
        others = d_all.at[q, pl.ds(0, nchips - 1)]
        for sem in (recv, send):
            pltpu.make_async_copy(others, others, sem.at[DIAGONAL + q]).wait()

        @pl.when(q == 0)
        def _():
            pair_of(2 * tile + GROUP).wait_send()

        @pl.when(jnp.logical_and(last, q == 0))
        def _():
            start_moves(*step_one)

        @pl.when(jnp.logical_and(last, q == 1))
        def _():
            end_moves(*step_one)
            start_moves(*step_two)

        phase("chol")

        def store(first, t, value):
            linv[q, k, pl.ds(first, GROUP), t * tile : (t + 1) * tile] = value

        diagonal = d_all[q, 0]
        for chip in range(1, nchips):
            diagonal = diagonal + d_all[q, chip]
        inverse_factor(g_all, diagonal / total_rows, work, store)
        phase("mul")

        @pl.when(last)
        def _():
            share_linv(q).start()

        @pl.when(q == 0)
        def _():
            y_one[0] = dot_f32(ycur[k], linv[0, k], NT)
            swap_y.wait()
            y_one[1] = dot_f32(y_in[...], linv[0, k], NT)

        phase()

    def launch(p):
        t = lax.rem(p, 2)

        def new_x(i):
            d_a[i] = dot_f32(y_one[i], linv[1, k], NT)
            return [d_a[i, h * hsub : (h + 1) * hsub] for h in range(2)]

        phase("launch")

        @pl.when(k == t)
        def _():
            sends, _, relays = gather_t()
            for i, core in enumerate((k, other)):
                for h, rows in enumerate(new_x(i)):
                    ag_t[x, h, core] = rows.T.astype(BF16)
            for n in ORDER:
                sends[n].start()
            relays[0].start()

        @pl.when(k != t)
        def _():
            sends, _, for_other, relay_a = gather_a()
            for h, rows in enumerate(new_x(0)):
                ag_a[y, h] = rows.astype(BF16)
            for n in ORDER:
                sends[n].start()
            for h, rows in enumerate(new_x(1)):
                x_half[0, h] = rows.astype(BF16)
            for n in ORDER:
                for_other[n].start()
            relay_a.start()

        phase()

    def sweep(p, carry):
        apply(p)

        @pl.when(p < SWEEPS)
        def _():
            def one(q, carry):
                normalize(p, q)
                return carry

            lax.fori_loop(0, 2, one, 0)
            launch(p + 1)

        return carry

    lax.fori_loop(0, SWEEPS + 1, sweep, 0)

    def rayleigh(op):
        full = dot_f32(x_move[op], ycur[op], TN)
        for n, (i, j) in enumerate(corners):
            g_loc[op, n * tile : (n + 1) * tile] = full[i * tile : (i + 1) * tile, j * tile : (j + 1) * tile]

    pair_sum(4 * tile, rayleigh)
    all_reduce(4 * tile)
    pair_of(4 * tile).wait_send()
    phase("h_swap")
    swap = push(SWAP_H, g_all, h_all, partner)
    swap.start()
    swap.wait()
    for n, (i, j) in enumerate(corners):
        rows, at = slice(n * tile, (n + 1) * tile), (slice(i * tile, (i + 1) * tile), slice(j * tile, (j + 1) * tile))
        for op in range(2):
            h_out[(op, *at)] = jnp.where(k == op, g_all[rows], h_all[rows])
    out_left.wait()
    out_right.wait()
    phase()


def hand_over(x_ref, h_ref, left_x, left_h, right_x, right_h, x_buf, h_buf, sem_in, sem_out):
    size = x_buf.shape[1] // 2
    routes = []
    for op, (x_to, h_to) in enumerate(((left_x, left_h), (right_x, right_h))):
        for h in range(2):
            rows = pl.ds(h * size, size)
            routes.append((x_ref.at[op, rows], x_buf.at[op, rows], x_to.at[rows]))
        routes.append((h_ref.at[op], h_buf.at[op], h_to))
    come = [pltpu.make_async_copy(src, buf, sem_in.at[n]) for n, (src, buf, _) in enumerate(routes)]
    go = [pltpu.make_async_copy(buf, dst, sem_out.at[n]) for n, (_, buf, dst) in enumerate(routes)]
    for copy in come:
        copy.start()
    for copy, nxt in zip(come, go):
        copy.wait()
        nxt.start()
    for copy in go:
        copy.wait()


def solution(mesh):
    nrow, ncol = mesh.shape["row"], mesh.shape["col"]
    assert nrow == RING and ncol == RING * CORES

    def local_program(left_op, left_start, right_op, right_start):
        rows, cols = left_op.shape
        sub, width = left_start.shape
        tile = width // 2
        vmem = pltpu.VMEM
        dma = pltpu.SemaphoreType.DMA
        basis, ray = jax.ShapeDtypeStruct((sub, width), F32), jax.ShapeDtypeStruct((width, width), F32)
        both_x, both_h = pl.pallas_call(
            functools.partial(kernel, (nrow, ncol, rows * nrow)),
            out_shape=[jax.ShapeDtypeStruct((2, sub, width), F32), jax.ShapeDtypeStruct((2, width, width), F32)],
            in_specs=[pl.BlockSpec(memory_space=pl.ANY)] * 4,
            out_specs=[pl.BlockSpec(memory_space=pl.ANY), pl.BlockSpec(memory_space=vmem)],
            scratch_shapes=[
                vmem((2, rows, cols), BF16),
                vmem((2, sub, width), F32),
                vmem((2, sub, width), F32),
                vmem((RING, 2, CORES, width, sub // 2), BF16),
                vmem((nrow, 2, sub // 2, width), BF16),
                vmem((nrow, width, sub), F32),
                vmem((ncol, sub, width), F32),
                vmem((RING, sub, width), F32),
                vmem((6, width // 2, sub), F32),
                vmem((6, sub // 2, width), F32),
                vmem((2, 2, sub // 2, width), BF16),
                vmem((2, sub, width), F32),
                vmem((2, sub, width), F32),
                vmem((sub, width), F32),
                vmem((2, 4 * tile, tile), F32),
                vmem((4 * tile, tile), F32),
                vmem((4 * tile, tile), F32),
                vmem((2, 4 * tile, tile), F32),
                vmem((4 * tile // (RING * RING), tile), F32),
                vmem((4 * tile, tile), F32),
                vmem((4 * tile, tile), F32),
                vmem((2, RING * RING, 1, tile), F32),
                vmem((width, 2 * width), F32),
                vmem((2, 2, width, width), F32),
                dma((KINDS.stop,)),
                dma((KINDS.stop,)),
                dma((10,)),
            ],
            compiler_params=pltpu.CompilerParams(collective_id=0, has_side_effects=True, vmem_limit_bytes=VMEM_BYTES),
            name="subspace",
        )(left_op, left_start, right_op, right_start)
        anywhere = pl.BlockSpec(memory_space=pl.ANY)
        return pl.pallas_call(
            hand_over,
            out_shape=[basis, ray, basis, ray],
            in_specs=[anywhere] * 2,
            out_specs=[anywhere] * 4,
            scratch_shapes=[vmem((2, sub, width), F32), vmem((2, width, width), F32), dma((6,)), dma((6,))],
            name="hand_over",
        )(both_x, both_h)

    op_spec = P(("batch", "row"), "col")
    vec_spec = P(("batch", "row", "col"), None)
    small_spec = P("batch", None)
    return jax.shard_map(
        local_program,
        mesh=mesh,
        in_specs=(op_spec, vec_spec, op_spec, vec_spec),
        out_specs=(vec_spec, small_spec, vec_spec, small_spec),
        check_vma=False,
    )
```

```python
import functools

import jax
import jax.numpy as jnp
from jax import lax
from jax.experimental import pallas as pl
from jax.experimental.pallas import tpu as pltpu
from jax.sharding import PartitionSpec as P

SWEEPS = 4
CORES = 2
RING = 4
PIVOTS = 32
STEP = 16
AHEAD = 2
LEFT_PARTS, RIGHT_PARTS = (2, 0, 1, 1, 0, 0), (0, 2, 1, 0, 1, 0)
GROUP = 8
VMEM_BYTES = 67043328
F32, BF16 = jnp.float32, jnp.bfloat16
TN = (((0,), (0,)), ((), ()))
NT = (((1,), (1,)), ((), ()))

SLOTS = 8
KINDS = range(0, 17 * SLOTS, SLOTS)
AG_T, AG_A, AG_B, RELAY, RELAY_A, RS_T, RS_A, PAIR, GRAM_PAIR, GRAM_RS, GRAM_AG, LINV, MOVE, START, SWAP_Y, SWAP_H, DIAGONAL = KINDS
ORDER = (0, 2, 1, 3)
OFFSETS = sorted(
    ((dy, dx) for dy in range(RING) for dx in range(RING) if dy or dx),
    key=lambda o: -min(o[0], RING - o[0]) - min(o[1], RING - o[1]),
)


def split3(v):
    high = v.astype(BF16)
    rest = v - high.astype(F32)
    mid = rest.astype(BF16)
    return high, mid, (rest - mid.astype(F32)).astype(BF16)


def halves_dot(lhs, rhs, dims):
    axis = 1 - dims[0][0][0]
    size = lhs.shape[axis] // 2
    parts = [lax.slice_in_dim(lhs, i * size, (i + 1) * size, axis=axis) for i in range(2)]
    return jnp.concatenate([lax.dot_general(part, rhs, dims, preferred_element_type=F32) for part in parts], axis=0)


def dot_f32(lhs, rhs, dims):
    left, right = split3(lhs), split3(rhs)
    (lk,), (rk,) = dims[0]
    lhs = jnp.concatenate([left[i] for i in LEFT_PARTS], axis=lk)
    rhs = jnp.concatenate([right[i] for i in RIGHT_PARTS], axis=rk)
    return halves_dot(lhs, rhs, dims)


def gram_f32(v):
    high, mid, low = split3(v)
    mixed = halves_dot(jnp.concatenate([high, high], axis=0), jnp.concatenate([low, mid], axis=0), TN)
    return (halves_dot(mid, mid, TN) + (mixed + mixed.T)) + halves_dot(high, high, TN)


class Phases:
    def __init__(self):
        self.scope = None

    def __call__(self, name=None):
        if self.scope is not None:
            self.scope.__exit__(None, None, None)
        self.scope = None
        if name is not None:
            self.scope = jax.named_scope(name)
            self.scope.__enter__()


def rows_of(ref, part, parts=2):
    size = ref.shape[0] // parts
    return ref.at[pl.ds(part * size, size)]


def set_identity(work):
    width = work.shape[0]
    at_row = lax.broadcasted_iota(jnp.int32, (width, width), 0)
    at_col = lax.broadcasted_iota(jnp.int32, (width, width), 1)
    work[:, width : 2 * width] = jnp.where(at_row == at_col, 1.0, 0.0).astype(F32)


def inverse_factor(gram, diagonal, work, store):
    tile = gram.shape[1]
    width = 2 * tile
    at_row, at_col = (lax.broadcasted_iota(jnp.int32, (tile, tile), i) for i in range(2))
    packed = gram[0:tile]
    turned = packed.T
    work[0:tile, 0:tile] = jnp.where(at_row <= at_col, packed, turned)
    work[0:tile, tile:width] = gram[tile : 2 * tile]
    work[tile:width, tile:width] = jnp.where(at_row == at_col, diagonal, jnp.where(at_row > at_col, packed, turned))
    sub = lax.broadcasted_iota(jnp.int32, (GROUP, tile), 0)
    groups = PIVOTS // GROUP
    full = (GROUP, tile)

    def lane(row):
        return jnp.broadcast_to(row, full)

    for first in range(0, width, PIVOTS):
        near = first // tile
        gram_tiles = list(range(near, 2))
        tiles = gram_tiles + [2 + i for i in range(near + 1)]
        data = {
            t: [work[pl.ds(first + GROUP * g, GROUP), t * tile : (t + 1) * tile] for g in range(groups)] for t in tiles
        }
        pivots = [jnp.ones(full, F32) for _ in range(groups)]
        def spread_columns(start, end):
            at = first - near * tile
            return {
                j: {g: jnp.broadcast_to(data[near][g][:, at + j : at + j + 1], full) for g in range(j // GROUP, groups)}
                for j in range(start, end)
            }

        cols = spread_columns(0, STEP)
        for j in range(PIVOTS):
            if j == STEP - AHEAD:
                cols |= spread_columns(STEP, PIVOTS)
            gj, rj = divmod(j, GROUP)
            col = cols[j]
            pivot = lane(col[gj][rj : rj + 1])
            inv = 1.0 / pivot
            pivots[gj] = jnp.where(sub == rj, pivot, pivots[gj])
            for nxt in range(j + 1, PIVOTS if j >= STEP - AHEAD else STEP):
                gn, rn = divmod(nxt, GROUP)
                entry = lane(col[gn][rn : rn + 1])
                if nxt == j + 1:
                    for g in range(gn, groups):
                        cols[nxt][g] = cols[nxt][g] - (col[g] * entry) * inv
                else:
                    scaled = entry * inv
                    for g in range(gn, groups):
                        cols[nxt][g] = cols[nxt][g] - col[g] * scaled
            for g in range(gj, groups):
                factor = col[g] * inv
                if g == gj:
                    if rj == GROUP - 1:
                        continue
                    factor = jnp.where(sub > rj, factor, 0.0)
                for t in tiles:
                    data[t][g] = data[t][g] - factor * lane(data[t][gj][rj : rj + 1])
        scale = [lax.rsqrt(p) for p in pivots]
        for t in tiles:
            data[t] = [d * s for d, s in zip(data[t], scale, strict=True)]
        for t in tiles:
            if t >= 2:
                for g in range(groups):
                    store(first + GROUP * g, t - 2, data[t][g])
        nxt = first + PIVOTS
        if nxt == width:
            break
        parts = {t: split3(jnp.concatenate(data[t], axis=0)) for t in tiles}
        below = [t for t in gram_tiles if (t + 1) * tile > nxt]
        low = below[0] * tile
        lhs = jnp.concatenate([jnp.concatenate([parts[t][i] for i in LEFT_PARTS], axis=0) for t in below], axis=1)
        right_tiles = below + [t for t in tiles if t >= 2]
        rhs = jnp.concatenate([jnp.concatenate([parts[t][i] for i in RIGHT_PARTS], axis=0) for t in right_tiles], axis=1)
        upd = lax.dot_general(lhs, rhs, TN, preferred_element_type=F32)
        for n, t in enumerate(right_tiles):
            where = pl.ds(nxt, width - nxt), slice(t * tile, (t + 1) * tile)
            work[where] = work[where] - upd[nxt - low :, n * tile : (n + 1) * tile]


def kernel(
    sizes, left_op, left_start, right_op, right_start, x_out, h_out,
    ops, ycur, y_one, ag_t, ag_a, p_t, p_a, d_a, r_t, r_a, x_half, x_via, x_move, y_in, g_loc, g_pair, g_sum, g_in, g_red, g_all, h_all, d_all, work, linv,
    send, recv, load_sem,
):
    nrow, ncol, total_rows = sizes
    sub, width = ycur.shape[1:]
    tile, hsub = width // 2, sub // 2
    nchips = RING * RING
    y = lax.axis_index("row")
    c = lax.axis_index("col")
    x, k = lax.div(c, CORES), lax.rem(c, CORES)
    other = 1 - k
    xp, xm, xf = (lax.rem(x + d, RING) for d in (1, 3, 2))
    yp, ym, yf = (lax.rem(y + d, RING) for d in (1, 3, 2))

    def dev(row, chip, core):
        return {"row": row, "col": chip * CORES + core}

    partner = dev(y, x, other)

    def push(i, src, dst, to):
        return pltpu.make_async_remote_copy(
            src_ref=src, dst_ref=dst, send_sem=send.at[i], recv_sem=recv.at[i], device_id=to, device_id_type=pl.DeviceIdType.MESH
        )

    def spot(i):
        return lax.rem(i + RING - x, RING)

    def run(index, size):
        return pl.ds(pl.multiple_of(index * size, size), size)

    phase = Phases()
    phase("boot")
    barrier = pltpu.get_barrier_semaphore()
    here = y * ncol + c
    for o in range(1, nrow * ncol):
        there = lax.rem(here + o, nrow * ncol)
        pl.semaphore_signal(
            barrier, inc=1, device_id={"row": lax.div(there, ncol), "col": lax.rem(there, ncol)}, device_id_type=pl.DeviceIdType.MESH
        )

    starts = [
        pltpu.make_async_copy(left_start, ycur.at[0], load_sem.at[8]),
        pltpu.make_async_copy(right_start, ycur.at[1], load_sem.at[9]),
    ]
    loads_t, loads_a = [], []
    for n, (xi, yi) in enumerate(((x, y), (xm, ym), (xp, yp), (xf, yf))):
        take = run(xi, CORES * sub)
        loads_t.append(pltpu.make_async_copy(left_op.at[take], ops.at[0, take], load_sem.at[2 * n]))
        take = run(spot(yi), sub)
        loads_a.append(pltpu.make_async_copy(right_op.at[:, take], ops.at[1, :, take], load_sem.at[2 * n + 1]))
    for copy in starts + loads_t + loads_a:
        copy.start()

    shift = CORES * lax.rem(x, 2) + k
    behind = spot(y)
    up, down = lax.rem(y + shift, RING), lax.rem(y + RING - shift, RING)

    def move(i, src, dst, row, chip, core):
        stays = jnp.logical_and(row == y, jnp.logical_and(chip == x, core == k))
        return push(i, src, dst, dev(row, chip, core)), stays, src, dst

    def start_moves(*moves):
        for copy, stays, src, dst in moves:

            @pl.when(stays)
            def _():
                dst[...] = src[...]

            @pl.when(jnp.logical_not(stays))
            def _():
                copy.start()

    def end_moves(*moves):
        for copy, stays, _, _ in moves:

            @pl.when(jnp.logical_not(stays))
            def _():
                copy.wait()

    for copy in starts:
        copy.wait()
    for h in range(2):
        ag_t[x, h, k] = ycur[0, h * hsub : (h + 1) * hsub].T.astype(BF16)
    for h in range(2):
        x_half[0, h] = ycur[1, h * hsub : (h + 1) * hsub].astype(BF16)
    pl.semaphore_wait(barrier, nrow * ncol - 1)
    first_one = [move(MOVE + h, x_half.at[0, h], x_half.at[1, h], up, x, k) for h in range(2)]
    first_two = [move(MOVE + 2 + h, x_half.at[1, h], ag_a.at[y, h], y, down, lax.div(x, 2)) for h in range(2)]
    start_moves(*first_one)
    first_swap = [push(START + h, ag_t.at[x, h, k], ag_t.at[x, h, k], partner) for h in range(2)]
    for copy in first_swap:
        copy.start()
    phase()

    def piece_t(chip, h):
        return ag_t.at[chip, h]

    def gather_t():
        to_p, to_m = dev(y, xp, k), dev(y, xm, k)
        sends = [
            push(AG_T + n, piece_t(x, h), piece_t(x, h), to) for n, (h, to) in enumerate(((0, to_p), (1, to_p), (1, to_m), (0, to_m)))
        ]
        onward = [
            push(AG_T + 4, piece_t(xm, 0), piece_t(xm, 0), to_p),
            push(AG_T + 5, piece_t(xp, 1), piece_t(xp, 1), to_m),
        ]
        relays = [push(RELAY, ag_t.at[x], ag_t.at[x], partner)] + [
            push(RELAY + 1 + n, piece_t(i, h), piece_t(i, h), partner)
            for n, (i, h) in enumerate(((xm, 0), (xp, 1), (xm, 1), (xp, 0), (xf, 0), (xf, 1)))
        ]
        return sends, onward, relays

    def gather_a():
        routes = ((0, yp), (1, yp), (1, ym), (0, ym))
        sends = [push(AG_A + n, ag_a.at[y, h], ag_a.at[y, h], dev(i, x, k)) for n, (h, i) in enumerate(routes)]
        onward = [
            push(AG_A + 4, ag_a.at[ym, 0], ag_a.at[ym, 0], dev(yp, x, k)),
            push(AG_A + 5, ag_a.at[yp, 1], ag_a.at[yp, 1], dev(ym, x, k)),
        ]
        for_other = [
            pltpu.make_async_remote_copy(
                src_ref=x_half.at[0, h], dst_ref=ag_a.at[y, h], send_sem=send.at[AG_B + n], recv_sem=recv.at[AG_A + n],
                device_id=dev(i, x, other), device_id_type=pl.DeviceIdType.MESH,
            )
            for n, (h, i) in enumerate(routes)
        ]
        return sends, onward, for_other, push(RELAY_A, x_half.at[0], ag_a.at[y], partner)

    def ring_scatter(base, part, got, plus, minus, far, to):
        def half(i, h):
            return rows_of(part(i), h)

        return [
            push(base + 0, half(far, 0), got.at[0], to(plus)),
            push(base + 1, half(far, 1), got.at[1], to(minus)),
            push(base + 2, half(plus, 1), got.at[2], to(plus)),
            push(base + 3, half(minus, 0), got.at[3], to(minus)),
            push(base + 4, half(plus, 0), got.at[4], to(plus)),
            push(base + 5, half(minus, 1), got.at[5], to(minus)),
        ]

    step_one = [
        move(MOVE, ycur.at[0], x_via.at[0], up, x, k),
        move(MOVE + 1, ycur.at[1], x_via.at[1], y, CORES * k + lax.div(behind, 2), lax.rem(behind, 2)),
    ]
    step_two = [
        move(MOVE + 2, x_via.at[0], x_move.at[0], y, down, lax.div(x, 2)),
        move(MOVE + 3, x_via.at[1], x_move.at[1], down, x, k),
    ]
    out_left = pltpu.make_async_copy(x_via.at[0], x_out.at[0], load_sem.at[0])
    out_right = pltpu.make_async_copy(x_move.at[1], x_out.at[1], load_sem.at[1])

    def share_linv(q):
        return push(LINV + q, linv.at[q, k], linv.at[q, k], partner)

    swap_y = push(SWAP_Y, ycur.at[other], y_in, partner)

    def apply(p):
        t = lax.rem(p, 2)
        a = 1 - t

        def mm_t(pieces, owner, first=False, cuts=1):
            size = sub // cuts
            for n in range(cuts):
                acc, lanes = None, slice(n * size, (n + 1) * size)
                for chip, h in pieces:
                    for core in range(CORES):
                        rows = run((chip * CORES + core) * 2 + h, hsub)
                        one = jnp.dot(ag_t[chip, h, core], ops[t, rows, run(spot(owner) * cuts + n, size)], preferred_element_type=F32)
                        acc = one if acc is None else acc + one
                p_t[owner, :, lanes] = acc if first else p_t[owner, :, lanes] + acc

        def mm_a(pieces, owner, first=False, cuts=1):
            size = sub // cuts
            for n in range(cuts):
                acc, rows = None, slice(n * size, (n + 1) * size)
                for i, h in pieces:
                    one = jnp.dot(ops[a, run(owner * cuts + n, size), run(spot(i) * 2 + h, hsub)], ag_a[i, h], preferred_element_type=F32)
                    acc = one if acc is None else acc + one
                p_a[owner, rows] = acc if first else p_a[owner, rows] + acc

        def loaded(copy):
            @pl.when(p == 0)
            def _():
                copy.wait()

        send_t, fwd_t, relays = gather_t()
        send_a, fwd_a, send_b, relay_a = gather_a()
        drives_t, drives_a = k == t, k == a
        own_y = [(y, 0), (y, 1)]
        phase("ag_own")

        @pl.when(p == 0)
        def _():
            for h in range(2):
                end_moves(first_one[h])
                start_moves(first_two[h])
            for copy in first_swap:
                copy.wait()

            @pl.when(drives_t)
            def _():
                for n in ORDER:
                    send_t[n].start()

        @pl.when(p > 0)
        def _():
            @pl.when(jnp.logical_not(drives_a))
            def _():
                relay_a.wait_recv()

            for owner in range(RING * CORES):
                mm_a(own_y, owner, True)

            @pl.when(jnp.logical_not(drives_t))
            def _():
                relays[0].wait_recv()

        loaded(loads_t[0])
        for owner in range(RING):
            mm_t([(x, 0), (x, 1)], owner, True)

        @pl.when(p == 0)
        def _():
            end_moves(first_two[0])
            send_a[0].start()
            send_a[3].start()
            end_moves(first_two[1])
            send_a[2].start()
            send_a[1].start()
            loads_a[0].wait()
            for owner in range(RING * CORES):
                mm_a(own_y, owner, True)

        def take_t(arrived, then):
            @pl.when(drives_t)
            def _():
                for copy, follow in zip(arrived, then):
                    copy.wait_recv()
                    for nxt in follow:
                        nxt.start()

        def relayed(*copies):
            @pl.when(jnp.logical_not(drives_t))
            def _():
                for copy in copies:
                    copy.wait_recv()

        phase("ag_wait1")
        take_t([send_t[n] for n in ORDER[:2]], zip(fwd_t, relays[1:3]))
        for n, copy in zip(ORDER, fwd_a):
            send_a[n].wait_recv()
            copy.start()
        phase("mm_near1")
        loaded(loads_a[1])
        loaded(loads_a[2])
        for owner in range(RING * CORES):
            mm_a([(ym, 0), (yp, 1)], owner)
        relayed(*relays[1:3])
        loaded(loads_t[1])
        loaded(loads_t[2])
        for owner in range(RING):
            mm_t([(xm, 0), (xp, 1)], owner)
        phase("mm_near2")
        take_t([send_t[n] for n in ORDER[2:]], zip(relays[3:5]))
        for n in ORDER[2:]:
            send_a[n].wait_recv()
        for owner in range(RING * CORES):
            mm_a([(ym, 1), (yp, 0)], owner)
        relayed(*relays[3:5])
        for owner in range(RING):
            mm_t([(xm, 1), (xp, 0)], owner)
        phase("ag_far")
        take_t(fwd_t, zip(relays[5:]))
        for copy in fwd_a:
            copy.wait_recv()
        phase("mm_far")

        loaded(loads_a[3])
        pairs = []
        far_y = [(yf, 0), (yf, 1)]
        out_t = ring_scatter(RS_T, lambda i: p_t.at[i], r_t, yp, ym, yf, lambda i: dev(i, x, k))
        out_a = ring_scatter(RS_A, lambda i: p_a.at[i * CORES + k], r_a, xp, xm, xf, lambda i: dev(y, i, k))

        def pair(n, i, rows):
            pairs.append(push(PAIR + n, p_a.at[i * CORES + other, rows], d_a.at[i, rows], partner))
            pairs[n].start()

        def add_pair(n, i, rows):
            pairs[n].wait_recv()
            p_a[i * CORES + k, rows] = p_a[i * CORES + k, rows] + d_a[i, rows]

        every, half_rows = pl.ds(0, sub), [pl.ds(h * hsub, hsub) for h in range(2)]
        far_x = [(xf, 0), (xf, 1)]
        mm_a(far_y, xf * CORES + other, cuts=2)
        for h in range(2):
            pair(h, xf, half_rows[h])
        relayed(*relays[5:])
        loaded(loads_t[3])
        mm_t(far_x, yf, cuts=2)
        out_t[0].start()
        out_t[1].start()
        mm_a(far_y, xf * CORES + k, cuts=2)
        for h in range(2):
            add_pair(h, xf, half_rows[h])
            out_a[h].start()
        for n, i in enumerate((xp, xm, x)):
            mm_a(far_y, i * CORES + other)
        for n, i in enumerate((xp, xm, x)):
            pair(2 + n, i, every)
        mm_t(far_x, yp)
        mm_t(far_x, ym)
        out_t[2].start()
        out_t[3].start()
        for i in (xp, xm, x):
            mm_a(far_y, i * CORES + k)
        add_pair(2, xp, every)
        add_pair(3, xm, every)
        out_a[2].start()
        out_a[3].start()
        mm_t(far_x, y)
        phase("rs_mid")

        ht = width // 2
        out_t[0].wait_recv()
        p_t[yp, 0:ht] = p_t[yp, 0:ht] + r_t[0]
        out_t[4].start()
        out_t[1].wait_recv()
        p_t[ym, ht:width] = p_t[ym, ht:width] + r_t[1]
        out_t[5].start()
        out_a[0].wait_recv()
        kp, km, kk = xp * CORES + k, xm * CORES + k, x * CORES + k
        p_a[kp, 0:hsub] = p_a[kp, 0:hsub] + r_a[0]
        out_a[4].start()
        out_a[1].wait_recv()
        p_a[km, hsub:sub] = p_a[km, hsub:sub] + r_a[1]
        out_a[5].start()
        phase("rs_end")

        @pl.when(p == SWEEPS)
        def _():
            end_moves(*step_two)
            for q in range(2):
                share_linv(q).wait()
            for op in range(2):
                y_one[op] = dot_f32(x_move[op], linv[0, op], NT)
                x_move[op] = dot_f32(y_one[op], linv[1, op], NT)
            out_right.start()
            y_one[0] = dot_f32(ycur[0], linv[0, 0], NT)
            x_via[0] = dot_f32(y_one[0], linv[1, 0], NT)
            out_left.start()

        add_pair(4, x, every)
        for copy in out_t[2:] + out_a[2:]:
            copy.wait_recv()
        phase("rs_sum")
        ycur[t, :, 0:ht] = (p_t[y, 0:ht] + r_t[3] + r_t[4]).T
        ycur[t, :, ht:width] = (p_t[y, ht:width] + r_t[2] + r_t[5]).T
        ycur[a, 0:hsub] = p_a[kk, 0:hsub] + r_a[3] + r_a[4]
        ycur[a, hsub:sub] = p_a[kk, hsub:sub] + r_a[2] + r_a[5]
        phase("rs_drain")
        for copy in fwd_a + pairs + out_t + out_a:
            copy.wait_send()

        @pl.when(drives_t)
        def _():
            for copy in send_t + fwd_t + relays[1:]:
                copy.wait_send()

            @pl.when(p > 0)
            def _():
                relays[0].wait_send()

        @pl.when(jnp.logical_or(p == 0, drives_a))
        def _():
            for copy in send_a:
                copy.wait_send()

        @pl.when(jnp.logical_and(p > 0, drives_a))
        def _():
            for copy in send_b + [relay_a]:
                copy.wait_send()

        phase()

    def routes():
        for dy, dx in OFFSETS:
            to_y, to_x = (y, yp, yf, ym)[dy], (x, xp, xf, xm)[dx]
            yield dy * RING + dx, to_y * RING + to_x, to_y, to_x

    def pair_of(rows):
        return push(GRAM_PAIR, g_loc.at[other, pl.ds(0, rows)], g_pair.at[pl.ds(0, rows)], partner)

    def pair_sum(rows, local, behind=None):
        phase("ar_pair")
        local(other)
        pair = pair_of(rows)
        pair.start()
        local(k)
        pair.wait_recv()
        if behind is not None:
            behind.start()
        g_sum[0:rows] = g_loc[k, 0:rows] + g_pair[0:rows]
        phase()

    def all_reduce(rows, meanwhile=None):
        piece = rows // nchips

        def chunk(ref, q):
            return ref.at[pl.ds(pl.multiple_of(q * piece, GROUP), piece)]

        def count(copies):
            return g_all.at[pl.ds(0, copies * piece)]

        def await_copies(sem, copies):
            pltpu.make_async_copy(count(copies), count(copies), sem).wait()

        phase("ar_rs")
        mine = y * RING + x
        owner = CORES - 1

        def spread(o, q, to_y, to_x):
            pltpu.make_async_remote_copy(
                src_ref=chunk(g_sum, q), dst_ref=g_in.at[k, pl.ds(o * piece, piece)], send_sem=send.at[GRAM_RS],
                recv_sem=recv.at[GRAM_RS + k], device_id=dev(to_y, to_x, owner), device_id_type=pl.DeviceIdType.MESH,
            ).start()

        for route in routes():
            spread(*route)
        if meanwhile is not None:
            meanwhile()

        @pl.when(k == 0)
        def _():
            spread(0, mine, y, x)
            await_copies(send.at[GRAM_RS], nchips)
            phase("ar_ag")
            await_copies(recv.at[GRAM_AG], nchips)
            phase("ar_drain")

        @pl.when(k == 1)
        def _():
            def hand_out(i, src, q, to_y, to_x, core):
                pltpu.make_async_remote_copy(
                    src_ref=src, dst_ref=chunk(g_all, q), send_sem=send.at[GRAM_AG + i], recv_sem=recv.at[GRAM_AG],
                    device_id=dev(to_y, to_x, core), device_id_type=pl.DeviceIdType.MESH,
                ).start()

            await_copies(recv.at[GRAM_RS], nchips)
            total = g_in[0, 0:piece]
            for o in range(1, nchips):
                total = total + g_in[0, o * piece : (o + 1) * piece]
            g_red[0:piece] = total / total_rows
            for _, _, to_y, to_x in routes():
                hand_out(1, g_red.at[pl.ds(0, piece)], mine, to_y, to_x, 0)
            hand_out(1, g_red.at[pl.ds(0, piece)], mine, y, x, 0)
            phase("ar_ag")
            await_copies(recv.at[GRAM_RS + 1], nchips - 1)
            total = chunk(g_sum, mine)[...]
            for o in range(1, nchips):
                total = total + g_in[1, o * piece : (o + 1) * piece]
            chunk(g_all, mine)[...] = total / total_rows
            for _, _, to_y, to_x in routes():
                hand_out(0, chunk(g_all, mine), mine, to_y, to_x, 1)
            await_copies(recv.at[GRAM_AG], nchips - 1)
            phase("ar_drain")
            await_copies(send.at[GRAM_RS], nchips - 1)
            await_copies(send.at[GRAM_AG], nchips - 1)
            await_copies(send.at[GRAM_AG + 1], nchips)

        phase()

    corners = ((0, 0), (0, 1), (1, 1), (1, 0))

    def put_gram(into, full):
        at_row, at_col = (lax.broadcasted_iota(jnp.int32, (tile, tile), i) for i in range(2))
        low = full[tile:width, tile:width]
        into[0:tile] = jnp.where(at_row <= at_col, full[0:tile, 0:tile], low)
        into[tile : 2 * tile] = full[0:tile, tile:width]
        diagonal = jnp.sum(jnp.where(at_row == at_col, low, 0.0), axis=0, keepdims=True)
        into[2 * tile : 2 * tile + GROUP] = jnp.broadcast_to(diagonal, (GROUP, tile))

    def half_gram(op):
        half = ycur[op].astype(BF16)
        put_gram(g_loc.at[op], lax.dot_general(half, half, TN, preferred_element_type=F32))

    def normalize(p, q):
        @pl.when(q == 0)
        def _():
            pair_sum(2 * tile + GROUP, half_gram, swap_y)
            phase()

        @pl.when(q == 1)
        def _():
            phase("gram2")
            put_gram(g_sum, gram_f32(y_one[0]) + gram_f32(y_one[1]))
            phase()

        last = p == SWEEPS - 1

        def clear():
            own = d_all.at[q, y * RING + x]
            own[...] = g_sum[2 * tile : 2 * tile + 1]
            for _, _, to_y, to_x in routes():
                push(DIAGONAL + q, own, own, dev(to_y, to_x, k)).start()
            set_identity(work)
            linv[q, k, 0:tile, tile:width] = jnp.zeros((tile, tile), F32)


        all_reduce(2 * tile, clear)
        others = d_all.at[q, pl.ds(0, nchips - 1)]
        for sem in (recv, send):
            pltpu.make_async_copy(others, others, sem.at[DIAGONAL + q]).wait()

        @pl.when(q == 0)
        def _():
            pair_of(2 * tile + GROUP).wait_send()

        @pl.when(jnp.logical_and(last, q == 0))
        def _():
            start_moves(*step_one)

        @pl.when(jnp.logical_and(last, q == 1))
        def _():
            end_moves(*step_one)
            start_moves(*step_two)

        phase("chol")

        def store(first, t, value):
            linv[q, k, pl.ds(first, GROUP), t * tile : (t + 1) * tile] = value

        diagonal = d_all[q, 0]
        for chip in range(1, nchips):
            diagonal = diagonal + d_all[q, chip]
        inverse_factor(g_all, diagonal / total_rows, work, store)
        phase("mul")

        @pl.when(last)
        def _():
            share_linv(q).start()

        @pl.when(q == 0)
        def _():
            y_one[0] = dot_f32(ycur[k], linv[0, k], NT)
            swap_y.wait()
            y_one[1] = dot_f32(y_in[...], linv[0, k], NT)

        phase()

    def launch(p):
        t = lax.rem(p, 2)

        def new_x(i):
            d_a[i] = dot_f32(y_one[i], linv[1, k], NT)
            return [d_a[i, h * hsub : (h + 1) * hsub] for h in range(2)]

        phase("launch")

        @pl.when(k == t)
        def _():
            sends, _, relays = gather_t()
            for i, core in enumerate((k, other)):
                for h, rows in enumerate(new_x(i)):
                    ag_t[x, h, core] = rows.T.astype(BF16)
            for n in ORDER:
                sends[n].start()
            relays[0].start()

        @pl.when(k != t)
        def _():
            sends, _, for_other, relay_a = gather_a()
            for h, rows in enumerate(new_x(0)):
                ag_a[y, h] = rows.astype(BF16)
            for n in ORDER:
                sends[n].start()
            for h, rows in enumerate(new_x(1)):
                x_half[0, h] = rows.astype(BF16)
            for n in ORDER:
                for_other[n].start()
            relay_a.start()

        phase()

    def sweep(p, carry):
        apply(p)

        @pl.when(p < SWEEPS)
        def _():
            def one(q, carry):
                normalize(p, q)
                return carry

            lax.fori_loop(0, 2, one, 0)
            launch(p + 1)

        return carry

    lax.fori_loop(0, SWEEPS + 1, sweep, 0)

    def rayleigh(op):
        full = dot_f32(x_move[op], ycur[op], TN)
        for n, (i, j) in enumerate(corners):
            g_loc[op, n * tile : (n + 1) * tile] = full[i * tile : (i + 1) * tile, j * tile : (j + 1) * tile]

    pair_sum(4 * tile, rayleigh)
    all_reduce(4 * tile)
    pair_of(4 * tile).wait_send()
    phase("h_swap")
    swap = push(SWAP_H, g_all, h_all, partner)
    swap.start()
    swap.wait()
    for n, (i, j) in enumerate(corners):
        rows, at = slice(n * tile, (n + 1) * tile), (slice(i * tile, (i + 1) * tile), slice(j * tile, (j + 1) * tile))
        for op in range(2):
            h_out[(op, *at)] = jnp.where(k == op, g_all[rows], h_all[rows])
    out_left.wait()
    out_right.wait()
    phase()


def hand_over(x_ref, h_ref, left_x, left_h, right_x, right_h, x_buf, h_buf, sem_in, sem_out):
    size = x_buf.shape[1] // 2
    routes = []
    for op, (x_to, h_to) in enumerate(((left_x, left_h), (right_x, right_h))):
        for h in range(2):
            rows = pl.ds(h * size, size)
            routes.append((x_ref.at[op, rows], x_buf.at[op, rows], x_to.at[rows]))
        routes.append((h_ref.at[op], h_buf.at[op], h_to))
    come = [pltpu.make_async_copy(src, buf, sem_in.at[n]) for n, (src, buf, _) in enumerate(routes)]
    go = [pltpu.make_async_copy(buf, dst, sem_out.at[n]) for n, (_, buf, dst) in enumerate(routes)]
    for copy in come:
        copy.start()
    for copy, nxt in zip(come, go):
        copy.wait()
        nxt.start()
    for copy in go:
        copy.wait()


def solution(mesh):
    nrow, ncol = mesh.shape["row"], mesh.shape["col"]
    assert nrow == RING and ncol == RING * CORES

    def local_program(left_op, left_start, right_op, right_start):
        rows, cols = left_op.shape
        sub, width = left_start.shape
        tile = width // 2
        vmem = pltpu.VMEM
        dma = pltpu.SemaphoreType.DMA
        basis, ray = jax.ShapeDtypeStruct((sub, width), F32), jax.ShapeDtypeStruct((width, width), F32)
        both_x, both_h = pl.pallas_call(
            functools.partial(kernel, (nrow, ncol, rows * nrow)),
            out_shape=[jax.ShapeDtypeStruct((2, sub, width), F32), jax.ShapeDtypeStruct((2, width, width), F32)],
            in_specs=[pl.BlockSpec(memory_space=pl.ANY)] * 4,
            out_specs=[pl.BlockSpec(memory_space=pl.ANY), pl.BlockSpec(memory_space=vmem)],
            scratch_shapes=[
                vmem((2, rows, cols), BF16),
                vmem((2, sub, width), F32),
                vmem((2, sub, width), F32),
                vmem((RING, 2, CORES, width, sub // 2), BF16),
                vmem((nrow, 2, sub // 2, width), BF16),
                vmem((nrow, width, sub), F32),
                vmem((ncol, sub, width), F32),
                vmem((RING, sub, width), F32),
                vmem((6, width // 2, sub), F32),
                vmem((6, sub // 2, width), F32),
                vmem((2, 2, sub // 2, width), BF16),
                vmem((2, sub, width), F32),
                vmem((2, sub, width), F32),
                vmem((sub, width), F32),
                vmem((2, 4 * tile, tile), F32),
                vmem((4 * tile, tile), F32),
                vmem((4 * tile, tile), F32),
                vmem((2, 4 * tile, tile), F32),
                vmem((4 * tile // (RING * RING), tile), F32),
                vmem((4 * tile, tile), F32),
                vmem((4 * tile, tile), F32),
                vmem((2, RING * RING, 1, tile), F32),
                vmem((width, 2 * width), F32),
                vmem((2, 2, width, width), F32),
                dma((KINDS.stop,)),
                dma((KINDS.stop,)),
                dma((10,)),
            ],
            compiler_params=pltpu.CompilerParams(collective_id=0, has_side_effects=True, vmem_limit_bytes=VMEM_BYTES),
            name="subspace",
        )(left_op, left_start, right_op, right_start)
        anywhere = pl.BlockSpec(memory_space=pl.ANY)
        return pl.pallas_call(
            hand_over,
            out_shape=[basis, ray, basis, ray],
            in_specs=[anywhere] * 2,
            out_specs=[anywhere] * 4,
            scratch_shapes=[vmem((2, sub, width), F32), vmem((2, width, width), F32), dma((6,)), dma((6,))],
            name="hand_over",
        )(both_x, both_h)

    op_spec = P(("batch", "row"), "col")
    vec_spec = P(("batch", "row", "col"), None)
    small_spec = P("batch", None)
    return jax.shard_map(
        local_program,
        mesh=mesh,
        in_specs=(op_spec, vec_spec, op_spec, vec_spec),
        out_specs=(vec_spec, small_spec, vec_spec, small_spec),
        check_vma=False,
    )
```

```python
import functools

import jax
import jax.numpy as jnp
from jax import lax
from jax.experimental import pallas as pl
from jax.experimental.pallas import tpu as pltpu
from jax.sharding import PartitionSpec as P

SWEEPS = 4
CORES = 2
RING = 4
PIVOTS = 32
STEP = 16
AHEAD = 2
LEFT_PARTS, RIGHT_PARTS = (2, 0, 1, 1, 0, 0), (0, 2, 1, 0, 1, 0)
GROUP = 8
VMEM_BYTES = 67043328
F32, BF16 = jnp.float32, jnp.bfloat16
TN = (((0,), (0,)), ((), ()))
NT = (((1,), (1,)), ((), ()))

SLOTS = 8
KINDS = range(0, 17 * SLOTS, SLOTS)
AG_T, AG_A, AG_B, RELAY, RELAY_A, RS_T, RS_A, PAIR, GRAM_PAIR, GRAM_RS, GRAM_AG, LINV, MOVE, START, SWAP_Y, SWAP_H, DIAGONAL = KINDS
ORDER = (0, 2, 1, 3)
OFFSETS = sorted(
    ((dy, dx) for dy in range(RING) for dx in range(RING) if dy or dx),
    key=lambda o: -min(o[0], RING - o[0]) - min(o[1], RING - o[1]),
)


def split3(v):
    high = v.astype(BF16)
    rest = v - high.astype(F32)
    mid = rest.astype(BF16)
    return high, mid, (rest - mid.astype(F32)).astype(BF16)


def halves_dot(lhs, rhs, dims):
    axis = 1 - dims[0][0][0]
    size = lhs.shape[axis] // 2
    parts = [lax.slice_in_dim(lhs, i * size, (i + 1) * size, axis=axis) for i in range(2)]
    return jnp.concatenate([lax.dot_general(part, rhs, dims, preferred_element_type=F32) for part in parts], axis=0)


def dot_f32(lhs, rhs, dims):
    left, right = split3(lhs), split3(rhs)
    (lk,), (rk,) = dims[0]
    lhs = jnp.concatenate([left[i] for i in LEFT_PARTS], axis=lk)
    rhs = jnp.concatenate([right[i] for i in RIGHT_PARTS], axis=rk)
    return halves_dot(lhs, rhs, dims)


def gram_f32(v):
    high, mid, low = split3(v)
    mixed = halves_dot(jnp.concatenate([high, high], axis=0), jnp.concatenate([low, mid], axis=0), TN)
    return (halves_dot(mid, mid, TN) + (mixed + mixed.T)) + halves_dot(high, high, TN)


class Phases:
    def __init__(self):
        self.scope = None

    def __call__(self, name=None):
        if self.scope is not None:
            self.scope.__exit__(None, None, None)
        self.scope = None
        if name is not None:
            self.scope = jax.named_scope(name)
            self.scope.__enter__()


def rows_of(ref, part, parts=2):
    size = ref.shape[0] // parts
    return ref.at[pl.ds(part * size, size)]


def set_identity(work):
    width = work.shape[0]
    at_row = lax.broadcasted_iota(jnp.int32, (width, width), 0)
    at_col = lax.broadcasted_iota(jnp.int32, (width, width), 1)
    work[:, width : 2 * width] = jnp.where(at_row == at_col, 1.0, 0.0).astype(F32)


def inverse_factor(gram, diagonal, work, store):
    tile = gram.shape[1]
    width = 2 * tile
    at_row, at_col = (lax.broadcasted_iota(jnp.int32, (tile, tile), i) for i in range(2))
    packed = gram[0:tile]
    turned = packed.T
    work[0:tile, 0:tile] = jnp.where(at_row <= at_col, packed, turned)
    work[0:tile, tile:width] = gram[tile : 2 * tile]
    work[tile:width, tile:width] = jnp.where(at_row == at_col, diagonal, jnp.where(at_row > at_col, packed, turned))
    sub = lax.broadcasted_iota(jnp.int32, (GROUP, tile), 0)
    groups = PIVOTS // GROUP
    full = (GROUP, tile)

    def lane(row):
        return jnp.broadcast_to(row, full)

    for first in range(0, width, PIVOTS):
        near = first // tile
        gram_tiles = list(range(near, 2))
        tiles = gram_tiles + [2 + i for i in range(near + 1)]
        data = {
            t: [work[pl.ds(first + GROUP * g, GROUP), t * tile : (t + 1) * tile] for g in range(groups)] for t in tiles
        }
        pivots = [jnp.ones(full, F32) for _ in range(groups)]
        def spread_columns(start, end):
            at = first - near * tile
            return {
                j: {g: jnp.broadcast_to(data[near][g][:, at + j : at + j + 1], full) for g in range(j // GROUP, groups)}
                for j in range(start, end)
            }

        cols = spread_columns(0, STEP)
        for j in range(PIVOTS):
            if j == STEP - AHEAD:
                cols |= spread_columns(STEP, PIVOTS)
            gj, rj = divmod(j, GROUP)
            col = cols[j]
            pivot = lane(col[gj][rj : rj + 1])
            inv = 1.0 / pivot
            pivots[gj] = jnp.where(sub == rj, pivot, pivots[gj])
            for nxt in range(j + 1, PIVOTS if j >= STEP - AHEAD else STEP):
                gn, rn = divmod(nxt, GROUP)
                entry = lane(col[gn][rn : rn + 1])
                if nxt == j + 1:
                    for g in range(gn, groups):
                        cols[nxt][g] = cols[nxt][g] - (col[g] * entry) * inv
                else:
                    scaled = entry * inv
                    for g in range(gn, groups):
                        cols[nxt][g] = cols[nxt][g] - col[g] * scaled
            for g in range(gj, groups):
                factor = col[g] * inv
                if g == gj:
                    if rj == GROUP - 1:
                        continue
                    factor = jnp.where(sub > rj, factor, 0.0)
                for t in tiles:
                    data[t][g] = data[t][g] - factor * lane(data[t][gj][rj : rj + 1])
        scale = [lax.rsqrt(p) for p in pivots]
        for t in tiles:
            data[t] = [d * s for d, s in zip(data[t], scale, strict=True)]
        for t in tiles:
            if t >= 2:
                for g in range(groups):
                    store(first + GROUP * g, t - 2, data[t][g])
        nxt = first + PIVOTS
        if nxt == width:
            break
        parts = {t: split3(jnp.concatenate(data[t], axis=0)) for t in tiles}
        below = [t for t in gram_tiles if (t + 1) * tile > nxt]
        low = below[0] * tile
        lhs = jnp.concatenate([jnp.concatenate([parts[t][i] for i in LEFT_PARTS], axis=0) for t in below], axis=1)
        right_tiles = below + [t for t in tiles if t >= 2]
        rhs = jnp.concatenate([jnp.concatenate([parts[t][i] for i in RIGHT_PARTS], axis=0) for t in right_tiles], axis=1)
        upd = lax.dot_general(lhs, rhs, TN, preferred_element_type=F32)
        for n, t in enumerate(right_tiles):
            where = pl.ds(nxt, width - nxt), slice(t * tile, (t + 1) * tile)
            work[where] = work[where] - upd[nxt - low :, n * tile : (n + 1) * tile]


def kernel(
    sizes, left_op, left_start, right_op, right_start, x_out, h_out,
    ops, ycur, y_one, ag_t, ag_a, p_t, p_a, d_a, r_t, r_a, x_half, x_via, x_move, y_in, g_loc, g_pair, g_sum, g_in, g_red, g_all, h_all, d_all, work, linv,
    send, recv, load_sem,
):
    nrow, ncol, total_rows = sizes
    sub, width = ycur.shape[1:]
    tile, hsub = width // 2, sub // 2
    nchips = RING * RING
    y = lax.axis_index("row")
    c = lax.axis_index("col")
    x, k = lax.div(c, CORES), lax.rem(c, CORES)
    other = 1 - k
    xp, xm, xf = (lax.rem(x + d, RING) for d in (1, 3, 2))
    yp, ym, yf = (lax.rem(y + d, RING) for d in (1, 3, 2))

    def dev(row, chip, core):
        return {"row": row, "col": chip * CORES + core}

    partner = dev(y, x, other)

    def push(i, src, dst, to):
        return pltpu.make_async_remote_copy(
            src_ref=src, dst_ref=dst, send_sem=send.at[i], recv_sem=recv.at[i], device_id=to, device_id_type=pl.DeviceIdType.MESH
        )

    def spot(i):
        return lax.rem(i + RING - x, RING)

    def run(index, size):
        return pl.ds(pl.multiple_of(index * size, size), size)

    phase = Phases()
    phase("boot")
    barrier = pltpu.get_barrier_semaphore()
    here = y * ncol + c
    for o in range(1, nrow * ncol):
        there = lax.rem(here + o, nrow * ncol)
        pl.semaphore_signal(
            barrier, inc=1, device_id={"row": lax.div(there, ncol), "col": lax.rem(there, ncol)}, device_id_type=pl.DeviceIdType.MESH
        )

    starts = [
        pltpu.make_async_copy(left_start, ycur.at[0], load_sem.at[8]),
        pltpu.make_async_copy(right_start, ycur.at[1], load_sem.at[9]),
    ]
    loads_t, loads_a = [], []
    for n, (xi, yi) in enumerate(((x, y), (xm, ym), (xp, yp), (xf, yf))):
        take = run(xi, CORES * sub)
        loads_t.append(pltpu.make_async_copy(left_op.at[take], ops.at[0, take], load_sem.at[2 * n]))
        take = run(spot(yi), sub)
        loads_a.append(pltpu.make_async_copy(right_op.at[:, take], ops.at[1, :, take], load_sem.at[2 * n + 1]))
    for copy in starts + loads_t + loads_a:
        copy.start()

    shift = CORES * lax.rem(x, 2) + k
    behind = spot(y)
    up, down = lax.rem(y + shift, RING), lax.rem(y + RING - shift, RING)

    def move(i, src, dst, row, chip, core):
        stays = jnp.logical_and(row == y, jnp.logical_and(chip == x, core == k))
        return push(i, src, dst, dev(row, chip, core)), stays, src, dst

    def start_moves(*moves):
        for copy, stays, src, dst in moves:

            @pl.when(stays)
            def _():
                dst[...] = src[...]

            @pl.when(jnp.logical_not(stays))
            def _():
                copy.start()

    def end_moves(*moves):
        for copy, stays, _, _ in moves:

            @pl.when(jnp.logical_not(stays))
            def _():
                copy.wait()

    for copy in starts:
        copy.wait()
    for h in range(2):
        ag_t[x, h, k] = ycur[0, h * hsub : (h + 1) * hsub].T.astype(BF16)
    for h in range(2):
        x_half[0, h] = ycur[1, h * hsub : (h + 1) * hsub].astype(BF16)
    pl.semaphore_wait(barrier, nrow * ncol - 1)
    first_one = [move(MOVE + h, x_half.at[0, h], x_half.at[1, h], up, x, k) for h in range(2)]
    first_two = [move(MOVE + 2 + h, x_half.at[1, h], ag_a.at[y, h], y, down, lax.div(x, 2)) for h in range(2)]
    start_moves(*first_one)
    first_swap = [push(START + h, ag_t.at[x, h, k], ag_t.at[x, h, k], partner) for h in range(2)]
    for copy in first_swap:
        copy.start()
    phase()

    def piece_t(chip, h):
        return ag_t.at[chip, h]

    def gather_t():
        to_p, to_m = dev(y, xp, k), dev(y, xm, k)
        sends = [
            push(AG_T + n, piece_t(x, h), piece_t(x, h), to) for n, (h, to) in enumerate(((0, to_p), (1, to_p), (1, to_m), (0, to_m)))
        ]
        onward = [
            push(AG_T + 4, piece_t(xm, 0), piece_t(xm, 0), to_p),
            push(AG_T + 5, piece_t(xp, 1), piece_t(xp, 1), to_m),
        ]
        relays = [push(RELAY, ag_t.at[x], ag_t.at[x], partner)] + [
            push(RELAY + 1 + n, piece_t(i, h), piece_t(i, h), partner)
            for n, (i, h) in enumerate(((xm, 0), (xp, 1), (xm, 1), (xp, 0), (xf, 0), (xf, 1)))
        ]
        return sends, onward, relays

    def gather_a():
        routes = ((0, yp), (1, yp), (1, ym), (0, ym))
        sends = [push(AG_A + n, ag_a.at[y, h], ag_a.at[y, h], dev(i, x, k)) for n, (h, i) in enumerate(routes)]
        onward = [
            push(AG_A + 4, ag_a.at[ym, 0], ag_a.at[ym, 0], dev(yp, x, k)),
            push(AG_A + 5, ag_a.at[yp, 1], ag_a.at[yp, 1], dev(ym, x, k)),
        ]
        for_other = [
            pltpu.make_async_remote_copy(
                src_ref=x_half.at[0, h], dst_ref=ag_a.at[y, h], send_sem=send.at[AG_B + n], recv_sem=recv.at[AG_A + n],
                device_id=dev(i, x, other), device_id_type=pl.DeviceIdType.MESH,
            )
            for n, (h, i) in enumerate(routes)
        ]
        return sends, onward, for_other, push(RELAY_A, x_half.at[0], ag_a.at[y], partner)

    def ring_scatter(base, part, got, plus, minus, far, to):
        def half(i, h):
            return rows_of(part(i), h)

        return [
            push(base + 0, half(far, 0), got.at[0], to(plus)),
            push(base + 1, half(far, 1), got.at[1], to(minus)),
            push(base + 2, half(plus, 1), got.at[2], to(plus)),
            push(base + 3, half(minus, 0), got.at[3], to(minus)),
            push(base + 4, half(plus, 0), got.at[4], to(plus)),
            push(base + 5, half(minus, 1), got.at[5], to(minus)),
        ]

    step_one = [
        move(MOVE, ycur.at[0], x_via.at[0], up, x, k),
        move(MOVE + 1, ycur.at[1], x_via.at[1], y, CORES * k + lax.div(behind, 2), lax.rem(behind, 2)),
    ]
    step_two = [
        move(MOVE + 2, x_via.at[0], x_move.at[0], y, down, lax.div(x, 2)),
        move(MOVE + 3, x_via.at[1], x_move.at[1], down, x, k),
    ]
    out_left = pltpu.make_async_copy(x_via.at[0], x_out.at[0], load_sem.at[0])
    out_right = pltpu.make_async_copy(x_move.at[1], x_out.at[1], load_sem.at[1])

    def share_linv(q):
        return push(LINV + q, linv.at[q, k], linv.at[q, k], partner)

    swap_y = push(SWAP_Y, ycur.at[other], y_in, partner)

    def apply(p):
        t = lax.rem(p, 2)
        a = 1 - t

        def mm_t(pieces, owner, first=False, cuts=1):
            size = sub // cuts
            for n in range(cuts):
                acc, lanes = None, slice(n * size, (n + 1) * size)
                for chip, h in pieces:
                    for core in range(CORES):
                        rows = run((chip * CORES + core) * 2 + h, hsub)
                        one = jnp.dot(ag_t[chip, h, core], ops[t, rows, run(spot(owner) * cuts + n, size)], preferred_element_type=F32)
                        acc = one if acc is None else acc + one
                p_t[owner, :, lanes] = acc if first else p_t[owner, :, lanes] + acc

        def mm_a(pieces, owner, first=False, cuts=1):
            size = sub // cuts
            for n in range(cuts):
                acc, rows = None, slice(n * size, (n + 1) * size)
                for i, h in pieces:
                    one = jnp.dot(ops[a, run(owner * cuts + n, size), run(spot(i) * 2 + h, hsub)], ag_a[i, h], preferred_element_type=F32)
                    acc = one if acc is None else acc + one
                p_a[owner, rows] = acc if first else p_a[owner, rows] + acc

        def loaded(copy):
            @pl.when(p == 0)
            def _():
                copy.wait()

        send_t, fwd_t, relays = gather_t()
        send_a, fwd_a, send_b, relay_a = gather_a()
        drives_t, drives_a = k == t, k == a
        own_y = [(y, 0), (y, 1)]
        phase("ag_own")

        @pl.when(p == 0)
        def _():
            for h in range(2):
                end_moves(first_one[h])
                start_moves(first_two[h])
            for copy in first_swap:
                copy.wait()

            @pl.when(drives_t)
            def _():
                for n in ORDER:
                    send_t[n].start()

        @pl.when(p > 0)
        def _():
            @pl.when(jnp.logical_not(drives_a))
            def _():
                relay_a.wait_recv()

            for owner in range(RING * CORES):
                mm_a(own_y, owner, True)

            @pl.when(jnp.logical_not(drives_t))
            def _():
                relays[0].wait_recv()

        loaded(loads_t[0])
        for owner in range(RING):
            mm_t([(x, 0), (x, 1)], owner, True)

        @pl.when(p == 0)
        def _():
            end_moves(first_two[0])
            send_a[0].start()
            send_a[3].start()
            end_moves(first_two[1])
            send_a[2].start()
            send_a[1].start()
            loads_a[0].wait()
            for owner in range(RING * CORES):
                mm_a(own_y, owner, True)

        def take_t(arrived, then):
            @pl.when(drives_t)
            def _():
                for copy, follow in zip(arrived, then):
                    copy.wait_recv()
                    for nxt in follow:
                        nxt.start()

        def relayed(*copies):
            @pl.when(jnp.logical_not(drives_t))
            def _():
                for copy in copies:
                    copy.wait_recv()

        phase("ag_wait1")
        take_t([send_t[n] for n in ORDER[:2]], zip(fwd_t, relays[1:3]))
        for n, copy in zip(ORDER, fwd_a):
            send_a[n].wait_recv()
            copy.start()
        phase("mm_near1")
        loaded(loads_a[1])
        loaded(loads_a[2])
        for owner in range(RING * CORES):
            mm_a([(ym, 0), (yp, 1)], owner)
        relayed(*relays[1:3])
        loaded(loads_t[1])
        loaded(loads_t[2])
        for owner in range(RING):
            mm_t([(xm, 0), (xp, 1)], owner)
        phase("mm_near2")
        take_t([send_t[n] for n in ORDER[2:]], zip(relays[3:5]))
        for n in ORDER[2:]:
            send_a[n].wait_recv()
        for owner in range(RING * CORES):
            mm_a([(ym, 1), (yp, 0)], owner)
        relayed(*relays[3:5])
        for owner in range(RING):
            mm_t([(xm, 1), (xp, 0)], owner)
        phase("ag_far")
        take_t(fwd_t, zip(relays[5:]))
        for copy in fwd_a:
            copy.wait_recv()
        phase("mm_far")

        loaded(loads_a[3])
        pairs = []
        far_y = [(yf, 0), (yf, 1)]
        out_t = ring_scatter(RS_T, lambda i: p_t.at[i], r_t, yp, ym, yf, lambda i: dev(i, x, k))
        out_a = ring_scatter(RS_A, lambda i: p_a.at[i * CORES + k], r_a, xp, xm, xf, lambda i: dev(y, i, k))

        def pair(n, i, rows):
            pairs.append(push(PAIR + n, p_a.at[i * CORES + other, rows], d_a.at[i, rows], partner))
            pairs[n].start()

        def add_pair(n, i, rows):
            pairs[n].wait_recv()
            p_a[i * CORES + k, rows] = p_a[i * CORES + k, rows] + d_a[i, rows]

        every, half_rows = pl.ds(0, sub), [pl.ds(h * hsub, hsub) for h in range(2)]
        far_x = [(xf, 0), (xf, 1)]
        mm_a(far_y, xf * CORES + other, cuts=2)
        for h in range(2):
            pair(h, xf, half_rows[h])
        relayed(*relays[5:])
        loaded(loads_t[3])
        mm_t(far_x, yf, cuts=2)
        out_t[0].start()
        out_t[1].start()
        mm_a(far_y, xf * CORES + k, cuts=2)
        for h in range(2):
            add_pair(h, xf, half_rows[h])
            out_a[h].start()
        for n, i in enumerate((xp, xm, x)):
            mm_a(far_y, i * CORES + other)
        for n, i in enumerate((xp, xm, x)):
            pair(2 + n, i, every)
        mm_t(far_x, yp)
        mm_t(far_x, ym)
        out_t[2].start()
        out_t[3].start()
        for i in (xp, xm, x):
            mm_a(far_y, i * CORES + k)
        add_pair(2, xp, every)
        add_pair(3, xm, every)
        out_a[2].start()
        out_a[3].start()
        mm_t(far_x, y)
        phase("rs_mid")

        ht = width // 2
        out_t[0].wait_recv()
        p_t[yp, 0:ht] = p_t[yp, 0:ht] + r_t[0]
        out_t[4].start()
        out_t[1].wait_recv()
        p_t[ym, ht:width] = p_t[ym, ht:width] + r_t[1]
        out_t[5].start()
        out_a[0].wait_recv()
        kp, km, kk = xp * CORES + k, xm * CORES + k, x * CORES + k
        p_a[kp, 0:hsub] = p_a[kp, 0:hsub] + r_a[0]
        out_a[4].start()
        out_a[1].wait_recv()
        p_a[km, hsub:sub] = p_a[km, hsub:sub] + r_a[1]
        out_a[5].start()
        phase("rs_end")

        @pl.when(p == SWEEPS)
        def _():
            end_moves(*step_two)
            for q in range(2):
                share_linv(q).wait()
            for op in range(2):
                y_one[op] = dot_f32(x_move[op], linv[0, op], NT)
                x_move[op] = dot_f32(y_one[op], linv[1, op], NT)
            out_right.start()
            y_one[0] = dot_f32(ycur[0], linv[0, 0], NT)
            x_via[0] = dot_f32(y_one[0], linv[1, 0], NT)
            out_left.start()

        add_pair(4, x, every)
        for copy in out_t[2:] + out_a[2:]:
            copy.wait_recv()
        phase("rs_sum")
        ycur[t, :, 0:ht] = (p_t[y, 0:ht] + r_t[3] + r_t[4]).T
        ycur[t, :, ht:width] = (p_t[y, ht:width] + r_t[2] + r_t[5]).T
        ycur[a, 0:hsub] = p_a[kk, 0:hsub] + r_a[3] + r_a[4]
        ycur[a, hsub:sub] = p_a[kk, hsub:sub] + r_a[2] + r_a[5]
        phase("rs_drain")
        for copy in fwd_a + pairs + out_t + out_a:
            copy.wait_send()

        @pl.when(drives_t)
        def _():
            for copy in send_t + fwd_t + relays[1:]:
                copy.wait_send()

            @pl.when(p > 0)
            def _():
                relays[0].wait_send()

        @pl.when(jnp.logical_or(p == 0, drives_a))
        def _():
            for copy in send_a:
                copy.wait_send()

        @pl.when(jnp.logical_and(p > 0, drives_a))
        def _():
            for copy in send_b + [relay_a]:
                copy.wait_send()

        phase()

    def routes():
        for dy, dx in OFFSETS:
            to_y, to_x = (y, yp, yf, ym)[dy], (x, xp, xf, xm)[dx]
            yield dy * RING + dx, to_y * RING + to_x, to_y, to_x

    def pair_of(rows):
        return push(GRAM_PAIR, g_loc.at[other, pl.ds(0, rows)], g_pair.at[pl.ds(0, rows)], partner)

    def pair_sum(rows, local, behind=None):
        phase("ar_pair")
        local(other)
        pair = pair_of(rows)
        pair.start()
        local(k)
        pair.wait_recv()
        if behind is not None:
            behind.start()
        g_sum[0:rows] = g_loc[k, 0:rows] + g_pair[0:rows]
        phase()

    def all_reduce(rows, meanwhile=None):
        piece = rows // nchips

        def chunk(ref, q):
            return ref.at[pl.ds(pl.multiple_of(q * piece, GROUP), piece)]

        def count(copies):
            return g_all.at[pl.ds(0, copies * piece)]

        def await_copies(sem, copies):
            pltpu.make_async_copy(count(copies), count(copies), sem).wait()

        phase("ar_rs")
        mine = y * RING + x
        owner = CORES - 1

        def spread(o, q, to_y, to_x):
            pltpu.make_async_remote_copy(
                src_ref=chunk(g_sum, q), dst_ref=g_in.at[k, pl.ds(o * piece, piece)], send_sem=send.at[GRAM_RS],
                recv_sem=recv.at[GRAM_RS + k], device_id=dev(to_y, to_x, owner), device_id_type=pl.DeviceIdType.MESH,
            ).start()

        for route in routes():
            spread(*route)
        if meanwhile is not None:
            meanwhile()

        @pl.when(k == 0)
        def _():
            spread(0, mine, y, x)
            await_copies(send.at[GRAM_RS], nchips)
            phase("ar_ag")
            await_copies(recv.at[GRAM_AG], nchips)
            phase("ar_drain")

        @pl.when(k == 1)
        def _():
            def hand_out(i, src, q, to_y, to_x, core):
                pltpu.make_async_remote_copy(
                    src_ref=src, dst_ref=chunk(g_all, q), send_sem=send.at[GRAM_AG + i], recv_sem=recv.at[GRAM_AG],
                    device_id=dev(to_y, to_x, core), device_id_type=pl.DeviceIdType.MESH,
                ).start()

            await_copies(recv.at[GRAM_RS], nchips)
            total = g_in[0, 0:piece]
            for o in range(1, nchips):
                total = total + g_in[0, o * piece : (o + 1) * piece]
            g_red[0:piece] = total / total_rows
            for _, _, to_y, to_x in routes():
                hand_out(1, g_red.at[pl.ds(0, piece)], mine, to_y, to_x, 0)
            hand_out(1, g_red.at[pl.ds(0, piece)], mine, y, x, 0)
            phase("ar_ag")
            await_copies(recv.at[GRAM_RS + 1], nchips - 1)
            total = chunk(g_sum, mine)[...]
            for o in range(1, nchips):
                total = total + g_in[1, o * piece : (o + 1) * piece]
            chunk(g_all, mine)[...] = total / total_rows
            for _, _, to_y, to_x in routes():
                hand_out(0, chunk(g_all, mine), mine, to_y, to_x, 1)
            await_copies(recv.at[GRAM_AG], nchips - 1)
            phase("ar_drain")
            await_copies(send.at[GRAM_RS], nchips - 1)
            await_copies(send.at[GRAM_AG], nchips - 1)
            await_copies(send.at[GRAM_AG + 1], nchips)

        phase()

    corners = ((0, 0), (0, 1), (1, 1), (1, 0))

    def put_gram(into, full):
        at_row, at_col = (lax.broadcasted_iota(jnp.int32, (tile, tile), i) for i in range(2))
        low = full[tile:width, tile:width]
        into[0:tile] = jnp.where(at_row <= at_col, full[0:tile, 0:tile], low)
        into[tile : 2 * tile] = full[0:tile, tile:width]
        diagonal = jnp.sum(jnp.where(at_row == at_col, low, 0.0), axis=0, keepdims=True)
        into[2 * tile : 2 * tile + GROUP] = jnp.broadcast_to(diagonal, (GROUP, tile))

    def half_gram(op):
        half = ycur[op].astype(BF16)
        put_gram(g_loc.at[op], lax.dot_general(half, half, TN, preferred_element_type=F32))

    def normalize(p, q):
        @pl.when(q == 0)
        def _():
            pair_sum(2 * tile + GROUP, half_gram, swap_y)
            phase()

        @pl.when(q == 1)
        def _():
            phase("gram2")
            put_gram(g_sum, gram_f32(y_one[0]) + gram_f32(y_one[1]))
            phase()

        last = p == SWEEPS - 1

        def clear():
            own = d_all.at[q, y * RING + x]
            own[...] = g_sum[2 * tile : 2 * tile + 1]
            for _, _, to_y, to_x in routes():
                push(DIAGONAL + q, own, own, dev(to_y, to_x, k)).start()
            set_identity(work)
            linv[q, k, 0:tile, tile:width] = jnp.zeros((tile, tile), F32)


        all_reduce(2 * tile, clear)
        others = d_all.at[q, pl.ds(0, nchips - 1)]
        for sem in (recv, send):
            pltpu.make_async_copy(others, others, sem.at[DIAGONAL + q]).wait()

        @pl.when(q == 0)
        def _():
            pair_of(2 * tile + GROUP).wait_send()

        @pl.when(jnp.logical_and(last, q == 0))
        def _():
            start_moves(*step_one)

        @pl.when(jnp.logical_and(last, q == 1))
        def _():
            end_moves(*step_one)
            start_moves(*step_two)

        phase("chol")

        def store(first, t, value):
            linv[q, k, pl.ds(first, GROUP), t * tile : (t + 1) * tile] = value

        diagonal = d_all[q, 0]
        for chip in range(1, nchips):
            diagonal = diagonal + d_all[q, chip]
        inverse_factor(g_all, diagonal / total_rows, work, store)
        phase("mul")

        @pl.when(last)
        def _():
            share_linv(q).start()

        @pl.when(q == 0)
        def _():
            swap_y.wait()
            both = jnp.concatenate([ycur[k], y_in[...]], axis=0)
            y_one[...] = dot_f32(both, linv[0, k], NT).reshape(y_one.shape)

        phase()

    def launch(p):
        t = lax.rem(p, 2)

        def new_x(i):
            d_a[i] = dot_f32(y_one[i], linv[1, k], NT)
            return [d_a[i, h * hsub : (h + 1) * hsub] for h in range(2)]

        phase("launch")

        @pl.when(k == t)
        def _():
            sends, _, relays = gather_t()
            for i, core in enumerate((k, other)):
                for h, rows in enumerate(new_x(i)):
                    ag_t[x, h, core] = rows.T.astype(BF16)
            for n in ORDER:
                sends[n].start()
            relays[0].start()

        @pl.when(k != t)
        def _():
            sends, _, for_other, relay_a = gather_a()
            for h, rows in enumerate(new_x(0)):
                ag_a[y, h] = rows.astype(BF16)
            for n in ORDER:
                sends[n].start()
            for h, rows in enumerate(new_x(1)):
                x_half[0, h] = rows.astype(BF16)
            for n in ORDER:
                for_other[n].start()
            relay_a.start()

        phase()

    def sweep(p, carry):
        apply(p)

        @pl.when(p < SWEEPS)
        def _():
            def one(q, carry):
                normalize(p, q)
                return carry

            lax.fori_loop(0, 2, one, 0)
            launch(p + 1)

        return carry

    lax.fori_loop(0, SWEEPS + 1, sweep, 0)

    def rayleigh(op):
        full = dot_f32(x_move[op], ycur[op], TN)
        for n, (i, j) in enumerate(corners):
            g_loc[op, n * tile : (n + 1) * tile] = full[i * tile : (i + 1) * tile, j * tile : (j + 1) * tile]

    pair_sum(4 * tile, rayleigh)
    all_reduce(4 * tile)
    pair_of(4 * tile).wait_send()
    phase("h_swap")
    swap = push(SWAP_H, g_all, h_all, partner)
    swap.start()
    swap.wait()
    for n, (i, j) in enumerate(corners):
        rows, at = slice(n * tile, (n + 1) * tile), (slice(i * tile, (i + 1) * tile), slice(j * tile, (j + 1) * tile))
        for op in range(2):
            h_out[(op, *at)] = jnp.where(k == op, g_all[rows], h_all[rows])
    out_left.wait()
    out_right.wait()
    phase()


def hand_over(x_ref, h_ref, left_x, left_h, right_x, right_h, x_buf, h_buf, sem_in, sem_out):
    size = x_buf.shape[1] // 2
    routes = []
    for op, (x_to, h_to) in enumerate(((left_x, left_h), (right_x, right_h))):
        for h in range(2):
            rows = pl.ds(h * size, size)
            routes.append((x_ref.at[op, rows], x_buf.at[op, rows], x_to.at[rows]))
        routes.append((h_ref.at[op], h_buf.at[op], h_to))
    come = [pltpu.make_async_copy(src, buf, sem_in.at[n]) for n, (src, buf, _) in enumerate(routes)]
    go = [pltpu.make_async_copy(buf, dst, sem_out.at[n]) for n, (_, buf, dst) in enumerate(routes)]
    for copy in come:
        copy.start()
    for copy, nxt in zip(come, go):
        copy.wait()
        nxt.start()
    for copy in go:
        copy.wait()


def solution(mesh):
    nrow, ncol = mesh.shape["row"], mesh.shape["col"]
    assert nrow == RING and ncol == RING * CORES

    def local_program(left_op, left_start, right_op, right_start):
        rows, cols = left_op.shape
        sub, width = left_start.shape
        tile = width // 2
        vmem = pltpu.VMEM
        dma = pltpu.SemaphoreType.DMA
        basis, ray = jax.ShapeDtypeStruct((sub, width), F32), jax.ShapeDtypeStruct((width, width), F32)
        both_x, both_h = pl.pallas_call(
            functools.partial(kernel, (nrow, ncol, rows * nrow)),
            out_shape=[jax.ShapeDtypeStruct((2, sub, width), F32), jax.ShapeDtypeStruct((2, width, width), F32)],
            in_specs=[pl.BlockSpec(memory_space=pl.ANY)] * 4,
            out_specs=[pl.BlockSpec(memory_space=pl.ANY), pl.BlockSpec(memory_space=vmem)],
            scratch_shapes=[
                vmem((2, rows, cols), BF16),
                vmem((2, sub, width), F32),
                vmem((2, sub, width), F32),
                vmem((RING, 2, CORES, width, sub // 2), BF16),
                vmem((nrow, 2, sub // 2, width), BF16),
                vmem((nrow, width, sub), F32),
                vmem((ncol, sub, width), F32),
                vmem((RING, sub, width), F32),
                vmem((6, width // 2, sub), F32),
                vmem((6, sub // 2, width), F32),
                vmem((2, 2, sub // 2, width), BF16),
                vmem((2, sub, width), F32),
                vmem((2, sub, width), F32),
                vmem((sub, width), F32),
                vmem((2, 4 * tile, tile), F32),
                vmem((4 * tile, tile), F32),
                vmem((4 * tile, tile), F32),
                vmem((2, 4 * tile, tile), F32),
                vmem((4 * tile // (RING * RING), tile), F32),
                vmem((4 * tile, tile), F32),
                vmem((4 * tile, tile), F32),
                vmem((2, RING * RING, 1, tile), F32),
                vmem((width, 2 * width), F32),
                vmem((2, 2, width, width), F32),
                dma((KINDS.stop,)),
                dma((KINDS.stop,)),
                dma((10,)),
            ],
            compiler_params=pltpu.CompilerParams(collective_id=0, has_side_effects=True, vmem_limit_bytes=VMEM_BYTES),
            name="subspace",
        )(left_op, left_start, right_op, right_start)
        anywhere = pl.BlockSpec(memory_space=pl.ANY)
        return pl.pallas_call(
            hand_over,
            out_shape=[basis, ray, basis, ray],
            in_specs=[anywhere] * 2,
            out_specs=[anywhere] * 4,
            scratch_shapes=[vmem((2, sub, width), F32), vmem((2, width, width), F32), dma((6,)), dma((6,))],
            name="hand_over",
        )(both_x, both_h)

    op_spec = P(("batch", "row"), "col")
    vec_spec = P(("batch", "row", "col"), None)
    small_spec = P("batch", None)
    return jax.shard_map(
        local_program,
        mesh=mesh,
        in_specs=(op_spec, vec_spec, op_spec, vec_spec),
        out_specs=(vec_spec, small_spec, vec_spec, small_spec),
        check_vma=False,
    )
```

```python
import functools

import jax
import jax.numpy as jnp
from jax import lax
from jax.experimental import pallas as pl
from jax.experimental.pallas import tpu as pltpu
from jax.sharding import PartitionSpec as P

SWEEPS = 4
CORES = 2
RING = 4
PIVOTS = 32
STEP = 16
AHEAD = 2
LEFT_PARTS, RIGHT_PARTS = (2, 0, 1, 1, 0, 0), (0, 2, 1, 0, 1, 0)
GROUP = 8
VMEM_BYTES = 67043328
F32, BF16 = jnp.float32, jnp.bfloat16
TN = (((0,), (0,)), ((), ()))
NT = (((1,), (1,)), ((), ()))

SLOTS = 8
KINDS = range(0, 17 * SLOTS, SLOTS)
AG_T, AG_A, AG_B, RELAY, RELAY_A, RS_T, RS_A, PAIR, GRAM_PAIR, GRAM_RS, GRAM_AG, LINV, MOVE, START, SWAP_Y, SWAP_H, DIAGONAL = KINDS
ORDER = (0, 2, 1, 3)
OFFSETS = sorted(
    ((dy, dx) for dy in range(RING) for dx in range(RING) if dy or dx),
    key=lambda o: -min(o[0], RING - o[0]) - min(o[1], RING - o[1]),
)


def split3(v):
    high = v.astype(BF16)
    rest = v - high.astype(F32)
    mid = rest.astype(BF16)
    return high, mid, (rest - mid.astype(F32)).astype(BF16)


def halves_dot(lhs, rhs, dims):
    axis = 1 - dims[0][0][0]
    size = lhs.shape[axis] // 2
    parts = [lax.slice_in_dim(lhs, i * size, (i + 1) * size, axis=axis) for i in range(2)]
    return jnp.concatenate([lax.dot_general(part, rhs, dims, preferred_element_type=F32) for part in parts], axis=0)


def dot_f32(lhs, rhs, dims):
    left, right = split3(lhs), split3(rhs)
    (lk,), (rk,) = dims[0]
    lhs = jnp.concatenate([left[i] for i in LEFT_PARTS], axis=lk)
    rhs = jnp.concatenate([right[i] for i in RIGHT_PARTS], axis=rk)
    return halves_dot(lhs, rhs, dims)


def gram_f32(v):
    high, mid, low = split3(v)
    mixed = halves_dot(jnp.concatenate([high, high], axis=0), jnp.concatenate([low, mid], axis=0), TN)
    return (halves_dot(mid, mid, TN) + (mixed + mixed.T)) + halves_dot(high, high, TN)


class Phases:
    def __init__(self):
        self.scope = None

    def __call__(self, name=None):
        if self.scope is not None:
            self.scope.__exit__(None, None, None)
        self.scope = None
        if name is not None:
            self.scope = jax.named_scope(name)
            self.scope.__enter__()


def rows_of(ref, part, parts=2):
    size = ref.shape[0] // parts
    return ref.at[pl.ds(part * size, size)]


def set_identity(work):
    width = work.shape[0]
    at_row = lax.broadcasted_iota(jnp.int32, (width, width), 0)
    at_col = lax.broadcasted_iota(jnp.int32, (width, width), 1)
    work[:, width : 2 * width] = jnp.where(at_row == at_col, 1.0, 0.0).astype(F32)


def inverse_factor(gram, diagonal, work, store):
    tile = gram.shape[1]
    width = 2 * tile
    at_row, at_col = (lax.broadcasted_iota(jnp.int32, (tile, tile), i) for i in range(2))
    packed = gram[0:tile]
    turned = packed.T
    work[0:tile, 0:tile] = jnp.where(at_row <= at_col, packed, turned)
    work[0:tile, tile:width] = gram[tile : 2 * tile]
    work[tile:width, tile:width] = jnp.where(at_row == at_col, diagonal, jnp.where(at_row > at_col, packed, turned))
    sub = lax.broadcasted_iota(jnp.int32, (GROUP, tile), 0)
    groups = PIVOTS // GROUP
    full = (GROUP, tile)

    def lane(row):
        return jnp.broadcast_to(row, full)

    for first in range(0, width, PIVOTS):
        near = first // tile
        gram_tiles = list(range(near, 2))
        tiles = gram_tiles + [2 + i for i in range(near + 1)]
        data = {
            t: [work[pl.ds(first + GROUP * g, GROUP), t * tile : (t + 1) * tile] for g in range(groups)] for t in tiles
        }
        pivots = [jnp.ones(full, F32) for _ in range(groups)]
        def spread_columns(start, end):
            at = first - near * tile
            return {
                j: {g: jnp.broadcast_to(data[near][g][:, at + j : at + j + 1], full) for g in range(j // GROUP, groups)}
                for j in range(start, end)
            }

        cols = spread_columns(0, STEP)
        for j in range(PIVOTS):
            if j == STEP - AHEAD:
                cols |= spread_columns(STEP, PIVOTS)
            gj, rj = divmod(j, GROUP)
            col = cols[j]
            pivot = lane(col[gj][rj : rj + 1])
            inv = 1.0 / pivot
            pivots[gj] = jnp.where(sub == rj, pivot, pivots[gj])
            for nxt in range(j + 1, PIVOTS if j >= STEP - AHEAD else STEP):
                gn, rn = divmod(nxt, GROUP)
                entry = lane(col[gn][rn : rn + 1])
                if nxt == j + 1:
                    for g in range(gn, groups):
                        cols[nxt][g] = cols[nxt][g] - (col[g] * entry) * inv
                else:
                    scaled = entry * inv
                    for g in range(gn, groups):
                        cols[nxt][g] = cols[nxt][g] - col[g] * scaled
            for g in range(gj, groups):
                factor = col[g] * inv
                if g == gj:
                    if rj == GROUP - 1:
                        continue
                    factor = jnp.where(sub > rj, factor, 0.0)
                for t in tiles:
                    data[t][g] = data[t][g] - factor * lane(data[t][gj][rj : rj + 1])
        scale = [lax.rsqrt(p) for p in pivots]
        for t in tiles:
            data[t] = [d * s for d, s in zip(data[t], scale, strict=True)]
        for t in tiles:
            if t >= 2:
                for g in range(groups):
                    store(first + GROUP * g, t - 2, data[t][g])
        nxt = first + PIVOTS
        if nxt == width:
            break
        parts = {t: split3(jnp.concatenate(data[t], axis=0)) for t in tiles}
        below = [t for t in gram_tiles if (t + 1) * tile > nxt]
        low = below[0] * tile
        lhs = jnp.concatenate([jnp.concatenate([parts[t][i] for i in LEFT_PARTS], axis=0) for t in below], axis=1)
        right_tiles = below + [t for t in tiles if t >= 2]
        rhs = jnp.concatenate([jnp.concatenate([parts[t][i] for i in RIGHT_PARTS], axis=0) for t in right_tiles], axis=1)
        upd = lax.dot_general(lhs, rhs, TN, preferred_element_type=F32)
        for n, t in enumerate(right_tiles):
            where = pl.ds(nxt, width - nxt), slice(t * tile, (t + 1) * tile)
            work[where] = work[where] - upd[nxt - low :, n * tile : (n + 1) * tile]


def kernel(
    sizes, left_op, left_start, right_op, right_start, x_out, h_out,
    ops, ycur, y_one, ag_t, ag_a, p_t, p_a, d_a, r_t, r_a, x_half, x_via, x_move, y_in, g_loc, g_pair, g_sum, g_in, g_red, g_all, h_all, d_all, work, linv,
    send, recv, load_sem,
):
    nrow, ncol, total_rows = sizes
    sub, width = ycur.shape[1:]
    tile, hsub = width // 2, sub // 2
    nchips = RING * RING
    y = lax.axis_index("row")
    c = lax.axis_index("col")
    x, k = lax.div(c, CORES), lax.rem(c, CORES)
    other = 1 - k
    xp, xm, xf = (lax.rem(x + d, RING) for d in (1, 3, 2))
    yp, ym, yf = (lax.rem(y + d, RING) for d in (1, 3, 2))

    def dev(row, chip, core):
        return {"row": row, "col": chip * CORES + core}

    partner = dev(y, x, other)

    def push(i, src, dst, to):
        return pltpu.make_async_remote_copy(
            src_ref=src, dst_ref=dst, send_sem=send.at[i], recv_sem=recv.at[i], device_id=to, device_id_type=pl.DeviceIdType.MESH
        )

    def spot(i):
        return lax.rem(i + RING - x, RING)

    def run(index, size):
        return pl.ds(pl.multiple_of(index * size, size), size)

    phase = Phases()
    phase("boot")
    barrier = pltpu.get_barrier_semaphore()
    here = y * ncol + c
    for o in range(1, nrow * ncol):
        there = lax.rem(here + o, nrow * ncol)
        pl.semaphore_signal(
            barrier, inc=1, device_id={"row": lax.div(there, ncol), "col": lax.rem(there, ncol)}, device_id_type=pl.DeviceIdType.MESH
        )

    starts = [
        pltpu.make_async_copy(left_start, ycur.at[0], load_sem.at[8]),
        pltpu.make_async_copy(right_start, ycur.at[1], load_sem.at[9]),
    ]
    loads_t, loads_a = [], []
    for n, (xi, yi) in enumerate(((x, y), (xm, ym), (xp, yp), (xf, yf))):
        take = run(xi, CORES * sub)
        loads_t.append(pltpu.make_async_copy(left_op.at[take], ops.at[0, take], load_sem.at[2 * n]))
        take = run(spot(yi), sub)
        loads_a.append(pltpu.make_async_copy(right_op.at[:, take], ops.at[1, :, take], load_sem.at[2 * n + 1]))
    for copy in starts + loads_t + loads_a:
        copy.start()

    shift = CORES * lax.rem(x, 2) + k
    behind = spot(y)
    up, down = lax.rem(y + shift, RING), lax.rem(y + RING - shift, RING)

    def move(i, src, dst, row, chip, core):
        stays = jnp.logical_and(row == y, jnp.logical_and(chip == x, core == k))
        return push(i, src, dst, dev(row, chip, core)), stays, src, dst

    def start_moves(*moves):
        for copy, stays, src, dst in moves:

            @pl.when(stays)
            def _():
                dst[...] = src[...]

            @pl.when(jnp.logical_not(stays))
            def _():
                copy.start()

    def end_moves(*moves):
        for copy, stays, _, _ in moves:

            @pl.when(jnp.logical_not(stays))
            def _():
                copy.wait()

    for copy in starts:
        copy.wait()
    for h in range(2):
        ag_t[x, h, k] = ycur[0, h * hsub : (h + 1) * hsub].T.astype(BF16)
    for h in range(2):
        x_half[0, h] = ycur[1, h * hsub : (h + 1) * hsub].astype(BF16)
    pl.semaphore_wait(barrier, nrow * ncol - 1)
    first_one = [move(MOVE + h, x_half.at[0, h], x_half.at[1, h], up, x, k) for h in range(2)]
    first_two = [move(MOVE + 2 + h, x_half.at[1, h], ag_a.at[y, h], y, down, lax.div(x, 2)) for h in range(2)]
    start_moves(*first_one)
    first_swap = [push(START + h, ag_t.at[x, h, k], ag_t.at[x, h, k], partner) for h in range(2)]
    for copy in first_swap:
        copy.start()
    phase()

    def piece_t(chip, h):
        return ag_t.at[chip, h]

    def gather_t():
        to_p, to_m = dev(y, xp, k), dev(y, xm, k)
        sends = [
            push(AG_T + n, piece_t(x, h), piece_t(x, h), to) for n, (h, to) in enumerate(((0, to_p), (1, to_p), (1, to_m), (0, to_m)))
        ]
        onward = [
            push(AG_T + 4, piece_t(xm, 0), piece_t(xm, 0), to_p),
            push(AG_T + 5, piece_t(xp, 1), piece_t(xp, 1), to_m),
        ]
        relays = [push(RELAY, ag_t.at[x], ag_t.at[x], partner)] + [
            push(RELAY + 1 + n, piece_t(i, h), piece_t(i, h), partner)
            for n, (i, h) in enumerate(((xm, 0), (xp, 1), (xm, 1), (xp, 0), (xf, 0), (xf, 1)))
        ]
        return sends, onward, relays

    def gather_a():
        routes = ((0, yp), (1, yp), (1, ym), (0, ym))
        sends = [push(AG_A + n, ag_a.at[y, h], ag_a.at[y, h], dev(i, x, k)) for n, (h, i) in enumerate(routes)]
        onward = [
            push(AG_A + 4, ag_a.at[ym, 0], ag_a.at[ym, 0], dev(yp, x, k)),
            push(AG_A + 5, ag_a.at[yp, 1], ag_a.at[yp, 1], dev(ym, x, k)),
        ]
        for_other = [
            pltpu.make_async_remote_copy(
                src_ref=x_half.at[0, h], dst_ref=ag_a.at[y, h], send_sem=send.at[AG_B + n], recv_sem=recv.at[AG_A + n],
                device_id=dev(i, x, other), device_id_type=pl.DeviceIdType.MESH,
            )
            for n, (h, i) in enumerate(routes)
        ]
        return sends, onward, for_other, push(RELAY_A, x_half.at[0], ag_a.at[y], partner)

    def ring_scatter(base, part, got, plus, minus, far, to):
        def half(i, h):
            return rows_of(part(i), h)

        return [
            push(base + 0, half(far, 0), got.at[0], to(plus)),
            push(base + 1, half(far, 1), got.at[1], to(minus)),
            push(base + 2, half(plus, 1), got.at[2], to(plus)),
            push(base + 3, half(minus, 0), got.at[3], to(minus)),
            push(base + 4, half(plus, 0), got.at[4], to(plus)),
            push(base + 5, half(minus, 1), got.at[5], to(minus)),
        ]

    step_one = [
        move(MOVE, ycur.at[0], x_via.at[0], up, x, k),
        move(MOVE + 1, ycur.at[1], x_via.at[1], y, CORES * k + lax.div(behind, 2), lax.rem(behind, 2)),
    ]
    step_two = []
    for h in range(2):
        rows = pl.ds(h * hsub, hsub)
        step_two += [
            move(MOVE + 2 + h, x_via.at[0, rows], x_move.at[0, rows], y, down, lax.div(x, 2)),
            move(MOVE + 4 + h, x_via.at[1, rows], x_move.at[1, rows], down, x, k),
        ]
    out_left = pltpu.make_async_copy(x_via.at[0], x_out.at[0], load_sem.at[0])
    out_right = pltpu.make_async_copy(x_move.at[1], x_out.at[1], load_sem.at[1])

    def share_linv(q):
        return push(LINV + q, linv.at[q, k], linv.at[q, k], partner)

    swap_y = push(SWAP_Y, ycur.at[other], y_in, partner)

    def apply(p):
        t = lax.rem(p, 2)
        a = 1 - t

        def mm_t(pieces, owner, first=False, cuts=1):
            size = sub // cuts
            for n in range(cuts):
                acc, lanes = None, slice(n * size, (n + 1) * size)
                for chip, h in pieces:
                    for core in range(CORES):
                        rows = run((chip * CORES + core) * 2 + h, hsub)
                        one = jnp.dot(ag_t[chip, h, core], ops[t, rows, run(spot(owner) * cuts + n, size)], preferred_element_type=F32)
                        acc = one if acc is None else acc + one
                p_t[owner, :, lanes] = acc if first else p_t[owner, :, lanes] + acc

        def mm_a(pieces, owner, first=False, cuts=1):
            size = sub // cuts
            for n in range(cuts):
                acc, rows = None, slice(n * size, (n + 1) * size)
                for i, h in pieces:
                    one = jnp.dot(ops[a, run(owner * cuts + n, size), run(spot(i) * 2 + h, hsub)], ag_a[i, h], preferred_element_type=F32)
                    acc = one if acc is None else acc + one
                p_a[owner, rows] = acc if first else p_a[owner, rows] + acc

        def loaded(copy):
            @pl.when(p == 0)
            def _():
                copy.wait()

        send_t, fwd_t, relays = gather_t()
        send_a, fwd_a, send_b, relay_a = gather_a()
        drives_t, drives_a = k == t, k == a
        own_y = [(y, 0), (y, 1)]
        phase("ag_own")

        @pl.when(p == 0)
        def _():
            for h in range(2):
                end_moves(first_one[h])
                start_moves(first_two[h])
            for copy in first_swap:
                copy.wait()

            @pl.when(drives_t)
            def _():
                for n in ORDER:
                    send_t[n].start()

        @pl.when(p > 0)
        def _():
            @pl.when(jnp.logical_not(drives_a))
            def _():
                relay_a.wait_recv()

            for owner in range(RING * CORES):
                mm_a(own_y, owner, True)

            @pl.when(jnp.logical_not(drives_t))
            def _():
                relays[0].wait_recv()

        loaded(loads_t[0])
        for owner in range(RING):
            mm_t([(x, 0), (x, 1)], owner, True)

        @pl.when(p == 0)
        def _():
            end_moves(first_two[0])
            send_a[0].start()
            send_a[3].start()
            end_moves(first_two[1])
            send_a[2].start()
            send_a[1].start()
            loads_a[0].wait()
            for owner in range(RING * CORES):
                mm_a(own_y, owner, True)

        def take_t(arrived, then):
            @pl.when(drives_t)
            def _():
                for copy, follow in zip(arrived, then):
                    copy.wait_recv()
                    for nxt in follow:
                        nxt.start()

        def relayed(*copies):
            @pl.when(jnp.logical_not(drives_t))
            def _():
                for copy in copies:
                    copy.wait_recv()

        phase("ag_wait1")
        take_t([send_t[n] for n in ORDER[:2]], zip(fwd_t, relays[1:3]))
        for n, copy in zip(ORDER, fwd_a):
            send_a[n].wait_recv()
            copy.start()

        @pl.when(p == SWEEPS)
        def _():
            start_moves(*step_two[2:])

        phase("mm_near1")
        loaded(loads_a[1])
        loaded(loads_a[2])
        for owner in range(RING * CORES):
            mm_a([(ym, 0), (yp, 1)], owner)
        relayed(*relays[1:3])
        loaded(loads_t[1])
        loaded(loads_t[2])
        for owner in range(RING):
            mm_t([(xm, 0), (xp, 1)], owner)
        phase("mm_near2")
        take_t([send_t[n] for n in ORDER[2:]], zip(relays[3:5]))
        for n in ORDER[2:]:
            send_a[n].wait_recv()
        for owner in range(RING * CORES):
            mm_a([(ym, 1), (yp, 0)], owner)
        relayed(*relays[3:5])
        for owner in range(RING):
            mm_t([(xm, 1), (xp, 0)], owner)
        phase("ag_far")
        take_t(fwd_t, zip(relays[5:]))
        for copy in fwd_a:
            copy.wait_recv()
        phase("mm_far")

        loaded(loads_a[3])
        pairs = []
        far_y = [(yf, 0), (yf, 1)]
        out_t = ring_scatter(RS_T, lambda i: p_t.at[i], r_t, yp, ym, yf, lambda i: dev(i, x, k))
        out_a = ring_scatter(RS_A, lambda i: p_a.at[i * CORES + k], r_a, xp, xm, xf, lambda i: dev(y, i, k))

        def pair(n, i, rows):
            pairs.append(push(PAIR + n, p_a.at[i * CORES + other, rows], d_a.at[i, rows], partner))
            pairs[n].start()

        def add_pair(n, i, rows):
            pairs[n].wait_recv()
            p_a[i * CORES + k, rows] = p_a[i * CORES + k, rows] + d_a[i, rows]

        every, half_rows = pl.ds(0, sub), [pl.ds(h * hsub, hsub) for h in range(2)]
        far_x = [(xf, 0), (xf, 1)]
        mm_a(far_y, xf * CORES + other, cuts=2)
        for h in range(2):
            pair(h, xf, half_rows[h])
        relayed(*relays[5:])
        loaded(loads_t[3])
        mm_t(far_x, yf, cuts=2)
        out_t[0].start()
        out_t[1].start()
        mm_a(far_y, xf * CORES + k, cuts=2)
        for h in range(2):
            add_pair(h, xf, half_rows[h])
            out_a[h].start()
        for n, i in enumerate((xp, xm, x)):
            mm_a(far_y, i * CORES + other)
        for n, i in enumerate((xp, xm, x)):
            pair(2 + n, i, every)
        mm_t(far_x, yp)
        mm_t(far_x, ym)
        out_t[2].start()
        out_t[3].start()
        for i in (xp, xm, x):
            mm_a(far_y, i * CORES + k)
        add_pair(2, xp, every)
        add_pair(3, xm, every)
        out_a[2].start()
        out_a[3].start()
        mm_t(far_x, y)
        phase("rs_mid")

        ht = width // 2
        out_t[0].wait_recv()
        p_t[yp, 0:ht] = p_t[yp, 0:ht] + r_t[0]
        out_t[4].start()
        out_t[1].wait_recv()
        p_t[ym, ht:width] = p_t[ym, ht:width] + r_t[1]
        out_t[5].start()
        out_a[0].wait_recv()
        kp, km, kk = xp * CORES + k, xm * CORES + k, x * CORES + k
        p_a[kp, 0:hsub] = p_a[kp, 0:hsub] + r_a[0]
        out_a[4].start()
        out_a[1].wait_recv()
        p_a[km, hsub:sub] = p_a[km, hsub:sub] + r_a[1]
        out_a[5].start()
        phase("rs_end")

        @pl.when(p == SWEEPS)
        def _():
            end_moves(*step_two)
            for q in range(2):
                share_linv(q).wait()
            for op in range(2):
                y_one[op] = dot_f32(x_move[op], linv[0, op], NT)
                x_move[op] = dot_f32(y_one[op], linv[1, op], NT)
            out_right.start()
            y_one[0] = dot_f32(ycur[0], linv[0, 0], NT)
            x_via[0] = dot_f32(y_one[0], linv[1, 0], NT)
            out_left.start()

        add_pair(4, x, every)
        for copy in out_t[2:] + out_a[2:]:
            copy.wait_recv()
        phase("rs_sum")
        ycur[t, :, 0:ht] = (p_t[y, 0:ht] + r_t[3] + r_t[4]).T
        ycur[t, :, ht:width] = (p_t[y, ht:width] + r_t[2] + r_t[5]).T
        ycur[a, 0:hsub] = p_a[kk, 0:hsub] + r_a[3] + r_a[4]
        ycur[a, hsub:sub] = p_a[kk, hsub:sub] + r_a[2] + r_a[5]
        phase("rs_drain")
        for copy in fwd_a + pairs + out_t + out_a:
            copy.wait_send()

        @pl.when(drives_t)
        def _():
            for copy in send_t + fwd_t + relays[1:]:
                copy.wait_send()

            @pl.when(p > 0)
            def _():
                relays[0].wait_send()

        @pl.when(jnp.logical_or(p == 0, drives_a))
        def _():
            for copy in send_a:
                copy.wait_send()

        @pl.when(jnp.logical_and(p > 0, drives_a))
        def _():
            for copy in send_b + [relay_a]:
                copy.wait_send()

        phase()

    def routes():
        for dy, dx in OFFSETS:
            to_y, to_x = (y, yp, yf, ym)[dy], (x, xp, xf, xm)[dx]
            yield dy * RING + dx, to_y * RING + to_x, to_y, to_x

    def pair_of(rows):
        return push(GRAM_PAIR, g_loc.at[other, pl.ds(0, rows)], g_pair.at[pl.ds(0, rows)], partner)

    def pair_sum(rows, local, behind=None):
        phase("ar_pair")
        local(other)
        pair = pair_of(rows)
        pair.start()
        local(k)
        pair.wait_recv()
        if behind is not None:
            behind.start()
        g_sum[0:rows] = g_loc[k, 0:rows] + g_pair[0:rows]
        phase()

    def all_reduce(rows, meanwhile=None):
        piece = rows // nchips

        def chunk(ref, q):
            return ref.at[pl.ds(pl.multiple_of(q * piece, GROUP), piece)]

        def count(copies):
            return g_all.at[pl.ds(0, copies * piece)]

        def await_copies(sem, copies):
            pltpu.make_async_copy(count(copies), count(copies), sem).wait()

        phase("ar_rs")
        mine = y * RING + x
        owner = CORES - 1

        def spread(o, q, to_y, to_x):
            pltpu.make_async_remote_copy(
                src_ref=chunk(g_sum, q), dst_ref=g_in.at[k, pl.ds(o * piece, piece)], send_sem=send.at[GRAM_RS],
                recv_sem=recv.at[GRAM_RS + k], device_id=dev(to_y, to_x, owner), device_id_type=pl.DeviceIdType.MESH,
            ).start()

        for route in routes():
            spread(*route)
        if meanwhile is not None:
            meanwhile()

        @pl.when(k == 0)
        def _():
            spread(0, mine, y, x)
            await_copies(send.at[GRAM_RS], nchips)
            phase("ar_ag")
            await_copies(recv.at[GRAM_AG], nchips)
            phase("ar_drain")

        @pl.when(k == 1)
        def _():
            def hand_out(i, src, q, to_y, to_x, core):
                pltpu.make_async_remote_copy(
                    src_ref=src, dst_ref=chunk(g_all, q), send_sem=send.at[GRAM_AG + i], recv_sem=recv.at[GRAM_AG],
                    device_id=dev(to_y, to_x, core), device_id_type=pl.DeviceIdType.MESH,
                ).start()

            await_copies(recv.at[GRAM_RS], nchips)
            total = g_in[0, 0:piece]
            for o in range(1, nchips):
                total = total + g_in[0, o * piece : (o + 1) * piece]
            g_red[0:piece] = total / total_rows
            for _, _, to_y, to_x in routes():
                hand_out(1, g_red.at[pl.ds(0, piece)], mine, to_y, to_x, 0)
            hand_out(1, g_red.at[pl.ds(0, piece)], mine, y, x, 0)
            phase("ar_ag")
            await_copies(recv.at[GRAM_RS + 1], nchips - 1)
            total = chunk(g_sum, mine)[...]
            for o in range(1, nchips):
                total = total + g_in[1, o * piece : (o + 1) * piece]
            chunk(g_all, mine)[...] = total / total_rows
            for _, _, to_y, to_x in routes():
                hand_out(0, chunk(g_all, mine), mine, to_y, to_x, 1)
            await_copies(recv.at[GRAM_AG], nchips - 1)
            phase("ar_drain")
            await_copies(send.at[GRAM_RS], nchips - 1)
            await_copies(send.at[GRAM_AG], nchips - 1)
            await_copies(send.at[GRAM_AG + 1], nchips)

        phase()

    corners = ((0, 0), (0, 1), (1, 1), (1, 0))

    def put_gram(into, full):
        at_row, at_col = (lax.broadcasted_iota(jnp.int32, (tile, tile), i) for i in range(2))
        low = full[tile:width, tile:width]
        into[0:tile] = jnp.where(at_row <= at_col, full[0:tile, 0:tile], low)
        into[tile : 2 * tile] = full[0:tile, tile:width]
        diagonal = jnp.sum(jnp.where(at_row == at_col, low, 0.0), axis=0, keepdims=True)
        into[2 * tile : 2 * tile + GROUP] = jnp.broadcast_to(diagonal, (GROUP, tile))

    def half_gram(op):
        half = ycur[op].astype(BF16)
        put_gram(g_loc.at[op], lax.dot_general(half, half, TN, preferred_element_type=F32))

    def normalize(p, q):
        @pl.when(q == 0)
        def _():
            pair_sum(2 * tile + GROUP, half_gram, swap_y)
            phase()

        @pl.when(q == 1)
        def _():
            phase("gram2")
            put_gram(g_sum, gram_f32(y_one[0]) + gram_f32(y_one[1]))
            phase()

        last = p == SWEEPS - 1

        def clear():
            own = d_all.at[q, y * RING + x]
            own[...] = g_sum[2 * tile : 2 * tile + 1]
            for _, _, to_y, to_x in routes():
                push(DIAGONAL + q, own, own, dev(to_y, to_x, k)).start()
            set_identity(work)
            linv[q, k, 0:tile, tile:width] = jnp.zeros((tile, tile), F32)


        all_reduce(2 * tile, clear)
        others = d_all.at[q, pl.ds(0, nchips - 1)]
        for sem in (recv, send):
            pltpu.make_async_copy(others, others, sem.at[DIAGONAL + q]).wait()

        @pl.when(q == 0)
        def _():
            pair_of(2 * tile + GROUP).wait_send()

        @pl.when(jnp.logical_and(last, q == 0))
        def _():
            start_moves(*step_one)

        @pl.when(jnp.logical_and(last, q == 1))
        def _():
            end_moves(*step_one)
            start_moves(*step_two[:2])

        phase("chol")

        def store(first, t, value):
            linv[q, k, pl.ds(first, GROUP), t * tile : (t + 1) * tile] = value

        diagonal = d_all[q, 0]
        for chip in range(1, nchips):
            diagonal = diagonal + d_all[q, chip]
        inverse_factor(g_all, diagonal / total_rows, work, store)
        phase("mul")

        @pl.when(last)
        def _():
            share_linv(q).start()

        @pl.when(q == 0)
        def _():
            swap_y.wait()
            both = jnp.concatenate([ycur[k], y_in[...]], axis=0)
            y_one[...] = dot_f32(both, linv[0, k], NT).reshape(y_one.shape)

        phase()

    def launch(p):
        t = lax.rem(p, 2)

        def new_x(i):
            d_a[i] = dot_f32(y_one[i], linv[1, k], NT)
            return [d_a[i, h * hsub : (h + 1) * hsub] for h in range(2)]

        phase("launch")

        @pl.when(k == t)
        def _():
            sends, _, relays = gather_t()
            for i, core in enumerate((k, other)):
                for h, rows in enumerate(new_x(i)):
                    ag_t[x, h, core] = rows.T.astype(BF16)
            for n in ORDER:
                sends[n].start()
            relays[0].start()

        @pl.when(k != t)
        def _():
            sends, _, for_other, relay_a = gather_a()
            for h, rows in enumerate(new_x(0)):
                ag_a[y, h] = rows.astype(BF16)
            for n in ORDER:
                sends[n].start()
            for h, rows in enumerate(new_x(1)):
                x_half[0, h] = rows.astype(BF16)
            for n in ORDER:
                for_other[n].start()
            relay_a.start()

        phase()

    def sweep(p, carry):
        apply(p)

        @pl.when(p < SWEEPS)
        def _():
            def one(q, carry):
                normalize(p, q)
                return carry

            lax.fori_loop(0, 2, one, 0)
            launch(p + 1)

        return carry

    lax.fori_loop(0, SWEEPS + 1, sweep, 0)

    def rayleigh(op):
        full = dot_f32(x_move[op], ycur[op], TN)
        for n, (i, j) in enumerate(corners):
            g_loc[op, n * tile : (n + 1) * tile] = full[i * tile : (i + 1) * tile, j * tile : (j + 1) * tile]

    pair_sum(4 * tile, rayleigh)
    all_reduce(4 * tile)
    pair_of(4 * tile).wait_send()
    phase("h_swap")
    swap = push(SWAP_H, g_all, h_all, partner)
    swap.start()
    swap.wait()
    for n, (i, j) in enumerate(corners):
        rows, at = slice(n * tile, (n + 1) * tile), (slice(i * tile, (i + 1) * tile), slice(j * tile, (j + 1) * tile))
        for op in range(2):
            h_out[(op, *at)] = jnp.where(k == op, g_all[rows], h_all[rows])
    out_left.wait()
    out_right.wait()
    phase()


def hand_over(x_ref, h_ref, left_x, left_h, right_x, right_h, x_buf, h_buf, sem_in, sem_out):
    size = x_buf.shape[1] // 2
    routes = []
    for op, (x_to, h_to) in enumerate(((left_x, left_h), (right_x, right_h))):
        for h in range(2):
            rows = pl.ds(h * size, size)
            routes.append((x_ref.at[op, rows], x_buf.at[op, rows], x_to.at[rows]))
        routes.append((h_ref.at[op], h_buf.at[op], h_to))
    come = [pltpu.make_async_copy(src, buf, sem_in.at[n]) for n, (src, buf, _) in enumerate(routes)]
    go = [pltpu.make_async_copy(buf, dst, sem_out.at[n]) for n, (_, buf, dst) in enumerate(routes)]
    for copy in come:
        copy.start()
    for copy, nxt in zip(come, go):
        copy.wait()
        nxt.start()
    for copy in go:
        copy.wait()


def solution(mesh):
    nrow, ncol = mesh.shape["row"], mesh.shape["col"]
    assert nrow == RING and ncol == RING * CORES

    def local_program(left_op, left_start, right_op, right_start):
        rows, cols = left_op.shape
        sub, width = left_start.shape
        tile = width // 2
        vmem = pltpu.VMEM
        dma = pltpu.SemaphoreType.DMA
        basis, ray = jax.ShapeDtypeStruct((sub, width), F32), jax.ShapeDtypeStruct((width, width), F32)
        both_x, both_h = pl.pallas_call(
            functools.partial(kernel, (nrow, ncol, rows * nrow)),
            out_shape=[jax.ShapeDtypeStruct((2, sub, width), F32), jax.ShapeDtypeStruct((2, width, width), F32)],
            in_specs=[pl.BlockSpec(memory_space=pl.ANY)] * 4,
            out_specs=[pl.BlockSpec(memory_space=pl.ANY), pl.BlockSpec(memory_space=vmem)],
            scratch_shapes=[
                vmem((2, rows, cols), BF16),
                vmem((2, sub, width), F32),
                vmem((2, sub, width), F32),
                vmem((RING, 2, CORES, width, sub // 2), BF16),
                vmem((nrow, 2, sub // 2, width), BF16),
                vmem((nrow, width, sub), F32),
                vmem((ncol, sub, width), F32),
                vmem((RING, sub, width), F32),
                vmem((6, width // 2, sub), F32),
                vmem((6, sub // 2, width), F32),
                vmem((2, 2, sub // 2, width), BF16),
                vmem((2, sub, width), F32),
                vmem((2, sub, width), F32),
                vmem((sub, width), F32),
                vmem((2, 4 * tile, tile), F32),
                vmem((4 * tile, tile), F32),
                vmem((4 * tile, tile), F32),
                vmem((2, 4 * tile, tile), F32),
                vmem((4 * tile // (RING * RING), tile), F32),
                vmem((4 * tile, tile), F32),
                vmem((4 * tile, tile), F32),
                vmem((2, RING * RING, 1, tile), F32),
                vmem((width, 2 * width), F32),
                vmem((2, 2, width, width), F32),
                dma((KINDS.stop,)),
                dma((KINDS.stop,)),
                dma((10,)),
            ],
            compiler_params=pltpu.CompilerParams(collective_id=0, has_side_effects=True, vmem_limit_bytes=VMEM_BYTES),
            name="subspace",
        )(left_op, left_start, right_op, right_start)
        anywhere = pl.BlockSpec(memory_space=pl.ANY)
        return pl.pallas_call(
            hand_over,
            out_shape=[basis, ray, basis, ray],
            in_specs=[anywhere] * 2,
            out_specs=[anywhere] * 4,
            scratch_shapes=[vmem((2, sub, width), F32), vmem((2, width, width), F32), dma((6,)), dma((6,))],
            name="hand_over",
        )(both_x, both_h)

    op_spec = P(("batch", "row"), "col")
    vec_spec = P(("batch", "row", "col"), None)
    small_spec = P("batch", None)
    return jax.shard_map(
        local_program,
        mesh=mesh,
        in_specs=(op_spec, vec_spec, op_spec, vec_spec),
        out_specs=(vec_spec, small_spec, vec_spec, small_spec),
        check_vma=False,
    )
```

```python
import functools

import jax
import jax.numpy as jnp
from jax import lax
from jax.experimental import pallas as pl
from jax.experimental.pallas import tpu as pltpu
from jax.sharding import PartitionSpec as P

SWEEPS = 4
CORES = 2
RING = 4
PIVOTS = 32
STEP = 16
AHEAD = 2
LEFT_PARTS, RIGHT_PARTS = (2, 0, 1, 1, 0, 0), (0, 2, 1, 0, 1, 0)
GROUP = 8
VMEM_BYTES = 67043328
F32, BF16 = jnp.float32, jnp.bfloat16
TN = (((0,), (0,)), ((), ()))
NT = (((1,), (1,)), ((), ()))

SLOTS = 8
KINDS = range(0, 17 * SLOTS, SLOTS)
AG_T, AG_A, AG_B, RELAY, RELAY_A, RS_T, RS_A, PAIR, GRAM_PAIR, GRAM_RS, GRAM_AG, LINV, MOVE, START, SWAP_Y, SWAP_H, DIAGONAL = KINDS
ORDER = (0, 2, 1, 3)
OFFSETS = sorted(
    ((dy, dx) for dy in range(RING) for dx in range(RING) if dy or dx),
    key=lambda o: -min(o[0], RING - o[0]) - min(o[1], RING - o[1]),
)


def split3(v):
    high = v.astype(BF16)
    rest = v - high.astype(F32)
    mid = rest.astype(BF16)
    return high, mid, (rest - mid.astype(F32)).astype(BF16)


def halves_dot(lhs, rhs, dims):
    axis = 1 - dims[0][0][0]
    size = lhs.shape[axis] // 2
    parts = [lax.slice_in_dim(lhs, i * size, (i + 1) * size, axis=axis) for i in range(2)]
    return jnp.concatenate([lax.dot_general(part, rhs, dims, preferred_element_type=F32) for part in parts], axis=0)


def dot_f32(lhs, rhs, dims):
    left, right = split3(lhs), split3(rhs)
    (lk,), (rk,) = dims[0]
    lhs = jnp.concatenate([left[i] for i in LEFT_PARTS], axis=lk)
    rhs = jnp.concatenate([right[i] for i in RIGHT_PARTS], axis=rk)
    return halves_dot(lhs, rhs, dims)


def gram_f32(v):
    high, mid, low = split3(v)
    mixed = halves_dot(jnp.concatenate([high, high], axis=0), jnp.concatenate([low, mid], axis=0), TN)
    return (halves_dot(mid, mid, TN) + (mixed + mixed.T)) + halves_dot(high, high, TN)


class Phases:
    def __init__(self):
        self.scope = None

    def __call__(self, name=None):
        if self.scope is not None:
            self.scope.__exit__(None, None, None)
        self.scope = None
        if name is not None:
            self.scope = jax.named_scope(name)
            self.scope.__enter__()


def rows_of(ref, part, parts=2):
    size = ref.shape[0] // parts
    return ref.at[pl.ds(part * size, size)]


def set_identity(work):
    width = work.shape[0]
    at_row = lax.broadcasted_iota(jnp.int32, (width, width), 0)
    at_col = lax.broadcasted_iota(jnp.int32, (width, width), 1)
    work[:, width : 2 * width] = jnp.where(at_row == at_col, 1.0, 0.0).astype(F32)


def inverse_factor(gram, diagonal, work, store):
    tile = gram.shape[1]
    width = 2 * tile
    at_row, at_col = (lax.broadcasted_iota(jnp.int32, (tile, tile), i) for i in range(2))
    packed = gram[0:tile]
    turned = packed.T
    work[0:tile, 0:tile] = jnp.where(at_row <= at_col, packed, turned)
    work[0:tile, tile:width] = gram[tile : 2 * tile]
    work[tile:width, tile:width] = jnp.where(at_row == at_col, diagonal, jnp.where(at_row > at_col, packed, turned))
    sub = lax.broadcasted_iota(jnp.int32, (GROUP, tile), 0)
    groups = PIVOTS // GROUP
    full = (GROUP, tile)

    def lane(row):
        return jnp.broadcast_to(row, full)

    for first in range(0, width, PIVOTS):
        near = first // tile
        gram_tiles = list(range(near, 2))
        tiles = gram_tiles + [2 + i for i in range(near + 1)]
        data = {
            t: [work[pl.ds(first + GROUP * g, GROUP), t * tile : (t + 1) * tile] for g in range(groups)] for t in tiles
        }
        roots = [jnp.ones(full, F32) for _ in range(groups)]
        def spread_columns(start, end):
            at = first - near * tile
            return {
                j: {g: jnp.broadcast_to(data[near][g][:, at + j : at + j + 1], full) for g in range(j // GROUP, groups)}
                for j in range(start, end)
            }

        cols = spread_columns(0, STEP)
        for j in range(PIVOTS):
            if j == STEP - AHEAD:
                cols |= spread_columns(STEP, PIVOTS)
            gj, rj = divmod(j, GROUP)
            col = cols[j]
            root = lax.rsqrt(lane(col[gj][rj : rj + 1]))
            roots[gj] = jnp.where(sub == rj, root, roots[gj])
            low = {g: col[g] * root for g in range(gj, groups)}
            for nxt in range(j + 1, PIVOTS if j >= STEP - AHEAD else STEP):
                gn, rn = divmod(nxt, GROUP)
                entry = lane(col[gn][rn : rn + 1]) * root
                for g in range(gn, groups):
                    cols[nxt][g] = cols[nxt][g] - low[g] * entry
            for g in range(gj, groups):
                factor = low[g] * root
                if g == gj:
                    if rj == GROUP - 1:
                        continue
                    factor = jnp.where(sub > rj, factor, 0.0)
                for t in tiles:
                    data[t][g] = data[t][g] - factor * lane(data[t][gj][rj : rj + 1])
        for t in tiles:
            data[t] = [d * s for d, s in zip(data[t], roots, strict=True)]
        for t in tiles:
            if t >= 2:
                for g in range(groups):
                    store(first + GROUP * g, t - 2, data[t][g])
        nxt = first + PIVOTS
        if nxt == width:
            break
        parts = {t: split3(jnp.concatenate(data[t], axis=0)) for t in tiles}
        below = [t for t in gram_tiles if (t + 1) * tile > nxt]
        low = below[0] * tile
        lhs = jnp.concatenate([jnp.concatenate([parts[t][i] for i in LEFT_PARTS], axis=0) for t in below], axis=1)
        right_tiles = below + [t for t in tiles if t >= 2]
        rhs = jnp.concatenate([jnp.concatenate([parts[t][i] for i in RIGHT_PARTS], axis=0) for t in right_tiles], axis=1)
        upd = lax.dot_general(lhs, rhs, TN, preferred_element_type=F32)
        for n, t in enumerate(right_tiles):
            where = pl.ds(nxt, width - nxt), slice(t * tile, (t + 1) * tile)
            work[where] = work[where] - upd[nxt - low :, n * tile : (n + 1) * tile]


def kernel(
    sizes, left_op, left_start, right_op, right_start, x_out, h_out,
    ops, ycur, y_one, ag_t, ag_a, p_t, p_a, d_a, r_t, r_a, x_half, x_via, x_move, y_in, g_loc, g_pair, g_sum, g_in, g_red, g_all, h_all, d_all, work, linv,
    send, recv, load_sem,
):
    nrow, ncol, total_rows = sizes
    sub, width = ycur.shape[1:]
    tile, hsub = width // 2, sub // 2
    nchips = RING * RING
    y = lax.axis_index("row")
    c = lax.axis_index("col")
    x, k = lax.div(c, CORES), lax.rem(c, CORES)
    other = 1 - k
    xp, xm, xf = (lax.rem(x + d, RING) for d in (1, 3, 2))
    yp, ym, yf = (lax.rem(y + d, RING) for d in (1, 3, 2))

    def dev(row, chip, core):
        return {"row": row, "col": chip * CORES + core}

    partner = dev(y, x, other)

    def push(i, src, dst, to):
        return pltpu.make_async_remote_copy(
            src_ref=src, dst_ref=dst, send_sem=send.at[i], recv_sem=recv.at[i], device_id=to, device_id_type=pl.DeviceIdType.MESH
        )

    def spot(i):
        return lax.rem(i + RING - x, RING)

    def run(index, size):
        return pl.ds(pl.multiple_of(index * size, size), size)

    phase = Phases()
    phase("boot")
    barrier = pltpu.get_barrier_semaphore()
    here = y * ncol + c
    for o in range(1, nrow * ncol):
        there = lax.rem(here + o, nrow * ncol)
        pl.semaphore_signal(
            barrier, inc=1, device_id={"row": lax.div(there, ncol), "col": lax.rem(there, ncol)}, device_id_type=pl.DeviceIdType.MESH
        )

    starts = [
        pltpu.make_async_copy(left_start, ycur.at[0], load_sem.at[8]),
        pltpu.make_async_copy(right_start, ycur.at[1], load_sem.at[9]),
    ]
    loads_t, loads_a = [], []
    for n, (xi, yi) in enumerate(((x, y), (xm, ym), (xp, yp), (xf, yf))):
        take = run(xi, CORES * sub)
        loads_t.append(pltpu.make_async_copy(left_op.at[take], ops.at[0, take], load_sem.at[2 * n]))
        take = run(spot(yi), sub)
        loads_a.append(pltpu.make_async_copy(right_op.at[:, take], ops.at[1, :, take], load_sem.at[2 * n + 1]))
    for copy in starts + loads_t + loads_a:
        copy.start()

    shift = CORES * lax.rem(x, 2) + k
    behind = spot(y)
    up, down = lax.rem(y + shift, RING), lax.rem(y + RING - shift, RING)

    def move(i, src, dst, row, chip, core):
        stays = jnp.logical_and(row == y, jnp.logical_and(chip == x, core == k))
        return push(i, src, dst, dev(row, chip, core)), stays, src, dst

    def start_moves(*moves):
        for copy, stays, src, dst in moves:

            @pl.when(stays)
            def _():
                dst[...] = src[...]

            @pl.when(jnp.logical_not(stays))
            def _():
                copy.start()

    def end_moves(*moves):
        for copy, stays, _, _ in moves:

            @pl.when(jnp.logical_not(stays))
            def _():
                copy.wait()

    for copy in starts:
        copy.wait()
    for h in range(2):
        ag_t[x, h, k] = ycur[0, h * hsub : (h + 1) * hsub].T.astype(BF16)
    for h in range(2):
        x_half[0, h] = ycur[1, h * hsub : (h + 1) * hsub].astype(BF16)
    pl.semaphore_wait(barrier, nrow * ncol - 1)
    first_one = [move(MOVE + h, x_half.at[0, h], x_half.at[1, h], up, x, k) for h in range(2)]
    first_two = [move(MOVE + 2 + h, x_half.at[1, h], ag_a.at[y, h], y, down, lax.div(x, 2)) for h in range(2)]
    start_moves(*first_one)
    first_swap = [push(START + h, ag_t.at[x, h, k], ag_t.at[x, h, k], partner) for h in range(2)]
    for copy in first_swap:
        copy.start()
    phase()

    def piece_t(chip, h):
        return ag_t.at[chip, h]

    def gather_t():
        to_p, to_m = dev(y, xp, k), dev(y, xm, k)
        sends = [
            push(AG_T + n, piece_t(x, h), piece_t(x, h), to) for n, (h, to) in enumerate(((0, to_p), (1, to_p), (1, to_m), (0, to_m)))
        ]
        onward = [
            push(AG_T + 4, piece_t(xm, 0), piece_t(xm, 0), to_p),
            push(AG_T + 5, piece_t(xp, 1), piece_t(xp, 1), to_m),
        ]
        relays = [push(RELAY, ag_t.at[x], ag_t.at[x], partner)] + [
            push(RELAY + 1 + n, piece_t(i, h), piece_t(i, h), partner)
            for n, (i, h) in enumerate(((xm, 0), (xp, 1), (xm, 1), (xp, 0), (xf, 0), (xf, 1)))
        ]
        return sends, onward, relays

    def gather_a():
        routes = ((0, yp), (1, yp), (1, ym), (0, ym))
        sends = [push(AG_A + n, ag_a.at[y, h], ag_a.at[y, h], dev(i, x, k)) for n, (h, i) in enumerate(routes)]
        onward = [
            push(AG_A + 4, ag_a.at[ym, 0], ag_a.at[ym, 0], dev(yp, x, k)),
            push(AG_A + 5, ag_a.at[yp, 1], ag_a.at[yp, 1], dev(ym, x, k)),
        ]
        for_other = [
            pltpu.make_async_remote_copy(
                src_ref=x_half.at[0, h], dst_ref=ag_a.at[y, h], send_sem=send.at[AG_B + n], recv_sem=recv.at[AG_A + n],
                device_id=dev(i, x, other), device_id_type=pl.DeviceIdType.MESH,
            )
            for n, (h, i) in enumerate(routes)
        ]
        return sends, onward, for_other, push(RELAY_A, x_half.at[0], ag_a.at[y], partner)

    def ring_scatter(base, part, got, plus, minus, far, to):
        def half(i, h):
            return rows_of(part(i), h)

        return [
            push(base + 0, half(far, 0), got.at[0], to(plus)),
            push(base + 1, half(far, 1), got.at[1], to(minus)),
            push(base + 2, half(plus, 1), got.at[2], to(plus)),
            push(base + 3, half(minus, 0), got.at[3], to(minus)),
            push(base + 4, half(plus, 0), got.at[4], to(plus)),
            push(base + 5, half(minus, 1), got.at[5], to(minus)),
        ]

    step_one = [
        move(MOVE, ycur.at[0], x_via.at[0], up, x, k),
        move(MOVE + 1, ycur.at[1], x_via.at[1], y, CORES * k + lax.div(behind, 2), lax.rem(behind, 2)),
    ]
    step_two = []
    for h in range(2):
        rows = pl.ds(h * hsub, hsub)
        step_two += [
            move(MOVE + 2 + h, x_via.at[0, rows], x_move.at[0, rows], y, down, lax.div(x, 2)),
            move(MOVE + 4 + h, x_via.at[1, rows], x_move.at[1, rows], down, x, k),
        ]
    out_left = pltpu.make_async_copy(x_via.at[0], x_out.at[0], load_sem.at[0])
    out_right = pltpu.make_async_copy(x_move.at[1], x_out.at[1], load_sem.at[1])

    def share_linv(q):
        return push(LINV + q, linv.at[q, k], linv.at[q, k], partner)

    swap_y = push(SWAP_Y, ycur.at[other], y_in, partner)

    def apply(p):
        t = lax.rem(p, 2)
        a = 1 - t

        def mm_t(pieces, owner, first=False, cuts=1):
            size = sub // cuts
            for n in range(cuts):
                acc, lanes = None, slice(n * size, (n + 1) * size)
                for chip, h in pieces:
                    for core in range(CORES):
                        rows = run((chip * CORES + core) * 2 + h, hsub)
                        one = jnp.dot(ag_t[chip, h, core], ops[t, rows, run(spot(owner) * cuts + n, size)], preferred_element_type=F32)
                        acc = one if acc is None else acc + one
                p_t[owner, :, lanes] = acc if first else p_t[owner, :, lanes] + acc

        def mm_a(pieces, owner, first=False, cuts=1):
            size = sub // cuts
            for n in range(cuts):
                acc, rows = None, slice(n * size, (n + 1) * size)
                for i, h in pieces:
                    one = jnp.dot(ops[a, run(owner * cuts + n, size), run(spot(i) * 2 + h, hsub)], ag_a[i, h], preferred_element_type=F32)
                    acc = one if acc is None else acc + one
                p_a[owner, rows] = acc if first else p_a[owner, rows] + acc

        def loaded(copy):
            @pl.when(p == 0)
            def _():
                copy.wait()

        send_t, fwd_t, relays = gather_t()
        send_a, fwd_a, send_b, relay_a = gather_a()
        drives_t, drives_a = k == t, k == a
        own_y = [(y, 0), (y, 1)]
        phase("ag_own")

        @pl.when(p == 0)
        def _():
            for h in range(2):
                end_moves(first_one[h])
                start_moves(first_two[h])
            for copy in first_swap:
                copy.wait()

            @pl.when(drives_t)
            def _():
                for n in ORDER:
                    send_t[n].start()

        @pl.when(p > 0)
        def _():
            @pl.when(jnp.logical_not(drives_a))
            def _():
                relay_a.wait_recv()

            for owner in range(RING * CORES):
                mm_a(own_y, owner, True)

            @pl.when(jnp.logical_not(drives_t))
            def _():
                relays[0].wait_recv()

        loaded(loads_t[0])
        for owner in range(RING):
            mm_t([(x, 0), (x, 1)], owner, True)

        @pl.when(p == 0)
        def _():
            end_moves(first_two[0])
            send_a[0].start()
            send_a[3].start()
            end_moves(first_two[1])
            send_a[2].start()
            send_a[1].start()
            loads_a[0].wait()
            for owner in range(RING * CORES):
                mm_a(own_y, owner, True)

        def take_t(arrived, then):
            @pl.when(drives_t)
            def _():
                for copy, follow in zip(arrived, then):
                    copy.wait_recv()
                    for nxt in follow:
                        nxt.start()

        def relayed(*copies):
            @pl.when(jnp.logical_not(drives_t))
            def _():
                for copy in copies:
                    copy.wait_recv()

        phase("ag_wait1")
        take_t([send_t[n] for n in ORDER[:2]], zip(fwd_t, relays[1:3]))
        for n, copy in zip(ORDER, fwd_a):
            send_a[n].wait_recv()
            copy.start()

        @pl.when(p == SWEEPS)
        def _():
            start_moves(*step_two[2:])

        phase("mm_near1")
        loaded(loads_a[1])
        loaded(loads_a[2])
        for owner in range(RING * CORES):
            mm_a([(ym, 0), (yp, 1)], owner)
        relayed(*relays[1:3])
        loaded(loads_t[1])
        loaded(loads_t[2])
        for owner in range(RING):
            mm_t([(xm, 0), (xp, 1)], owner)
        phase("mm_near2")
        take_t([send_t[n] for n in ORDER[2:]], zip(relays[3:5]))
        for n in ORDER[2:]:
            send_a[n].wait_recv()
        for owner in range(RING * CORES):
            mm_a([(ym, 1), (yp, 0)], owner)
        relayed(*relays[3:5])
        for owner in range(RING):
            mm_t([(xm, 1), (xp, 0)], owner)
        phase("ag_far")
        take_t(fwd_t, zip(relays[5:]))
        for copy in fwd_a:
            copy.wait_recv()
        phase("mm_far")

        loaded(loads_a[3])
        pairs = []
        far_y = [(yf, 0), (yf, 1)]
        out_t = ring_scatter(RS_T, lambda i: p_t.at[i], r_t, yp, ym, yf, lambda i: dev(i, x, k))
        out_a = ring_scatter(RS_A, lambda i: p_a.at[i * CORES + k], r_a, xp, xm, xf, lambda i: dev(y, i, k))

        def pair(n, i, rows):
            pairs.append(push(PAIR + n, p_a.at[i * CORES + other, rows], d_a.at[i, rows], partner))
            pairs[n].start()

        def add_pair(n, i, rows):
            pairs[n].wait_recv()
            p_a[i * CORES + k, rows] = p_a[i * CORES + k, rows] + d_a[i, rows]

        every, half_rows = pl.ds(0, sub), [pl.ds(h * hsub, hsub) for h in range(2)]
        far_x = [(xf, 0), (xf, 1)]
        mm_a(far_y, xf * CORES + other, cuts=2)
        for h in range(2):
            pair(h, xf, half_rows[h])
        relayed(*relays[5:])
        loaded(loads_t[3])
        mm_t(far_x, yf, cuts=2)
        out_t[0].start()
        out_t[1].start()
        mm_a(far_y, xf * CORES + k, cuts=2)
        for h in range(2):
            add_pair(h, xf, half_rows[h])
            out_a[h].start()
        for n, i in enumerate((xp, xm, x)):
            mm_a(far_y, i * CORES + other)
        for n, i in enumerate((xp, xm, x)):
            pair(2 + n, i, every)
        mm_t(far_x, yp)
        mm_t(far_x, ym)
        out_t[2].start()
        out_t[3].start()
        for i in (xp, xm, x):
            mm_a(far_y, i * CORES + k)
        add_pair(2, xp, every)
        add_pair(3, xm, every)
        out_a[2].start()
        out_a[3].start()
        mm_t(far_x, y)
        phase("rs_mid")

        ht = width // 2
        out_t[0].wait_recv()
        p_t[yp, 0:ht] = p_t[yp, 0:ht] + r_t[0]
        out_t[4].start()
        out_t[1].wait_recv()
        p_t[ym, ht:width] = p_t[ym, ht:width] + r_t[1]
        out_t[5].start()
        out_a[0].wait_recv()
        kp, km, kk = xp * CORES + k, xm * CORES + k, x * CORES + k
        p_a[kp, 0:hsub] = p_a[kp, 0:hsub] + r_a[0]
        out_a[4].start()
        out_a[1].wait_recv()
        p_a[km, hsub:sub] = p_a[km, hsub:sub] + r_a[1]
        out_a[5].start()
        phase("rs_end")

        @pl.when(p == SWEEPS)
        def _():
            end_moves(*step_two)
            for q in range(2):
                share_linv(q).wait()
            for op in range(2):
                y_one[op] = dot_f32(x_move[op], linv[0, op], NT)
                x_move[op] = dot_f32(y_one[op], linv[1, op], NT)
            out_right.start()
            y_one[0] = dot_f32(ycur[0], linv[0, 0], NT)
            x_via[0] = dot_f32(y_one[0], linv[1, 0], NT)
            out_left.start()

        add_pair(4, x, every)
        for copy in out_t[2:] + out_a[2:]:
            copy.wait_recv()
        phase("rs_sum")
        ycur[t, :, 0:ht] = (p_t[y, 0:ht] + r_t[3] + r_t[4]).T
        ycur[t, :, ht:width] = (p_t[y, ht:width] + r_t[2] + r_t[5]).T
        ycur[a, 0:hsub] = p_a[kk, 0:hsub] + r_a[3] + r_a[4]
        ycur[a, hsub:sub] = p_a[kk, hsub:sub] + r_a[2] + r_a[5]
        phase("rs_drain")
        for copy in fwd_a + pairs + out_t + out_a:
            copy.wait_send()

        @pl.when(drives_t)
        def _():
            for copy in send_t + fwd_t + relays[1:]:
                copy.wait_send()

            @pl.when(p > 0)
            def _():
                relays[0].wait_send()

        @pl.when(jnp.logical_or(p == 0, drives_a))
        def _():
            for copy in send_a:
                copy.wait_send()

        @pl.when(jnp.logical_and(p > 0, drives_a))
        def _():
            for copy in send_b + [relay_a]:
                copy.wait_send()

        phase()

    def routes():
        for dy, dx in OFFSETS:
            to_y, to_x = (y, yp, yf, ym)[dy], (x, xp, xf, xm)[dx]
            yield dy * RING + dx, to_y * RING + to_x, to_y, to_x

    def pair_of(rows):
        return push(GRAM_PAIR, g_loc.at[other, pl.ds(0, rows)], g_pair.at[pl.ds(0, rows)], partner)

    def pair_sum(rows, local, behind=None):
        phase("ar_pair")
        local(other)
        pair = pair_of(rows)
        pair.start()
        local(k)
        pair.wait_recv()
        if behind is not None:
            behind.start()
        g_sum[0:rows] = g_loc[k, 0:rows] + g_pair[0:rows]
        phase()

    def all_reduce(rows, meanwhile=None):
        piece = rows // nchips

        def chunk(ref, q):
            return ref.at[pl.ds(pl.multiple_of(q * piece, GROUP), piece)]

        def count(copies):
            return g_all.at[pl.ds(0, copies * piece)]

        def await_copies(sem, copies):
            pltpu.make_async_copy(count(copies), count(copies), sem).wait()

        phase("ar_rs")
        mine = y * RING + x
        owner = CORES - 1

        def spread(o, q, to_y, to_x):
            pltpu.make_async_remote_copy(
                src_ref=chunk(g_sum, q), dst_ref=g_in.at[k, pl.ds(o * piece, piece)], send_sem=send.at[GRAM_RS],
                recv_sem=recv.at[GRAM_RS + k], device_id=dev(to_y, to_x, owner), device_id_type=pl.DeviceIdType.MESH,
            ).start()

        for route in routes():
            spread(*route)
        if meanwhile is not None:
            meanwhile()

        @pl.when(k == 0)
        def _():
            spread(0, mine, y, x)
            await_copies(send.at[GRAM_RS], nchips)
            phase("ar_ag")
            await_copies(recv.at[GRAM_AG], nchips)
            phase("ar_drain")

        @pl.when(k == 1)
        def _():
            def hand_out(i, src, q, to_y, to_x, core):
                pltpu.make_async_remote_copy(
                    src_ref=src, dst_ref=chunk(g_all, q), send_sem=send.at[GRAM_AG + i], recv_sem=recv.at[GRAM_AG],
                    device_id=dev(to_y, to_x, core), device_id_type=pl.DeviceIdType.MESH,
                ).start()

            await_copies(recv.at[GRAM_RS], nchips)
            total = g_in[0, 0:piece]
            for o in range(1, nchips):
                total = total + g_in[0, o * piece : (o + 1) * piece]
            g_red[0:piece] = total / total_rows
            for _, _, to_y, to_x in routes():
                hand_out(1, g_red.at[pl.ds(0, piece)], mine, to_y, to_x, 0)
            hand_out(1, g_red.at[pl.ds(0, piece)], mine, y, x, 0)
            phase("ar_ag")
            await_copies(recv.at[GRAM_RS + 1], nchips - 1)
            total = chunk(g_sum, mine)[...]
            for o in range(1, nchips):
                total = total + g_in[1, o * piece : (o + 1) * piece]
            chunk(g_all, mine)[...] = total / total_rows
            for _, _, to_y, to_x in routes():
                hand_out(0, chunk(g_all, mine), mine, to_y, to_x, 1)
            await_copies(recv.at[GRAM_AG], nchips - 1)
            phase("ar_drain")
            await_copies(send.at[GRAM_RS], nchips - 1)
            await_copies(send.at[GRAM_AG], nchips - 1)
            await_copies(send.at[GRAM_AG + 1], nchips)

        phase()

    corners = ((0, 0), (0, 1), (1, 1), (1, 0))

    def put_gram(into, full):
        at_row, at_col = (lax.broadcasted_iota(jnp.int32, (tile, tile), i) for i in range(2))
        low = full[tile:width, tile:width]
        into[0:tile] = jnp.where(at_row <= at_col, full[0:tile, 0:tile], low)
        into[tile : 2 * tile] = full[0:tile, tile:width]
        diagonal = jnp.sum(jnp.where(at_row == at_col, low, 0.0), axis=0, keepdims=True)
        into[2 * tile : 2 * tile + GROUP] = jnp.broadcast_to(diagonal, (GROUP, tile))

    def half_gram(op):
        half = ycur[op].astype(BF16)
        put_gram(g_loc.at[op], lax.dot_general(half, half, TN, preferred_element_type=F32))

    def normalize(p, q):
        @pl.when(q == 0)
        def _():
            pair_sum(2 * tile + GROUP, half_gram, swap_y)
            phase()

        @pl.when(q == 1)
        def _():
            phase("gram2")
            put_gram(g_sum, gram_f32(y_one[0]) + gram_f32(y_one[1]))
            phase()

        last = p == SWEEPS - 1

        def clear():
            own = d_all.at[q, y * RING + x]
            own[...] = g_sum[2 * tile : 2 * tile + 1]
            for _, _, to_y, to_x in routes():
                push(DIAGONAL + q, own, own, dev(to_y, to_x, k)).start()
            set_identity(work)
            linv[q, k, 0:tile, tile:width] = jnp.zeros((tile, tile), F32)


        all_reduce(2 * tile, clear)
        others = d_all.at[q, pl.ds(0, nchips - 1)]
        for sem in (recv, send):
            pltpu.make_async_copy(others, others, sem.at[DIAGONAL + q]).wait()

        @pl.when(q == 0)
        def _():
            pair_of(2 * tile + GROUP).wait_send()

        @pl.when(jnp.logical_and(last, q == 0))
        def _():
            start_moves(*step_one)

        @pl.when(jnp.logical_and(last, q == 1))
        def _():
            end_moves(*step_one)
            start_moves(*step_two[:2])

        phase("chol")

        def store(first, t, value):
            linv[q, k, pl.ds(first, GROUP), t * tile : (t + 1) * tile] = value

        diagonal = d_all[q, 0]
        for chip in range(1, nchips):
            diagonal = diagonal + d_all[q, chip]
        inverse_factor(g_all, diagonal / total_rows, work, store)
        phase("mul")

        @pl.when(last)
        def _():
            share_linv(q).start()

        @pl.when(q == 0)
        def _():
            swap_y.wait()
            both = jnp.concatenate([ycur[k], y_in[...]], axis=0)
            y_one[...] = dot_f32(both, linv[0, k], NT).reshape(y_one.shape)

        phase()

    def launch(p):
        t = lax.rem(p, 2)

        def new_x(i):
            d_a[i] = dot_f32(y_one[i], linv[1, k], NT)
            return [d_a[i, h * hsub : (h + 1) * hsub] for h in range(2)]

        phase("launch")

        @pl.when(k == t)
        def _():
            sends, _, relays = gather_t()
            for i, core in enumerate((k, other)):
                for h, rows in enumerate(new_x(i)):
                    ag_t[x, h, core] = rows.T.astype(BF16)
            for n in ORDER:
                sends[n].start()
            relays[0].start()

        @pl.when(k != t)
        def _():
            sends, _, for_other, relay_a = gather_a()
            for h, rows in enumerate(new_x(0)):
                ag_a[y, h] = rows.astype(BF16)
            for n in ORDER:
                sends[n].start()
            for h, rows in enumerate(new_x(1)):
                x_half[0, h] = rows.astype(BF16)
            for n in ORDER:
                for_other[n].start()
            relay_a.start()

        phase()

    def sweep(p, carry):
        apply(p)

        @pl.when(p < SWEEPS)
        def _():
            def one(q, carry):
                normalize(p, q)
                return carry

            lax.fori_loop(0, 2, one, 0)
            launch(p + 1)

        return carry

    lax.fori_loop(0, SWEEPS + 1, sweep, 0)

    def rayleigh(op):
        full = dot_f32(x_move[op], ycur[op], TN)
        for n, (i, j) in enumerate(corners):
            g_loc[op, n * tile : (n + 1) * tile] = full[i * tile : (i + 1) * tile, j * tile : (j + 1) * tile]

    pair_sum(4 * tile, rayleigh)
    all_reduce(4 * tile)
    pair_of(4 * tile).wait_send()
    phase("h_swap")
    swap = push(SWAP_H, g_all, h_all, partner)
    swap.start()
    swap.wait()
    for n, (i, j) in enumerate(corners):
        rows, at = slice(n * tile, (n + 1) * tile), (slice(i * tile, (i + 1) * tile), slice(j * tile, (j + 1) * tile))
        for op in range(2):
            h_out[(op, *at)] = jnp.where(k == op, g_all[rows], h_all[rows])
    out_left.wait()
    out_right.wait()
    phase()


def hand_over(x_ref, h_ref, left_x, left_h, right_x, right_h, x_buf, h_buf, sem_in, sem_out):
    size = x_buf.shape[1] // 2
    routes = []
    for op, (x_to, h_to) in enumerate(((left_x, left_h), (right_x, right_h))):
        for h in range(2):
            rows = pl.ds(h * size, size)
            routes.append((x_ref.at[op, rows], x_buf.at[op, rows], x_to.at[rows]))
        routes.append((h_ref.at[op], h_buf.at[op], h_to))
    come = [pltpu.make_async_copy(src, buf, sem_in.at[n]) for n, (src, buf, _) in enumerate(routes)]
    go = [pltpu.make_async_copy(buf, dst, sem_out.at[n]) for n, (_, buf, dst) in enumerate(routes)]
    for copy in come:
        copy.start()
    for copy, nxt in zip(come, go):
        copy.wait()
        nxt.start()
    for copy in go:
        copy.wait()


def solution(mesh):
    nrow, ncol = mesh.shape["row"], mesh.shape["col"]
    assert nrow == RING and ncol == RING * CORES

    def local_program(left_op, left_start, right_op, right_start):
        rows, cols = left_op.shape
        sub, width = left_start.shape
        tile = width // 2
        vmem = pltpu.VMEM
        dma = pltpu.SemaphoreType.DMA
        basis, ray = jax.ShapeDtypeStruct((sub, width), F32), jax.ShapeDtypeStruct((width, width), F32)
        both_x, both_h = pl.pallas_call(
            functools.partial(kernel, (nrow, ncol, rows * nrow)),
            out_shape=[jax.ShapeDtypeStruct((2, sub, width), F32), jax.ShapeDtypeStruct((2, width, width), F32)],
            in_specs=[pl.BlockSpec(memory_space=pl.ANY)] * 4,
            out_specs=[pl.BlockSpec(memory_space=pl.ANY), pl.BlockSpec(memory_space=vmem)],
            scratch_shapes=[
                vmem((2, rows, cols), BF16),
                vmem((2, sub, width), F32),
                vmem((2, sub, width), F32),
                vmem((RING, 2, CORES, width, sub // 2), BF16),
                vmem((nrow, 2, sub // 2, width), BF16),
                vmem((nrow, width, sub), F32),
                vmem((ncol, sub, width), F32),
                vmem((RING, sub, width), F32),
                vmem((6, width // 2, sub), F32),
                vmem((6, sub // 2, width), F32),
                vmem((2, 2, sub // 2, width), BF16),
                vmem((2, sub, width), F32),
                vmem((2, sub, width), F32),
                vmem((sub, width), F32),
                vmem((2, 4 * tile, tile), F32),
                vmem((4 * tile, tile), F32),
                vmem((4 * tile, tile), F32),
                vmem((2, 4 * tile, tile), F32),
                vmem((4 * tile // (RING * RING), tile), F32),
                vmem((4 * tile, tile), F32),
                vmem((4 * tile, tile), F32),
                vmem((2, RING * RING, 1, tile), F32),
                vmem((width, 2 * width), F32),
                vmem((2, 2, width, width), F32),
                dma((KINDS.stop,)),
                dma((KINDS.stop,)),
                dma((10,)),
            ],
            compiler_params=pltpu.CompilerParams(collective_id=0, has_side_effects=True, vmem_limit_bytes=VMEM_BYTES),
            name="subspace",
        )(left_op, left_start, right_op, right_start)
        anywhere = pl.BlockSpec(memory_space=pl.ANY)
        return pl.pallas_call(
            hand_over,
            out_shape=[basis, ray, basis, ray],
            in_specs=[anywhere] * 2,
            out_specs=[anywhere] * 4,
            scratch_shapes=[vmem((2, sub, width), F32), vmem((2, width, width), F32), dma((6,)), dma((6,))],
            name="hand_over",
        )(both_x, both_h)

    op_spec = P(("batch", "row"), "col")
    vec_spec = P(("batch", "row", "col"), None)
    small_spec = P("batch", None)
    return jax.shard_map(
        local_program,
        mesh=mesh,
        in_specs=(op_spec, vec_spec, op_spec, vec_spec),
        out_specs=(vec_spec, small_spec, vec_spec, small_spec),
        check_vma=False,
    )
```

```python
import functools

import jax
import jax.numpy as jnp
from jax import lax
from jax.experimental import pallas as pl
from jax.experimental.pallas import tpu as pltpu
from jax.sharding import PartitionSpec as P

SWEEPS = 4
CORES = 2
RING = 4
PIVOTS = 32
STEP = 16
AHEAD = 2
LEFT_PARTS, RIGHT_PARTS = (2, 0, 1, 1, 0, 0), (0, 2, 1, 0, 1, 0)
GROUP = 8
VMEM_BYTES = 67043328
F32, BF16 = jnp.float32, jnp.bfloat16
TN = (((0,), (0,)), ((), ()))
NT = (((1,), (1,)), ((), ()))

SLOTS = 8
KINDS = range(0, 19 * SLOTS, SLOTS)
AG_T, AG_A, AG_B, RELAY, RELAY_A, RS_T, RS_A, PAIR, GRAM_PAIR, GRAM_RS, GRAM_AG, LINV, MOVE, START, SWAP_Y, SWAP_H, DIAGONAL, ON_T, ON_A = KINDS
ORDER = (0, 2, 1, 3)
OFFSETS = sorted(
    ((dy, dx) for dy in range(RING) for dx in range(RING) if dy or dx),
    key=lambda o: -min(o[0], RING - o[0]) - min(o[1], RING - o[1]),
)


def split3(v):
    high = v.astype(BF16)
    rest = v - high.astype(F32)
    mid = rest.astype(BF16)
    return high, mid, (rest - mid.astype(F32)).astype(BF16)


def halves_dot(lhs, rhs, dims):
    axis = 1 - dims[0][0][0]
    size = lhs.shape[axis] // 2
    parts = [lax.slice_in_dim(lhs, i * size, (i + 1) * size, axis=axis) for i in range(2)]
    return jnp.concatenate([lax.dot_general(part, rhs, dims, preferred_element_type=F32) for part in parts], axis=0)


def dot_f32(lhs, rhs, dims):
    left, right = split3(lhs), split3(rhs)
    (lk,), (rk,) = dims[0]
    lhs = jnp.concatenate([left[i] for i in LEFT_PARTS], axis=lk)
    rhs = jnp.concatenate([right[i] for i in RIGHT_PARTS], axis=rk)
    return halves_dot(lhs, rhs, dims)


def gram_f32(v):
    high, mid, low = split3(v)
    mixed = halves_dot(jnp.concatenate([high, high], axis=0), jnp.concatenate([low, mid], axis=0), TN)
    return (halves_dot(mid, mid, TN) + (mixed + mixed.T)) + halves_dot(high, high, TN)


class Phases:
    def __init__(self):
        self.scope = None

    def __call__(self, name=None):
        if self.scope is not None:
            self.scope.__exit__(None, None, None)
        self.scope = None
        if name is not None:
            self.scope = jax.named_scope(name)
            self.scope.__enter__()


def rows_of(ref, part, parts=2):
    size = ref.shape[0] // parts
    return ref.at[pl.ds(part * size, size)]


def set_identity(work):
    width = work.shape[0]
    at_row = lax.broadcasted_iota(jnp.int32, (width, width), 0)
    at_col = lax.broadcasted_iota(jnp.int32, (width, width), 1)
    work[:, width : 2 * width] = jnp.where(at_row == at_col, 1.0, 0.0).astype(F32)


def inverse_factor(gram, diagonal, work, store):
    tile = gram.shape[1]
    width = 2 * tile
    at_row, at_col = (lax.broadcasted_iota(jnp.int32, (tile, tile), i) for i in range(2))
    packed = gram[0:tile]
    turned = packed.T
    work[0:tile, 0:tile] = jnp.where(at_row <= at_col, packed, turned)
    work[0:tile, tile:width] = gram[tile : 2 * tile]
    work[tile:width, tile:width] = jnp.where(at_row == at_col, diagonal, jnp.where(at_row > at_col, packed, turned))
    sub = lax.broadcasted_iota(jnp.int32, (GROUP, tile), 0)
    groups = PIVOTS // GROUP
    full = (GROUP, tile)

    def lane(row):
        return jnp.broadcast_to(row, full)

    for first in range(0, width, PIVOTS):
        near = first // tile
        gram_tiles = list(range(near, 2))
        tiles = gram_tiles + [2 + i for i in range(near + 1)]
        data = {
            t: [work[pl.ds(first + GROUP * g, GROUP), t * tile : (t + 1) * tile] for g in range(groups)] for t in tiles
        }
        roots = [jnp.ones(full, F32) for _ in range(groups)]
        def spread_columns(start, end):
            at = first - near * tile
            return {
                j: {g: jnp.broadcast_to(data[near][g][:, at + j : at + j + 1], full) for g in range(j // GROUP, groups)}
                for j in range(start, end)
            }

        cols = spread_columns(0, STEP)
        for j in range(PIVOTS):
            if j == STEP - AHEAD:
                cols |= spread_columns(STEP, PIVOTS)
            gj, rj = divmod(j, GROUP)
            col = cols[j]
            root = lax.rsqrt(lane(col[gj][rj : rj + 1]))
            roots[gj] = jnp.where(sub == rj, root, roots[gj])
            low = {g: col[g] * root for g in range(gj, groups)}
            for nxt in range(j + 1, PIVOTS if j >= STEP - AHEAD else STEP):
                gn, rn = divmod(nxt, GROUP)
                entry = lane(col[gn][rn : rn + 1]) * root
                for g in range(gn, groups):
                    cols[nxt][g] = cols[nxt][g] - low[g] * entry
            for g in range(gj, groups):
                factor = low[g] * root
                if g == gj:
                    if rj == GROUP - 1:
                        continue
                    factor = jnp.where(sub > rj, factor, 0.0)
                for t in tiles:
                    data[t][g] = data[t][g] - factor * lane(data[t][gj][rj : rj + 1])
        for t in tiles:
            data[t] = [d * s for d, s in zip(data[t], roots, strict=True)]
        for t in tiles:
            if t >= 2:
                for g in range(groups):
                    store(first + GROUP * g, t - 2, data[t][g])
        nxt = first + PIVOTS
        if nxt == width:
            break
        parts = {t: split3(jnp.concatenate(data[t], axis=0)) for t in tiles}
        below = [t for t in gram_tiles if (t + 1) * tile > nxt]
        low = below[0] * tile
        lhs = jnp.concatenate([jnp.concatenate([parts[t][i] for i in LEFT_PARTS], axis=0) for t in below], axis=1)
        right_tiles = below + [t for t in tiles if t >= 2]
        rhs = jnp.concatenate([jnp.concatenate([parts[t][i] for i in RIGHT_PARTS], axis=0) for t in right_tiles], axis=1)
        upd = lax.dot_general(lhs, rhs, TN, preferred_element_type=F32)
        for n, t in enumerate(right_tiles):
            where = pl.ds(nxt, width - nxt), slice(t * tile, (t + 1) * tile)
            work[where] = work[where] - upd[nxt - low :, n * tile : (n + 1) * tile]


def kernel(
    sizes, left_op, left_start, right_op, right_start, x_out, h_out,
    ops, ycur, y_one, ag_t, ag_a, p_t, p_a, d_a, r_t, r_a, x_half, x_via, x_move, y_in, g_loc, g_pair, g_sum, g_in, g_red, g_all, h_all, d_all, work, linv,
    send, recv, load_sem,
):
    nrow, ncol, total_rows = sizes
    sub, width = ycur.shape[1:]
    tile, hsub = width // 2, sub // 2
    nchips = RING * RING
    y = lax.axis_index("row")
    c = lax.axis_index("col")
    x, k = lax.div(c, CORES), lax.rem(c, CORES)
    other = 1 - k
    xp, xm, xf = (lax.rem(x + d, RING) for d in (1, 3, 2))
    yp, ym, yf = (lax.rem(y + d, RING) for d in (1, 3, 2))

    def dev(row, chip, core):
        return {"row": row, "col": chip * CORES + core}

    partner = dev(y, x, other)

    def push(i, src, dst, to):
        return pltpu.make_async_remote_copy(
            src_ref=src, dst_ref=dst, send_sem=send.at[i], recv_sem=recv.at[i], device_id=to, device_id_type=pl.DeviceIdType.MESH
        )

    def spot(i):
        return lax.rem(i + RING - x, RING)

    def run(index, size):
        return pl.ds(pl.multiple_of(index * size, size), size)

    phase = Phases()
    phase("boot")
    def routes():
        for dy, dx in OFFSETS:
            to_y, to_x = (y, yp, yf, ym)[dy], (x, xp, xf, xm)[dx]
            yield dy * RING + dx, to_y * RING + to_x, to_y, to_x

    barrier = pltpu.get_barrier_semaphore()
    peers = [dev(to_y, to_x, core) for _, _, to_y, to_x in routes() for core in range(CORES)] + [partner]
    for peer in peers:
        pl.semaphore_signal(barrier, inc=1, device_id=peer, device_id_type=pl.DeviceIdType.MESH)

    starts = [
        pltpu.make_async_copy(left_start, ycur.at[0], load_sem.at[8]),
        pltpu.make_async_copy(right_start, ycur.at[1], load_sem.at[9]),
    ]
    loads_t, loads_a = [], []
    for n, (xi, yi) in enumerate(((x, y), (xm, ym), (xp, yp), (xf, yf))):
        take = run(xi, CORES * sub)
        loads_t.append(pltpu.make_async_copy(left_op.at[take], ops.at[0, take], load_sem.at[2 * n]))
        take = run(spot(yi), sub)
        loads_a.append(pltpu.make_async_copy(right_op.at[:, take], ops.at[1, :, take], load_sem.at[2 * n + 1]))
    for copy in starts + loads_t + loads_a:
        copy.start()

    shift = CORES * lax.rem(x, 2) + k
    behind = spot(y)
    up, down = lax.rem(y + shift, RING), lax.rem(y + RING - shift, RING)

    def move(i, src, dst, row, chip, core):
        stays = jnp.logical_and(row == y, jnp.logical_and(chip == x, core == k))
        return push(i, src, dst, dev(row, chip, core)), stays, src, dst

    def start_moves(*moves):
        for copy, stays, src, dst in moves:

            @pl.when(stays)
            def _():
                dst[...] = src[...]

            @pl.when(jnp.logical_not(stays))
            def _():
                copy.start()

    def end_moves(*moves):
        for copy, stays, _, _ in moves:

            @pl.when(jnp.logical_not(stays))
            def _():
                copy.wait()

    for copy in starts:
        copy.wait()
    for h in range(2):
        ag_t[x, h, k] = ycur[0, h * hsub : (h + 1) * hsub].T.astype(BF16)
    for h in range(2):
        x_half[0, h] = ycur[1, h * hsub : (h + 1) * hsub].astype(BF16)
    pl.semaphore_wait(barrier, len(peers))
    first_one = [move(MOVE + h, x_half.at[0, h], x_half.at[1, h], up, x, k) for h in range(2)]
    first_two = [move(MOVE + 2 + h, x_half.at[1, h], ag_a.at[y, h], y, down, lax.div(x, 2)) for h in range(2)]
    start_moves(*first_one)
    first_swap = [push(START + h, ag_t.at[x, h, k], ag_t.at[x, h, k], partner) for h in range(2)]
    for copy in first_swap:
        copy.start()
    phase()

    def piece_t(chip, h):
        return ag_t.at[chip, h]

    def start_all(copies):
        for n in ORDER:
            for copy in copies[n]:
                copy.start()

    def gather_t():
        to_p, to_m = dev(y, xp, k), dev(y, xm, k)

        def parts(kind, n, chip, h, to):
            pieces = [ag_t.at[chip, h, core] for core in (k, other)]
            return [push(kind + CORES * n + part, piece, piece, to) for part, piece in enumerate(pieces)]

        sends = [parts(AG_T, n, x, h, to) for n, (h, to) in enumerate(((0, to_p), (1, to_p), (1, to_m), (0, to_m)))]
        onward = [parts(ON_T, 0, xm, 0, to_p), parts(ON_T, 1, xp, 1, to_m)]
        relays = [push(RELAY, ag_t.at[x], ag_t.at[x], partner)] + [
            push(RELAY + 1 + n, piece_t(i, h), piece_t(i, h), partner)
            for n, (i, h) in enumerate(((xm, 0), (xp, 1), (xm, 1), (xp, 0), (xf, 0), (xf, 1)))
        ]
        return sends, onward, relays

    def gather_a():
        def parts(kind, took, n, src, i, h, row, core):
            pieces = [pl.ds(part * hsub // 2, hsub // 2) for part in range(2)]
            return [
                pltpu.make_async_remote_copy(
                    src_ref=src.at[h, rows], dst_ref=ag_a.at[i, h, rows], send_sem=send.at[kind + 2 * n + part],
                    recv_sem=recv.at[took + 2 * n + part], device_id=dev(row, x, core), device_id_type=pl.DeviceIdType.MESH,
                )
                for part, rows in enumerate(pieces)
            ]

        routes = ((0, yp), (1, yp), (1, ym), (0, ym))
        sends = [parts(AG_A, AG_A, n, ag_a.at[y], y, h, row, k) for n, (h, row) in enumerate(routes)]
        for_other = [parts(AG_B, AG_A, n, x_half.at[0], y, h, row, other) for n, (h, row) in enumerate(routes)]
        onward = [parts(ON_A, ON_A, 0, ag_a.at[ym], ym, 0, yp, k), parts(ON_A, ON_A, 1, ag_a.at[yp], yp, 1, ym, k)]
        return sends, onward, for_other, push(RELAY_A, x_half.at[0], ag_a.at[y], partner)

    def ring_scatter(base, part, got, plus, minus, far, to):
        def half(i, h):
            return rows_of(part(i), h)

        return [
            push(base + 0, half(far, 0), got.at[0], to(plus)),
            push(base + 1, half(far, 1), got.at[1], to(minus)),
            push(base + 2, half(plus, 1), got.at[2], to(plus)),
            push(base + 3, half(minus, 0), got.at[3], to(minus)),
            push(base + 4, half(plus, 0), got.at[4], to(plus)),
            push(base + 5, half(minus, 1), got.at[5], to(minus)),
        ]

    step_one = [
        move(MOVE, ycur.at[0], x_via.at[0], up, x, k),
        move(MOVE + 1, ycur.at[1], x_via.at[1], y, CORES * k + lax.div(behind, 2), lax.rem(behind, 2)),
    ]
    step_two = []
    for h in range(2):
        rows = pl.ds(h * hsub, hsub)
        step_two += [
            move(MOVE + 2 + h, x_via.at[0, rows], x_move.at[0, rows], y, down, lax.div(x, 2)),
            move(MOVE + 4 + h, x_via.at[1, rows], x_move.at[1, rows], down, x, k),
        ]
    out_left = pltpu.make_async_copy(x_via.at[0], x_out.at[0], load_sem.at[0])
    out_right = pltpu.make_async_copy(x_move.at[1], x_out.at[1], load_sem.at[1])

    def share_linv(q):
        return push(LINV + q, linv.at[q, k], linv.at[q, k], partner)

    swap_y = push(SWAP_Y, ycur.at[other], y_in, partner)

    def apply(p):
        t = lax.rem(p, 2)
        a = 1 - t

        def mm_t(pieces, owner, first=False, cuts=1):
            size = sub // cuts
            for n in range(cuts):
                acc, lanes = None, slice(n * size, (n + 1) * size)
                for chip, h in pieces:
                    for core in range(CORES):
                        rows = run((chip * CORES + core) * 2 + h, hsub)
                        one = jnp.dot(ag_t[chip, h, core], ops[t, rows, run(spot(owner) * cuts + n, size)], preferred_element_type=F32)
                        acc = one if acc is None else acc + one
                p_t[owner, :, lanes] = acc if first else p_t[owner, :, lanes] + acc

        def mm_a(pieces, owner, first=False, cuts=1):
            size = sub // cuts
            for n in range(cuts):
                acc, rows = None, slice(n * size, (n + 1) * size)
                for i, h in pieces:
                    one = jnp.dot(ops[a, run(owner * cuts + n, size), run(spot(i) * 2 + h, hsub)], ag_a[i, h], preferred_element_type=F32)
                    acc = one if acc is None else acc + one
                p_a[owner, rows] = acc if first else p_a[owner, rows] + acc

        def loaded(copy):
            @pl.when(p == 0)
            def _():
                copy.wait()

        send_t, fwd_t, relays = gather_t()
        send_a, fwd_a, send_b, relay_a = gather_a()
        drives_t, drives_a = k == t, k == a
        own_y = [(y, 0), (y, 1)]
        phase("ag_own")

        @pl.when(p == 0)
        def _():
            for h in range(2):
                end_moves(first_one[h])
                start_moves(first_two[h])
            for copy in first_swap:
                copy.wait()

            @pl.when(drives_t)
            def _():
                start_all(send_t)

        @pl.when(p > 0)
        def _():
            @pl.when(jnp.logical_not(drives_a))
            def _():
                relay_a.wait_recv()

            for owner in range(RING * CORES):
                mm_a(own_y, owner, True)

            @pl.when(jnp.logical_not(drives_t))
            def _():
                relays[0].wait_recv()

        loaded(loads_t[0])
        for owner in range(RING):
            mm_t([(x, 0), (x, 1)], owner, True)

        @pl.when(p == 0)
        def _():
            for h, copies in enumerate(((send_a[0], send_a[3]), (send_a[2], send_a[1]))):
                end_moves(first_two[h])
                for copy in copies[0] + copies[1]:
                    copy.start()
            loads_a[0].wait()
            for owner in range(RING * CORES):
                mm_a(own_y, owner, True)

        def take(arrived, onward=(), relays=()):
            for part in range(2):
                for n, copies in enumerate(arrived):
                    copies[part].wait_recv()
                    for copies in onward[n : n + 1]:
                        copies[part].start()
            for copy in relays:
                copy.start()

        def take_t(*args):
            @pl.when(drives_t)
            def _():
                take(*args)

        def relayed(*copies):
            @pl.when(jnp.logical_not(drives_t))
            def _():
                for copy in copies:
                    copy.wait_recv()

        phase("ag_wait1")
        take_t([send_t[n] for n in ORDER[:2]], fwd_t, relays[1:3])
        take([send_a[n] for n in ORDER[:2]], fwd_a)

        @pl.when(p == SWEEPS)
        def _():
            start_moves(*step_two[2:])

        phase("mm_near1")
        loaded(loads_a[1])
        loaded(loads_a[2])
        for owner in range(RING * CORES):
            mm_a([(ym, 0), (yp, 1)], owner)
        relayed(*relays[1:3])
        loaded(loads_t[1])
        loaded(loads_t[2])
        for owner in range(RING):
            mm_t([(xm, 0), (xp, 1)], owner)
        phase("mm_near2")
        take_t([send_t[n] for n in ORDER[2:]], (), relays[3:5])
        take([send_a[n] for n in ORDER[2:]])
        for owner in range(RING * CORES):
            mm_a([(ym, 1), (yp, 0)], owner)
        relayed(*relays[3:5])
        for owner in range(RING):
            mm_t([(xm, 1), (xp, 0)], owner)
        phase("ag_far")
        take_t(fwd_t, (), relays[5:])
        take(fwd_a)
        phase("mm_far")

        loaded(loads_a[3])
        pairs = []
        far_y = [(yf, 0), (yf, 1)]
        out_t = ring_scatter(RS_T, lambda i: p_t.at[i], r_t, yp, ym, yf, lambda i: dev(i, x, k))
        out_a = ring_scatter(RS_A, lambda i: p_a.at[i * CORES + k], r_a, xp, xm, xf, lambda i: dev(y, i, k))

        def pair(n, i, rows):
            pairs.append(push(PAIR + n, p_a.at[i * CORES + other, rows], d_a.at[i, rows], partner))
            pairs[n].start()

        def add_pair(n, i, rows):
            pairs[n].wait_recv()
            p_a[i * CORES + k, rows] = p_a[i * CORES + k, rows] + d_a[i, rows]

        every, half_rows = pl.ds(0, sub), [pl.ds(h * hsub, hsub) for h in range(2)]
        far_x = [(xf, 0), (xf, 1)]
        mm_a(far_y, xf * CORES + other, cuts=2)
        for h in range(2):
            pair(h, xf, half_rows[h])
        relayed(*relays[5:])
        loaded(loads_t[3])
        mm_t(far_x, yf, cuts=2)
        out_t[0].start()
        out_t[1].start()
        mm_a(far_y, xf * CORES + k, cuts=2)
        for h in range(2):
            add_pair(h, xf, half_rows[h])
            out_a[h].start()
        for n, i in enumerate((xp, xm, x)):
            mm_a(far_y, i * CORES + other)
        for n, i in enumerate((xp, xm, x)):
            pair(2 + n, i, every)
        mm_t(far_x, yp)
        mm_t(far_x, ym)
        out_t[2].start()
        out_t[3].start()
        for i in (xp, xm, x):
            mm_a(far_y, i * CORES + k)
        add_pair(2, xp, every)
        add_pair(3, xm, every)
        out_a[2].start()
        out_a[3].start()
        mm_t(far_x, y)
        phase("rs_mid")

        ht = width // 2
        out_t[0].wait_recv()
        p_t[yp, 0:ht] = p_t[yp, 0:ht] + r_t[0]
        out_t[4].start()
        out_t[1].wait_recv()
        p_t[ym, ht:width] = p_t[ym, ht:width] + r_t[1]
        out_t[5].start()
        out_a[0].wait_recv()
        kp, km, kk = xp * CORES + k, xm * CORES + k, x * CORES + k
        p_a[kp, 0:hsub] = p_a[kp, 0:hsub] + r_a[0]
        out_a[4].start()
        out_a[1].wait_recv()
        p_a[km, hsub:sub] = p_a[km, hsub:sub] + r_a[1]
        out_a[5].start()
        phase("rs_end")

        @pl.when(p == SWEEPS)
        def _():
            end_moves(*step_two)
            for q in range(2):
                share_linv(q).wait()
            for op in range(2):
                y_one[op] = dot_f32(x_move[op], linv[0, op], NT)
                x_move[op] = dot_f32(y_one[op], linv[1, op], NT)
            out_right.start()
            y_one[0] = dot_f32(ycur[0], linv[0, 0], NT)
            x_via[0] = dot_f32(y_one[0], linv[1, 0], NT)
            out_left.start()

        add_pair(4, x, every)
        for copy in out_t[2:] + out_a[2:]:
            copy.wait_recv()
        phase("rs_sum")
        ycur[t, :, 0:ht] = (p_t[y, 0:ht] + r_t[3] + r_t[4]).T
        ycur[t, :, ht:width] = (p_t[y, ht:width] + r_t[2] + r_t[5]).T
        ycur[a, 0:hsub] = p_a[kk, 0:hsub] + r_a[3] + r_a[4]
        ycur[a, hsub:sub] = p_a[kk, hsub:sub] + r_a[2] + r_a[5]
        phase("rs_drain")
        for copy in sum(fwd_a, pairs + out_t + out_a):
            copy.wait_send()

        @pl.when(drives_t)
        def _():
            for copy in sum(send_t + fwd_t, relays[1:]):
                copy.wait_send()

            @pl.when(p > 0)
            def _():
                relays[0].wait_send()

        @pl.when(jnp.logical_or(p == 0, drives_a))
        def _():
            for copy in sum(send_a, []):
                copy.wait_send()

        @pl.when(jnp.logical_and(p > 0, drives_a))
        def _():
            for copy in sum(send_b, [relay_a]):
                copy.wait_send()

        phase()

    def pair_of(rows):
        return push(GRAM_PAIR, g_loc.at[other, pl.ds(0, rows)], g_pair.at[pl.ds(0, rows)], partner)

    def pair_sum(rows, local, behind=None):
        phase("ar_pair")
        local(other)
        pair = pair_of(rows)
        pair.start()
        local(k)
        pair.wait_recv()
        if behind is not None:
            behind.start()
        g_sum[0:rows] = g_loc[k, 0:rows] + g_pair[0:rows]
        phase()

    def all_reduce(rows, meanwhile=None):
        piece = rows // nchips

        def chunk(ref, q):
            return ref.at[pl.ds(pl.multiple_of(q * piece, GROUP), piece)]

        def count(copies):
            return g_all.at[pl.ds(0, copies * piece)]

        def await_copies(sem, copies):
            pltpu.make_async_copy(count(copies), count(copies), sem).wait()

        phase("ar_rs")
        mine = y * RING + x
        owner = CORES - 1

        def spread(o, q, to_y, to_x):
            pltpu.make_async_remote_copy(
                src_ref=chunk(g_sum, q), dst_ref=g_in.at[k, pl.ds(o * piece, piece)], send_sem=send.at[GRAM_RS],
                recv_sem=recv.at[GRAM_RS + k], device_id=dev(to_y, to_x, owner), device_id_type=pl.DeviceIdType.MESH,
            ).start()

        for route in routes():
            spread(*route)
        if meanwhile is not None:
            meanwhile()

        @pl.when(k == 0)
        def _():
            spread(0, mine, y, x)
            await_copies(send.at[GRAM_RS], nchips)
            phase("ar_ag")
            await_copies(recv.at[GRAM_AG], nchips)
            phase("ar_drain")

        @pl.when(k == 1)
        def _():
            def hand_out(i, src, q, to_y, to_x, core):
                pltpu.make_async_remote_copy(
                    src_ref=src, dst_ref=chunk(g_all, q), send_sem=send.at[GRAM_AG + i], recv_sem=recv.at[GRAM_AG],
                    device_id=dev(to_y, to_x, core), device_id_type=pl.DeviceIdType.MESH,
                ).start()

            await_copies(recv.at[GRAM_RS], nchips)
            total = g_in[0, 0:piece]
            for o in range(1, nchips):
                total = total + g_in[0, o * piece : (o + 1) * piece]
            g_red[0:piece] = total / total_rows
            for _, _, to_y, to_x in routes():
                hand_out(1, g_red.at[pl.ds(0, piece)], mine, to_y, to_x, 0)
            hand_out(1, g_red.at[pl.ds(0, piece)], mine, y, x, 0)
            phase("ar_ag")
            await_copies(recv.at[GRAM_RS + 1], nchips - 1)
            total = chunk(g_sum, mine)[...]
            for o in range(1, nchips):
                total = total + g_in[1, o * piece : (o + 1) * piece]
            chunk(g_all, mine)[...] = total / total_rows
            for _, _, to_y, to_x in routes():
                hand_out(0, chunk(g_all, mine), mine, to_y, to_x, 1)
            await_copies(recv.at[GRAM_AG], nchips - 1)
            phase("ar_drain")
            await_copies(send.at[GRAM_RS], nchips - 1)
            await_copies(send.at[GRAM_AG], nchips - 1)
            await_copies(send.at[GRAM_AG + 1], nchips)

        phase()

    corners = ((0, 0), (0, 1), (1, 1), (1, 0))

    def put_gram(into, full):
        at_row, at_col = (lax.broadcasted_iota(jnp.int32, (tile, tile), i) for i in range(2))
        low = full[tile:width, tile:width]
        into[0:tile] = jnp.where(at_row <= at_col, full[0:tile, 0:tile], low)
        into[tile : 2 * tile] = full[0:tile, tile:width]
        diagonal = jnp.sum(jnp.where(at_row == at_col, low, 0.0), axis=0, keepdims=True)
        into[2 * tile : 2 * tile + GROUP] = jnp.broadcast_to(diagonal, (GROUP, tile))

    def half_gram(op):
        half = ycur[op].astype(BF16)
        put_gram(g_loc.at[op], lax.dot_general(half, half, TN, preferred_element_type=F32))

    def normalize(p, q):
        @pl.when(q == 0)
        def _():
            pair_sum(2 * tile + GROUP, half_gram, swap_y)
            phase()

        @pl.when(q == 1)
        def _():
            phase("gram2")
            put_gram(g_sum, gram_f32(y_one[0]) + gram_f32(y_one[1]))
            phase()

        last = p == SWEEPS - 1

        def clear():
            own = d_all.at[q, y * RING + x]
            own[...] = g_sum[2 * tile : 2 * tile + 1]
            for _, _, to_y, to_x in routes():
                push(DIAGONAL + q, own, own, dev(to_y, to_x, k)).start()
            set_identity(work)
            linv[q, k, 0:tile, tile:width] = jnp.zeros((tile, tile), F32)


        all_reduce(2 * tile, clear)
        others = d_all.at[q, pl.ds(0, nchips - 1)]
        for sem in (recv, send):
            pltpu.make_async_copy(others, others, sem.at[DIAGONAL + q]).wait()

        @pl.when(q == 0)
        def _():
            pair_of(2 * tile + GROUP).wait_send()

        @pl.when(jnp.logical_and(last, q == 0))
        def _():
            start_moves(*step_one)

        @pl.when(jnp.logical_and(last, q == 1))
        def _():
            end_moves(*step_one)
            start_moves(*step_two[:2])

        phase("chol")

        def store(first, t, value):
            linv[q, k, pl.ds(first, GROUP), t * tile : (t + 1) * tile] = value

        diagonal = d_all[q, 0]
        for chip in range(1, nchips):
            diagonal = diagonal + d_all[q, chip]
        inverse_factor(g_all, diagonal / total_rows, work, store)
        phase("mul")

        @pl.when(last)
        def _():
            share_linv(q).start()

        @pl.when(q == 0)
        def _():
            swap_y.wait()
            both = jnp.concatenate([ycur[k], y_in[...]], axis=0)
            y_one[...] = dot_f32(both, linv[0, k], NT).reshape(y_one.shape)

        phase()

    def launch(p):
        t = lax.rem(p, 2)

        def new_x(i):
            d_a[i] = dot_f32(y_one[i], linv[1, k], NT)
            return [d_a[i, h * hsub : (h + 1) * hsub] for h in range(2)]

        phase("launch")

        @pl.when(k == t)
        def _():
            sends, _, relays = gather_t()
            for i, core in enumerate((k, other)):
                for h, rows in enumerate(new_x(i)):
                    ag_t[x, h, core] = rows.T.astype(BF16)

                for n in ORDER[:2]:
                    sends[n][i].start()
            for n in ORDER[2:]:
                for copy in sends[n]:
                    copy.start()
            relays[0].start()

        @pl.when(k != t)
        def _():
            sends, _, for_other, relay_a = gather_a()
            for h, rows in enumerate(new_x(0)):
                ag_a[y, h] = rows.astype(BF16)
            start_all(sends)
            for h, rows in enumerate(new_x(1)):
                x_half[0, h] = rows.astype(BF16)
            start_all(for_other)
            relay_a.start()

        phase()

    def sweep(p, carry):
        apply(p)

        @pl.when(p < SWEEPS)
        def _():
            def one(q, carry):
                normalize(p, q)
                return carry

            lax.fori_loop(0, 2, one, 0)
            launch(p + 1)

        return carry

    lax.fori_loop(0, SWEEPS + 1, sweep, 0)

    def rayleigh(op):
        full = dot_f32(x_move[op], ycur[op], TN)
        for n, (i, j) in enumerate(corners):
            g_loc[op, n * tile : (n + 1) * tile] = full[i * tile : (i + 1) * tile, j * tile : (j + 1) * tile]

    pair_sum(4 * tile, rayleigh)
    all_reduce(4 * tile)
    pair_of(4 * tile).wait_send()
    phase("h_swap")
    swap = push(SWAP_H, g_all, h_all, partner)
    swap.start()
    swap.wait()
    for n, (i, j) in enumerate(corners):
        rows, at = slice(n * tile, (n + 1) * tile), (slice(i * tile, (i + 1) * tile), slice(j * tile, (j + 1) * tile))
        for op in range(2):
            h_out[(op, *at)] = jnp.where(k == op, g_all[rows], h_all[rows])
    out_left.wait()
    out_right.wait()
    phase()


def hand_over(x_ref, h_ref, left_x, left_h, right_x, right_h, x_buf, h_buf, sem_in, sem_out):
    size = x_buf.shape[1] // 2
    routes = []
    for op, (x_to, h_to) in enumerate(((left_x, left_h), (right_x, right_h))):
        for h in range(2):
            rows = pl.ds(h * size, size)
            routes.append((x_ref.at[op, rows], x_buf.at[op, rows], x_to.at[rows]))
        routes.append((h_ref.at[op], h_buf.at[op], h_to))
    come = [pltpu.make_async_copy(src, buf, sem_in.at[n]) for n, (src, buf, _) in enumerate(routes)]
    go = [pltpu.make_async_copy(buf, dst, sem_out.at[n]) for n, (_, buf, dst) in enumerate(routes)]
    for copy in come:
        copy.start()
    for copy, nxt in zip(come, go):
        copy.wait()
        nxt.start()
    for copy in go:
        copy.wait()


def solution(mesh):
    nrow, ncol = mesh.shape["row"], mesh.shape["col"]
    assert nrow == RING and ncol == RING * CORES

    def local_program(left_op, left_start, right_op, right_start):
        rows, cols = left_op.shape
        sub, width = left_start.shape
        tile = width // 2
        vmem = pltpu.VMEM
        dma = pltpu.SemaphoreType.DMA
        basis, ray = jax.ShapeDtypeStruct((sub, width), F32), jax.ShapeDtypeStruct((width, width), F32)
        both_x, both_h = pl.pallas_call(
            functools.partial(kernel, (nrow, ncol, rows * nrow)),
            out_shape=[jax.ShapeDtypeStruct((2, sub, width), F32), jax.ShapeDtypeStruct((2, width, width), F32)],
            in_specs=[pl.BlockSpec(memory_space=pl.ANY)] * 4,
            out_specs=[pl.BlockSpec(memory_space=pl.ANY), pl.BlockSpec(memory_space=vmem)],
            scratch_shapes=[
                vmem((2, rows, cols), BF16),
                vmem((2, sub, width), F32),
                vmem((2, sub, width), F32),
                vmem((RING, 2, CORES, width, sub // 2), BF16),
                vmem((nrow, 2, sub // 2, width), BF16),
                vmem((nrow, width, sub), F32),
                vmem((ncol, sub, width), F32),
                vmem((RING, sub, width), F32),
                vmem((6, width // 2, sub), F32),
                vmem((6, sub // 2, width), F32),
                vmem((2, 2, sub // 2, width), BF16),
                vmem((2, sub, width), F32),
                vmem((2, sub, width), F32),
                vmem((sub, width), F32),
                vmem((2, 4 * tile, tile), F32),
                vmem((4 * tile, tile), F32),
                vmem((4 * tile, tile), F32),
                vmem((2, 4 * tile, tile), F32),
                vmem((4 * tile // (RING * RING), tile), F32),
                vmem((4 * tile, tile), F32),
                vmem((4 * tile, tile), F32),
                vmem((2, RING * RING, 1, tile), F32),
                vmem((width, 2 * width), F32),
                vmem((2, 2, width, width), F32),
                dma((KINDS.stop,)),
                dma((KINDS.stop,)),
                dma((10,)),
            ],
            compiler_params=pltpu.CompilerParams(collective_id=0, has_side_effects=True, vmem_limit_bytes=VMEM_BYTES),
            name="subspace",
        )(left_op, left_start, right_op, right_start)
        anywhere = pl.BlockSpec(memory_space=pl.ANY)
        return pl.pallas_call(
            hand_over,
            out_shape=[basis, ray, basis, ray],
            in_specs=[anywhere] * 2,
            out_specs=[anywhere] * 4,
            scratch_shapes=[vmem((2, sub, width), F32), vmem((2, width, width), F32), dma((6,)), dma((6,))],
            name="hand_over",
        )(both_x, both_h)

    op_spec = P(("batch", "row"), "col")
    vec_spec = P(("batch", "row", "col"), None)
    small_spec = P("batch", None)
    return jax.shard_map(
        local_program,
        mesh=mesh,
        in_specs=(op_spec, vec_spec, op_spec, vec_spec),
        out_specs=(vec_spec, small_spec, vec_spec, small_spec),
        check_vma=False,
    )
```
